32 devices in a mesh: dp: 8 (over y, x, core), tensor: 4 (over z).
Axes of the slice: x: 2, y: 2, z: 4, core: 2. Of those that a mesh axis runs over, the one named last changes fastest.
Arguments:
- tokens: bfloat16 [32, 256, 1152], P(('dp', 'tensor')), may hold values from -6 to 6
- timesteps: int32 [32], P('dp'), may hold values from 0 to 999
- labels: int32 [32], P('dp'), may hold values from 0 to 999
- item_counts: int32 [8], P('dp'), may hold values from 1 to 4
- cotangent: bfloat16 [32, 256, 1152], P(('dp', 'tensor')), may hold values from -6 to 6
- project_weight: bfloat16 [1152, 3, 1152], P(None, None, 'tensor'), may hold values from -0.1875 to 0.1875
- query_gain: bfloat16 [72], replicated, may hold values from 0.099609375 to 1.8984375
- key_gain: bfloat16 [72], replicated, may hold values from 0.099609375 to 1.8984375
- output_weight: bfloat16 [1152, 1152], P('tensor'), may hold values from -0.5 to 0.5
- output_bias: bfloat16 [1152], replicated, may hold values from -3 to 3
- expand_weight: bfloat16 [1152, 2, 3072], P(None, None, 'tensor'), may hold values from -0.1875 to 0.1875
- down_weight: bfloat16 [3072, 1152], P('tensor'), may hold values from -0.15625 to 0.15625
- down_bias: bfloat16 [1152], replicated, may hold values from -3 to 3
- modulate_weight: bfloat16 [1152, 6, 1152], P(None, None, 'tensor'), may hold values from -0.1875 to 0.1875
- modulate_bias: bfloat16 [6, 1152], P(None, 'tensor'), may hold values from -3 to 3
- time_weight: bfloat16 [256, 1152], replicated, may hold values from -0.5 to 0.5
- time_bias: bfloat16 [1152], replicated, may hold values from -3 to 3
- embed_weight: bfloat16 [1152, 1152], replicated, may hold values from -0.25 to 0.25
- embed_bias: bfloat16 [1152], replicated, may hold values from -3 to 3
- class_table: bfloat16 [1000, 1152], replicated, may hold values from -6 to 6
Outputs:
- result: bfloat16 [32, 256, 1152], P(('dp', 'tensor'))
- tokens_grad: bfloat16 [32, 256, 1152], P(('dp', 'tensor'))
- project_grad: float32 [1152, 3, 1152], P('dp', None, 'tensor')
- query_gain_grad: float32 [72], replicated
- key_gain_grad: float32 [72], replicated
- output_weight_grad: float32 [1152, 1152], P('tensor', 'dp')
- output_bias_grad: float32 [1152], replicated
- expand_grad: float32 [1152, 2, 3072], P('dp', None, 'tensor')
- down_grad: float32 [3072, 1152], P('tensor', 'dp')
- down_bias_grad: float32 [1152], replicated
- modulate_grad: float32 [1152, 6, 1152], P('dp', None, 'tensor')
- modulate_bias_grad: float32 [6, 1152], replicated
- time_grad: float32 [256, 1152], P(None, 'dp')
- time_bias_grad: float32 [1152], P('dp')
- embed_grad: float32 [1152, 1152], P('dp')
- embed_bias_grad: float32 [1152], P('dp')
- class_grad: float32 [1000, 1152], P(None, 'dp')
The draws below stay inside these ranges and needn't reach their ends.
Inputs may be any that keep to these rules, and one draw needn't show every extreme that they name: `item_counts`: entry i counts the real items among the 4 items of index i of dp; they are its first ones.
All inputs are finite; a program needn't handle non-finite values.
Results may differ from the reference program's by a relative error of at most 0.03.
Values may be sent and summed in bfloat16 or wider, within the bound.
A program may use at most 256 MiB of HBM per device.

```python
import math
import jax
import jax.numpy as jnp
from jax import lax

D = 1152
HEADS = 16
HD = 72
FF = 3072
FREQ = 256
CLASSES = 1000
GRID = 16
ITEMS = 4
ITEM_LEN = 256
BATCH = 32
N_DP = 8


def set_ends(array, stream_key, smallest, high):
    longest = array.shape.index(max(array.shape))
    spots = []
    for shift in (0, 1):
        where = [jax.random.randint(jax.random.fold_in(stream_key, axis), (), 0, length) for axis, length in enumerate(array.shape)]
        where[longest] = (where[longest] + shift) % array.shape[longest]
        spots.append(tuple(where))
    return array.at[spots[0]].set(smallest).at[spots[1]].set(high)


def levels(rng, dims, shards, least, high):
    level, own = 1.0, jax.random.fold_in(rng, 6)
    for dim, blocks in shards:
        heights = jnp.exp(jax.random.uniform(jax.random.fold_in(own, dim), (blocks,), jnp.float32, least / len(shards), high / len(shards)))
        level = level * jnp.repeat(heights, dims[dim] // blocks).reshape([-1 if axis == dim else 1 for axis in range(len(dims))])
    return level


def centred(own_key, extent, scale, limit, cuts=(), kind=jnp.bfloat16):
    drawn = jax.random.normal(own_key, extent, jnp.float32) * scale
    if len(cuts) > 0:
        drawn = levels(own_key, extent, cuts, -0.22, 0.18) * drawn
    return jnp.clip(drawn, min=-limit, max=limit).astype(kind)


def setup_inputs(seed: int = 0) -> dict:
    key_list = jax.random.split(jax.random.key(seed), 21)
    tokens = centred(key_list[0], (BATCH, ITEM_LEN, D), 1.0, 6.0, ((0, 32),))
    timesteps = set_ends(jax.random.randint(key_list[1], (BATCH,), 0, 1000), jax.random.fold_in(key_list[1], 1), 0, 999).astype(jnp.int32)
    labels = set_ends(jax.random.randint(key_list[2], (BATCH,), 0, CLASSES), jax.random.fold_in(key_list[2], 1), 0, CLASSES - 1).astype(jnp.int32)
    item_counts = set_ends(jax.random.randint(key_list[3], (N_DP,), 1, ITEMS + 1), jax.random.fold_in(key_list[3], 1), 1, ITEMS).astype(jnp.int32)
    cotangent = centred(key_list[4], (BATCH, ITEM_LEN, D), 1.0, 6.0, ((0, 32),))
    project_weight = centred(key_list[5], (D, 3, D), D ** -0.5, 0.1875, ((2, 4),))
    query_gain = jnp.clip(1.0 + 0.18 * jax.random.normal(key_list[6], (HD,), jnp.float32), 0.099609375, 1.8984375).astype(jnp.bfloat16)
    key_gain = jnp.clip(1.0 + 0.18 * jax.random.normal(key_list[7], (HD,), jnp.float32), 0.099609375, 1.8984375).astype(jnp.bfloat16)
    output_weight = centred(key_list[8], (D, D), (D // 8) ** -0.5, 0.5, ((0, 4),))
    output_bias = centred(key_list[9], (D,), 0.5, 3.0)
    expand_weight = centred(key_list[10], (D, 2, FF), D ** -0.5, 0.1875, ((2, 4),))
    down_weight = centred(key_list[11], (FF, D), (FF // 2) ** -0.5, 0.15625, ((0, 4),))
    down_bias = centred(key_list[12], (D,), 0.5, 3.0)
    modulate_weight = centred(key_list[13], (D, 6, D), D ** -0.5, 0.1875, ((2, 4),))
    modulate_bias = centred(key_list[14], (6, D), 0.5, 3.0, ((1, 4),))
    time_weight = centred(key_list[15], (FREQ, D), (FREQ // 2) ** -0.5, 0.5)
    time_bias = centred(key_list[16], (D,), 0.5, 3.0)
    embed_weight = centred(key_list[17], (D, D), (D // 2) ** -0.5, 0.25)
    embed_bias = centred(key_list[18], (D,), 0.5, 3.0)
    class_table = centred(key_list[19], (CLASSES, D), 1.0, 6.0)
    return dict(tokens=tokens, timesteps=timesteps, labels=labels, item_counts=item_counts, cotangent=cotangent, project_weight=project_weight, query_gain=query_gain, key_gain=key_gain, output_weight=output_weight, output_bias=output_bias, expand_weight=expand_weight, down_weight=down_weight, down_bias=down_bias, modulate_weight=modulate_weight, modulate_bias=modulate_bias, time_weight=time_weight, time_bias=time_bias, embed_weight=embed_weight, embed_bias=embed_bias, class_table=class_table)


@jax.custom_vjp
def low(v):
    return lax.optimization_barrier(v.astype(jnp.bfloat16)).astype(jnp.float32)

@jax.custom_vjp
def low_back(v):
    return v

def low_keep(v):
    return (low(v), None)

def low_pass(kept, grad):
    return (grad,)

def back_keep(v):
    return (v, None)

def back_low(kept, grad):
    return (low(grad),)
low.defvjp(low_keep, low_pass)
low_back.defvjp(back_keep, back_low)
HIGH = lax.Precision.HIGHEST
EPS = 1e-06

def layer_norm(value):
    center = value - lax.optimization_barrier(jnp.mean(value, axis=-1, keepdims=True))
    return center * lax.rsqrt(lax.optimization_barrier(jnp.mean(center * center, axis=-1, keepdims=True)) + EPS)

def rotate(value, positions):
    quarter = HD // 4
    rates = 10000.0 ** (-jnp.arange(quarter, dtype=jnp.float32) / quarter)
    places = ((positions // GRID).astype(jnp.float32), (positions % GRID).astype(jnp.float32))
    pieces = []
    for which_half in range(2):
        half_value = value[..., which_half * 2 * quarter:(which_half + 1) * 2 * quarter]
        angle = places[which_half][:, None] * rates[None, :]
        cosine = jnp.cos(angle)[None, :, None, :]
        sine = jnp.sin(angle)[None, :, None, :]
        first = half_value[..., :quarter]
        second = half_value[..., quarter:]
        pieces.append(first * cosine - second * sine)
        pieces.append(second * cosine + first * sine)
    return jnp.concatenate(pieces, axis=-1)

def head_prepare(raw, gain, positions):
    scaled = raw * lax.rsqrt(lax.optimization_barrier(jnp.mean(raw * raw, axis=-1, keepdims=True)) + EPS) * gain
    return rotate(scaled, positions)

def time_features(steps_in):
    half = FREQ // 2
    rates = jnp.exp(-math.log(10000.0) * jnp.arange(half, dtype=jnp.float32) / half)
    angle = steps_in.astype(jnp.float32)[:, None] * rates[None, :]
    return jnp.concatenate([jnp.cos(angle), jnp.sin(angle)], axis=-1)

def block(tokens, params, timesteps, labels, live):
    project_weight, query_gain, key_gain, output_weight, output_bias, expand_weight, down_weight, down_bias, modulate_weight, modulate_bias, time_weight, time_bias, embed_weight, embed_bias, class_table = params
    number = tokens.shape[0]
    length = tokens.shape[1]
    time_feat = low(time_features(timesteps))
    pre_hidden = low_back(jnp.dot(time_feat, time_weight, precision=HIGH) + time_bias)
    time_hidden = low(jax.nn.silu(pre_hidden))
    condition = low_back(jnp.dot(time_hidden, embed_weight, precision=HIGH) + embed_bias + jnp.take(class_table, labels, axis=0))
    cond_act = low(jax.nn.silu(condition))
    modulation = low(low_back(jnp.einsum('bd,dke->bke', cond_act, modulate_weight, precision=HIGH) + modulate_bias))
    parts = [modulation[:, which][:, None, :] for which in range(6)]
    attend_shift, attend_scale, attend_gate, feed_shift, feed_scale, feed_gate = parts
    positions = jnp.arange(length)
    mod_in = low(layer_norm(tokens) * (1.0 + attend_scale) + attend_shift)
    projected = low_back(jnp.einsum('bld,dke->blke', mod_in, project_weight, precision=HIGH))
    split = projected.reshape(number, length, 3, HEADS, HD)
    queries = low(head_prepare(split[:, :, 0], query_gain, positions))
    keys = low(head_prepare(split[:, :, 1], key_gain, positions))
    values = low(split[:, :, 2])
    scores = low_back(jnp.einsum('bqhd,bkhd->bhqk', queries, keys, precision=HIGH) * HD ** (-0.5))
    probs = low(jax.nn.softmax(scores, axis=-1))
    mixed = jnp.einsum('bhqk,bkhd->bqhd', probs, values, precision=HIGH).reshape(number, length, D)
    mixed = low_back(low(mixed))
    attend_branch = low_back(jnp.dot(mixed, output_weight, precision=HIGH) + output_bias)
    residual = tokens + attend_gate * attend_branch
    mod_two = low(layer_norm(residual) * (1.0 + feed_scale) + feed_shift)
    gate_up = low_back(jnp.einsum('bld,dkf->blkf', mod_two, expand_weight, precision=HIGH))
    hidden = low(jax.nn.silu(gate_up[:, :, 0]) * gate_up[:, :, 1])
    feed_branch = low_back(jnp.dot(hidden, down_weight, precision=HIGH) + down_bias)
    return live[:, None, None] * (residual + feed_gate * feed_branch)

def reference(tokens, timesteps, labels, item_counts, cotangent, project_weight, query_gain, key_gain, output_weight, output_bias, expand_weight, down_weight, down_bias, modulate_weight, modulate_bias, time_weight, time_bias, embed_weight, embed_bias, class_table):
    params = tuple((weight.astype(jnp.float32) for weight in (project_weight, query_gain, key_gain, output_weight, output_bias, expand_weight, down_weight, down_bias, modulate_weight, modulate_bias, time_weight, time_bias, embed_weight, embed_bias, class_table)))
    group = math.gcd(BATCH, 16)
    blocks = BATCH // group
    item_ids = jnp.arange(BATCH)
    live = (item_ids % ITEMS < item_counts[item_ids // ITEMS]).astype(jnp.float32)

    def regroup(value):
        return value.reshape(blocks, group, ITEM_LEN, D)
    inputs_all = (regroup(tokens.astype(jnp.float32)), regroup(cotangent.astype(jnp.float32)), timesteps.reshape(blocks, group), labels.reshape(blocks, group), live.reshape(blocks, group))

    def advance(totals, inputs):
        block_tokens, block_cot, block_steps, block_labels, block_live = inputs

        def forward(token_values, *weights):
            return block(token_values, weights, block_steps, block_labels, block_live)
        outcome, pullback = jax.vjp(forward, block_tokens, *params)
        grads = pullback(block_cot)
        totals = tuple((total + grad for total, grad in zip(totals, grads[1:])))
        return (totals, (outcome.astype(jnp.bfloat16), grads[0].astype(jnp.bfloat16)))
    zeros = tuple((jnp.zeros_like(weight) for weight in params))
    totals, (outcomes, token_grads) = lax.scan(advance, zeros, inputs_all)

    def ungroup(value):
        return value.reshape(BATCH, ITEM_LEN, D)
    return (ungroup(outcomes), ungroup(token_grads), totals[0], totals[1], totals[2], totals[3], totals[4], totals[5], totals[6], totals[7], totals[8], totals[9], totals[10], totals[11], totals[12], totals[13], totals[14])
```

```python
import math

import jax
import jax.numpy as jnp
from jax import lax
from jax.sharding import PartitionSpec as P

HD = 72
FREQ = 256
GRID = 16


EPS = 1e-06


def layer_norm(value):
    center = value - jnp.mean(value, axis=-1, keepdims=True)
    inverse = lax.rsqrt(jnp.mean(center * center, axis=-1, keepdims=True) + EPS)
    return (center * inverse, inverse)


def layer_norm_back(normed, inverse, grad):
    return inverse * (
        grad
        - jnp.mean(grad, axis=-1, keepdims=True)
        - normed * jnp.mean(grad * normed, axis=-1, keepdims=True)
    )


def silu_slope(value):
    sigma = jax.nn.sigmoid(value)
    return sigma * (1.0 + value * (1.0 - sigma))


def rotate(value, positions):
    quarter = HD // 4
    rates = 10000.0 ** (-jnp.arange(quarter, dtype=jnp.float32) / quarter)
    places = ((positions // GRID).astype(jnp.float32), (positions % GRID).astype(jnp.float32))
    pieces = []
    for which_half in range(2):
        half_value = value[..., which_half * 2 * quarter : (which_half + 1) * 2 * quarter]
        angle = places[which_half][:, None] * rates[None, :]
        cosine = jnp.cos(angle)[None, :, None, :]
        sine = jnp.sin(angle)[None, :, None, :]
        first = half_value[..., :quarter]
        second = half_value[..., quarter:]
        pieces.append(first * cosine - second * sine)
        pieces.append(second * cosine + first * sine)
    return jnp.concatenate(pieces, axis=-1)


def head_prepare(raw, gain, positions):
    scaled = raw * lax.rsqrt(jnp.mean(raw * raw, axis=-1, keepdims=True) + EPS) * gain
    return rotate(scaled, positions)


def time_features(steps_in):
    half = FREQ // 2
    rates = jnp.exp(-math.log(10000.0) * jnp.arange(half, dtype=jnp.float32) / half)
    angle = steps_in.astype(jnp.float32)[:, None] * rates[None, :]
    return jnp.concatenate([jnp.cos(angle), jnp.sin(angle)], axis=-1)


def shards(
    tokens,
    timesteps,
    labels,
    item_counts,
    cotangent,
    project_weight,
    query_gain,
    key_gain,
    output_weight,
    output_bias,
    expand_weight,
    down_weight,
    down_bias,
    modulate_weight,
    modulate_bias,
    time_weight,
    time_bias,
    embed_weight,
    embed_bias,
    class_table,
):
    local_items, length, width = tokens.shape
    items = timesteps.shape[0]
    slab = modulate_weight.shape[2]
    heads_here = project_weight.shape[2] // HD
    scale = HD ** (-0.5)
    lane = lax.axis_index("tensor")
    first_item = lane * local_items
    live = (first_item + jnp.arange(local_items) < item_counts[0]).astype(jnp.float32)[
        :, None, None
    ]
    index = lax.axis_index("dp")
    tags = lax.all_gather(jnp.stack([timesteps, labels]), "dp", axis=1, tiled=True)
    time_feat = time_features(tags[0]).astype(jnp.bfloat16)
    pre_hidden = jnp.dot(
        time_feat, time_weight, preferred_element_type=jnp.float32
    ) + time_bias.astype(jnp.float32)
    time_hidden = jax.nn.silu(pre_hidden).astype(jnp.bfloat16)
    condition = (
        jnp.dot(time_hidden, embed_weight, preferred_element_type=jnp.float32)
        + embed_bias.astype(jnp.float32)
        + jnp.take(class_table, tags[1], axis=0).astype(jnp.float32)
    )
    cond_act = jax.nn.silu(condition).astype(jnp.bfloat16)
    cond_act_here = lax.dynamic_slice_in_dim(cond_act, index * items, items, 0)
    condition_here = lax.dynamic_slice_in_dim(condition, index * items, items, 0)
    modulation_part = (
        jnp.einsum("bd,dke->bke", cond_act_here, modulate_weight, preferred_element_type=jnp.float32)
        + modulate_bias.astype(jnp.float32)
    ).astype(jnp.bfloat16)
    modulation_local = lax.all_to_all(
        modulation_part, "tensor", split_axis=0, concat_axis=2, tiled=True
    ).astype(jnp.float32)
    local_parts = [modulation_local[:, which][:, None, :] for which in range(6)]
    attend_shift, attend_scale, attend_gate, feed_shift, feed_scale, feed_gate = local_parts
    positions = jnp.arange(length)
    token_local = tokens.astype(jnp.float32)
    normed_local, inverse_local = layer_norm(token_local)
    mod_in = lax.all_gather(
        (normed_local * (1.0 + attend_scale) + attend_shift).astype(jnp.bfloat16),
        "tensor",
        axis=0,
        tiled=True,
    )
    projected = jnp.einsum(
        "bld,dke->blke", mod_in, project_weight, preferred_element_type=jnp.float32
    )
    split = projected.reshape(items, length, 3, heads_here, HD)
    query_gain_f = query_gain.astype(jnp.float32)
    key_gain_f = key_gain.astype(jnp.float32)
    queries = head_prepare(split[:, :, 0], query_gain_f, positions).astype(jnp.bfloat16)
    keys = head_prepare(split[:, :, 1], key_gain_f, positions).astype(jnp.bfloat16)
    values = split[:, :, 2].astype(jnp.bfloat16)
    scores = (
        jnp.einsum("bqhd,bkhd->bhqk", queries, keys, preferred_element_type=jnp.float32) * scale
    )
    top = jnp.max(scores, axis=-1, keepdims=True)
    logsum = top + jnp.log(jnp.sum(jnp.exp(scores - top), axis=-1, keepdims=True))
    probs = jnp.exp(scores - logsum).astype(jnp.bfloat16)
    mixed = jnp.einsum("bhqk,bkhd->bqhd", probs, values, preferred_element_type=jnp.float32)
    mixed = mixed.reshape(items, length, heads_here * HD).astype(jnp.bfloat16)
    piece = mixed
    attend_branch = lax.psum_scatter(
        jnp.einsum("blh,hd->bld", piece, output_weight, preferred_element_type=jnp.float32).astype(
            jnp.bfloat16
        ),
        "tensor",
        scatter_dimension=0,
        tiled=True,
    ).astype(jnp.float32) + output_bias.astype(jnp.float32)
    residual = token_local + attend_gate * attend_branch
    normed_two, inverse_two = layer_norm(residual)
    mod_two = (normed_two * (1.0 + feed_scale) + feed_shift).astype(jnp.bfloat16)
    mod_two_all = lax.all_gather(mod_two, "tensor", axis=0, tiled=True)
    gate_up = jnp.einsum(
        "bld,dkf->blkf", mod_two_all, expand_weight, preferred_element_type=jnp.float32
    )
    gate = gate_up[:, :, 0]
    upper = gate_up[:, :, 1]
    hidden = (jax.nn.silu(gate) * upper).astype(jnp.bfloat16)
    piece = hidden
    feed_branch = lax.psum_scatter(
        jnp.einsum("blf,fd->bld", piece, down_weight, preferred_element_type=jnp.float32).astype(
            jnp.bfloat16
        ),
        "tensor",
        scatter_dimension=0,
        tiled=True,
    ).astype(jnp.float32) + down_bias.astype(jnp.float32)
    result = (live * (residual + feed_gate * feed_branch)).astype(jnp.bfloat16)
    out_grad = cotangent.astype(jnp.float32) * live
    branch_grad = (out_grad * feed_gate).astype(jnp.bfloat16)
    down_bias_part = jnp.sum(branch_grad.astype(jnp.float32), axis=(0, 1))
    piece = lax.all_gather(branch_grad, "tensor", axis=0, tiled=True)
    weight_total = jnp.einsum("blf,bld->fd", hidden, piece, preferred_element_type=jnp.float32)
    rows_grad = jnp.einsum("bld,fd->blf", piece, down_weight, preferred_element_type=jnp.float32)
    hidden_total = rows_grad
    down_grad = weight_total
    gate_up_grad = jnp.stack(
        [hidden_total * upper * silu_slope(gate), hidden_total * jax.nn.silu(gate)], axis=2
    ).astype(jnp.bfloat16)
    expand_grad = jnp.einsum(
        "bld,blkf->dkf", mod_two_all, gate_up_grad, preferred_element_type=jnp.float32
    )
    piece = gate_up_grad
    mod_two_grad = lax.psum_scatter(
        jnp.einsum(
            "blkf,dkf->bld", piece, expand_weight, preferred_element_type=jnp.float32
        ).astype(jnp.bfloat16),
        "tensor",
        scatter_dimension=0,
        tiled=True,
    ).astype(jnp.float32)
    residual_grad = out_grad + layer_norm_back(
        normed_two, inverse_two, mod_two_grad * (1.0 + feed_scale)
    )
    attend_grad = (residual_grad * attend_gate).astype(jnp.bfloat16)
    output_bias_part = jnp.sum(attend_grad.astype(jnp.float32), axis=(0, 1))
    piece = lax.all_gather(attend_grad, "tensor", axis=0, tiled=True)
    weight_total = jnp.einsum("blh,bld->hd", mixed, piece, preferred_element_type=jnp.float32)
    rows_grad = jnp.einsum("bld,hd->blh", piece, output_weight, preferred_element_type=jnp.float32)
    output_weight_grad = weight_total
    mixed_grad = rows_grad
    mixed_grad = mixed_grad.reshape(items, length, heads_here, HD).astype(jnp.bfloat16)
    again = jnp.einsum("bqhd,bkhd->bhqk", queries, keys, preferred_element_type=jnp.float32) * scale
    prob_float = jnp.exp(again - logsum)
    prob_low = prob_float.astype(jnp.bfloat16)
    prob_grad = jnp.einsum(
        "bqhd,bkhd->bhqk", mixed_grad, values, preferred_element_type=jnp.float32
    )
    score_grad = (
        prob_float * (prob_grad - jnp.sum(prob_float * prob_grad, axis=-1, keepdims=True))
    ).astype(jnp.bfloat16)
    query_grad = (
        jnp.einsum("bhqk,bkhd->bqhd", score_grad, keys, preferred_element_type=jnp.float32) * scale
    )
    key_grad = (
        jnp.einsum("bhqk,bqhd->bkhd", score_grad, queries, preferred_element_type=jnp.float32)
        * scale
    )
    value_grad = jnp.einsum(
        "bhqk,bqhd->bkhd", prob_low, mixed_grad, preferred_element_type=jnp.float32
    )

    def prepare_here(raw, gain):
        return head_prepare(raw, gain, positions)

    _, query_back = jax.vjp(prepare_here, split[:, :, 0], query_gain_f)
    raw_query_grad, query_gain_part = query_back(query_grad)
    _, key_back = jax.vjp(prepare_here, split[:, :, 1], key_gain_f)
    raw_key_grad, key_gain_part = key_back(key_grad)
    projected_grad = jnp.stack([raw_query_grad, raw_key_grad, value_grad], axis=2)
    projected_grad = projected_grad.reshape(items, length, 3, heads_here * HD).astype(jnp.bfloat16)
    project_grad = jnp.einsum(
        "bld,blke->dke", mod_in, projected_grad, preferred_element_type=jnp.float32
    )
    piece = projected_grad
    mod_in_grad = lax.psum_scatter(
        jnp.einsum(
            "blke,dke->bld", piece, project_weight, preferred_element_type=jnp.float32
        ).astype(jnp.bfloat16),
        "tensor",
        scatter_dimension=0,
        tiled=True,
    ).astype(jnp.float32)
    tokens_grad = (
        residual_grad
        + layer_norm_back(normed_local, inverse_local, mod_in_grad * (1.0 + attend_scale))
    ).astype(jnp.bfloat16)
    modulation_grad_part = jnp.stack(
        [
            jnp.sum(mod_in_grad, axis=1),
            jnp.sum(mod_in_grad * normed_local, axis=1),
            jnp.sum(residual_grad * attend_branch, axis=1),
            jnp.sum(mod_two_grad, axis=1),
            jnp.sum(mod_two_grad * normed_two, axis=1),
            jnp.sum(out_grad * feed_branch, axis=1),
        ],
        axis=1,
    )
    modulation_grad = lax.all_to_all(
        modulation_grad_part, "tensor", split_axis=2, concat_axis=0, tiled=True
    ).astype(jnp.bfloat16)
    modulate_bias_part = jnp.sum(modulation_grad.astype(jnp.float32), axis=0)
    cond_part = jnp.einsum(
        "bke,dke->bd", modulation_grad, modulate_weight, preferred_element_type=jnp.float32
    )
    cond_total = lax.psum(cond_part, "tensor")
    cond_grad_here = (cond_total * silu_slope(condition_here)).astype(jnp.bfloat16)
    packed = jnp.concatenate([cond_grad_here, modulation_grad.reshape(items, 6 * slab)], axis=1)
    packed = lax.all_gather(packed, "dp", axis=0, tiled=True)
    cond_grad = packed[:, :width]
    modulation_grad_all = packed[:, width:].reshape(-1, 6, slab)
    share = width // lax.axis_size("dp")

    def mine(value, axis):
        return lax.dynamic_slice_in_dim(value, index * share, share, axis)

    one_hot = (tags[1][:, None] == jnp.arange(class_table.shape[0])[None, :]).astype(jnp.bfloat16)
    cond_grad_mine = mine(cond_grad, 1)
    class_grad = jnp.einsum(
        "bc,bd->cd", one_hot, cond_grad_mine, preferred_element_type=jnp.float32
    )
    pre_grad = (
        jnp.einsum(
            "be,de->bd", cond_grad, mine(embed_weight, 0), preferred_element_type=jnp.float32
        )
        * silu_slope(mine(pre_hidden, 1))
    ).astype(jnp.bfloat16)
    modulate_grad = jnp.einsum(
        "bd,bke->dke", mine(cond_act, 1), modulation_grad_all, preferred_element_type=jnp.float32
    )
    embed_grad = jnp.einsum(
        "bd,be->de", mine(time_hidden, 1), cond_grad, preferred_element_type=jnp.float32
    )
    embed_bias_grad = jnp.sum(cond_grad_mine.astype(jnp.float32), axis=0)
    time_grad = jnp.einsum("bf,bd->fd", time_feat, pre_grad, preferred_element_type=jnp.float32)
    time_bias_grad = jnp.sum(pre_grad.astype(jnp.float32), axis=0)
    bias_wide = lax.dynamic_update_slice_in_dim(
        jnp.zeros((6, width), jnp.float32), modulate_bias_part, lane * slab, 1
    )
    small = jnp.concatenate(
        [
            output_bias_part,
            down_bias_part,
            bias_wide.reshape(-1),
            query_gain_part,
            key_gain_part,
        ]
    )
    small = lax.psum(small, ("dp", "tensor"))
    output_bias_grad = small[:width]
    down_bias_grad = small[width : 2 * width]
    modulate_bias_grad = small[2 * width : 8 * width].reshape(6, width)
    query_gain_grad = small[8 * width : 8 * width + HD]
    key_gain_grad = small[8 * width + HD :]

    def scatter(value, axis):
        value = value.astype(jnp.bfloat16)
        return lax.psum_scatter(value, "dp", scatter_dimension=axis, tiled=True).astype(
            jnp.float32
        )

    project_grad = scatter(project_grad, 0)
    output_weight_grad = scatter(output_weight_grad, 1)
    expand_grad = scatter(expand_grad, 0)
    down_grad = scatter(down_grad, 1)
    return (
        result,
        tokens_grad,
        project_grad,
        query_gain_grad,
        key_gain_grad,
        output_weight_grad,
        output_bias_grad,
        expand_grad,
        down_grad,
        down_bias_grad,
        modulate_grad,
        modulate_bias_grad,
        time_grad,
        time_bias_grad,
        embed_grad,
        embed_bias_grad,
        class_grad,
    )


def solution(mesh):
    return jax.shard_map(
        shards,
        mesh=mesh,
        in_specs=(
            P(("dp", "tensor"), None, None),
            P("dp"),
            P("dp"),
            P("dp"),
            P(("dp", "tensor"), None, None),
            P(None, None, "tensor"),
            P(),
            P(),
            P("tensor", None),
            P(),
            P(None, None, "tensor"),
            P("tensor", None),
            P(),
            P(None, None, "tensor"),
            P(None, "tensor"),
            P(),
            P(),
            P(),
            P(),
            P(),
        ),
        out_specs=(
            P(("dp", "tensor"), None, None),
            P(("dp", "tensor"), None, None),
            P("dp", None, "tensor"),
            P(),
            P(),
            P("tensor", "dp"),
            P(),
            P("dp", None, "tensor"),
            P("tensor", "dp"),
            P(),
            P("dp", None, "tensor"),
            P(),
            P(None, "dp"),
            P("dp"),
            P("dp", None),
            P("dp"),
            P(None, "dp"),
        ),
        check_vma=False,
    )
```

```python
import functools
import math

import jax
import jax.numpy as jnp
from jax import lax
from jax.experimental import pallas as pl
from jax.experimental.pallas import tpu as pltpu
from jax.sharding import PartitionSpec as P

HD = 72
FREQ = 256
GRID = 16


EPS = 1e-06


def layer_norm(value):
    center = value - jnp.mean(value, axis=-1, keepdims=True)
    inverse = lax.rsqrt(jnp.mean(center * center, axis=-1, keepdims=True) + EPS)
    return (center * inverse, inverse)


def layer_norm_back(normed, inverse, grad):
    return inverse * (
        grad
        - jnp.mean(grad, axis=-1, keepdims=True)
        - normed * jnp.mean(grad * normed, axis=-1, keepdims=True)
    )


def silu_slope(value):
    sigma = jax.nn.sigmoid(value)
    return sigma * (1.0 + value * (1.0 - sigma))


def rotate(value, positions):
    quarter = HD // 4
    rates = 10000.0 ** (-jnp.arange(quarter, dtype=jnp.float32) / quarter)
    places = ((positions // GRID).astype(jnp.float32), (positions % GRID).astype(jnp.float32))
    pieces = []
    for which_half in range(2):
        half_value = value[..., which_half * 2 * quarter : (which_half + 1) * 2 * quarter]
        angle = places[which_half][:, None] * rates[None, :]
        cosine = jnp.cos(angle)[None, :, None, :]
        sine = jnp.sin(angle)[None, :, None, :]
        first = half_value[..., :quarter]
        second = half_value[..., quarter:]
        pieces.append(first * cosine - second * sine)
        pieces.append(second * cosine + first * sine)
    return jnp.concatenate(pieces, axis=-1)


def head_prepare(raw, gain, positions):
    scaled = raw * lax.rsqrt(jnp.mean(raw * raw, axis=-1, keepdims=True) + EPS) * gain
    return rotate(scaled, positions)


def time_features(steps_in):
    half = FREQ // 2
    rates = jnp.exp(-math.log(10000.0) * jnp.arange(half, dtype=jnp.float32) / half)
    angle = steps_in.astype(jnp.float32)[:, None] * rates[None, :]
    return jnp.concatenate([jnp.cos(angle), jnp.sin(angle)], axis=-1)


CHUNKS = 4


def rows_of(block, total):
    size = total // CHUNKS
    return pl.ds(pl.multiple_of(block * size, size), size)


class Line:
    def __init__(self, count, gathered, summed, ag_sems, rs_sems):
        self.count = count
        self.place = lax.axis_index("tensor")
        self.gathered = gathered
        self.summed = summed
        self.ag_send, self.ag_recv = ag_sems
        self.rs_send, self.rs_recv = rs_sems

    def barrier(self):
        place, count = self.place, self.count
        sem = pltpu.get_barrier_semaphore()

        @pl.when(place > 0)
        def _():
            pl.semaphore_signal(sem, inc=1, device_id={"tensor": place - 1})

        @pl.when(place < count - 1)
        def _():
            pl.semaphore_signal(sem, inc=1, device_id={"tensor": place + 1})

        peers = jnp.where(place > 0, 1, 0) + jnp.where(place < count - 1, 1, 0)
        pl.semaphore_wait(sem, peers)

    def item_copy(self, which, way, item, own=False):
        mine, everyone = self.gathered[which]
        target = self.place + (1 if way == 0 else -1)
        return pltpu.make_async_remote_copy(
            src_ref=mine if own else everyone.at[item],
            dst_ref=everyone.at[item],
            send_sem=self.ag_send.at[which, way, item],
            recv_sem=self.ag_recv.at[which, way, item],
            device_id={"tensor": target},
        )

    def can(self, way):
        return self.place < self.count - 1 if way == 0 else self.place > 0

    def sum_copy(self, which, way, item, block):
        part, landed = self.summed[which]
        target = self.place + (1 if way == 0 else -1)
        slot = item
        if way == 1:
            slot = jnp.where(item == target, self.count, item)
        rows = rows_of(block, part.shape[1])
        return pltpu.make_async_remote_copy(
            src_ref=part.at[item, rows],
            dst_ref=landed.at[slot, rows],
            send_sem=self.rs_send.at[which, way, item, block],
            recv_sem=self.rs_recv.at[which, way, item, block],
            device_id={"tensor": target},
        )

    def landed_slot(self, way, item):
        return jnp.where(item == self.place, self.count, item) if way == 1 else item

    def wait_sum(self, which, way, item, block):
        part, landed = self.summed[which]
        rows = rows_of(block, part.shape[1])
        view = landed.at[self.landed_slot(way, item), rows]
        pltpu.make_async_remote_copy(
            src_ref=view,
            dst_ref=view,
            send_sem=self.rs_send.at[which, way, item, block],
            recv_sem=self.rs_recv.at[which, way, item, block],
            device_id={"tensor": self.place},
        ).wait_recv()
        return view

    def start_own(self):
        for which in range(len(self.gathered)):
            for way in range(2):

                @pl.when(self.can(way))
                def _():
                    self.item_copy(which, way, self.place, own=True).start()

    def receive(self, step):
        place, count = self.place, self.count
        for which in range(len(self.gathered)):
            for way in range(2):
                item = place - step if way == 0 else place + step

                @pl.when((item >= 0) & (item < count))
                def _():
                    self.item_copy(which, way, item).wait_recv()

                    @pl.when(self.can(way))
                    def _():
                        self.item_copy(which, way, item).start()

    def items(self, step):
        place, count = self.place, self.count
        low, high = place - step, place + step
        return ((low, (low >= 0)), (high, (high < count) & (step > 0)))

    def pass_sums(self, step):
        place, count = self.place, self.count

        @pl.loop(0, CHUNKS)
        def _(block):
            for which in range(len(self.summed)):
                part, landed = self.summed[which]
                rows = rows_of(block, part.shape[1])
                for way in range(2):
                    item = step if way == 0 else count - 1 - step
                    further = item > place if way == 0 else item < place
                    first = place == 0 if way == 0 else place == count - 1

                    @pl.when(further & jnp.logical_not(first))
                    def _():
                        view = self.wait_sum(which, way, item, block)
                        total = part[item, rows].astype(jnp.float32) + view[...].astype(
                            jnp.float32
                        )
                        part[item, rows] = total.astype(part.dtype)

                    @pl.when(further)
                    def _():
                        self.sum_copy(which, way, item, block).start()

    def finish(self, which, out):
        place, count = self.place, self.count
        part, landed = self.summed[which]

        @pl.loop(0, CHUNKS)
        def _(block):
            rows = rows_of(block, part.shape[1])
            out[rows] = part[place, rows].astype(jnp.float32)
            for way in range(2):

                @pl.when(place > 0 if way == 0 else place < count - 1)
                def _():
                    view = self.wait_sum(which, way, place, block)
                    out[rows] += view[...].astype(jnp.float32)

    def drain(self):
        place, count = self.place, self.count

        @pl.loop(0, count)
        def _(item):
            for way in range(2):
                passed = item <= place if way == 0 else item >= place

                @pl.when(passed & self.can(way))
                def _():
                    for which in range(len(self.gathered)):
                        self.item_copy(which, way, item).wait_send()

                further = item > place if way == 0 else item < place

                @pl.when(further)
                def _():
                    @pl.loop(0, CHUNKS)
                    def _(block):
                        for which in range(len(self.summed)):
                            self.sum_copy(which, way, item, block).wait_send()


def dot(left, right):
    return jnp.dot(left, right, preferred_element_type=jnp.float32)


def dot_rt(left, right):
    return lax.dot_general(
        left, right, (((1,), (1,)), ((), ())), preferred_element_type=jnp.float32
    )


def dot_lt(left, right):
    return lax.dot_general(
        left, right, (((0,), (0,)), ((), ())), preferred_element_type=jnp.float32
    )


def cut(total, most):
    size = max(s for s in range(128, most + 1, 128) if total % s == 0)
    return size, total // size


def span(index, size):
    return pl.ds(pl.multiple_of(index * size, size), size)


def feed_kernel(
    count,
    mod_ref,
    grad_ref,
    expand_hbm,
    down_hbm,
    feed_out,
    back_out,
    weight_out,
    expand,
    down,
    mod_all,
    grad_all,
    hidden,
    slopes,
    feed_part,
    back_part,
    feed_land,
    back_land,
    total,
    load_sem,
    ag_send,
    ag_recv,
    rs_send,
    rs_recv,
):
    line = Line(
        count,
        [(mod_ref, mod_all), (grad_ref, grad_all)],
        [(back_part, back_land), (feed_part, feed_land)],
        (ag_send, ag_recv),
        (rs_send, rs_recv),
    )
    width, units = expand.shape[1], expand.shape[2]
    loads = (
        pltpu.make_async_copy(expand_hbm, expand, load_sem.at[0]),
        pltpu.make_async_copy(down_hbm, down, load_sem.at[1]),
    )
    for load in loads:
        load.start()
    line.barrier()
    line.start_own()
    mod_all[line.place] = mod_ref[...]
    grad_all[line.place] = grad_ref[...]
    total[...] = jnp.zeros_like(total)
    for load in loads:
        load.wait()
    unit_size, unit_count = cut(units, 256)
    wide_size, wide_count = cut(width, 384)
    tall_size, tall_count = cut(width, 128)

    def compute(item):
        @pl.loop(0, unit_count)
        def _(index):
            cols = span(index, unit_size)
            mod = mod_all[item]
            gate = dot(mod, expand[0, :, cols])
            upper = dot(mod, expand[1, :, cols])
            back = dot_rt(grad_all[item], down[cols, :])
            sigma = jax.nn.sigmoid(gate)
            active = gate * sigma
            hidden[item, :, cols] = (active * upper).astype(jnp.bfloat16)
            slopes[0, item, :, cols] = (
                back * upper * (sigma * (1.0 + gate * (1.0 - sigma)))
            ).astype(jnp.bfloat16)
            slopes[1, item, :, cols] = (back * active).astype(jnp.bfloat16)

        @pl.loop(0, wide_count)
        def _(index):
            cols = span(index, wide_size)
            back_part[item, :, cols] = (
                dot_rt(slopes[0, item], expand[0, cols, :])
                + dot_rt(slopes[1, item], expand[1, cols, :])
            ).astype(jnp.bfloat16)
            feed_part[item, :, cols] = dot(hidden[item], down[:, cols]).astype(jnp.bfloat16)

    def weigh(item):
        @pl.loop(0, tall_count)
        def _(index):
            rows = span(index, tall_size)
            mod = mod_all[item, :, rows]
            total[0, rows, :] += dot_lt(mod, slopes[0, item])
            total[1, rows, :] += dot_lt(mod, slopes[1, item])
            total[2, rows, :] += dot_lt(grad_all[item, :, rows], hidden[item])

    @pl.loop(0, count)
    def _(step):
        @pl.when(step > 0)
        def _():
            for item, valid in line.items(step - 1):

                @pl.when(valid)
                def _():
                    weigh(item)

            line.receive(step)

        for item, valid in line.items(step):

            @pl.when(valid)
            def _():
                compute(item)

        @pl.when(step > 0)
        def _():
            line.pass_sums(step)

    for item, valid in line.items(count - 1):

        @pl.when(valid)
        def _():
            weigh(item)

    weight_out[...] = total[...].astype(jnp.bfloat16)
    line.finish(0, back_out)
    line.finish(1, feed_out)
    line.drain()


def feed_pass(mod_two, branch_grad, expand_weight, down_weight):
    count = lax.axis_size("tensor")
    length, width = mod_two.shape
    units = down_weight.shape[0]
    expand = jnp.transpose(expand_weight, (1, 0, 2))
    vmem, any_space = pl.BlockSpec(memory_space=pltpu.VMEM), pl.BlockSpec(memory_space=pl.ANY)
    low = jnp.bfloat16
    item = (length, width)
    return pl.pallas_call(
        functools.partial(feed_kernel, count),
        out_shape=(
            jax.ShapeDtypeStruct(item, jnp.float32),
            jax.ShapeDtypeStruct(item, jnp.float32),
            jax.ShapeDtypeStruct((3, width, units), low),
        ),
        in_specs=[vmem, vmem, any_space, any_space],
        out_specs=(vmem, vmem, vmem),
        scratch_shapes=[
            pltpu.VMEM((2, width, units), low),
            pltpu.VMEM((units, width), low),
            pltpu.VMEM((count, *item), low),
            pltpu.VMEM((count, *item), low),
            pltpu.VMEM((count, length, units), low),
            pltpu.VMEM((2, count, length, units), low),
            pltpu.VMEM((count, *item), low),
            pltpu.VMEM((count, *item), low),
            pltpu.VMEM((count + 1, *item), low),
            pltpu.VMEM((count + 1, *item), low),
            pltpu.VMEM((3, width, units), jnp.float32),
            pltpu.SemaphoreType.DMA((2,)),
            pltpu.SemaphoreType.DMA((2, 2, count)),
            pltpu.SemaphoreType.DMA((2, 2, count)),
            pltpu.SemaphoreType.DMA((2, 2, count, CHUNKS)),
            pltpu.SemaphoreType.DMA((2, 2, count, CHUNKS)),
        ],
        compiler_params=pltpu.CompilerParams(
            collective_id=1, has_side_effects=True, vmem_limit_bytes=64000000
        ),
        name="feed_pass",
    )(mod_two, branch_grad, expand, down_weight)


def shards(
    tokens,
    timesteps,
    labels,
    item_counts,
    cotangent,
    project_weight,
    query_gain,
    key_gain,
    output_weight,
    output_bias,
    expand_weight,
    down_weight,
    down_bias,
    modulate_weight,
    modulate_bias,
    time_weight,
    time_bias,
    embed_weight,
    embed_bias,
    class_table,
):
    local_items, length, width = tokens.shape
    items = timesteps.shape[0]
    slab = modulate_weight.shape[2]
    heads_here = project_weight.shape[2] // HD
    scale = HD ** (-0.5)
    lane = lax.axis_index("tensor")
    first_item = lane * local_items
    live = (first_item + jnp.arange(local_items) < item_counts[0]).astype(jnp.float32)[
        :, None, None
    ]
    index = lax.axis_index("dp")
    tags = lax.all_gather(jnp.stack([timesteps, labels]), "dp", axis=1, tiled=True)
    time_feat = time_features(tags[0]).astype(jnp.bfloat16)
    pre_hidden = jnp.dot(
        time_feat, time_weight, preferred_element_type=jnp.float32
    ) + time_bias.astype(jnp.float32)
    time_hidden = jax.nn.silu(pre_hidden).astype(jnp.bfloat16)
    condition = (
        jnp.dot(time_hidden, embed_weight, preferred_element_type=jnp.float32)
        + embed_bias.astype(jnp.float32)
        + jnp.take(class_table, tags[1], axis=0).astype(jnp.float32)
    )
    cond_act = jax.nn.silu(condition).astype(jnp.bfloat16)
    cond_act_here = lax.dynamic_slice_in_dim(cond_act, index * items, items, 0)
    condition_here = lax.dynamic_slice_in_dim(condition, index * items, items, 0)
    modulation_part = (
        jnp.einsum("bd,dke->bke", cond_act_here, modulate_weight, preferred_element_type=jnp.float32)
        + modulate_bias.astype(jnp.float32)
    ).astype(jnp.bfloat16)
    modulation_local = lax.all_to_all(
        modulation_part, "tensor", split_axis=0, concat_axis=2, tiled=True
    ).astype(jnp.float32)
    local_parts = [modulation_local[:, which][:, None, :] for which in range(6)]
    attend_shift, attend_scale, attend_gate, feed_shift, feed_scale, feed_gate = local_parts
    positions = jnp.arange(length)
    token_local = tokens.astype(jnp.float32)
    normed_local, inverse_local = layer_norm(token_local)
    mod_in = lax.all_gather(
        (normed_local * (1.0 + attend_scale) + attend_shift).astype(jnp.bfloat16),
        "tensor",
        axis=0,
        tiled=True,
    )
    projected = jnp.einsum(
        "bld,dke->blke", mod_in, project_weight, preferred_element_type=jnp.float32
    )
    split = projected.reshape(items, length, 3, heads_here, HD)
    query_gain_f = query_gain.astype(jnp.float32)
    key_gain_f = key_gain.astype(jnp.float32)
    queries = head_prepare(split[:, :, 0], query_gain_f, positions).astype(jnp.bfloat16)
    keys = head_prepare(split[:, :, 1], key_gain_f, positions).astype(jnp.bfloat16)
    values = split[:, :, 2].astype(jnp.bfloat16)
    scores = (
        jnp.einsum("bqhd,bkhd->bhqk", queries, keys, preferred_element_type=jnp.float32) * scale
    )
    top = jnp.max(scores, axis=-1, keepdims=True)
    logsum = top + jnp.log(jnp.sum(jnp.exp(scores - top), axis=-1, keepdims=True))
    probs = jnp.exp(scores - logsum).astype(jnp.bfloat16)
    mixed = jnp.einsum("bhqk,bkhd->bqhd", probs, values, preferred_element_type=jnp.float32)
    mixed = mixed.reshape(items, length, heads_here * HD).astype(jnp.bfloat16)
    piece = mixed
    attend_branch = lax.psum_scatter(
        jnp.einsum("blh,hd->bld", piece, output_weight, preferred_element_type=jnp.float32).astype(
            jnp.bfloat16
        ),
        "tensor",
        scatter_dimension=0,
        tiled=True,
    ).astype(jnp.float32) + output_bias.astype(jnp.float32)
    residual = token_local + attend_gate * attend_branch
    normed_two, inverse_two = layer_norm(residual)
    mod_two = (normed_two * (1.0 + feed_scale) + feed_shift).astype(jnp.bfloat16)
    out_grad = cotangent.astype(jnp.float32) * live
    branch_grad = (out_grad * feed_gate).astype(jnp.bfloat16)
    down_bias_part = jnp.sum(branch_grad.astype(jnp.float32), axis=(0, 1))
    feed_total, mod_two_grad, feed_weights = feed_pass(
        mod_two[0], branch_grad[0], expand_weight, down_weight
    )
    feed_branch = feed_total[None] + down_bias.astype(jnp.float32)
    result = (live * (residual + feed_gate * feed_branch)).astype(jnp.bfloat16)
    mod_two_grad = mod_two_grad[None]
    residual_grad = out_grad + layer_norm_back(
        normed_two, inverse_two, mod_two_grad * (1.0 + feed_scale)
    )
    attend_grad = (residual_grad * attend_gate).astype(jnp.bfloat16)
    output_bias_part = jnp.sum(attend_grad.astype(jnp.float32), axis=(0, 1))
    piece = lax.all_gather(attend_grad, "tensor", axis=0, tiled=True)
    weight_total = jnp.einsum("blh,bld->hd", mixed, piece, preferred_element_type=jnp.float32)
    rows_grad = jnp.einsum("bld,hd->blh", piece, output_weight, preferred_element_type=jnp.float32)
    output_weight_grad = weight_total
    mixed_grad = rows_grad
    mixed_grad = mixed_grad.reshape(items, length, heads_here, HD).astype(jnp.bfloat16)
    again = jnp.einsum("bqhd,bkhd->bhqk", queries, keys, preferred_element_type=jnp.float32) * scale
    prob_float = jnp.exp(again - logsum)
    prob_low = prob_float.astype(jnp.bfloat16)
    prob_grad = jnp.einsum(
        "bqhd,bkhd->bhqk", mixed_grad, values, preferred_element_type=jnp.float32
    )
    score_grad = (
        prob_float * (prob_grad - jnp.sum(prob_float * prob_grad, axis=-1, keepdims=True))
    ).astype(jnp.bfloat16)
    query_grad = (
        jnp.einsum("bhqk,bkhd->bqhd", score_grad, keys, preferred_element_type=jnp.float32) * scale
    )
    key_grad = (
        jnp.einsum("bhqk,bqhd->bkhd", score_grad, queries, preferred_element_type=jnp.float32)
        * scale
    )
    value_grad = jnp.einsum(
        "bhqk,bqhd->bkhd", prob_low, mixed_grad, preferred_element_type=jnp.float32
    )

    def prepare_here(raw, gain):
        return head_prepare(raw, gain, positions)

    _, query_back = jax.vjp(prepare_here, split[:, :, 0], query_gain_f)
    raw_query_grad, query_gain_part = query_back(query_grad)
    _, key_back = jax.vjp(prepare_here, split[:, :, 1], key_gain_f)
    raw_key_grad, key_gain_part = key_back(key_grad)
    projected_grad = jnp.stack([raw_query_grad, raw_key_grad, value_grad], axis=2)
    projected_grad = projected_grad.reshape(items, length, 3, heads_here * HD).astype(jnp.bfloat16)
    project_grad = jnp.einsum(
        "bld,blke->dke", mod_in, projected_grad, preferred_element_type=jnp.float32
    )
    piece = projected_grad
    mod_in_grad = lax.psum_scatter(
        jnp.einsum(
            "blke,dke->bld", piece, project_weight, preferred_element_type=jnp.float32
        ).astype(jnp.bfloat16),
        "tensor",
        scatter_dimension=0,
        tiled=True,
    ).astype(jnp.float32)
    tokens_grad = (
        residual_grad
        + layer_norm_back(normed_local, inverse_local, mod_in_grad * (1.0 + attend_scale))
    ).astype(jnp.bfloat16)
    modulation_grad_part = jnp.stack(
        [
            jnp.sum(mod_in_grad, axis=1),
            jnp.sum(mod_in_grad * normed_local, axis=1),
            jnp.sum(residual_grad * attend_branch, axis=1),
            jnp.sum(mod_two_grad, axis=1),
            jnp.sum(mod_two_grad * normed_two, axis=1),
            jnp.sum(out_grad * feed_branch, axis=1),
        ],
        axis=1,
    )
    modulation_grad = lax.all_to_all(
        modulation_grad_part, "tensor", split_axis=2, concat_axis=0, tiled=True
    ).astype(jnp.bfloat16)
    modulate_bias_part = jnp.sum(modulation_grad.astype(jnp.float32), axis=0)
    cond_part = jnp.einsum(
        "bke,dke->bd", modulation_grad, modulate_weight, preferred_element_type=jnp.float32
    )
    cond_total = lax.psum(cond_part, "tensor")
    cond_grad_here = (cond_total * silu_slope(condition_here)).astype(jnp.bfloat16)
    packed = jnp.concatenate([cond_grad_here, modulation_grad.reshape(items, 6 * slab)], axis=1)
    packed = lax.all_gather(packed, "dp", axis=0, tiled=True)
    cond_grad = packed[:, :width]
    modulation_grad_all = packed[:, width:].reshape(-1, 6, slab)
    share = width // lax.axis_size("dp")

    def mine(value, axis):
        return lax.dynamic_slice_in_dim(value, index * share, share, axis)

    one_hot = (tags[1][:, None] == jnp.arange(class_table.shape[0])[None, :]).astype(jnp.bfloat16)
    cond_grad_mine = mine(cond_grad, 1)
    class_grad = jnp.einsum(
        "bc,bd->cd", one_hot, cond_grad_mine, preferred_element_type=jnp.float32
    )
    pre_grad = (
        jnp.einsum(
            "be,de->bd", cond_grad, mine(embed_weight, 0), preferred_element_type=jnp.float32
        )
        * silu_slope(mine(pre_hidden, 1))
    ).astype(jnp.bfloat16)
    modulate_grad = jnp.einsum(
        "bd,bke->dke", mine(cond_act, 1), modulation_grad_all, preferred_element_type=jnp.float32
    )
    embed_grad = jnp.einsum(
        "bd,be->de", mine(time_hidden, 1), cond_grad, preferred_element_type=jnp.float32
    )
    embed_bias_grad = jnp.sum(cond_grad_mine.astype(jnp.float32), axis=0)
    time_grad = jnp.einsum("bf,bd->fd", time_feat, pre_grad, preferred_element_type=jnp.float32)
    time_bias_grad = jnp.sum(pre_grad.astype(jnp.float32), axis=0)
    bias_wide = lax.dynamic_update_slice_in_dim(
        jnp.zeros((6, width), jnp.float32), modulate_bias_part, lane * slab, 1
    )
    small = jnp.concatenate(
        [
            output_bias_part,
            down_bias_part,
            bias_wide.reshape(-1),
            query_gain_part,
            key_gain_part,
        ]
    )
    small = lax.psum(small, ("dp", "tensor"))
    output_bias_grad = small[:width]
    down_bias_grad = small[width : 2 * width]
    modulate_bias_grad = small[2 * width : 8 * width].reshape(6, width)
    query_gain_grad = small[8 * width : 8 * width + HD]
    key_gain_grad = small[8 * width + HD :]

    def scatter(value, axis):
        value = value.astype(jnp.bfloat16)
        return lax.psum_scatter(value, "dp", scatter_dimension=axis, tiled=True).astype(
            jnp.float32
        )

    project_grad = scatter(project_grad, 0)
    output_weight_grad = scatter(output_weight_grad, 1)
    feed_weights = scatter(feed_weights, 1)
    expand_grad = jnp.transpose(feed_weights[:2], (1, 0, 2))
    down_grad = feed_weights[2].T
    return (
        result,
        tokens_grad,
        project_grad,
        query_gain_grad,
        key_gain_grad,
        output_weight_grad,
        output_bias_grad,
        expand_grad,
        down_grad,
        down_bias_grad,
        modulate_grad,
        modulate_bias_grad,
        time_grad,
        time_bias_grad,
        embed_grad,
        embed_bias_grad,
        class_grad,
    )


def solution(mesh):
    return jax.shard_map(
        shards,
        mesh=mesh,
        in_specs=(
            P(("dp", "tensor"), None, None),
            P("dp"),
            P("dp"),
            P("dp"),
            P(("dp", "tensor"), None, None),
            P(None, None, "tensor"),
            P(),
            P(),
            P("tensor", None),
            P(),
            P(None, None, "tensor"),
            P("tensor", None),
            P(),
            P(None, None, "tensor"),
            P(None, "tensor"),
            P(),
            P(),
            P(),
            P(),
            P(),
        ),
        out_specs=(
            P(("dp", "tensor"), None, None),
            P(("dp", "tensor"), None, None),
            P("dp", None, "tensor"),
            P(),
            P(),
            P("tensor", "dp"),
            P(),
            P("dp", None, "tensor"),
            P("tensor", "dp"),
            P(),
            P("dp", None, "tensor"),
            P(),
            P(None, "dp"),
            P("dp"),
            P("dp", None),
            P("dp"),
            P(None, "dp"),
        ),
        check_vma=False,
    )
```

```python
import functools
import math

import jax
import jax.numpy as jnp
from jax import lax
from jax.experimental import pallas as pl
from jax.experimental.pallas import tpu as pltpu
from jax.sharding import PartitionSpec as P

HD = 72
FREQ = 256
GRID = 16


EPS = 1e-06


def layer_norm(value):
    center = value - jnp.mean(value, axis=-1, keepdims=True)
    inverse = lax.rsqrt(jnp.mean(center * center, axis=-1, keepdims=True) + EPS)
    return (center * inverse, inverse)


def layer_norm_back(normed, inverse, grad):
    return inverse * (
        grad
        - jnp.mean(grad, axis=-1, keepdims=True)
        - normed * jnp.mean(grad * normed, axis=-1, keepdims=True)
    )


def silu_slope(value):
    sigma = jax.nn.sigmoid(value)
    return sigma * (1.0 + value * (1.0 - sigma))


def rotate(value, positions):
    quarter = HD // 4
    rates = 10000.0 ** (-jnp.arange(quarter, dtype=jnp.float32) / quarter)
    places = ((positions // GRID).astype(jnp.float32), (positions % GRID).astype(jnp.float32))
    pieces = []
    for which_half in range(2):
        half_value = value[..., which_half * 2 * quarter : (which_half + 1) * 2 * quarter]
        angle = places[which_half][:, None] * rates[None, :]
        cosine = jnp.cos(angle)[None, :, None, :]
        sine = jnp.sin(angle)[None, :, None, :]
        first = half_value[..., :quarter]
        second = half_value[..., quarter:]
        pieces.append(first * cosine - second * sine)
        pieces.append(second * cosine + first * sine)
    return jnp.concatenate(pieces, axis=-1)


def head_prepare(raw, gain, positions):
    scaled = raw * lax.rsqrt(jnp.mean(raw * raw, axis=-1, keepdims=True) + EPS) * gain
    return rotate(scaled, positions)


def time_features(steps_in):
    half = FREQ // 2
    rates = jnp.exp(-math.log(10000.0) * jnp.arange(half, dtype=jnp.float32) / half)
    angle = steps_in.astype(jnp.float32)[:, None] * rates[None, :]
    return jnp.concatenate([jnp.cos(angle), jnp.sin(angle)], axis=-1)


CHUNKS = 8


def rows_of(block, total):
    size = total // CHUNKS
    return pl.ds(pl.multiple_of(block * size, size), size)


class Line:
    def __init__(self, count, gathered, summed, ag_sems, rs_sems):
        self.count = count
        self.place = lax.axis_index("tensor")
        self.gathered = gathered
        self.summed = summed
        self.ag_send, self.ag_recv = ag_sems
        self.rs_send, self.rs_recv = rs_sems

    def barrier(self):
        place, count = self.place, self.count
        sem = pltpu.get_barrier_semaphore()

        @pl.when(place > 0)
        def _():
            pl.semaphore_signal(sem, inc=1, device_id={"tensor": place - 1})

        @pl.when(place < count - 1)
        def _():
            pl.semaphore_signal(sem, inc=1, device_id={"tensor": place + 1})

        peers = jnp.where(place > 0, 1, 0) + jnp.where(place < count - 1, 1, 0)
        pl.semaphore_wait(sem, peers)

    def item_copy(self, which, way, item, own=False):
        mine, everyone = self.gathered[which]
        target = self.place + (1 if way == 0 else -1)
        return pltpu.make_async_remote_copy(
            src_ref=mine if own else everyone.at[item],
            dst_ref=everyone.at[item],
            send_sem=self.ag_send.at[which, way, item],
            recv_sem=self.ag_recv.at[which, way, item],
            device_id={"tensor": target},
        )

    def can(self, way):
        return self.place < self.count - 1 if way == 0 else self.place > 0

    def sum_copy(self, which, way, item, block):
        part, landed = self.summed[which]
        target = self.place + (1 if way == 0 else -1)
        slot = item
        if way == 1:
            slot = jnp.where(item == target, self.count, item)
        rows = rows_of(block, part.shape[1])
        return pltpu.make_async_remote_copy(
            src_ref=part.at[item, rows],
            dst_ref=landed.at[slot, rows],
            send_sem=self.rs_send.at[which, way, item, block],
            recv_sem=self.rs_recv.at[which, way, item, block],
            device_id={"tensor": target},
        )

    def landed_slot(self, way, item):
        return jnp.where(item == self.place, self.count, item) if way == 1 else item

    def wait_sum(self, which, way, item, block):
        part, landed = self.summed[which]
        rows = rows_of(block, part.shape[1])
        view = landed.at[self.landed_slot(way, item), rows]
        pltpu.make_async_remote_copy(
            src_ref=view,
            dst_ref=view,
            send_sem=self.rs_send.at[which, way, item, block],
            recv_sem=self.rs_recv.at[which, way, item, block],
            device_id={"tensor": self.place},
        ).wait_recv()
        return view

    def start_own(self):
        for which in range(len(self.gathered)):
            for way in range(2):

                @pl.when(self.can(way))
                def _():
                    self.item_copy(which, way, self.place, own=True).start()

    def receive(self, step):
        place, count = self.place, self.count
        for which in range(len(self.gathered)):
            for way in range(2):
                item = place - step if way == 0 else place + step

                @pl.when((item >= 0) & (item < count))
                def _():
                    self.item_copy(which, way, item).wait_recv()

                    @pl.when(self.can(way))
                    def _():
                        self.item_copy(which, way, item).start()

    def items(self, step):
        place, count = self.place, self.count
        low, high = place - step, place + step
        return ((low, (low >= 0)), (high, (high < count) & (step > 0)))

    def pass_sums(self, step):
        place, count = self.place, self.count
        ways = []
        for way in range(2):
            item = step if way == 0 else count - 1 - step
            ways.append(
                (
                    way,
                    item,
                    item > place if way == 0 else item < place,
                    place if way == 0 else count - 1 - place,
                )
            )

        @pl.loop(0, CHUNKS)
        def _(block):
            for way, item, further, hop in ways:

                @pl.when(further & (hop == 0))
                def _():
                    for which in range(len(self.summed)):
                        self.sum_copy(which, way, item, block).start()

        @pl.loop(0, CHUNKS + count - 3)
        def _(turn):
            for distance in range(1, count - 1):
                block = turn - (distance - 1)
                for way, item, further, hop in ways:

                    @pl.when(further & (hop == distance) & (block >= 0) & (block < CHUNKS))
                    def _():
                        for which in range(len(self.summed)):
                            part, landed = self.summed[which]
                            rows = rows_of(block, part.shape[1])
                            view = self.wait_sum(which, way, item, block)
                            total = part[item, rows].astype(jnp.float32) + view[...].astype(
                                jnp.float32
                            )
                            part[item, rows] = total.astype(part.dtype)
                            self.sum_copy(which, way, item, block).start()

    def finish(self, which, out):
        place, count = self.place, self.count
        part, landed = self.summed[which]

        @pl.loop(0, CHUNKS)
        def _(block):
            rows = rows_of(block, part.shape[1])
            out[rows] = part[place, rows].astype(jnp.float32)
            for way in range(2):

                @pl.when(place > 0 if way == 0 else place < count - 1)
                def _():
                    view = self.wait_sum(which, way, place, block)
                    out[rows] += view[...].astype(jnp.float32)

    def drain(self):
        place, count = self.place, self.count

        @pl.loop(0, count)
        def _(item):
            for way in range(2):
                passed = item <= place if way == 0 else item >= place

                @pl.when(passed & self.can(way))
                def _():
                    for which in range(len(self.gathered)):
                        self.item_copy(which, way, item).wait_send()

                further = item > place if way == 0 else item < place

                @pl.when(further)
                def _():
                    @pl.loop(0, CHUNKS)
                    def _(block):
                        for which in range(len(self.summed)):
                            self.sum_copy(which, way, item, block).wait_send()


def dot(left, right):
    return jnp.dot(left, right, preferred_element_type=jnp.float32)


def dot_rt(left, right):
    return lax.dot_general(
        left, right, (((1,), (1,)), ((), ())), preferred_element_type=jnp.float32
    )


def dot_lt(left, right):
    return lax.dot_general(
        left, right, (((0,), (0,)), ((), ())), preferred_element_type=jnp.float32
    )


def cut(total, most):
    size = max(s for s in range(128, most + 1, 128) if total % s == 0)
    return size, total // size


def span(index, size):
    return pl.ds(pl.multiple_of(index * size, size), size)


def feed_kernel(
    count,
    mod_ref,
    grad_ref,
    expand_hbm,
    down_hbm,
    feed_out,
    back_out,
    weight_out,
    expand,
    down,
    mod_all,
    grad_all,
    hidden,
    slopes,
    feed_part,
    back_part,
    feed_land,
    back_land,
    total,
    load_sem,
    ag_send,
    ag_recv,
    rs_send,
    rs_recv,
):
    line = Line(
        count,
        [(mod_ref, mod_all), (grad_ref, grad_all)],
        [(back_part, back_land), (feed_part, feed_land)],
        (ag_send, ag_recv),
        (rs_send, rs_recv),
    )
    width, units = expand.shape[1], expand.shape[2]
    loads = (
        pltpu.make_async_copy(expand_hbm, expand, load_sem.at[0]),
        pltpu.make_async_copy(down_hbm, down, load_sem.at[1]),
    )
    for load in loads:
        load.start()
    line.barrier()
    line.start_own()
    mod_all[line.place] = mod_ref[...]
    grad_all[line.place] = grad_ref[...]
    total[...] = jnp.zeros_like(total)
    for load in loads:
        load.wait()
    unit_size, unit_count = cut(units, 256)
    wide_size, wide_count = cut(width, 384)
    tall_size, tall_count = cut(width, 128)

    def compute(item):
        @pl.loop(0, unit_count)
        def _(index):
            cols = span(index, unit_size)
            mod = mod_all[item]
            gate = dot(mod, expand[0, :, cols])
            upper = dot(mod, expand[1, :, cols])
            back = dot_rt(grad_all[item], down[cols, :])
            sigma = jax.nn.sigmoid(gate)
            active = gate * sigma
            hidden[item, :, cols] = (active * upper).astype(jnp.bfloat16)
            slopes[0, item, :, cols] = (
                back * upper * (sigma * (1.0 + gate * (1.0 - sigma)))
            ).astype(jnp.bfloat16)
            slopes[1, item, :, cols] = (back * active).astype(jnp.bfloat16)

        @pl.loop(0, wide_count)
        def _(index):
            cols = span(index, wide_size)
            back_part[item, :, cols] = (
                dot_rt(slopes[0, item], expand[0, cols, :])
                + dot_rt(slopes[1, item], expand[1, cols, :])
            ).astype(jnp.bfloat16)
            feed_part[item, :, cols] = dot(hidden[item], down[:, cols]).astype(jnp.bfloat16)

    def weigh(item):
        @pl.loop(0, tall_count)
        def _(index):
            rows = span(index, tall_size)
            mod = mod_all[item, :, rows]
            total[0, rows, :] += dot_lt(mod, slopes[0, item])
            total[1, rows, :] += dot_lt(mod, slopes[1, item])
            total[2, rows, :] += dot_lt(grad_all[item, :, rows], hidden[item])

    @pl.loop(0, count)
    def _(step):
        @pl.when(step > 0)
        def _():
            for item, valid in line.items(step - 1):

                @pl.when(valid)
                def _():
                    weigh(item)

            line.receive(step)

        for item, valid in line.items(step):

            @pl.when(valid)
            def _():
                compute(item)

        @pl.when(step > 0)
        def _():
            line.pass_sums(step)

    for item, valid in line.items(count - 1):

        @pl.when(valid)
        def _():
            weigh(item)

    weight_out[...] = total[...].astype(jnp.bfloat16)
    line.finish(0, back_out)
    line.finish(1, feed_out)
    line.drain()


def feed_pass(mod_two, branch_grad, expand_weight, down_weight):
    count = lax.axis_size("tensor")
    length, width = mod_two.shape
    units = down_weight.shape[0]
    expand = jnp.transpose(expand_weight, (1, 0, 2))
    vmem, any_space = pl.BlockSpec(memory_space=pltpu.VMEM), pl.BlockSpec(memory_space=pl.ANY)
    low = jnp.bfloat16
    item = (length, width)
    return pl.pallas_call(
        functools.partial(feed_kernel, count),
        out_shape=(
            jax.ShapeDtypeStruct(item, jnp.float32),
            jax.ShapeDtypeStruct(item, jnp.float32),
            jax.ShapeDtypeStruct((3, width, units), low),
        ),
        in_specs=[vmem, vmem, any_space, any_space],
        out_specs=(vmem, vmem, vmem),
        scratch_shapes=[
            pltpu.VMEM((2, width, units), low),
            pltpu.VMEM((units, width), low),
            pltpu.VMEM((count, *item), low),
            pltpu.VMEM((count, *item), low),
            pltpu.VMEM((count, length, units), low),
            pltpu.VMEM((2, count, length, units), low),
            pltpu.VMEM((count, *item), low),
            pltpu.VMEM((count, *item), low),
            pltpu.VMEM((count + 1, *item), low),
            pltpu.VMEM((count + 1, *item), low),
            pltpu.VMEM((3, width, units), jnp.float32),
            pltpu.SemaphoreType.DMA((2,)),
            pltpu.SemaphoreType.DMA((2, 2, count)),
            pltpu.SemaphoreType.DMA((2, 2, count)),
            pltpu.SemaphoreType.DMA((2, 2, count, CHUNKS)),
            pltpu.SemaphoreType.DMA((2, 2, count, CHUNKS)),
        ],
        compiler_params=pltpu.CompilerParams(
            collective_id=1, has_side_effects=True, vmem_limit_bytes=64000000
        ),
        name="feed_pass",
    )(mod_two, branch_grad, expand, down_weight)


def swap_kernel(jobs, total, *refs):
    n = len(jobs)
    ins, outs = refs[:n], refs[n + total : 2 * n + total]
    sems = refs[2 * n + 2 * total :]
    places = [lax.axis_index(axis) for axis, _, _ in jobs]
    hello = pltpu.get_barrier_semaphore()
    axes = []
    for axis, count, _ in jobs:
        if (axis, count) not in axes:
            axes.append((axis, count))
    if total:
        axes = [("dp", lax.axis_size("dp")), ("tensor", lax.axis_size("tensor"))]
    for axis, count in axes:
        here = lax.axis_index(axis)

        @pl.loop(1, count)
        def _(offset):
            peer = lax.rem(here + offset, count)
            pl.semaphore_signal(hello, inc=1, device_id={axis: peer})

    pl.semaphore_wait(hello, sum(count - 1 for _, count in axes))

    def copy(source, target, send, recv, axis, peer, slot):
        return pltpu.make_async_remote_copy(
            src_ref=source,
            dst_ref=target.at[slot],
            send_sem=send.at[peer],
            recv_sem=recv.at[slot],
            device_id={axis: peer},
        )

    def start(source, target, send, recv, axis, count, split):
        here = lax.axis_index(axis)

        @pl.loop(1, count)
        def _(offset):
            peer = lax.rem(here + offset, count)
            piece = source.at[peer] if split else source
            copy(piece, target, send, recv, axis, peer, here).start()

        target[here] = source[here] if split else source[...]

    def finish(source, target, send, recv, axis, count, split):
        here = lax.axis_index(axis)

        @pl.loop(1, count)
        def _(offset):
            peer = lax.rem(here + offset, count)
            piece = source.at[peer] if split else source
            step = copy(piece, target, send, recv, axis, peer, peer)
            step.wait_recv()
            step.wait_send()

    work = []
    for index, (axis, count, split) in enumerate(jobs):
        work.append((ins[index], outs[index], sems[2 * index], sems[2 * index + 1], axis, count, split))
    if total:
        source, result = refs[n], refs[2 * n + total]
        one, two, middle, s1, r1, s2, r2 = sems[2 * n :]
        wide, deep = lax.axis_size("dp"), lax.axis_size("tensor")
        first = (source, one, s1, r1, "dp", wide, False)
        start(*first)
    for job in work:
        start(*job)
    if total:
        finish(*first)
        middle[...] = one[0]

        @pl.loop(1, wide)
        def _(index):
            middle[...] += one[index]

        second = (middle, two, s2, r2, "tensor", deep, False)
        start(*second)
    for job in work:
        finish(*job)
    if total:
        finish(*second)
        result[...] = two[0]

        @pl.loop(1, deep)
        def _(index):
            result[...] += two[index]


def swap(name, number, jobs, total=None):
    vmem = pl.BlockSpec(memory_space=pltpu.VMEM)
    plan, arrays, shapes, scratch = [], [], [], []
    for array, axis, split in jobs:
        count = lax.axis_size(axis)
        plan.append((axis, count, split))
        arrays.append(array)
        piece = array.shape[1:] if split else array.shape
        shapes.append(jax.ShapeDtypeStruct((count, *piece), array.dtype))
        scratch += [pltpu.SemaphoreType.DMA((count,)), pltpu.SemaphoreType.DMA((count,))]
    if total is not None:
        wide, deep = lax.axis_size("dp"), lax.axis_size("tensor")
        arrays.append(total)
        shapes.append(jax.ShapeDtypeStruct(total.shape, total.dtype))
        scratch += [
            pltpu.VMEM((wide, *total.shape), total.dtype),
            pltpu.VMEM((deep, *total.shape), total.dtype),
            pltpu.VMEM(total.shape, total.dtype),
        ]
        for count in (wide, wide, deep, deep):
            scratch.append(pltpu.SemaphoreType.DMA((count,)))
    return pl.pallas_call(
        functools.partial(swap_kernel, tuple(plan), int(total is not None)),
        out_shape=tuple(shapes),
        in_specs=[vmem] * len(arrays),
        out_specs=tuple([vmem] * len(shapes)),
        scratch_shapes=scratch,
        compiler_params=pltpu.CompilerParams(collective_id=number, has_side_effects=True),
        name=name,
    )(*arrays)


def shards(
    tokens,
    timesteps,
    labels,
    item_counts,
    cotangent,
    project_weight,
    query_gain,
    key_gain,
    output_weight,
    output_bias,
    expand_weight,
    down_weight,
    down_bias,
    modulate_weight,
    modulate_bias,
    time_weight,
    time_bias,
    embed_weight,
    embed_bias,
    class_table,
):
    local_items, length, width = tokens.shape
    items = timesteps.shape[0]
    slab = modulate_weight.shape[2]
    heads_here = project_weight.shape[2] // HD
    scale = HD ** (-0.5)
    first_item = lax.axis_index("tensor") * local_items
    live = (first_item + jnp.arange(local_items) < item_counts[0]).astype(jnp.float32)[
        :, None, None
    ]
    index = lax.axis_index("dp")
    time_feat = time_features(timesteps).astype(jnp.bfloat16)
    pre_hidden = jnp.dot(
        time_feat, time_weight, preferred_element_type=jnp.float32
    ) + time_bias.astype(jnp.float32)
    time_hidden = jax.nn.silu(pre_hidden).astype(jnp.bfloat16)
    condition = (
        jnp.dot(time_hidden, embed_weight, preferred_element_type=jnp.float32)
        + embed_bias.astype(jnp.float32)
        + jnp.take(class_table, labels, axis=0).astype(jnp.float32)
    )
    cond_act = jax.nn.silu(condition).astype(jnp.bfloat16)
    modulation_part = (
        jnp.einsum("bd,dke->bke", cond_act, modulate_weight, preferred_element_type=jnp.float32)
        + modulate_bias.astype(jnp.float32)
    ).astype(jnp.bfloat16)
    (modulation_local,) = swap("modulation_swap", 2, [(modulation_part, "tensor", True)])
    modulation_local = jnp.transpose(modulation_local, (1, 0, 2)).reshape(1, 6, width)
    modulation_local = modulation_local.astype(jnp.float32)
    local_parts = [modulation_local[:, which][:, None, :] for which in range(6)]
    attend_shift, attend_scale, attend_gate, feed_shift, feed_scale, feed_gate = local_parts
    positions = jnp.arange(length)
    token_local = tokens.astype(jnp.float32)
    normed_local, inverse_local = layer_norm(token_local)
    mod_in = lax.all_gather(
        (normed_local * (1.0 + attend_scale) + attend_shift).astype(jnp.bfloat16),
        "tensor",
        axis=0,
        tiled=True,
    )
    projected = jnp.einsum(
        "bld,dke->blke", mod_in, project_weight, preferred_element_type=jnp.float32
    )
    split = projected.reshape(items, length, 3, heads_here, HD)
    query_gain_f = query_gain.astype(jnp.float32)
    key_gain_f = key_gain.astype(jnp.float32)
    queries = head_prepare(split[:, :, 0], query_gain_f, positions).astype(jnp.bfloat16)
    keys = head_prepare(split[:, :, 1], key_gain_f, positions).astype(jnp.bfloat16)
    values = split[:, :, 2].astype(jnp.bfloat16)
    scores = (
        jnp.einsum("bqhd,bkhd->bhqk", queries, keys, preferred_element_type=jnp.float32) * scale
    )
    top = jnp.max(scores, axis=-1, keepdims=True)
    logsum = top + jnp.log(jnp.sum(jnp.exp(scores - top), axis=-1, keepdims=True))
    probs = jnp.exp(scores - logsum).astype(jnp.bfloat16)
    mixed = jnp.einsum("bhqk,bkhd->bqhd", probs, values, preferred_element_type=jnp.float32)
    mixed = mixed.reshape(items, length, heads_here * HD).astype(jnp.bfloat16)
    piece = mixed
    attend_branch = lax.psum_scatter(
        jnp.einsum("blh,hd->bld", piece, output_weight, preferred_element_type=jnp.float32).astype(
            jnp.bfloat16
        ),
        "tensor",
        scatter_dimension=0,
        tiled=True,
    ).astype(jnp.float32) + output_bias.astype(jnp.float32)
    residual = token_local + attend_gate * attend_branch
    normed_two, inverse_two = layer_norm(residual)
    mod_two = (normed_two * (1.0 + feed_scale) + feed_shift).astype(jnp.bfloat16)
    out_grad = cotangent.astype(jnp.float32) * live
    branch_grad = (out_grad * feed_gate).astype(jnp.bfloat16)
    down_bias_part = jnp.sum(branch_grad.astype(jnp.float32), axis=(0, 1))
    feed_total, mod_two_grad, feed_weights = feed_pass(
        mod_two[0], branch_grad[0], expand_weight, down_weight
    )
    feed_branch = feed_total[None] + down_bias.astype(jnp.float32)
    result = (live * (residual + feed_gate * feed_branch)).astype(jnp.bfloat16)
    mod_two_grad = mod_two_grad[None]
    residual_grad = out_grad + layer_norm_back(
        normed_two, inverse_two, mod_two_grad * (1.0 + feed_scale)
    )
    attend_grad = (residual_grad * attend_gate).astype(jnp.bfloat16)
    output_bias_part = jnp.sum(attend_grad.astype(jnp.float32), axis=(0, 1))
    piece = lax.all_gather(attend_grad, "tensor", axis=0, tiled=True)
    weight_total = jnp.einsum("blh,bld->hd", mixed, piece, preferred_element_type=jnp.float32)
    rows_grad = jnp.einsum("bld,hd->blh", piece, output_weight, preferred_element_type=jnp.float32)
    output_weight_grad = weight_total
    mixed_grad = rows_grad
    mixed_grad = mixed_grad.reshape(items, length, heads_here, HD).astype(jnp.bfloat16)
    again = jnp.einsum("bqhd,bkhd->bhqk", queries, keys, preferred_element_type=jnp.float32) * scale
    prob_float = jnp.exp(again - logsum)
    prob_low = prob_float.astype(jnp.bfloat16)
    prob_grad = jnp.einsum(
        "bqhd,bkhd->bhqk", mixed_grad, values, preferred_element_type=jnp.float32
    )
    score_grad = (
        prob_float * (prob_grad - jnp.sum(prob_float * prob_grad, axis=-1, keepdims=True))
    ).astype(jnp.bfloat16)
    query_grad = (
        jnp.einsum("bhqk,bkhd->bqhd", score_grad, keys, preferred_element_type=jnp.float32) * scale
    )
    key_grad = (
        jnp.einsum("bhqk,bqhd->bkhd", score_grad, queries, preferred_element_type=jnp.float32)
        * scale
    )
    value_grad = jnp.einsum(
        "bhqk,bqhd->bkhd", prob_low, mixed_grad, preferred_element_type=jnp.float32
    )

    def prepare_here(raw, gain):
        return head_prepare(raw, gain, positions)

    _, query_back = jax.vjp(prepare_here, split[:, :, 0], query_gain_f)
    raw_query_grad, query_gain_part = query_back(query_grad)
    _, key_back = jax.vjp(prepare_here, split[:, :, 1], key_gain_f)
    raw_key_grad, key_gain_part = key_back(key_grad)
    projected_grad = jnp.stack([raw_query_grad, raw_key_grad, value_grad], axis=2)
    projected_grad = projected_grad.reshape(items, length, 3, heads_here * HD).astype(jnp.bfloat16)
    project_grad = jnp.einsum(
        "bld,blke->dke", mod_in, projected_grad, preferred_element_type=jnp.float32
    )
    piece = projected_grad
    mod_in_grad = lax.psum_scatter(
        jnp.einsum(
            "blke,dke->bld", piece, project_weight, preferred_element_type=jnp.float32
        ).astype(jnp.bfloat16),
        "tensor",
        scatter_dimension=0,
        tiled=True,
    ).astype(jnp.float32)
    tokens_grad = (
        residual_grad
        + layer_norm_back(normed_local, inverse_local, mod_in_grad * (1.0 + attend_scale))
    ).astype(jnp.bfloat16)
    modulation_grad_part = jnp.stack(
        [
            jnp.sum(mod_in_grad, axis=1),
            jnp.sum(mod_in_grad * normed_local, axis=1),
            jnp.sum(residual_grad * attend_branch, axis=1),
            jnp.sum(mod_two_grad, axis=1),
            jnp.sum(mod_two_grad * normed_two, axis=1),
            jnp.sum(out_grad * feed_branch, axis=1),
        ],
        axis=1,
    )
    modulation_grad_part = modulation_grad_part[0].astype(jnp.bfloat16)
    small = jnp.concatenate(
        [
            output_bias_part,
            down_bias_part,
            modulation_grad_part.astype(jnp.float32).reshape(-1),
            query_gain_part,
            key_gain_part,
        ]
    )
    small_size = small.shape[0]
    small = jnp.pad(small, (0, -small_size % 1024)).reshape(-1, 128)
    tensor_size = width // slab
    modulation_grad, small = swap(
        "sums_swap",
        3,
        [
            (
                jnp.transpose(modulation_grad_part.reshape(6, tensor_size, slab), (1, 0, 2)),
                "tensor",
                True,
            )
        ],
        small,
    )
    small = small.reshape(-1)
    output_bias_grad = small[:width]
    down_bias_grad = small[width : 2 * width]
    modulate_bias_grad = small[2 * width : 8 * width].reshape(6, width)
    query_gain_grad = small[8 * width : 8 * width + HD]
    key_gain_grad = small[8 * width + HD : 8 * width + 2 * HD]
    cond_part = jnp.einsum(
        "bke,dke->bd", modulation_grad, modulate_weight, preferred_element_type=jnp.float32
    )
    (cond_parts,) = swap("condition_swap", 4, [(cond_part, "tensor", False)])
    cond_grad = (jnp.sum(cond_parts, axis=0) * silu_slope(condition)).astype(jnp.bfloat16)
    pre_grad = (
        jnp.einsum("be,de->bd", cond_grad, embed_weight, preferred_element_type=jnp.float32)
        * silu_slope(pre_hidden)
    ).astype(jnp.bfloat16)
    pieces = [
        cond_grad,
        cond_act,
        time_hidden,
        pre_grad,
        time_feat,
        modulation_grad.reshape(items, 6 * slab),
    ]
    packed = jnp.concatenate(pieces, axis=1)
    tags = jnp.broadcast_to(labels[:, None], (items, 128))
    packed, tags = swap("items_swap", 5, [(packed, "dp", False), (tags, "dp", False)])
    packed = packed.reshape(-1, packed.shape[2])
    tags = tags[:, :, 0].reshape(-1)
    edges = [0]
    for piece in pieces:
        edges.append(edges[-1] + piece.shape[1])
    cond_grad, cond_act, time_hidden, pre_grad, time_feat, modulation_grad = [
        packed[:, start:stop] for start, stop in zip(edges[:-1], edges[1:])
    ]
    modulation_grad = modulation_grad.reshape(-1, 6, slab)
    share = width // lax.axis_size("dp")

    def mine(value):
        return lax.dynamic_slice_in_dim(value, index * share, share, 1)

    one_hot = (tags[:, None] == jnp.arange(class_table.shape[0])[None, :]).astype(jnp.bfloat16)
    cond_grad_mine, pre_grad_mine = mine(cond_grad), mine(pre_grad)
    class_grad = jnp.einsum(
        "bc,bd->cd", one_hot, cond_grad_mine, preferred_element_type=jnp.float32
    )
    modulate_grad = jnp.einsum(
        "bd,bke->dke", mine(cond_act), modulation_grad, preferred_element_type=jnp.float32
    )
    embed_grad = jnp.einsum(
        "bd,be->de", mine(time_hidden), cond_grad, preferred_element_type=jnp.float32
    )
    embed_bias_grad = jnp.sum(cond_grad_mine.astype(jnp.float32), axis=0)
    time_grad = jnp.einsum(
        "bf,bd->fd", time_feat, pre_grad_mine, preferred_element_type=jnp.float32
    )
    time_bias_grad = jnp.sum(pre_grad_mine.astype(jnp.float32), axis=0)

    def scatter(value, axis):
        value = value.astype(jnp.bfloat16)
        return lax.psum_scatter(value, "dp", scatter_dimension=axis, tiled=True).astype(
            jnp.float32
        )

    project_grad = scatter(project_grad, 0)
    output_weight_grad = scatter(output_weight_grad, 1)
    feed_weights = scatter(feed_weights, 1)
    expand_grad = jnp.transpose(feed_weights[:2], (1, 0, 2))
    down_grad = feed_weights[2].T
    return (
        result,
        tokens_grad,
        project_grad,
        query_gain_grad,
        key_gain_grad,
        output_weight_grad,
        output_bias_grad,
        expand_grad,
        down_grad,
        down_bias_grad,
        modulate_grad,
        modulate_bias_grad,
        time_grad,
        time_bias_grad,
        embed_grad,
        embed_bias_grad,
        class_grad,
    )


def solution(mesh):
    return jax.shard_map(
        shards,
        mesh=mesh,
        in_specs=(
            P(("dp", "tensor"), None, None),
            P("dp"),
            P("dp"),
            P("dp"),
            P(("dp", "tensor"), None, None),
            P(None, None, "tensor"),
            P(),
            P(),
            P("tensor", None),
            P(),
            P(None, None, "tensor"),
            P("tensor", None),
            P(),
            P(None, None, "tensor"),
            P(None, "tensor"),
            P(),
            P(),
            P(),
            P(),
            P(),
        ),
        out_specs=(
            P(("dp", "tensor"), None, None),
            P(("dp", "tensor"), None, None),
            P("dp", None, "tensor"),
            P(),
            P(),
            P("tensor", "dp"),
            P(),
            P("dp", None, "tensor"),
            P("tensor", "dp"),
            P(),
            P("dp", None, "tensor"),
            P(),
            P(None, "dp"),
            P("dp"),
            P("dp", None),
            P("dp"),
            P(None, "dp"),
        ),
        check_vma=False,
    )
```

```python
import functools
import math

import jax
import jax.numpy as jnp
from jax import lax
from jax.experimental import pallas as pl
from jax.experimental.pallas import tpu as pltpu
from jax.sharding import PartitionSpec as P

HD = 72
FREQ = 256
GRID = 16


EPS = 1e-06


def layer_norm(value):
    center = value - jnp.mean(value, axis=-1, keepdims=True)
    inverse = lax.rsqrt(jnp.mean(center * center, axis=-1, keepdims=True) + EPS)
    return (center * inverse, inverse)


def layer_norm_back(normed, inverse, grad):
    return inverse * (
        grad
        - jnp.mean(grad, axis=-1, keepdims=True)
        - normed * jnp.mean(grad * normed, axis=-1, keepdims=True)
    )


def silu_slope(value):
    sigma = jax.nn.sigmoid(value)
    return sigma * (1.0 + value * (1.0 - sigma))


def rotate(value, positions):
    quarter = HD // 4
    rates = 10000.0 ** (-jnp.arange(quarter, dtype=jnp.float32) / quarter)
    places = ((positions // GRID).astype(jnp.float32), (positions % GRID).astype(jnp.float32))
    pieces = []
    for which_half in range(2):
        half_value = value[..., which_half * 2 * quarter : (which_half + 1) * 2 * quarter]
        angle = places[which_half][:, None] * rates[None, :]
        cosine = jnp.cos(angle)[None, :, None, :]
        sine = jnp.sin(angle)[None, :, None, :]
        first = half_value[..., :quarter]
        second = half_value[..., quarter:]
        pieces.append(first * cosine - second * sine)
        pieces.append(second * cosine + first * sine)
    return jnp.concatenate(pieces, axis=-1)


def head_prepare(raw, gain, positions):
    scaled = raw * lax.rsqrt(jnp.mean(raw * raw, axis=-1, keepdims=True) + EPS) * gain
    return rotate(scaled, positions)


def time_features(steps_in):
    half = FREQ // 2
    rates = jnp.exp(-math.log(10000.0) * jnp.arange(half, dtype=jnp.float32) / half)
    angle = steps_in.astype(jnp.float32)[:, None] * rates[None, :]
    return jnp.concatenate([jnp.cos(angle), jnp.sin(angle)], axis=-1)


CHUNKS = 8


def rows_of(block, total):
    size = total // CHUNKS
    return pl.ds(pl.multiple_of(block * size, size), size)


class Line:
    def __init__(self, count, gathered, summed, ag_sems, rs_sems):
        self.count = count
        self.place = lax.axis_index("tensor")
        self.gathered = gathered
        self.summed = summed
        self.ag_send, self.ag_recv = ag_sems
        self.rs_send, self.rs_recv = rs_sems

    def barrier(self):
        place, count = self.place, self.count
        sem = pltpu.get_barrier_semaphore()

        @pl.when(place > 0)
        def _():
            pl.semaphore_signal(sem, inc=1, device_id={"tensor": place - 1})

        @pl.when(place < count - 1)
        def _():
            pl.semaphore_signal(sem, inc=1, device_id={"tensor": place + 1})

        peers = jnp.where(place > 0, 1, 0) + jnp.where(place < count - 1, 1, 0)
        pl.semaphore_wait(sem, peers)

    def item_copy(self, which, way, item, own=False):
        mine, everyone = self.gathered[which]
        target = self.place + (1 if way == 0 else -1)
        return pltpu.make_async_remote_copy(
            src_ref=mine if own else everyone.at[item],
            dst_ref=everyone.at[item],
            send_sem=self.ag_send.at[which, way, item],
            recv_sem=self.ag_recv.at[which, way, item],
            device_id={"tensor": target},
        )

    def can(self, way):
        return self.place < self.count - 1 if way == 0 else self.place > 0

    def sum_copy(self, which, way, item, block):
        part, landed = self.summed[which]
        target = self.place + (1 if way == 0 else -1)
        slot = item
        if way == 1:
            slot = jnp.where(item == target, self.count, item)
        rows = rows_of(block, part.shape[1])
        return pltpu.make_async_remote_copy(
            src_ref=part.at[item, rows],
            dst_ref=landed.at[slot, rows],
            send_sem=self.rs_send.at[which, way, item, block],
            recv_sem=self.rs_recv.at[which, way, item, block],
            device_id={"tensor": target},
        )

    def landed_slot(self, way, item):
        return jnp.where(item == self.place, self.count, item) if way == 1 else item

    def wait_sum(self, which, way, item, block):
        part, landed = self.summed[which]
        rows = rows_of(block, part.shape[1])
        view = landed.at[self.landed_slot(way, item), rows]
        pltpu.make_async_remote_copy(
            src_ref=view,
            dst_ref=view,
            send_sem=self.rs_send.at[which, way, item, block],
            recv_sem=self.rs_recv.at[which, way, item, block],
            device_id={"tensor": self.place},
        ).wait_recv()
        return view

    def start_own(self):
        for which in range(len(self.gathered)):
            for way in range(2):

                @pl.when(self.can(way))
                def _():
                    self.item_copy(which, way, self.place, own=True).start()

    def receive(self, step):
        place, count = self.place, self.count
        for which in range(len(self.gathered)):
            for way in range(2):
                item = place - step if way == 0 else place + step

                @pl.when((item >= 0) & (item < count))
                def _():
                    self.item_copy(which, way, item).wait_recv()

                    @pl.when(self.can(way))
                    def _():
                        self.item_copy(which, way, item).start()

    def items(self, step):
        place, count = self.place, self.count
        low, high = place - step, place + step
        return ((low, (low >= 0)), (high, (high < count) & (step > 0)))

    def pass_sums(self, step):
        place, count = self.place, self.count
        ways = []
        for way in range(2):
            item = step if way == 0 else count - 1 - step
            ways.append(
                (
                    way,
                    item,
                    item > place if way == 0 else item < place,
                    place if way == 0 else count - 1 - place,
                )
            )

        @pl.loop(0, CHUNKS)
        def _(block):
            for way, item, further, hop in ways:

                @pl.when(further & (hop == 0))
                def _():
                    for which in range(len(self.summed)):
                        self.sum_copy(which, way, item, block).start()

        @pl.loop(0, CHUNKS + count - 3)
        def _(turn):
            for distance in range(1, count - 1):
                block = turn - (distance - 1)
                for way, item, further, hop in ways:

                    @pl.when(further & (hop == distance) & (block >= 0) & (block < CHUNKS))
                    def _():
                        for which in range(len(self.summed)):
                            part, landed = self.summed[which]
                            rows = rows_of(block, part.shape[1])
                            view = self.wait_sum(which, way, item, block)
                            total = part[item, rows].astype(jnp.float32) + view[...].astype(
                                jnp.float32
                            )
                            part[item, rows] = total.astype(part.dtype)
                            self.sum_copy(which, way, item, block).start()

    def finish(self, which, out):
        place, count = self.place, self.count
        part, landed = self.summed[which]

        @pl.loop(0, CHUNKS)
        def _(block):
            rows = rows_of(block, part.shape[1])
            out[rows] = part[place, rows].astype(jnp.float32)
            for way in range(2):

                @pl.when(place > 0 if way == 0 else place < count - 1)
                def _():
                    view = self.wait_sum(which, way, place, block)
                    out[rows] += view[...].astype(jnp.float32)

    def drain(self):
        place, count = self.place, self.count

        @pl.loop(0, count)
        def _(item):
            for way in range(2):
                passed = item <= place if way == 0 else item >= place

                @pl.when(passed & self.can(way))
                def _():
                    for which in range(len(self.gathered)):
                        self.item_copy(which, way, item).wait_send()

                further = item > place if way == 0 else item < place

                @pl.when(further)
                def _():
                    @pl.loop(0, CHUNKS)
                    def _(block):
                        for which in range(len(self.summed)):
                            self.sum_copy(which, way, item, block).wait_send()


def dot(left, right):
    return jnp.dot(left, right, preferred_element_type=jnp.float32)


def dot_rt(left, right):
    return lax.dot_general(
        left, right, (((1,), (1,)), ((), ())), preferred_element_type=jnp.float32
    )


def dot_lt(left, right):
    return lax.dot_general(
        left, right, (((0,), (0,)), ((), ())), preferred_element_type=jnp.float32
    )


def cut(total, most):
    size = max(s for s in range(128, most + 1, 128) if total % s == 0)
    return size, total // size


def span(index, size):
    return pl.ds(pl.multiple_of(index * size, size), size)


def feed_kernel(
    count,
    mod_ref,
    grad_ref,
    expand_hbm,
    down_hbm,
    feed_out,
    back_out,
    weight_out,
    expand,
    down,
    mod_all,
    grad_all,
    hidden,
    slopes,
    feed_part,
    back_part,
    feed_land,
    back_land,
    total,
    load_sem,
    ag_send,
    ag_recv,
    rs_send,
    rs_recv,
):
    line = Line(
        count,
        [(mod_ref, mod_all), (grad_ref, grad_all)],
        [(back_part, back_land), (feed_part, feed_land)],
        (ag_send, ag_recv),
        (rs_send, rs_recv),
    )
    width, units = expand.shape[1], expand.shape[2]
    loads = (
        pltpu.make_async_copy(expand_hbm, expand, load_sem.at[0]),
        pltpu.make_async_copy(down_hbm, down, load_sem.at[1]),
    )
    for load in loads:
        load.start()
    line.barrier()
    line.start_own()
    mod_all[line.place] = mod_ref[...]
    grad_all[line.place] = grad_ref[...]
    total[...] = jnp.zeros_like(total)
    for load in loads:
        load.wait()
    unit_size, unit_count = cut(units, 256)
    wide_size, wide_count = cut(width, 384)
    tall_size, tall_count = cut(width, 128)

    def compute(item):
        @pl.loop(0, unit_count)
        def _(index):
            cols = span(index, unit_size)
            mod = mod_all[item]
            gate = dot(mod, expand[0, :, cols])
            upper = dot(mod, expand[1, :, cols])
            back = dot_rt(grad_all[item], down[cols, :])
            sigma = jax.nn.sigmoid(gate)
            active = gate * sigma
            hidden[item, :, cols] = (active * upper).astype(jnp.bfloat16)
            slopes[0, item, :, cols] = (
                back * upper * (sigma * (1.0 + gate * (1.0 - sigma)))
            ).astype(jnp.bfloat16)
            slopes[1, item, :, cols] = (back * active).astype(jnp.bfloat16)

        @pl.loop(0, wide_count)
        def _(index):
            cols = span(index, wide_size)
            back_part[item, :, cols] = (
                dot_rt(slopes[0, item], expand[0, cols, :])
                + dot_rt(slopes[1, item], expand[1, cols, :])
            ).astype(jnp.bfloat16)
            feed_part[item, :, cols] = dot(hidden[item], down[:, cols]).astype(jnp.bfloat16)

    def weigh(item):
        @pl.loop(0, tall_count)
        def _(index):
            rows = span(index, tall_size)
            mod = mod_all[item, :, rows]
            total[0, rows, :] += dot_lt(mod, slopes[0, item])
            total[1, rows, :] += dot_lt(mod, slopes[1, item])
            total[2, rows, :] += dot_lt(grad_all[item, :, rows], hidden[item])

    @pl.loop(0, count)
    def _(step):
        @pl.when(step > 0)
        def _():
            for item, valid in line.items(step - 1):

                @pl.when(valid)
                def _():
                    weigh(item)

            line.receive(step)

        for item, valid in line.items(step):

            @pl.when(valid)
            def _():
                compute(item)

        @pl.when(step > 0)
        def _():
            line.pass_sums(step)

    for item, valid in line.items(count - 1):

        @pl.when(valid)
        def _():
            weigh(item)

    weight_out[...] = total[...].astype(jnp.bfloat16)
    line.finish(0, back_out)
    line.finish(1, feed_out)
    line.drain()


def feed_pass(mod_two, branch_grad, expand_weight, down_weight):
    count = lax.axis_size("tensor")
    length, width = mod_two.shape
    units = down_weight.shape[0]
    expand = jnp.transpose(expand_weight, (1, 0, 2))
    vmem, any_space = pl.BlockSpec(memory_space=pltpu.VMEM), pl.BlockSpec(memory_space=pl.ANY)
    low = jnp.bfloat16
    item = (length, width)
    return pl.pallas_call(
        functools.partial(feed_kernel, count),
        out_shape=(
            jax.ShapeDtypeStruct(item, jnp.float32),
            jax.ShapeDtypeStruct(item, jnp.float32),
            jax.ShapeDtypeStruct((3, width, units), low),
        ),
        in_specs=[vmem, vmem, any_space, any_space],
        out_specs=(vmem, vmem, vmem),
        scratch_shapes=[
            pltpu.VMEM((2, width, units), low),
            pltpu.VMEM((units, width), low),
            pltpu.VMEM((count, *item), low),
            pltpu.VMEM((count, *item), low),
            pltpu.VMEM((count, length, units), low),
            pltpu.VMEM((2, count, length, units), low),
            pltpu.VMEM((count, *item), low),
            pltpu.VMEM((count, *item), low),
            pltpu.VMEM((count + 1, *item), low),
            pltpu.VMEM((count + 1, *item), low),
            pltpu.VMEM((3, width, units), jnp.float32),
            pltpu.SemaphoreType.DMA((2,)),
            pltpu.SemaphoreType.DMA((2, 2, count)),
            pltpu.SemaphoreType.DMA((2, 2, count)),
            pltpu.SemaphoreType.DMA((2, 2, count, CHUNKS)),
            pltpu.SemaphoreType.DMA((2, 2, count, CHUNKS)),
        ],
        compiler_params=pltpu.CompilerParams(
            collective_id=1, has_side_effects=True, vmem_limit_bytes=64000000
        ),
        name="feed_pass",
    )(mod_two, branch_grad, expand, down_weight)


def swap_kernel(jobs, total, *refs):
    n = len(jobs)
    ins, outs = refs[:n], refs[n + total : 2 * n + total]
    sems = refs[2 * n + 2 * total :]
    places = [lax.axis_index(axis) for axis, _, _ in jobs]
    hello = pltpu.get_barrier_semaphore()
    axes = []
    for axis, count, _ in jobs:
        if (axis, count) not in axes:
            axes.append((axis, count))
    if total:
        axes = [("dp", lax.axis_size("dp")), ("tensor", lax.axis_size("tensor"))]
    for axis, count in axes:
        here = lax.axis_index(axis)

        @pl.loop(1, count)
        def _(offset):
            peer = lax.rem(here + offset, count)
            pl.semaphore_signal(hello, inc=1, device_id={axis: peer})

    pl.semaphore_wait(hello, sum(count - 1 for _, count in axes))

    def copy(source, target, send, recv, axis, peer, slot):
        return pltpu.make_async_remote_copy(
            src_ref=source,
            dst_ref=target.at[slot],
            send_sem=send.at[peer],
            recv_sem=recv.at[slot],
            device_id={axis: peer},
        )

    def start(source, target, send, recv, axis, count, split):
        here = lax.axis_index(axis)

        @pl.loop(1, count)
        def _(offset):
            peer = lax.rem(here + offset, count)
            piece = source.at[peer] if split else source
            copy(piece, target, send, recv, axis, peer, here).start()

        target[here] = source[here] if split else source[...]

    def finish(source, target, send, recv, axis, count, split):
        here = lax.axis_index(axis)

        @pl.loop(1, count)
        def _(offset):
            peer = lax.rem(here + offset, count)
            piece = source.at[peer] if split else source
            step = copy(piece, target, send, recv, axis, peer, peer)
            step.wait_recv()
            step.wait_send()

    work = []
    for index, (axis, count, split) in enumerate(jobs):
        work.append((ins[index], outs[index], sems[2 * index], sems[2 * index + 1], axis, count, split))
    if total:
        source, result = refs[n], refs[2 * n + total]
        one, two, middle, s1, r1, s2, r2 = sems[2 * n :]
        wide, deep = lax.axis_size("dp"), lax.axis_size("tensor")
        first = (source, one, s1, r1, "dp", wide, False)
        start(*first)
    for job in work:
        start(*job)
    if total:
        finish(*first)
        middle[...] = one[0]

        @pl.loop(1, wide)
        def _(index):
            middle[...] += one[index]

        second = (middle, two, s2, r2, "tensor", deep, False)
        start(*second)
    for job in work:
        finish(*job)
    if total:
        finish(*second)
        result[...] = two[0]

        @pl.loop(1, deep)
        def _(index):
            result[...] += two[index]


def swap(name, number, jobs, total=None):
    vmem = pl.BlockSpec(memory_space=pltpu.VMEM)
    plan, arrays, shapes, scratch = [], [], [], []
    for array, axis, split in jobs:
        count = lax.axis_size(axis)
        plan.append((axis, count, split))
        arrays.append(array)
        piece = array.shape[1:] if split else array.shape
        shapes.append(jax.ShapeDtypeStruct((count, *piece), array.dtype))
        scratch += [pltpu.SemaphoreType.DMA((count,)), pltpu.SemaphoreType.DMA((count,))]
    if total is not None:
        wide, deep = lax.axis_size("dp"), lax.axis_size("tensor")
        arrays.append(total)
        shapes.append(jax.ShapeDtypeStruct(total.shape, total.dtype))
        scratch += [
            pltpu.VMEM((wide, *total.shape), total.dtype),
            pltpu.VMEM((deep, *total.shape), total.dtype),
            pltpu.VMEM(total.shape, total.dtype),
        ]
        for count in (wide, wide, deep, deep):
            scratch.append(pltpu.SemaphoreType.DMA((count,)))
    return pl.pallas_call(
        functools.partial(swap_kernel, tuple(plan), int(total is not None)),
        out_shape=tuple(shapes),
        in_specs=[vmem] * len(arrays),
        out_specs=tuple([vmem] * len(shapes)),
        scratch_shapes=scratch,
        compiler_params=pltpu.CompilerParams(collective_id=number, has_side_effects=True),
        name=name,
    )(*arrays)


LANES = 128


def turn(value, tables):
    return (
        value * tables[0]
        + pltpu.roll(value, LANES - HD // 4, 1) * tables[1]
        + pltpu.roll(value, HD // 4, 1) * tables[2]
    )


def turn_back(grad, tables):
    return (
        grad * tables[0]
        + pltpu.roll(grad * tables[1], HD // 4, 1)
        + pltpu.roll(grad * tables[2], LANES - HD // 4, 1)
    )


def turn_tables(length):
    quarter = HD // 4
    lane = jnp.arange(LANES)
    rates = 10000.0 ** (-(lane % quarter).astype(jnp.float32) / quarter)
    positions = jnp.arange(length)[:, None]
    place = jnp.where(lane < 2 * quarter, positions // GRID, positions % GRID)
    angle = place.astype(jnp.float32) * rates
    real = lane < HD
    early = (lane // quarter) % 2 == 0
    cosine = jnp.where(real, jnp.cos(angle), 0.0)
    sine = jnp.sin(angle)
    return jnp.stack(
        [
            cosine,
            jnp.where(real & early, -sine, 0.0),
            jnp.where(real & ~early, sine, 0.0),
        ]
    )


def unit_norm(raw):
    inverse = lax.rsqrt(jnp.sum(raw * raw, axis=-1, keepdims=True) * (1.0 / HD) + EPS)
    return raw * inverse, inverse


def project(mod, weight, raw):
    size, number = cut(weight.shape[1], 512)

    @pl.loop(0, number)
    def _(index):
        cols = span(index, size)
        raw[:, cols] = dot(mod, weight[:, cols])


def soft(queries, keys):
    scores = dot_rt(queries, keys) * (HD ** (-0.5))
    shifted = jnp.exp(scores - jnp.max(scores, axis=-1, keepdims=True))
    return shifted * (1.0 / jnp.sum(shifted, axis=-1, keepdims=True))


def attend_kernel(
    count,
    mod_ref,
    tables_ref,
    gains_ref,
    weight_hbm,
    last_hbm,
    branch_out,
    mod_out,
    weight,
    last,
    mod_all,
    raw,
    mixed,
    part,
    land,
    load_sem,
    ag_send,
    ag_recv,
    rs_send,
    rs_recv,
):
    line = Line(count, [(mod_ref, mod_all)], [(part, land)], (ag_send, ag_recv), (rs_send, rs_recv))
    loads = (
        pltpu.make_async_copy(weight_hbm, weight, load_sem.at[0]),
        pltpu.make_async_copy(last_hbm, last, load_sem.at[1]),
    )
    for load in loads:
        load.start()
    line.barrier()
    line.start_own()
    mod_all[line.place] = mod_ref[...]
    for load in loads:
        load.wait()
    inner = last.shape[0]
    heads = inner // LANES
    wide_size, wide_count = cut(last.shape[1], 384)

    def compute(item):
        project(mod_all[item], weight, raw)
        tables = (tables_ref[0], tables_ref[1], tables_ref[2])

        @pl.loop(0, heads)
        def _(head):
            query_raw = raw[:, span(head, LANES)]
            key_raw = raw[:, span(heads + head, LANES)]
            values = raw[:, span(2 * heads + head, LANES)].astype(jnp.bfloat16)
            queries = turn(unit_norm(query_raw)[0] * gains_ref[0:1, :], tables)
            keys = turn(unit_norm(key_raw)[0] * gains_ref[1:2, :], tables)
            probs = soft(queries.astype(jnp.bfloat16), keys.astype(jnp.bfloat16))
            mixed[:, span(head, LANES)] = dot(probs.astype(jnp.bfloat16), values).astype(
                jnp.bfloat16
            )

        @pl.loop(0, wide_count)
        def _(index):
            cols = span(index, wide_size)
            part[item, :, cols] = dot(mixed[...], last[:, cols]).astype(jnp.bfloat16)

    @pl.loop(0, count)
    def _(step):
        @pl.when(step > 0)
        def _():
            line.receive(step)

        for item, valid in line.items(step):

            @pl.when(valid)
            def _():
                compute(item)

        @pl.when(step > 0)
        def _():
            line.pass_sums(step)

    mod_out[...] = mod_all[...]
    line.finish(0, branch_out)
    line.drain()


def attend_back_kernel(
    count,
    grad_ref,
    mod_all,
    tables_ref,
    gains_ref,
    weight_hbm,
    last_hbm,
    back_out,
    weight_out,
    gain_out,
    weight,
    last,
    grad_all,
    raw,
    mixed,
    mixed_grad,
    raw_grad,
    part,
    land,
    total,
    load_sem,
    ag_send,
    ag_recv,
    rs_send,
    rs_recv,
):
    line = Line(count, [(grad_ref, grad_all)], [(part, land)], (ag_send, ag_recv), (rs_send, rs_recv))
    loads = (
        pltpu.make_async_copy(weight_hbm, weight, load_sem.at[0]),
        pltpu.make_async_copy(last_hbm, last, load_sem.at[1]),
    )
    for load in loads:
        load.start()
    line.barrier()
    line.start_own()
    grad_all[line.place] = grad_ref[...]
    total[...] = jnp.zeros_like(total)
    gain_out[...] = jnp.zeros_like(gain_out)
    for load in loads:
        load.wait()
    inner, width = last.shape
    heads = inner // LANES
    scale = HD ** (-0.5)
    wide_size, wide_count = cut(width, 384)
    inner_size, inner_count = cut(inner, 256)
    tall_size, tall_count = cut(width, 128)

    def compute(item):
        project(mod_all[item], weight, raw)
        tables = (tables_ref[0], tables_ref[1], tables_ref[2])

        @pl.loop(0, inner_count)
        def _(index):
            cols = span(index, inner_size)
            mixed_grad[:, cols] = dot_rt(grad_all[item], last[cols, :]).astype(jnp.bfloat16)

        @pl.loop(0, heads)
        def _(head):
            query_norm, query_inverse = unit_norm(raw[:, span(head, LANES)])
            key_norm, key_inverse = unit_norm(raw[:, span(heads + head, LANES)])
            values = raw[:, span(2 * heads + head, LANES)].astype(jnp.bfloat16)
            queries = turn(query_norm * gains_ref[0:1, :], tables).astype(jnp.bfloat16)
            keys = turn(key_norm * gains_ref[1:2, :], tables).astype(jnp.bfloat16)
            probs = soft(queries, keys)
            probs_low = probs.astype(jnp.bfloat16)
            mixed[item, :, span(head, LANES)] = dot(probs_low, values).astype(jnp.bfloat16)
            grad = mixed_grad[:, span(head, LANES)]
            prob_grad = dot_rt(grad, values)
            score_grad = (
                probs * (prob_grad - jnp.sum(probs * prob_grad, axis=-1, keepdims=True))
            ).astype(jnp.bfloat16)

            def back(which, value_grad, norm, inverse):
                turned = turn_back(value_grad, tables)
                gained = turned * norm
                gain_out[which] += jnp.sum(gained.reshape(-1, 8, LANES), axis=0)
                scaled = turned * gains_ref[which : which + 1, :]
                mean = jnp.sum(scaled * norm, axis=-1, keepdims=True) * (1.0 / HD)
                raw_grad[item, :, span(which * heads + head, LANES)] = (
                    inverse * (scaled - norm * mean)
                ).astype(jnp.bfloat16)

            back(0, dot(score_grad, keys) * scale, query_norm, query_inverse)
            back(1, dot_lt(score_grad, queries) * scale, key_norm, key_inverse)
            raw_grad[item, :, span(2 * heads + head, LANES)] = dot_lt(probs_low, grad).astype(
                jnp.bfloat16
            )

        @pl.loop(0, wide_count)
        def _(index):
            cols = span(index, wide_size)
            part[item, :, cols] = dot_rt(raw_grad[item], weight[cols, :]).astype(jnp.bfloat16)

    def weigh(item):
        @pl.loop(0, tall_count)
        def _(index):
            rows = span(index, tall_size)
            total[rows, : 3 * inner] += dot_lt(mod_all[item, :, rows], raw_grad[item])
            total[rows, 3 * inner :] += dot_lt(grad_all[item, :, rows], mixed[item])

    @pl.loop(0, count)
    def _(step):
        @pl.when(step > 0)
        def _():
            for item, valid in line.items(step - 1):

                @pl.when(valid)
                def _():
                    weigh(item)

            line.receive(step)

        for item, valid in line.items(step):

            @pl.when(valid)
            def _():
                compute(item)

        @pl.when(step > 0)
        def _():
            line.pass_sums(step)

    for item, valid in line.items(count - 1):

        @pl.when(valid)
        def _():
            weigh(item)

    weight_out[...] = total[...].astype(jnp.bfloat16)
    line.finish(0, back_out)
    line.drain()


def attend_arrays(project_weight, output_weight, query_gain, key_gain, length):
    width, _, inner = project_weight.shape
    heads = inner // HD
    pad = LANES - HD
    weight = jnp.pad(project_weight.reshape(width, 3, heads, HD), ((0, 0),) * 3 + ((0, pad),))
    last = jnp.pad(output_weight.reshape(heads, HD, width), ((0, 0), (0, pad), (0, 0)))
    gains = jnp.pad(jnp.stack([query_gain, key_gain]).astype(jnp.float32), ((0, 6), (0, pad)))
    return (
        turn_tables(length),
        gains,
        weight.reshape(width, 3 * heads * LANES),
        last.reshape(heads * LANES, width),
    )


def line_sems(count, gathers, sums):
    return [
        pltpu.SemaphoreType.DMA((2,)),
        pltpu.SemaphoreType.DMA((gathers, 2, count)),
        pltpu.SemaphoreType.DMA((gathers, 2, count)),
        pltpu.SemaphoreType.DMA((sums, 2, count, CHUNKS)),
        pltpu.SemaphoreType.DMA((sums, 2, count, CHUNKS)),
    ]


def attend_pass(mod_in, arrays):
    count = lax.axis_size("tensor")
    weight, last = arrays[2:]
    item = mod_in.shape
    vmem, any_space = pl.BlockSpec(memory_space=pltpu.VMEM), pl.BlockSpec(memory_space=pl.ANY)
    low = jnp.bfloat16
    return pl.pallas_call(
        functools.partial(attend_kernel, count),
        out_shape=(
            jax.ShapeDtypeStruct(item, jnp.float32),
            jax.ShapeDtypeStruct((count, *item), low),
        ),
        in_specs=[vmem, vmem, vmem, any_space, any_space],
        out_specs=(vmem, vmem),
        scratch_shapes=[
            pltpu.VMEM(weight.shape, low),
            pltpu.VMEM(last.shape, low),
            pltpu.VMEM((count, *item), low),
            pltpu.VMEM((item[0], weight.shape[1]), jnp.float32),
            pltpu.VMEM((item[0], last.shape[0]), low),
            pltpu.VMEM((count, *item), low),
            pltpu.VMEM((count + 1, *item), low),
            *line_sems(count, 1, 1),
        ],
        compiler_params=pltpu.CompilerParams(
            collective_id=6, has_side_effects=True, vmem_limit_bytes=60000000
        ),
        name="attend_pass",
    )(mod_in, *arrays)


def attend_back_pass(attend_grad, mod_all, arrays):
    count = lax.axis_size("tensor")
    weight, last = arrays[2:]
    item = attend_grad.shape
    inner = last.shape[0]
    vmem, any_space = pl.BlockSpec(memory_space=pltpu.VMEM), pl.BlockSpec(memory_space=pl.ANY)
    low = jnp.bfloat16
    return pl.pallas_call(
        functools.partial(attend_back_kernel, count),
        out_shape=(
            jax.ShapeDtypeStruct(item, jnp.float32),
            jax.ShapeDtypeStruct((item[1], 4 * inner), low),
            jax.ShapeDtypeStruct((2, 8, LANES), jnp.float32),
        ),
        in_specs=[vmem, vmem, vmem, vmem, any_space, any_space],
        out_specs=(vmem, vmem, vmem),
        scratch_shapes=[
            pltpu.VMEM(weight.shape, low),
            pltpu.VMEM(last.shape, low),
            pltpu.VMEM((count, *item), low),
            pltpu.VMEM((item[0], weight.shape[1]), jnp.float32),
            pltpu.VMEM((count, item[0], inner), low),
            pltpu.VMEM((item[0], inner), low),
            pltpu.VMEM((count, item[0], 3 * inner), low),
            pltpu.VMEM((count, *item), low),
            pltpu.VMEM((count + 1, *item), low),
            pltpu.VMEM((item[1], 4 * inner), jnp.float32),
            *line_sems(count, 1, 1),
        ],
        compiler_params=pltpu.CompilerParams(
            collective_id=7, has_side_effects=True, vmem_limit_bytes=60000000
        ),
        cost_estimate=pl.CostEstimate(
            flops=int(4e10), bytes_accessed=int(2e8), transcendentals=int(1e6)
        ),
        name="attend_back_pass",
    )(attend_grad, mod_all, *arrays)


def shards(
    tokens,
    timesteps,
    labels,
    item_counts,
    cotangent,
    project_weight,
    query_gain,
    key_gain,
    output_weight,
    output_bias,
    expand_weight,
    down_weight,
    down_bias,
    modulate_weight,
    modulate_bias,
    time_weight,
    time_bias,
    embed_weight,
    embed_bias,
    class_table,
):
    local_items, length, width = tokens.shape
    items = timesteps.shape[0]
    slab = modulate_weight.shape[2]
    heads_here = project_weight.shape[2] // HD
    scale = HD ** (-0.5)
    first_item = lax.axis_index("tensor") * local_items
    live = (first_item + jnp.arange(local_items) < item_counts[0]).astype(jnp.float32)[
        :, None, None
    ]
    index = lax.axis_index("dp")
    time_feat = time_features(timesteps).astype(jnp.bfloat16)
    pre_hidden = jnp.dot(
        time_feat, time_weight, preferred_element_type=jnp.float32
    ) + time_bias.astype(jnp.float32)
    time_hidden = jax.nn.silu(pre_hidden).astype(jnp.bfloat16)
    condition = (
        jnp.dot(time_hidden, embed_weight, preferred_element_type=jnp.float32)
        + embed_bias.astype(jnp.float32)
        + jnp.take(class_table, labels, axis=0).astype(jnp.float32)
    )
    cond_act = jax.nn.silu(condition).astype(jnp.bfloat16)
    modulation_part = (
        jnp.einsum("bd,dke->bke", cond_act, modulate_weight, preferred_element_type=jnp.float32)
        + modulate_bias.astype(jnp.float32)
    ).astype(jnp.bfloat16)
    (modulation_local,) = swap("modulation_swap", 2, [(modulation_part, "tensor", True)])
    modulation_local = jnp.transpose(modulation_local, (1, 0, 2)).reshape(1, 6, width)
    modulation_local = modulation_local.astype(jnp.float32)
    local_parts = [modulation_local[:, which][:, None, :] for which in range(6)]
    attend_shift, attend_scale, attend_gate, feed_shift, feed_scale, feed_gate = local_parts
    positions = jnp.arange(length)
    token_local = tokens.astype(jnp.float32)
    normed_local, inverse_local = layer_norm(token_local)
    mod_in = normed_local * (1.0 + attend_scale) + attend_shift
    arrays = attend_arrays(project_weight, output_weight, query_gain, key_gain, length)
    attend_total, mod_all = attend_pass(mod_in[0].astype(jnp.bfloat16), arrays)
    attend_branch = attend_total[None] + output_bias.astype(jnp.float32)
    residual = token_local + attend_gate * attend_branch
    normed_two, inverse_two = layer_norm(residual)
    mod_two = (normed_two * (1.0 + feed_scale) + feed_shift).astype(jnp.bfloat16)
    out_grad = cotangent.astype(jnp.float32) * live
    branch_grad = (out_grad * feed_gate).astype(jnp.bfloat16)
    down_bias_part = jnp.sum(branch_grad.astype(jnp.float32), axis=(0, 1))
    feed_total, mod_two_grad, feed_weights = feed_pass(
        mod_two[0], branch_grad[0], expand_weight, down_weight
    )
    feed_branch = feed_total[None] + down_bias.astype(jnp.float32)
    result = (live * (residual + feed_gate * feed_branch)).astype(jnp.bfloat16)
    mod_two_grad = mod_two_grad[None]
    residual_grad = out_grad + layer_norm_back(
        normed_two, inverse_two, mod_two_grad * (1.0 + feed_scale)
    )
    attend_grad = (residual_grad * attend_gate).astype(jnp.bfloat16)
    output_bias_part = jnp.sum(attend_grad.astype(jnp.float32), axis=(0, 1))
    mod_in_grad, attend_weights, gain_parts = attend_back_pass(attend_grad[0], mod_all, arrays)
    mod_in_grad = mod_in_grad[None]
    query_gain_part, key_gain_part = jnp.sum(gain_parts, axis=1)[:, :HD]
    tokens_grad = (
        residual_grad
        + layer_norm_back(normed_local, inverse_local, mod_in_grad * (1.0 + attend_scale))
    ).astype(jnp.bfloat16)
    modulation_grad_part = jnp.stack(
        [
            jnp.sum(mod_in_grad, axis=1),
            jnp.sum(mod_in_grad * normed_local, axis=1),
            jnp.sum(residual_grad * attend_branch, axis=1),
            jnp.sum(mod_two_grad, axis=1),
            jnp.sum(mod_two_grad * normed_two, axis=1),
            jnp.sum(out_grad * feed_branch, axis=1),
        ],
        axis=1,
    )
    modulation_grad_part = modulation_grad_part[0].astype(jnp.bfloat16)
    small = jnp.concatenate(
        [
            output_bias_part,
            down_bias_part,
            modulation_grad_part.astype(jnp.float32).reshape(-1),
            query_gain_part,
            key_gain_part,
        ]
    )
    small_size = small.shape[0]
    small = jnp.pad(small, (0, -small_size % 1024)).reshape(-1, 128)
    tensor_size = width // slab
    modulation_grad, small = swap(
        "sums_swap",
        3,
        [
            (
                jnp.transpose(modulation_grad_part.reshape(6, tensor_size, slab), (1, 0, 2)),
                "tensor",
                True,
            )
        ],
        small,
    )
    small = small.reshape(-1)
    output_bias_grad = small[:width]
    down_bias_grad = small[width : 2 * width]
    modulate_bias_grad = small[2 * width : 8 * width].reshape(6, width)
    query_gain_grad = small[8 * width : 8 * width + HD]
    key_gain_grad = small[8 * width + HD : 8 * width + 2 * HD]
    cond_part = jnp.einsum(
        "bke,dke->bd", modulation_grad, modulate_weight, preferred_element_type=jnp.float32
    )
    (cond_parts,) = swap("condition_swap", 4, [(cond_part, "tensor", False)])
    cond_grad = (jnp.sum(cond_parts, axis=0) * silu_slope(condition)).astype(jnp.bfloat16)
    pre_grad = (
        jnp.einsum("be,de->bd", cond_grad, embed_weight, preferred_element_type=jnp.float32)
        * silu_slope(pre_hidden)
    ).astype(jnp.bfloat16)
    pieces = [
        cond_grad,
        cond_act,
        time_hidden,
        pre_grad,
        time_feat,
        modulation_grad.reshape(items, 6 * slab),
    ]
    packed = jnp.concatenate(pieces, axis=1)
    tags = jnp.broadcast_to(labels[:, None], (items, 128))
    packed, tags = swap("items_swap", 5, [(packed, "dp", False), (tags, "dp", False)])
    packed = packed.reshape(-1, packed.shape[2])
    tags = tags[:, :, 0].reshape(-1)
    edges = [0]
    for piece in pieces:
        edges.append(edges[-1] + piece.shape[1])
    cond_grad, cond_act, time_hidden, pre_grad, time_feat, modulation_grad = [
        packed[:, start:stop] for start, stop in zip(edges[:-1], edges[1:])
    ]
    modulation_grad = modulation_grad.reshape(-1, 6, slab)
    share = width // lax.axis_size("dp")

    def mine(value):
        return lax.dynamic_slice_in_dim(value, index * share, share, 1)

    one_hot = (tags[:, None] == jnp.arange(class_table.shape[0])[None, :]).astype(jnp.bfloat16)
    cond_grad_mine, pre_grad_mine = mine(cond_grad), mine(pre_grad)
    class_grad = jnp.einsum(
        "bc,bd->cd", one_hot, cond_grad_mine, preferred_element_type=jnp.float32
    )
    modulate_grad = jnp.einsum(
        "bd,bke->dke", mine(cond_act), modulation_grad, preferred_element_type=jnp.float32
    )
    embed_grad = jnp.einsum(
        "bd,be->de", mine(time_hidden), cond_grad, preferred_element_type=jnp.float32
    )
    embed_bias_grad = jnp.sum(cond_grad_mine.astype(jnp.float32), axis=0)
    time_grad = jnp.einsum(
        "bf,bd->fd", time_feat, pre_grad_mine, preferred_element_type=jnp.float32
    )
    time_bias_grad = jnp.sum(pre_grad_mine.astype(jnp.float32), axis=0)

    def scatter(value, axis):
        value = value.astype(jnp.bfloat16)
        return lax.psum_scatter(value, "dp", scatter_dimension=axis, tiled=True).astype(
            jnp.float32
        )

    inner = heads_here * HD
    attend_weights = attend_weights.reshape(width, 4 * heads_here, LANES)[:, :, :HD]
    attend_weights = scatter(attend_weights.reshape(width, 4 * inner), 0)
    project_grad = attend_weights[:, : 3 * inner].reshape(-1, 3, inner)
    output_weight_grad = attend_weights[:, 3 * inner :].T
    feed_weights = scatter(feed_weights, 1)
    expand_grad = jnp.transpose(feed_weights[:2], (1, 0, 2))
    down_grad = feed_weights[2].T
    return (
        result,
        tokens_grad,
        project_grad,
        query_gain_grad,
        key_gain_grad,
        output_weight_grad,
        output_bias_grad,
        expand_grad,
        down_grad,
        down_bias_grad,
        modulate_grad,
        modulate_bias_grad,
        time_grad,
        time_bias_grad,
        embed_grad,
        embed_bias_grad,
        class_grad,
    )


def solution(mesh):
    return jax.shard_map(
        shards,
        mesh=mesh,
        in_specs=(
            P(("dp", "tensor"), None, None),
            P("dp"),
            P("dp"),
            P("dp"),
            P(("dp", "tensor"), None, None),
            P(None, None, "tensor"),
            P(),
            P(),
            P("tensor", None),
            P(),
            P(None, None, "tensor"),
            P("tensor", None),
            P(),
            P(None, None, "tensor"),
            P(None, "tensor"),
            P(),
            P(),
            P(),
            P(),
            P(),
        ),
        out_specs=(
            P(("dp", "tensor"), None, None),
            P(("dp", "tensor"), None, None),
            P("dp", None, "tensor"),
            P(),
            P(),
            P("tensor", "dp"),
            P(),
            P("dp", None, "tensor"),
            P("tensor", "dp"),
            P(),
            P("dp", None, "tensor"),
            P(),
            P(None, "dp"),
            P("dp"),
            P("dp", None),
            P("dp"),
            P(None, "dp"),
        ),
        check_vma=False,
    )
```

```python
import functools
import math

import jax
import jax.numpy as jnp
from jax import lax
from jax.experimental import pallas as pl
from jax.experimental.pallas import tpu as pltpu
from jax.sharding import PartitionSpec as P

HD = 72
FREQ = 256
GRID = 16


EPS = 1e-06


def layer_norm(value):
    center = value - jnp.mean(value, axis=-1, keepdims=True)
    inverse = lax.rsqrt(jnp.mean(center * center, axis=-1, keepdims=True) + EPS)
    return (center * inverse, inverse)


def layer_norm_back(normed, inverse, grad):
    return inverse * (
        grad
        - jnp.mean(grad, axis=-1, keepdims=True)
        - normed * jnp.mean(grad * normed, axis=-1, keepdims=True)
    )


def silu_slope(value):
    sigma = jax.nn.sigmoid(value)
    return sigma * (1.0 + value * (1.0 - sigma))


def rotate(value, positions):
    quarter = HD // 4
    rates = 10000.0 ** (-jnp.arange(quarter, dtype=jnp.float32) / quarter)
    places = ((positions // GRID).astype(jnp.float32), (positions % GRID).astype(jnp.float32))
    pieces = []
    for which_half in range(2):
        half_value = value[..., which_half * 2 * quarter : (which_half + 1) * 2 * quarter]
        angle = places[which_half][:, None] * rates[None, :]
        cosine = jnp.cos(angle)[None, :, None, :]
        sine = jnp.sin(angle)[None, :, None, :]
        first = half_value[..., :quarter]
        second = half_value[..., quarter:]
        pieces.append(first * cosine - second * sine)
        pieces.append(second * cosine + first * sine)
    return jnp.concatenate(pieces, axis=-1)


def head_prepare(raw, gain, positions):
    scaled = raw * lax.rsqrt(jnp.mean(raw * raw, axis=-1, keepdims=True) + EPS) * gain
    return rotate(scaled, positions)


def time_features(steps_in):
    half = FREQ // 2
    rates = jnp.exp(-math.log(10000.0) * jnp.arange(half, dtype=jnp.float32) / half)
    angle = steps_in.astype(jnp.float32)[:, None] * rates[None, :]
    return jnp.concatenate([jnp.cos(angle), jnp.sin(angle)], axis=-1)


CHUNKS = 8


def rows_of(block, total):
    size = total // CHUNKS
    return pl.ds(pl.multiple_of(block * size, size), size)


class Line:
    def __init__(self, count, gathered, summed, ag_sems, rs_sems):
        self.count = count
        self.place = lax.axis_index("tensor")
        self.gathered = gathered
        self.summed = summed
        self.ag_send, self.ag_recv = ag_sems
        self.rs_send, self.rs_recv = rs_sems

    def barrier(self, wide=1):
        place, count = self.place, self.count
        sem = pltpu.get_barrier_semaphore()

        @pl.when(place > 0)
        def _():
            pl.semaphore_signal(sem, inc=1, device_id={"tensor": place - 1})

        @pl.when(place < count - 1)
        def _():
            pl.semaphore_signal(sem, inc=1, device_id={"tensor": place + 1})

        peers = jnp.where(place > 0, 1, 0) + jnp.where(place < count - 1, 1, 0)
        here = lax.axis_index("dp")

        @pl.loop(1, wide)
        def _(offset):
            peer = lax.rem(here + offset, wide)
            pl.semaphore_signal(sem, inc=1, device_id={"dp": peer})

        pl.semaphore_wait(sem, peers + (wide - 1))

    def item_copy(self, which, way, item, own=False):
        mine, everyone = self.gathered[which]
        target = self.place + (1 if way == 0 else -1)
        return pltpu.make_async_remote_copy(
            src_ref=mine if own else everyone.at[item],
            dst_ref=everyone.at[item],
            send_sem=self.ag_send.at[which, way, item],
            recv_sem=self.ag_recv.at[which, way, item],
            device_id={"tensor": target},
        )

    def can(self, way):
        return self.place < self.count - 1 if way == 0 else self.place > 0

    def sum_copy(self, which, way, item, block):
        part, landed = self.summed[which]
        target = self.place + (1 if way == 0 else -1)
        slot = item
        if way == 1:
            slot = jnp.where(item == target, self.count, item)
        rows = rows_of(block, part.shape[1])
        return pltpu.make_async_remote_copy(
            src_ref=part.at[item, rows],
            dst_ref=landed.at[slot, rows],
            send_sem=self.rs_send.at[which, way, item, block],
            recv_sem=self.rs_recv.at[which, way, item, block],
            device_id={"tensor": target},
        )

    def landed_slot(self, way, item):
        return jnp.where(item == self.place, self.count, item) if way == 1 else item

    def wait_sum(self, which, way, item, block):
        part, landed = self.summed[which]
        rows = rows_of(block, part.shape[1])
        view = landed.at[self.landed_slot(way, item), rows]
        pltpu.make_async_remote_copy(
            src_ref=view,
            dst_ref=view,
            send_sem=self.rs_send.at[which, way, item, block],
            recv_sem=self.rs_recv.at[which, way, item, block],
            device_id={"tensor": self.place},
        ).wait_recv()
        return view

    def start_own(self):
        for which in range(len(self.gathered)):
            for way in range(2):

                @pl.when(self.can(way))
                def _():
                    self.item_copy(which, way, self.place, own=True).start()

    def receive(self, step):
        place, count = self.place, self.count
        for which in range(len(self.gathered)):
            for way in range(2):
                item = place - step if way == 0 else place + step

                @pl.when((item >= 0) & (item < count))
                def _():
                    self.item_copy(which, way, item).wait_recv()

                    @pl.when(self.can(way))
                    def _():
                        self.item_copy(which, way, item).start()

    def items(self, step):
        place, count = self.place, self.count
        low, high = place - step, place + step
        return ((low, (low >= 0)), (high, (high < count) & (step > 0)))

    def moves(self, step):
        place, count = self.place, self.count
        return (
            (0, step, step > place, place),
            (1, count - 1 - step, count - 1 - step < place, count - 1 - place),
        )

    def first_sums(self, step):
        @pl.loop(0, CHUNKS)
        def _(block):
            for way, item, further, hop in self.moves(step):

                @pl.when(further & (hop == 0))
                def _():
                    for which in range(len(self.summed)):
                        self.sum_copy(which, way, item, block).start()

    def relay_sums(self, step):
        @pl.loop(0, CHUNKS + self.count - 3)
        def _(turn):
            for distance in range(1, self.count - 1):
                block = turn - (distance - 1)
                for way, item, further, hop in self.moves(step):

                    @pl.when(further & (hop == distance) & (block >= 0) & (block < CHUNKS))
                    def _():
                        for which in range(len(self.summed)):
                            part, landed = self.summed[which]
                            rows = rows_of(block, part.shape[1])
                            view = self.wait_sum(which, way, item, block)
                            total = part[item, rows].astype(jnp.float32) + view[...].astype(
                                jnp.float32
                            )
                            part[item, rows] = total.astype(part.dtype)
                            self.sum_copy(which, way, item, block).start()

    def near(self, step):
        place, count = self.place, self.count
        low = place >= step
        return jnp.where(low, place - step, place + step), low | (place + step < count)

    def far(self, step):
        place, count = self.place, self.count
        return place + step, (step > 0) & (place >= step) & (place + step < count)

    def finish(self, which, out):
        place, count = self.place, self.count
        part, landed = self.summed[which]

        @pl.loop(0, CHUNKS)
        def _(block):
            rows = rows_of(block, part.shape[1])
            out[rows] = part[place, rows].astype(jnp.float32)
            for way in range(2):

                @pl.when(place > 0 if way == 0 else place < count - 1)
                def _():
                    view = self.wait_sum(which, way, place, block)
                    out[rows] += view[...].astype(jnp.float32)

    def drain(self):
        place, count = self.place, self.count

        @pl.loop(0, count)
        def _(item):
            for way in range(2):
                passed = item <= place if way == 0 else item >= place

                @pl.when(passed & self.can(way))
                def _():
                    for which in range(len(self.gathered)):
                        self.item_copy(which, way, item).wait_send()

                further = item > place if way == 0 else item < place

                @pl.when(further)
                def _():
                    @pl.loop(0, CHUNKS)
                    def _(block):
                        for which in range(len(self.summed)):
                            self.sum_copy(which, way, item, block).wait_send()


def dot(left, right):
    return jnp.dot(left, right, preferred_element_type=jnp.float32)


def dot_rt(left, right):
    return lax.dot_general(
        left, right, (((1,), (1,)), ((), ())), preferred_element_type=jnp.float32
    )


def dot_lt(left, right):
    return lax.dot_general(
        left, right, (((0,), (0,)), ((), ())), preferred_element_type=jnp.float32
    )


def cut(total, most):
    size = max(s for s in range(128, most + 1, 128) if total % s == 0)
    return size, total // size


def span(index, size):
    return pl.ds(pl.multiple_of(index * size, size), size)


def feed_kernel(
    count,
    mod_ref,
    grad_ref,
    expand_hbm,
    down_hbm,
    feed_out,
    back_out,
    weight_out,
    expand,
    down,
    mod_all,
    grad_all,
    hidden,
    slopes,
    feed_part,
    back_part,
    feed_land,
    back_land,
    total,
    load_sem,
    ag_send,
    ag_recv,
    rs_send,
    rs_recv,
):
    line = Line(
        count,
        [(mod_ref, mod_all), (grad_ref, grad_all)],
        [(back_part, back_land), (feed_part, feed_land)],
        (ag_send, ag_recv),
        (rs_send, rs_recv),
    )
    width, units = expand.shape[1], expand.shape[2]
    loads = (
        pltpu.make_async_copy(expand_hbm, expand, load_sem.at[0]),
        pltpu.make_async_copy(down_hbm, down, load_sem.at[1]),
    )
    for load in loads:
        load.start()
    line.barrier()
    line.start_own()
    mod_all[line.place] = mod_ref[...]
    grad_all[line.place] = grad_ref[...]
    total[...] = jnp.zeros_like(total)
    for load in loads:
        load.wait()
    unit_size, unit_count = cut(units, 256)
    wide_size, wide_count = cut(width, 384)
    tall_size, tall_count = cut(width, 128)

    def compute(item):
        @pl.loop(0, unit_count)
        def _(index):
            cols = span(index, unit_size)
            mod = mod_all[item]
            gate = dot(mod, expand[0, :, cols])
            upper = dot(mod, expand[1, :, cols])
            back = dot_rt(grad_all[item], down[cols, :])
            sigma = jax.nn.sigmoid(gate)
            active = gate * sigma
            hidden[item, :, cols] = (active * upper).astype(jnp.bfloat16)
            slopes[0, item, :, cols] = (
                back * upper * (sigma * (1.0 + gate * (1.0 - sigma)))
            ).astype(jnp.bfloat16)
            slopes[1, item, :, cols] = (back * active).astype(jnp.bfloat16)

        @pl.loop(0, wide_count)
        def _(index):
            cols = span(index, wide_size)
            back_part[item, :, cols] = (
                dot_rt(slopes[0, item], expand[0, cols, :])
                + dot_rt(slopes[1, item], expand[1, cols, :])
            ).astype(jnp.bfloat16)
            feed_part[item, :, cols] = dot(hidden[item], down[:, cols]).astype(jnp.bfloat16)

    def weigh(item):
        @pl.loop(0, tall_count)
        def _(index):
            rows = span(index, tall_size)
            mod = mod_all[item, :, rows]
            total[0, rows, :] += dot_lt(mod, slopes[0, item])
            total[1, rows, :] += dot_lt(mod, slopes[1, item])
            total[2, rows, :] += dot_lt(grad_all[item, :, rows], hidden[item])

    @pl.loop(0, count)
    def _(step):
        @pl.when(step > 0)
        def _():
            for item, valid in line.items(step - 1):

                @pl.when(valid)
                def _():
                    weigh(item)

            line.receive(step)

        for item, valid in line.items(step):

            @pl.when(valid)
            def _():
                compute(item)

        @pl.when(step > 0)
        def _():
            line.first_sums(step)
            line.relay_sums(step)

    for item, valid in line.items(count - 1):

        @pl.when(valid)
        def _():
            weigh(item)

    weight_out[...] = total[...].astype(jnp.bfloat16)
    line.finish(0, back_out)
    line.finish(1, feed_out)
    line.drain()


def feed_pass(mod_two, branch_grad, expand_weight, down_weight):
    count = lax.axis_size("tensor")
    length, width = mod_two.shape
    units = down_weight.shape[0]
    expand = jnp.transpose(expand_weight, (1, 0, 2))
    vmem, any_space = pl.BlockSpec(memory_space=pltpu.VMEM), pl.BlockSpec(memory_space=pl.ANY)
    low = jnp.bfloat16
    item = (length, width)
    return pl.pallas_call(
        functools.partial(feed_kernel, count),
        out_shape=(
            jax.ShapeDtypeStruct(item, jnp.float32),
            jax.ShapeDtypeStruct(item, jnp.float32),
            jax.ShapeDtypeStruct((3, width, units), low),
        ),
        in_specs=[vmem, vmem, any_space, any_space],
        out_specs=(vmem, vmem, vmem),
        scratch_shapes=[
            pltpu.VMEM((2, width, units), low),
            pltpu.VMEM((units, width), low),
            pltpu.VMEM((count, *item), low),
            pltpu.VMEM((count, *item), low),
            pltpu.VMEM((count, length, units), low),
            pltpu.VMEM((2, count, length, units), low),
            pltpu.VMEM((count, *item), low),
            pltpu.VMEM((count, *item), low),
            pltpu.VMEM((count + 1, *item), low),
            pltpu.VMEM((count + 1, *item), low),
            pltpu.VMEM((3, width, units), jnp.float32),
            pltpu.SemaphoreType.DMA((2,)),
            pltpu.SemaphoreType.DMA((2, 2, count)),
            pltpu.SemaphoreType.DMA((2, 2, count)),
            pltpu.SemaphoreType.DMA((2, 2, count, CHUNKS)),
            pltpu.SemaphoreType.DMA((2, 2, count, CHUNKS)),
        ],
        compiler_params=pltpu.CompilerParams(
            collective_id=1, has_side_effects=True, vmem_limit_bytes=64000000
        ),
        name="feed_pass",
    )(mod_two, branch_grad, expand, down_weight)


def swap_kernel(jobs, total, *refs):
    n = len(jobs)
    ins, outs = refs[:n], refs[n + total : 2 * n + total]
    sems = refs[2 * n + 2 * total :]
    places = [lax.axis_index(axis) for axis, _, _ in jobs]
    hello = pltpu.get_barrier_semaphore()
    axes = []
    for axis, count, _ in jobs:
        if (axis, count) not in axes:
            axes.append((axis, count))
    if total:
        axes = [("dp", lax.axis_size("dp")), ("tensor", lax.axis_size("tensor"))]
    for axis, count in axes:
        here = lax.axis_index(axis)

        @pl.loop(1, count)
        def _(offset):
            peer = lax.rem(here + offset, count)
            pl.semaphore_signal(hello, inc=1, device_id={axis: peer})

    pl.semaphore_wait(hello, sum(count - 1 for _, count in axes))

    def copy(source, target, send, recv, axis, peer, slot):
        return pltpu.make_async_remote_copy(
            src_ref=source,
            dst_ref=target.at[slot],
            send_sem=send.at[peer],
            recv_sem=recv.at[slot],
            device_id={axis: peer},
        )

    def start(source, target, send, recv, axis, count, split):
        here = lax.axis_index(axis)

        @pl.loop(1, count)
        def _(offset):
            peer = lax.rem(here + offset, count)
            piece = source.at[peer] if split else source
            copy(piece, target, send, recv, axis, peer, here).start()

        target[here] = source[here] if split else source[...]

    def finish(source, target, send, recv, axis, count, split):
        here = lax.axis_index(axis)

        @pl.loop(1, count)
        def _(offset):
            peer = lax.rem(here + offset, count)
            piece = source.at[peer] if split else source
            step = copy(piece, target, send, recv, axis, peer, peer)
            step.wait_recv()
            step.wait_send()

    work = []
    for index, (axis, count, split) in enumerate(jobs):
        work.append((ins[index], outs[index], sems[2 * index], sems[2 * index + 1], axis, count, split))
    if total:
        source, result = refs[n], refs[2 * n + total]
        one, two, middle, s1, r1, s2, r2 = sems[2 * n :]
        wide, deep = lax.axis_size("dp"), lax.axis_size("tensor")
        first = (source, one, s1, r1, "dp", wide, False)
        start(*first)
    for job in work:
        start(*job)
    if total:
        finish(*first)
        middle[...] = one[0]

        @pl.loop(1, wide)
        def _(index):
            middle[...] += one[index]

        second = (middle, two, s2, r2, "tensor", deep, False)
        start(*second)
    for job in work:
        finish(*job)
    if total:
        finish(*second)
        result[...] = two[0]

        @pl.loop(1, deep)
        def _(index):
            result[...] += two[index]


def swap(name, number, jobs, total=None):
    vmem = pl.BlockSpec(memory_space=pltpu.VMEM)
    plan, arrays, shapes, scratch = [], [], [], []
    for array, axis, split in jobs:
        count = lax.axis_size(axis)
        plan.append((axis, count, split))
        arrays.append(array)
        piece = array.shape[1:] if split else array.shape
        shapes.append(jax.ShapeDtypeStruct((count, *piece), array.dtype))
        scratch += [pltpu.SemaphoreType.DMA((count,)), pltpu.SemaphoreType.DMA((count,))]
    if total is not None:
        wide, deep = lax.axis_size("dp"), lax.axis_size("tensor")
        arrays.append(total)
        shapes.append(jax.ShapeDtypeStruct(total.shape, total.dtype))
        scratch += [
            pltpu.VMEM((wide, *total.shape), total.dtype),
            pltpu.VMEM((deep, *total.shape), total.dtype),
            pltpu.VMEM(total.shape, total.dtype),
        ]
        for count in (wide, wide, deep, deep):
            scratch.append(pltpu.SemaphoreType.DMA((count,)))
    return pl.pallas_call(
        functools.partial(swap_kernel, tuple(plan), int(total is not None)),
        out_shape=tuple(shapes),
        in_specs=[vmem] * len(arrays),
        out_specs=tuple([vmem] * len(shapes)),
        scratch_shapes=scratch,
        compiler_params=pltpu.CompilerParams(collective_id=number, has_side_effects=True),
        name=name,
    )(*arrays)


LANES = 128
HEAD_UNROLL = 2


def turn(value, tables):
    return (
        value * tables[0]
        + pltpu.roll(value, LANES - HD // 4, 1) * tables[1]
        + pltpu.roll(value, HD // 4, 1) * tables[2]
    )


def turn_back(grad, tables):
    return (
        grad * tables[0]
        + pltpu.roll(grad * tables[1], HD // 4, 1)
        + pltpu.roll(grad * tables[2], LANES - HD // 4, 1)
    )


def turn_tables(length):
    quarter = HD // 4
    lane = jnp.arange(LANES)
    rates = 10000.0 ** (-(lane % quarter).astype(jnp.float32) / quarter)
    positions = jnp.arange(length)[:, None]
    place = jnp.where(lane < 2 * quarter, positions // GRID, positions % GRID)
    angle = place.astype(jnp.float32) * rates
    real = lane < HD
    early = (lane // quarter) % 2 == 0
    cosine = jnp.where(real, jnp.cos(angle), 0.0)
    sine = jnp.sin(angle)
    return jnp.stack(
        [
            cosine,
            jnp.where(real & early, -sine, 0.0),
            jnp.where(real & ~early, sine, 0.0),
        ]
    )


def unit_norm(raw):
    inverse = lax.rsqrt(jnp.sum(raw * raw, axis=-1, keepdims=True) * (1.0 / HD) + EPS)
    return raw * inverse, inverse


def project(mod, weight, raw):
    @pl.loop(0, weight.shape[0])
    def _(index):
        raw[index] = dot(mod, weight[index])


def soft(queries, keys):
    grown = jnp.exp2(dot_rt(queries, keys) * (HD ** (-0.5) / math.log(2.0)))
    return grown * (1.0 / jnp.sum(grown, axis=-1, keepdims=True))


def attend_kernel(
    count,
    mod_ref,
    tables_ref,
    gains_ref,
    weight_hbm,
    last_hbm,
    branch_out,
    mod_out,
    weight,
    last,
    mod_all,
    raw,
    mixed,
    part,
    land,
    load_sem,
    ag_send,
    ag_recv,
    rs_send,
    rs_recv,
):
    line = Line(count, [(mod_ref, mod_all)], [(part, land)], (ag_send, ag_recv), (rs_send, rs_recv))
    loads = (
        pltpu.make_async_copy(weight_hbm, weight, load_sem.at[0]),
        pltpu.make_async_copy(last_hbm, last, load_sem.at[1]),
    )
    for load in loads:
        load.start()
    line.barrier()
    line.start_own()
    mod_all[line.place] = mod_ref[...]
    for load in loads:
        load.wait()
    heads = last.shape[0] // LANES
    wide_size, wide_count = cut(last.shape[1], 384)

    def compute(item):
        project(mod_all[item], weight, raw)
        tables = (tables_ref[0], tables_ref[1], tables_ref[2])

        @pl.loop(0, heads, unroll=HEAD_UNROLL)
        def _(head):
            lanes = span(head, LANES)
            queries = turn(unit_norm(raw[0, :, lanes])[0] * gains_ref[0:1, :], tables)
            keys = turn(unit_norm(raw[1, :, lanes])[0] * gains_ref[1:2, :], tables)
            probs = soft(queries.astype(jnp.bfloat16), keys.astype(jnp.bfloat16))
            values = raw[2, :, lanes].astype(jnp.bfloat16)
            mixed[:, lanes] = dot(probs.astype(jnp.bfloat16), values).astype(jnp.bfloat16)

        @pl.loop(0, wide_count)
        def _(index):
            cols = span(index, wide_size)
            part[item, :, cols] = dot(mixed[...], last[:, cols]).astype(jnp.bfloat16)

    @pl.loop(0, count)
    def _(step):
        late, owed = line.far(step - 1)
        item, valid = line.near(step)

        @pl.when(step > 0)
        def _():
            line.receive(step)

            @pl.when(owed)
            def _():
                compute(late)

        @pl.when(valid)
        def _():
            compute(item)

        @pl.when(step > 0)
        def _():
            line.first_sums(step)
            line.relay_sums(step)

    mod_out[...] = mod_all[...]
    line.finish(0, branch_out)
    line.drain()


def block_copy(array, target, slot, block, size, send, recv, peer):
    rows = pl.ds(pl.multiple_of(block * size, size), size)
    source = array.at[rows] if len(array.shape) == 2 else array.at[:, rows]
    return pltpu.make_async_remote_copy(
        src_ref=source,
        dst_ref=target.at[slot],
        send_sem=send,
        recv_sem=recv,
        device_id={"dp": peer},
    )


def attend_back_kernel(
    count,
    wide,
    grad_ref,
    mod_all,
    tables_ref,
    gains_ref,
    narrow_ref,
    weight_hbm,
    last_hbm,
    *rest,
):
    if wide:
        feed_hbm, back_out, weight_out, gain_out, feed_out, *rest = rest
    else:
        back_out, weight_out, gain_out, *rest = rest
    (
        weight,
        last,
        grad_all,
        raw,
        mixed,
        mixed_grad,
        raw_grad,
        kept,
        kept_mixed,
        part,
        land,
        total,
        load_sem,
        ag_send,
        ag_recv,
        rs_send,
        rs_recv,
        *rest,
    ) = rest
    line = Line(count, [(grad_ref, grad_all)], [(part, land)], (ag_send, ag_recv), (rs_send, rs_recv))
    loads = (
        pltpu.make_async_copy(weight_hbm, weight, load_sem.at[0]),
        pltpu.make_async_copy(last_hbm, last, load_sem.at[1]),
    )
    for load in loads:
        load.start()
    line.barrier(wide or 1)
    line.start_own()
    width = last.shape[1]
    here = lax.axis_index("dp")
    if wide:
        feed_land, staged, pair_land, quad_land, fs, fr, ps, pr, qs, qr = rest
        size = width // wide
        half = wide // 2
        parity, seat = lax.rem(here, 2), here // 2
        partner = here + 1 - 2 * parity

        def feed_copy(peer, slot):
            return block_copy(feed_hbm, feed_land, slot, peer, size, fs.at[peer], fr.at[slot], peer)

        def pair_copy(index):
            block = 2 * index + 1 - parity
            return block_copy(
                staged, pair_land, index, block, size, ps.at[index], pr.at[index], partner
            )

        def quad_copy(index, slot):
            block = 2 * index + parity
            return block_copy(
                staged, quad_land, slot, block, size, qs.at[index], qr.at[slot], block
            )

        @pl.loop(1, wide)
        def _(offset):
            peer = lax.rem(here + offset, wide)
            feed_copy(peer, here).start()

    grad_all[line.place] = grad_ref[...]
    total[...] = jnp.zeros_like(total)
    gain_out[...] = jnp.zeros_like(gain_out)
    for load in loads:
        load.wait()
    inner = last.shape[0]
    heads = inner // LANES
    scale = HD ** (-0.5)
    wide_size, wide_count = cut(width, 384)
    inner_size, inner_count = cut(inner, 256)
    tall_size, tall_count = cut(width, 128)
    first_width = kept.shape[2]

    def compute(item):
        project(mod_all[item], weight, raw)
        tables = (tables_ref[0], tables_ref[1], tables_ref[2])

        @pl.loop(0, inner_count)
        def _(index):
            cols = span(index, inner_size)
            mixed_grad[:, cols] = dot_rt(grad_all[item], last[cols, :]).astype(jnp.bfloat16)

        @pl.loop(0, heads, unroll=HEAD_UNROLL)
        def _(head):
            lanes = span(head, LANES)
            query_norm, query_inverse = unit_norm(raw[0, :, lanes])
            key_norm, key_inverse = unit_norm(raw[1, :, lanes])
            values = raw[2, :, lanes].astype(jnp.bfloat16)
            queries = turn(query_norm * gains_ref[0:1, :], tables).astype(jnp.bfloat16)
            keys = turn(key_norm * gains_ref[1:2, :], tables).astype(jnp.bfloat16)
            probs = soft(queries, keys)
            probs_low = probs.astype(jnp.bfloat16)
            mixed[:, lanes] = dot(probs_low, values).astype(jnp.bfloat16)
            grad = mixed_grad[:, lanes]
            prob_grad = dot_rt(grad, values)
            score_grad = (
                probs * (prob_grad - jnp.sum(probs * prob_grad, axis=-1, keepdims=True))
            ).astype(jnp.bfloat16)

            def back(which, value_grad, norm, inverse):
                turned = turn_back(value_grad, tables)
                gained = turned * norm
                gain_out[which] += jnp.sum(gained.reshape(-1, 8, LANES), axis=0)
                scaled = turned * gains_ref[which : which + 1, :]
                mean = jnp.sum(scaled * norm, axis=-1, keepdims=True) * (1.0 / HD)
                raw_grad[which, :, lanes] = (inverse * (scaled - norm * mean)).astype(
                    jnp.bfloat16
                )

            back(0, dot(score_grad, keys) * scale, query_norm, query_inverse)
            back(1, dot_lt(score_grad, queries) * scale, key_norm, key_inverse)
            raw_grad[2, :, lanes] = dot_lt(probs_low, grad).astype(jnp.bfloat16)

        @pl.loop(0, wide_count)
        def _(index):
            cols = span(index, wide_size)
            sums = dot_rt(raw_grad[0], weight[0, cols, :])
            sums += dot_rt(raw_grad[1], weight[1, cols, :])
            sums += dot_rt(raw_grad[2], weight[2, cols, :])
            part[item, :, cols] = sums.astype(jnp.bfloat16)

    def keep(item):
        one = dot(raw_grad[0], narrow_ref[0])
        two = dot(raw_grad[1], narrow_ref[1])
        three = dot(raw_grad[2], narrow_ref[2])
        side = one.shape[1] - LANES
        low = jnp.bfloat16
        kept[item, :, :side] = one[:, :side].astype(low)
        kept[item, :, side : side + LANES] = (one[:, side:] + two[:, :LANES]).astype(low)
        kept[item, :, side + LANES : 2 * side] = two[:, LANES:side].astype(low)
        kept[item, :, 2 * side : 2 * side + LANES] = (two[:, side:] + three[:, :LANES]).astype(low)
        kept[item, :, 2 * side + LANES :] = three[:, LANES:].astype(low)
        kept_mixed[item] = dot(mixed[...], narrow_ref[0]).astype(low)

    def weigh(item):
        @pl.loop(0, tall_count)
        def _(index):
            rows = span(index, tall_size)
            total[rows, :first_width] += dot_lt(mod_all[item, :, rows], kept[item])
            total[rows, first_width:] += dot_lt(grad_all[item, :, rows], kept_mixed[item])

    @pl.loop(0, count)
    def _(step):
        late, owed = line.far(step - 1)
        item, valid = line.near(step)

        @pl.when(step > 0)
        def _():
            older, kept_older = line.far(step - 2)
            old, kept_old = line.near(step - 1)

            @pl.when((step > 1) & kept_older)
            def _():
                weigh(older)

            @pl.when(kept_old)
            def _():
                weigh(old)

            line.receive(step)

            @pl.when(owed)
            def _():
                compute(late)
                keep(late)

        @pl.when(valid)
        def _():
            compute(item)

            @pl.when(step > 0)
            def _():
                line.first_sums(step)

            keep(item)

        @pl.when(step == count - 1)
        def _():
            @pl.when(valid)
            def _():
                weigh(item)

            if wide:
                staged[...] = total[...].astype(jnp.bfloat16)

                @pl.loop(0, half)
                def _(index):
                    pair_copy(index).start()

        @pl.when(step > 0)
        def _():
            line.relay_sums(step)

    if wide:

        @pl.loop(0, half)
        def _(index):
            pair_copy(index).wait_send()
            pair_copy(index).wait_recv()
            rows = pl.ds(pl.multiple_of((2 * index + parity) * size, size), size)
            staged[rows] = (
                staged[rows].astype(jnp.float32) + pair_land[index].astype(jnp.float32)
            ).astype(jnp.bfloat16)

        @pl.loop(1, half)
        def _(offset):
            index = lax.rem(seat + offset, half)
            quad_copy(index, seat).start()

    line.finish(0, back_out)
    line.drain()
    if wide:
        rows = pl.ds(pl.multiple_of(here * size, size), size)
        own = pltpu.make_async_copy(feed_hbm.at[:, rows], feed_land.at[here], load_sem.at[0])
        own.start()

        @pl.loop(1, wide)
        def _(offset):
            peer = lax.rem(here + offset, wide)
            feed_copy(peer, here).wait_send()
            feed_copy(here, peer).wait_recv()

        own.wait()
        for which in range(feed_out.shape[0]):
            feed_out[which] = feed_land[0, which].astype(jnp.float32)

            @pl.loop(1, wide)
            def _(index):
                feed_out[which] += feed_land[index, which].astype(jnp.float32)

        weight_out[...] = staged[rows].astype(jnp.float32)

        @pl.loop(1, half)
        def _(offset):
            index = lax.rem(seat + offset, half)
            quad_copy(index, seat).wait_send()
            quad_copy(seat, index).wait_recv()
            weight_out[...] += quad_land[index].astype(jnp.float32)

    else:
        weight_out[...] = total[...].astype(jnp.bfloat16)


def attend_arrays(project_weight, output_weight, query_gain, key_gain, length):
    inner = project_weight.shape[2]
    heads = inner // HD
    low = jnp.bfloat16
    spot = jnp.arange(heads * LANES)
    real = spot % LANES < HD
    column = spot // LANES * HD + spot % LANES
    spread = (real[None] & (column[None] == jnp.arange(inner)[:, None])).astype(low)
    window = -(-inner // LANES) * LANES
    narrow = jnp.stack(
        [
            real[:, None]
            & (column[:, None] + index * (inner % LANES) == jnp.arange(window)[None, :])
            for index in range(3)
        ]
    ).astype(low)
    weight = jnp.einsum("dke,eh->kdh", project_weight, spread, preferred_element_type=low)
    last = jnp.einsum("ed,eh->hd", output_weight, spread, preferred_element_type=low)
    pad = LANES - HD
    gains = jnp.pad(jnp.stack([query_gain, key_gain]).astype(jnp.float32), ((0, 6), (0, pad)))
    return turn_tables(length), gains, narrow, weight, last


def line_sems(count, gathers, sums):
    return [
        pltpu.SemaphoreType.DMA((2,)),
        pltpu.SemaphoreType.DMA((gathers, 2, count)),
        pltpu.SemaphoreType.DMA((gathers, 2, count)),
        pltpu.SemaphoreType.DMA((sums, 2, count, CHUNKS)),
        pltpu.SemaphoreType.DMA((sums, 2, count, CHUNKS)),
    ]


def attend_pass(mod_in, arrays):
    count = lax.axis_size("tensor")
    tables, gains, _, weight, last = arrays
    item = mod_in.shape
    inner = last.shape[0]
    vmem, any_space = pl.BlockSpec(memory_space=pltpu.VMEM), pl.BlockSpec(memory_space=pl.ANY)
    low = jnp.bfloat16
    return pl.pallas_call(
        functools.partial(attend_kernel, count),
        out_shape=(
            jax.ShapeDtypeStruct(item, jnp.float32),
            jax.ShapeDtypeStruct((count, *item), low),
        ),
        in_specs=[vmem, vmem, vmem, any_space, any_space],
        out_specs=(vmem, vmem),
        scratch_shapes=[
            pltpu.VMEM(weight.shape, low),
            pltpu.VMEM(last.shape, low),
            pltpu.VMEM((count, *item), low),
            pltpu.VMEM((3, item[0], inner), jnp.float32),
            pltpu.VMEM((item[0], inner), low),
            pltpu.VMEM((count, *item), low),
            pltpu.VMEM((count + 1, *item), low),
            *line_sems(count, 1, 1),
        ],
        compiler_params=pltpu.CompilerParams(
            collective_id=6, has_side_effects=True, vmem_limit_bytes=60000000
        ),
        name="attend_pass",
    )(mod_in, tables, gains, weight, last)


def attend_back_pass(attend_grad, mod_all, arrays, feed_weights):
    count, wide = lax.axis_size("tensor"), lax.axis_size("dp")
    tables, gains, narrow, weight, last = arrays
    item = attend_grad.shape
    length, width = item
    inner = last.shape[0]
    vmem, any_space = pl.BlockSpec(memory_space=pltpu.VMEM), pl.BlockSpec(memory_space=pl.ANY)
    low, high = jnp.bfloat16, jnp.float32
    window = narrow.shape[2]
    first_width = 3 * window - 2 * LANES
    columns = first_width + window
    if width % (16 * wide):
        wide = 0
    size = width // wide if wide else width
    outs = [
        jax.ShapeDtypeStruct(item, high),
        jax.ShapeDtypeStruct((size, columns), high if wide else low),
        jax.ShapeDtypeStruct((2, 8, LANES), high),
    ]
    scratch = [
        pltpu.VMEM(weight.shape, low),
        pltpu.VMEM(last.shape, low),
        pltpu.VMEM((count, *item), low),
        pltpu.VMEM((3, length, inner), high),
        pltpu.VMEM((length, inner), low),
        pltpu.VMEM((length, inner), low),
        pltpu.VMEM((3, length, inner), low),
        pltpu.VMEM((count, length, first_width), low),
        pltpu.VMEM((count, length, window), low),
        pltpu.VMEM((count, *item), low),
        pltpu.VMEM((count + 1, *item), low),
        pltpu.VMEM((width, columns), high),
        *line_sems(count, 1, 1),
    ]
    ins = [attend_grad, mod_all, tables, gains, narrow, weight, last]
    specs = [vmem, vmem, vmem, vmem, vmem, any_space, any_space]
    if wide:
        ins.append(feed_weights)
        specs.append(any_space)
        kinds, _, units = feed_weights.shape
        outs.append(jax.ShapeDtypeStruct((kinds, size, units), high))
        half = wide // 2
        scratch += [
            pltpu.VMEM((wide, kinds, size, units), low),
            pltpu.VMEM((width, columns), low),
            pltpu.VMEM((half, size, columns), low),
            pltpu.VMEM((half, size, columns), low),
        ]
        for number in (wide, wide, half, half, half, half):
            scratch.append(pltpu.SemaphoreType.DMA((number,)))
    results = pl.pallas_call(
        functools.partial(attend_back_kernel, count, wide),
        out_shape=tuple(outs),
        in_specs=specs,
        out_specs=tuple([vmem] * len(outs)),
        scratch_shapes=scratch,
        compiler_params=pltpu.CompilerParams(
            collective_id=7, has_side_effects=True, vmem_limit_bytes=66000000
        ),
        name="attend_back_pass",
    )(*ins)
    if wide:
        return results

    def scatter(value, axis):
        return lax.psum_scatter(value, "dp", scatter_dimension=axis, tiled=True).astype(high)

    back, weights, gain_parts = results
    return back, scatter(weights, 0), gain_parts, scatter(feed_weights, 1)


def shards(
    tokens,
    timesteps,
    labels,
    item_counts,
    cotangent,
    project_weight,
    query_gain,
    key_gain,
    output_weight,
    output_bias,
    expand_weight,
    down_weight,
    down_bias,
    modulate_weight,
    modulate_bias,
    time_weight,
    time_bias,
    embed_weight,
    embed_bias,
    class_table,
):
    local_items, length, width = tokens.shape
    items = timesteps.shape[0]
    slab = modulate_weight.shape[2]
    heads_here = project_weight.shape[2] // HD
    scale = HD ** (-0.5)
    first_item = lax.axis_index("tensor") * local_items
    live = (first_item + jnp.arange(local_items) < item_counts[0]).astype(jnp.float32)[
        :, None, None
    ]
    index = lax.axis_index("dp")
    time_feat = time_features(timesteps).astype(jnp.bfloat16)
    pre_hidden = jnp.dot(
        time_feat, time_weight, preferred_element_type=jnp.float32
    ) + time_bias.astype(jnp.float32)
    time_hidden = jax.nn.silu(pre_hidden).astype(jnp.bfloat16)
    condition = (
        jnp.dot(time_hidden, embed_weight, preferred_element_type=jnp.float32)
        + embed_bias.astype(jnp.float32)
        + jnp.take(class_table, labels, axis=0).astype(jnp.float32)
    )
    cond_act = jax.nn.silu(condition).astype(jnp.bfloat16)
    modulation_part = (
        jnp.einsum("bd,dke->bke", cond_act, modulate_weight, preferred_element_type=jnp.float32)
        + modulate_bias.astype(jnp.float32)
    ).astype(jnp.bfloat16)
    (modulation_local,) = swap("modulation_swap", 2, [(modulation_part, "tensor", True)])
    modulation_local = jnp.transpose(modulation_local, (1, 0, 2)).reshape(1, 6, width)
    modulation_local = modulation_local.astype(jnp.float32)
    local_parts = [modulation_local[:, which][:, None, :] for which in range(6)]
    attend_shift, attend_scale, attend_gate, feed_shift, feed_scale, feed_gate = local_parts
    positions = jnp.arange(length)
    token_local = tokens.astype(jnp.float32)
    normed_local, inverse_local = layer_norm(token_local)
    mod_in = normed_local * (1.0 + attend_scale) + attend_shift
    arrays = attend_arrays(project_weight, output_weight, query_gain, key_gain, length)
    attend_total, mod_all = attend_pass(mod_in[0].astype(jnp.bfloat16), arrays)
    attend_branch = attend_total[None] + output_bias.astype(jnp.float32)
    residual = token_local + attend_gate * attend_branch
    normed_two, inverse_two = layer_norm(residual)
    mod_two = (normed_two * (1.0 + feed_scale) + feed_shift).astype(jnp.bfloat16)
    out_grad = cotangent.astype(jnp.float32) * live
    branch_grad = (out_grad * feed_gate).astype(jnp.bfloat16)
    down_bias_part = jnp.sum(branch_grad.astype(jnp.float32), axis=(0, 1))
    feed_total, mod_two_grad, feed_weights = feed_pass(
        mod_two[0], branch_grad[0], expand_weight, down_weight
    )
    feed_branch = feed_total[None] + down_bias.astype(jnp.float32)
    result = (live * (residual + feed_gate * feed_branch)).astype(jnp.bfloat16)
    mod_two_grad = mod_two_grad[None]
    residual_grad = out_grad + layer_norm_back(
        normed_two, inverse_two, mod_two_grad * (1.0 + feed_scale)
    )
    attend_grad = (residual_grad * attend_gate).astype(jnp.bfloat16)
    output_bias_part = jnp.sum(attend_grad.astype(jnp.float32), axis=(0, 1))
    mod_in_grad, attend_weights, gain_parts, feed_weights = attend_back_pass(
        attend_grad[0], mod_all, arrays, feed_weights
    )
    mod_in_grad = mod_in_grad[None]
    query_gain_part, key_gain_part = jnp.sum(gain_parts, axis=1)[:, :HD]
    tokens_grad = (
        residual_grad
        + layer_norm_back(normed_local, inverse_local, mod_in_grad * (1.0 + attend_scale))
    ).astype(jnp.bfloat16)
    modulation_grad_part = jnp.stack(
        [
            jnp.sum(mod_in_grad, axis=1),
            jnp.sum(mod_in_grad * normed_local, axis=1),
            jnp.sum(residual_grad * attend_branch, axis=1),
            jnp.sum(mod_two_grad, axis=1),
            jnp.sum(mod_two_grad * normed_two, axis=1),
            jnp.sum(out_grad * feed_branch, axis=1),
        ],
        axis=1,
    )
    modulation_grad_part = modulation_grad_part[0].astype(jnp.bfloat16)
    small = jnp.concatenate(
        [
            output_bias_part,
            down_bias_part,
            modulation_grad_part.astype(jnp.float32).reshape(-1),
            query_gain_part,
            key_gain_part,
        ]
    )
    small_size = small.shape[0]
    small = jnp.pad(small, (0, -small_size % 1024)).reshape(-1, 128)
    tensor_size = width // slab
    modulation_grad, small = swap(
        "sums_swap",
        3,
        [
            (
                jnp.transpose(modulation_grad_part.reshape(6, tensor_size, slab), (1, 0, 2)),
                "tensor",
                True,
            )
        ],
        small,
    )
    small = small.reshape(-1)
    output_bias_grad = small[:width]
    down_bias_grad = small[width : 2 * width]
    modulate_bias_grad = small[2 * width : 8 * width].reshape(6, width)
    query_gain_grad = small[8 * width : 8 * width + HD]
    key_gain_grad = small[8 * width + HD : 8 * width + 2 * HD]
    cond_part = jnp.einsum(
        "bke,dke->bd", modulation_grad, modulate_weight, preferred_element_type=jnp.float32
    )
    (cond_parts,) = swap("condition_swap", 4, [(cond_part, "tensor", False)])
    cond_grad = (jnp.sum(cond_parts, axis=0) * silu_slope(condition)).astype(jnp.bfloat16)
    pre_grad = (
        jnp.einsum("be,de->bd", cond_grad, embed_weight, preferred_element_type=jnp.float32)
        * silu_slope(pre_hidden)
    ).astype(jnp.bfloat16)
    pieces = [
        cond_grad,
        cond_act,
        time_hidden,
        pre_grad,
        time_feat,
        modulation_grad.reshape(items, 6 * slab),
    ]
    packed = jnp.concatenate(pieces, axis=1)
    tags = jnp.broadcast_to(labels[:, None], (items, 128))
    packed, tags = swap("items_swap", 5, [(packed, "dp", False), (tags, "dp", False)])
    packed = packed.reshape(-1, packed.shape[2])
    tags = tags[:, :, 0].reshape(-1)
    edges = [0]
    for piece in pieces:
        edges.append(edges[-1] + piece.shape[1])
    cond_grad, cond_act, time_hidden, pre_grad, time_feat, modulation_grad = [
        packed[:, start:stop] for start, stop in zip(edges[:-1], edges[1:])
    ]
    modulation_grad = modulation_grad.reshape(-1, 6, slab)
    share = width // lax.axis_size("dp")

    def mine(value):
        return lax.dynamic_slice_in_dim(value, index * share, share, 1)

    one_hot = (tags[:, None] == jnp.arange(class_table.shape[0])[None, :]).astype(jnp.bfloat16)
    cond_grad_mine, pre_grad_mine = mine(cond_grad), mine(pre_grad)
    class_grad = jnp.einsum(
        "bc,bd->cd", one_hot, cond_grad_mine, preferred_element_type=jnp.float32
    )
    modulate_grad = jnp.einsum(
        "bd,bke->dke", mine(cond_act), modulation_grad, preferred_element_type=jnp.float32
    )
    embed_grad = jnp.einsum(
        "bd,be->de", mine(time_hidden), cond_grad, preferred_element_type=jnp.float32
    )
    embed_bias_grad = jnp.sum(cond_grad_mine.astype(jnp.float32), axis=0)
    time_grad = jnp.einsum(
        "bf,bd->fd", time_feat, pre_grad_mine, preferred_element_type=jnp.float32
    )
    time_bias_grad = jnp.sum(pre_grad_mine.astype(jnp.float32), axis=0)

    inner = heads_here * HD
    first_width = attend_weights.shape[1] - -(-inner // LANES) * LANES
    project_grad = attend_weights[:, : 3 * inner].reshape(-1, 3, inner)
    output_weight_grad = attend_weights[:, first_width : first_width + inner].T
    expand_grad = jnp.transpose(feed_weights[:2], (1, 0, 2))
    down_grad = feed_weights[2].T
    return (
        result,
        tokens_grad,
        project_grad,
        query_gain_grad,
        key_gain_grad,
        output_weight_grad,
        output_bias_grad,
        expand_grad,
        down_grad,
        down_bias_grad,
        modulate_grad,
        modulate_bias_grad,
        time_grad,
        time_bias_grad,
        embed_grad,
        embed_bias_grad,
        class_grad,
    )


def solution(mesh):
    return jax.shard_map(
        shards,
        mesh=mesh,
        in_specs=(
            P(("dp", "tensor"), None, None),
            P("dp"),
            P("dp"),
            P("dp"),
            P(("dp", "tensor"), None, None),
            P(None, None, "tensor"),
            P(),
            P(),
            P("tensor", None),
            P(),
            P(None, None, "tensor"),
            P("tensor", None),
            P(),
            P(None, None, "tensor"),
            P(None, "tensor"),
            P(),
            P(),
            P(),
            P(),
            P(),
        ),
        out_specs=(
            P(("dp", "tensor"), None, None),
            P(("dp", "tensor"), None, None),
            P("dp", None, "tensor"),
            P(),
            P(),
            P("tensor", "dp"),
            P(),
            P("dp", None, "tensor"),
            P("tensor", "dp"),
            P(),
            P("dp", None, "tensor"),
            P(),
            P(None, "dp"),
            P("dp"),
            P("dp", None),
            P("dp"),
            P(None, "dp"),
        ),
        check_vma=False,
    )
```

```python
import functools
import math

import jax
import jax.numpy as jnp
from jax import lax
from jax.experimental import pallas as pl
from jax.experimental.pallas import tpu as pltpu
from jax.sharding import PartitionSpec as P

HD = 72
FREQ = 256
GRID = 16


EPS = 1e-06


def layer_norm(value):
    center = value - jnp.mean(value, axis=-1, keepdims=True)
    inverse = lax.rsqrt(jnp.mean(center * center, axis=-1, keepdims=True) + EPS)
    return (center * inverse, inverse)


def layer_norm_back(normed, inverse, grad):
    return inverse * (
        grad
        - jnp.mean(grad, axis=-1, keepdims=True)
        - normed * jnp.mean(grad * normed, axis=-1, keepdims=True)
    )


def silu_slope(value):
    sigma = jax.nn.sigmoid(value)
    return sigma * (1.0 + value * (1.0 - sigma))


def rotate(value, positions):
    quarter = HD // 4
    rates = 10000.0 ** (-jnp.arange(quarter, dtype=jnp.float32) / quarter)
    places = ((positions // GRID).astype(jnp.float32), (positions % GRID).astype(jnp.float32))
    pieces = []
    for which_half in range(2):
        half_value = value[..., which_half * 2 * quarter : (which_half + 1) * 2 * quarter]
        angle = places[which_half][:, None] * rates[None, :]
        cosine = jnp.cos(angle)[None, :, None, :]
        sine = jnp.sin(angle)[None, :, None, :]
        first = half_value[..., :quarter]
        second = half_value[..., quarter:]
        pieces.append(first * cosine - second * sine)
        pieces.append(second * cosine + first * sine)
    return jnp.concatenate(pieces, axis=-1)


def head_prepare(raw, gain, positions):
    scaled = raw * lax.rsqrt(jnp.mean(raw * raw, axis=-1, keepdims=True) + EPS) * gain
    return rotate(scaled, positions)


def time_features(steps_in):
    half = FREQ // 2
    rates = jnp.exp(-math.log(10000.0) * jnp.arange(half, dtype=jnp.float32) / half)
    angle = steps_in.astype(jnp.float32)[:, None] * rates[None, :]
    return jnp.concatenate([jnp.cos(angle), jnp.sin(angle)], axis=-1)


CHUNKS = 8


def rows_of(block, total):
    size = total // CHUNKS
    return pl.ds(pl.multiple_of(block * size, size), size)


class Line:
    def __init__(self, count, gathered, summed, ag_sems, rs_sems):
        self.count = count
        self.place = lax.axis_index("tensor")
        self.gathered = gathered
        self.summed = summed
        self.ag_send, self.ag_recv = ag_sems
        self.rs_send, self.rs_recv = rs_sems

    def barrier(self, wide=1):
        place, count = self.place, self.count
        sem = pltpu.get_barrier_semaphore()

        @pl.when(place > 0)
        def _():
            pl.semaphore_signal(sem, inc=1, device_id={"tensor": place - 1})

        @pl.when(place < count - 1)
        def _():
            pl.semaphore_signal(sem, inc=1, device_id={"tensor": place + 1})

        peers = jnp.where(place > 0, 1, 0) + jnp.where(place < count - 1, 1, 0)
        here = lax.axis_index("dp")

        @pl.loop(1, wide)
        def _(offset):
            peer = lax.rem(here + offset, wide)
            pl.semaphore_signal(sem, inc=1, device_id={"dp": peer})

        pl.semaphore_wait(sem, peers + (wide - 1))

    def item_copy(self, which, way, item, own=False):
        mine, everyone = self.gathered[which]
        target = self.place + (1 if way == 0 else -1)
        return pltpu.make_async_remote_copy(
            src_ref=mine if own else everyone.at[item],
            dst_ref=everyone.at[item],
            send_sem=self.ag_send.at[which, way, item],
            recv_sem=self.ag_recv.at[which, way, item],
            device_id={"tensor": target},
        )

    def can(self, way):
        return self.place < self.count - 1 if way == 0 else self.place > 0

    def sum_copy(self, which, way, item, block):
        part, landed = self.summed[which]
        target = self.place + (1 if way == 0 else -1)
        slot = item
        if way == 1:
            slot = jnp.where(item == target, self.count, item)
        rows = rows_of(block, part.shape[1])
        return pltpu.make_async_remote_copy(
            src_ref=part.at[item, rows],
            dst_ref=landed.at[slot, rows],
            send_sem=self.rs_send.at[which, way, item, block],
            recv_sem=self.rs_recv.at[which, way, item, block],
            device_id={"tensor": target},
        )

    def landed_slot(self, way, item):
        return jnp.where(item == self.place, self.count, item) if way == 1 else item

    def wait_sum(self, which, way, item, block):
        part, landed = self.summed[which]
        rows = rows_of(block, part.shape[1])
        view = landed.at[self.landed_slot(way, item), rows]
        pltpu.make_async_remote_copy(
            src_ref=view,
            dst_ref=view,
            send_sem=self.rs_send.at[which, way, item, block],
            recv_sem=self.rs_recv.at[which, way, item, block],
            device_id={"tensor": self.place},
        ).wait_recv()
        return view

    def start_own(self):
        for which in range(len(self.gathered)):
            for way in range(2):

                @pl.when(self.can(way))
                def _():
                    self.item_copy(which, way, self.place, own=True).start()

    def receive(self, step):
        place, count = self.place, self.count
        for which in range(len(self.gathered)):
            for way in range(2):
                item = place - step if way == 0 else place + step

                @pl.when((item >= 0) & (item < count))
                def _():
                    self.item_copy(which, way, item).wait_recv()

                    @pl.when(self.can(way))
                    def _():
                        self.item_copy(which, way, item).start()

    def items(self, step):
        place, count = self.place, self.count
        low, high = place - step, place + step
        return ((low, (low >= 0)), (high, (high < count) & (step > 0)))

    def moves(self, step):
        place, count = self.place, self.count
        return (
            (0, step, step > place, place),
            (1, count - 1 - step, count - 1 - step < place, count - 1 - place),
        )

    def first_sums(self, step):
        @pl.loop(0, CHUNKS)
        def _(block):
            for way, item, further, hop in self.moves(step):

                @pl.when(further & (hop == 0))
                def _():
                    for which in range(len(self.summed)):
                        self.sum_copy(which, way, item, block).start()

    def relay_sums(self, step):
        @pl.loop(0, CHUNKS + self.count - 3)
        def _(turn):
            for distance in range(1, self.count - 1):
                block = turn - (distance - 1)
                for way, item, further, hop in self.moves(step):

                    @pl.when(further & (hop == distance) & (block >= 0) & (block < CHUNKS))
                    def _():
                        for which in range(len(self.summed)):
                            part, landed = self.summed[which]
                            rows = rows_of(block, part.shape[1])
                            view = self.wait_sum(which, way, item, block)
                            total = part[item, rows].astype(jnp.float32) + view[...].astype(
                                jnp.float32
                            )
                            part[item, rows] = total.astype(part.dtype)
                            self.sum_copy(which, way, item, block).start()

    def near(self, step):
        place, count = self.place, self.count
        low = place >= step
        return jnp.where(low, place - step, place + step), low | (place + step < count)

    def far(self, step):
        place, count = self.place, self.count
        return place + step, (step > 0) & (place >= step) & (place + step < count)

    def finish(self, which, out):
        place, count = self.place, self.count
        part, landed = self.summed[which]

        @pl.loop(0, CHUNKS)
        def _(block):
            rows = rows_of(block, part.shape[1])
            out[rows] = part[place, rows].astype(jnp.float32)
            for way in range(2):

                @pl.when(place > 0 if way == 0 else place < count - 1)
                def _():
                    view = self.wait_sum(which, way, place, block)
                    out[rows] += view[...].astype(jnp.float32)

    def drain(self):
        place, count = self.place, self.count

        @pl.loop(0, count)
        def _(item):
            for way in range(2):
                passed = item <= place if way == 0 else item >= place

                @pl.when(passed & self.can(way))
                def _():
                    for which in range(len(self.gathered)):
                        self.item_copy(which, way, item).wait_send()

                further = item > place if way == 0 else item < place

                @pl.when(further)
                def _():
                    @pl.loop(0, CHUNKS)
                    def _(block):
                        for which in range(len(self.summed)):
                            self.sum_copy(which, way, item, block).wait_send()


def dot(left, right):
    return jnp.dot(left, right, preferred_element_type=jnp.float32)


def dot_rt(left, right):
    return lax.dot_general(
        left, right, (((1,), (1,)), ((), ())), preferred_element_type=jnp.float32
    )


def dot_lt(left, right):
    return lax.dot_general(
        left, right, (((0,), (0,)), ((), ())), preferred_element_type=jnp.float32
    )


def cut(total, most):
    size = max(s for s in range(128, most + 1, 128) if total % s == 0)
    return size, total // size


def span(index, size):
    return pl.ds(pl.multiple_of(index * size, size), size)


def feed_kernel(
    count,
    mod_ref,
    grad_ref,
    expand_hbm,
    down_hbm,
    feed_out,
    back_out,
    weight_out,
    expand,
    down,
    mod_all,
    grad_all,
    hidden,
    slopes,
    feed_part,
    back_part,
    feed_land,
    back_land,
    total,
    load_sem,
    ag_send,
    ag_recv,
    rs_send,
    rs_recv,
):
    line = Line(
        count,
        [(mod_ref, mod_all), (grad_ref, grad_all)],
        [(back_part, back_land), (feed_part, feed_land)],
        (ag_send, ag_recv),
        (rs_send, rs_recv),
    )
    width, units = expand.shape[1], expand.shape[2]
    loads = (
        pltpu.make_async_copy(expand_hbm, expand, load_sem.at[0]),
        pltpu.make_async_copy(down_hbm, down, load_sem.at[1]),
    )
    for load in loads:
        load.start()
    line.barrier()
    line.start_own()
    mod_all[line.place] = mod_ref[...]
    grad_all[line.place] = grad_ref[...]
    total[...] = jnp.zeros_like(total)
    for load in loads:
        load.wait()
    unit_size, unit_count = cut(units, 256)
    wide_size, wide_count = cut(width, 384)
    tall_size, tall_count = cut(width, 128)

    def compute(item):
        @pl.loop(0, unit_count)
        def _(index):
            cols = span(index, unit_size)
            mod = mod_all[item]
            gate = dot(mod, expand[0, :, cols])
            upper = dot(mod, expand[1, :, cols])
            back = dot_rt(grad_all[item], down[cols, :])
            sigma = jax.nn.sigmoid(gate)
            active = gate * sigma
            hidden[item, :, cols] = (active * upper).astype(jnp.bfloat16)
            slopes[0, item, :, cols] = (
                back * upper * (sigma * (1.0 + gate * (1.0 - sigma)))
            ).astype(jnp.bfloat16)
            slopes[1, item, :, cols] = (back * active).astype(jnp.bfloat16)

        @pl.loop(0, wide_count)
        def _(index):
            cols = span(index, wide_size)
            back_part[item, :, cols] = (
                dot_rt(slopes[0, item], expand[0, cols, :])
                + dot_rt(slopes[1, item], expand[1, cols, :])
            ).astype(jnp.bfloat16)
            feed_part[item, :, cols] = dot(hidden[item], down[:, cols]).astype(jnp.bfloat16)

    def weigh(item):
        @pl.loop(0, tall_count)
        def _(index):
            rows = span(index, tall_size)
            mod = mod_all[item, :, rows]
            total[0, rows, :] += dot_lt(mod, slopes[0, item])
            total[1, rows, :] += dot_lt(mod, slopes[1, item])
            total[2, rows, :] += dot_lt(grad_all[item, :, rows], hidden[item])

    @pl.loop(0, count)
    def _(step):
        @pl.when(step > 0)
        def _():
            for item, valid in line.items(step - 1):

                @pl.when(valid)
                def _():
                    weigh(item)

            line.receive(step)

        for item, valid in line.items(step):

            @pl.when(valid)
            def _():
                compute(item)

        @pl.when(step > 0)
        def _():
            line.first_sums(step)
            line.relay_sums(step)

    for item, valid in line.items(count - 1):

        @pl.when(valid)
        def _():
            weigh(item)

    weight_out[...] = total[...].astype(jnp.bfloat16)
    line.finish(0, back_out)
    line.finish(1, feed_out)
    line.drain()


def feed_pass(mod_two, branch_grad, expand_weight, down_weight):
    count = lax.axis_size("tensor")
    length, width = mod_two.shape
    units = down_weight.shape[0]
    expand = jnp.transpose(expand_weight, (1, 0, 2))
    vmem, any_space = pl.BlockSpec(memory_space=pltpu.VMEM), pl.BlockSpec(memory_space=pl.ANY)
    low = jnp.bfloat16
    item = (length, width)
    return pl.pallas_call(
        functools.partial(feed_kernel, count),
        out_shape=(
            jax.ShapeDtypeStruct(item, jnp.float32),
            jax.ShapeDtypeStruct(item, jnp.float32),
            jax.ShapeDtypeStruct((3, width, units), low),
        ),
        in_specs=[vmem, vmem, any_space, any_space],
        out_specs=(vmem, vmem, vmem),
        scratch_shapes=[
            pltpu.VMEM((2, width, units), low),
            pltpu.VMEM((units, width), low),
            pltpu.VMEM((count, *item), low),
            pltpu.VMEM((count, *item), low),
            pltpu.VMEM((count, length, units), low),
            pltpu.VMEM((2, count, length, units), low),
            pltpu.VMEM((count, *item), low),
            pltpu.VMEM((count, *item), low),
            pltpu.VMEM((count + 1, *item), low),
            pltpu.VMEM((count + 1, *item), low),
            pltpu.VMEM((3, width, units), jnp.float32),
            pltpu.SemaphoreType.DMA((2,)),
            pltpu.SemaphoreType.DMA((2, 2, count)),
            pltpu.SemaphoreType.DMA((2, 2, count)),
            pltpu.SemaphoreType.DMA((2, 2, count, CHUNKS)),
            pltpu.SemaphoreType.DMA((2, 2, count, CHUNKS)),
        ],
        compiler_params=pltpu.CompilerParams(
            collective_id=1, has_side_effects=True, vmem_limit_bytes=64000000
        ),
        name="feed_pass",
    )(mod_two, branch_grad, expand, down_weight)


def swap_kernel(jobs, total, *refs):
    n = len(jobs)
    ins, outs = refs[:n], refs[n + total : 2 * n + total]
    sems = refs[2 * n + 2 * total :]
    places = [lax.axis_index(axis) for axis, _, _ in jobs]
    hello = pltpu.get_barrier_semaphore()
    axes = []
    for axis, count, _ in jobs:
        if (axis, count) not in axes:
            axes.append((axis, count))
    if total:
        axes = [("dp", lax.axis_size("dp")), ("tensor", lax.axis_size("tensor"))]
    for axis, count in axes:
        here = lax.axis_index(axis)

        @pl.loop(1, count)
        def _(offset):
            peer = lax.rem(here + offset, count)
            pl.semaphore_signal(hello, inc=1, device_id={axis: peer})

    pl.semaphore_wait(hello, sum(count - 1 for _, count in axes))

    def copy(source, target, send, recv, axis, peer, slot):
        return pltpu.make_async_remote_copy(
            src_ref=source,
            dst_ref=target.at[slot],
            send_sem=send.at[peer],
            recv_sem=recv.at[slot],
            device_id={axis: peer},
        )

    def start(source, target, send, recv, axis, count, split):
        here = lax.axis_index(axis)

        @pl.loop(1, count)
        def _(offset):
            peer = lax.rem(here + offset, count)
            piece = source.at[peer] if split else source
            copy(piece, target, send, recv, axis, peer, here).start()

        target[here] = source[here] if split else source[...]

    def finish(source, target, send, recv, axis, count, split):
        here = lax.axis_index(axis)

        @pl.loop(1, count)
        def _(offset):
            peer = lax.rem(here + offset, count)
            piece = source.at[peer] if split else source
            step = copy(piece, target, send, recv, axis, peer, peer)
            step.wait_recv()
            step.wait_send()

    work = []
    for index, (axis, count, split) in enumerate(jobs):
        work.append((ins[index], outs[index], sems[2 * index], sems[2 * index + 1], axis, count, split))
    if total:
        source, result = refs[n], refs[2 * n + total]
        one, two, middle, s1, r1, s2, r2 = sems[2 * n :]
        wide, deep = lax.axis_size("dp"), lax.axis_size("tensor")
        first = (source, one, s1, r1, "dp", wide, False)
        start(*first)
    for job in work:
        start(*job)
    if total:
        finish(*first)
        middle[...] = one[0]

        @pl.loop(1, wide)
        def _(index):
            middle[...] += one[index]

        second = (middle, two, s2, r2, "tensor", deep, False)
        start(*second)
    for job in work:
        finish(*job)
    if total:
        finish(*second)
        result[...] = two[0]

        @pl.loop(1, deep)
        def _(index):
            result[...] += two[index]


def swap(name, number, jobs, total=None):
    vmem = pl.BlockSpec(memory_space=pltpu.VMEM)
    plan, arrays, shapes, scratch = [], [], [], []
    for array, axis, split in jobs:
        count = lax.axis_size(axis)
        plan.append((axis, count, split))
        arrays.append(array)
        piece = array.shape[1:] if split else array.shape
        shapes.append(jax.ShapeDtypeStruct((count, *piece), array.dtype))
        scratch += [pltpu.SemaphoreType.DMA((count,)), pltpu.SemaphoreType.DMA((count,))]
    if total is not None:
        wide, deep = lax.axis_size("dp"), lax.axis_size("tensor")
        arrays.append(total)
        shapes.append(jax.ShapeDtypeStruct(total.shape, total.dtype))
        scratch += [
            pltpu.VMEM((wide, *total.shape), total.dtype),
            pltpu.VMEM((deep, *total.shape), total.dtype),
            pltpu.VMEM(total.shape, total.dtype),
        ]
        for count in (wide, wide, deep, deep):
            scratch.append(pltpu.SemaphoreType.DMA((count,)))
    return pl.pallas_call(
        functools.partial(swap_kernel, tuple(plan), int(total is not None)),
        out_shape=tuple(shapes),
        in_specs=[vmem] * len(arrays),
        out_specs=tuple([vmem] * len(shapes)),
        scratch_shapes=scratch,
        compiler_params=pltpu.CompilerParams(collective_id=number, has_side_effects=True),
        name=name,
    )(*arrays)


LANES = 128
HEAD_UNROLL = 2


def turn(value, tables):
    return (
        value * tables[0]
        + pltpu.roll(value, LANES - HD // 4, 1) * tables[1]
        + pltpu.roll(value, HD // 4, 1) * tables[2]
    )


def turn_back(grad, tables):
    return (
        grad * tables[0]
        + pltpu.roll(grad * tables[1], HD // 4, 1)
        + pltpu.roll(grad * tables[2], LANES - HD // 4, 1)
    )


def turn_tables(length):
    quarter = HD // 4
    lane = jnp.arange(LANES)
    rates = 10000.0 ** (-(lane % quarter).astype(jnp.float32) / quarter)
    positions = jnp.arange(length)[:, None]
    place = jnp.where(lane < 2 * quarter, positions // GRID, positions % GRID)
    angle = place.astype(jnp.float32) * rates
    real = lane < HD
    early = (lane // quarter) % 2 == 0
    cosine = jnp.where(real, jnp.cos(angle), 0.0)
    sine = jnp.sin(angle)
    return jnp.stack(
        [
            cosine,
            jnp.where(real & early, -sine, 0.0),
            jnp.where(real & ~early, sine, 0.0),
        ]
    )


def unit_norm(raw):
    inverse = lax.rsqrt(jnp.sum(raw * raw, axis=-1, keepdims=True) * (1.0 / HD) + EPS)
    return raw * inverse, inverse


def project(mod, weight, raw):
    @pl.loop(0, weight.shape[0])
    def _(index):
        raw[index] = dot(mod, weight[index])


def soft(queries, keys):
    grown = jnp.exp2(dot_rt(queries, keys) * (HD ** (-0.5) / math.log(2.0)))
    return grown * (1.0 / jnp.sum(grown, axis=-1, keepdims=True))


def attend_kernel(
    count,
    mod_ref,
    tables_ref,
    gains_ref,
    weight_hbm,
    last_hbm,
    branch_out,
    mod_out,
    weight,
    last,
    mod_all,
    raw,
    mixed,
    part,
    land,
    load_sem,
    ag_send,
    ag_recv,
    rs_send,
    rs_recv,
):
    line = Line(count, [(mod_ref, mod_all)], [(part, land)], (ag_send, ag_recv), (rs_send, rs_recv))
    loads = (
        pltpu.make_async_copy(weight_hbm, weight, load_sem.at[0]),
        pltpu.make_async_copy(last_hbm, last, load_sem.at[1]),
    )
    for load in loads:
        load.start()
    line.barrier()
    line.start_own()
    mod_all[line.place] = mod_ref[...]
    for load in loads:
        load.wait()
    heads = last.shape[0] // LANES
    wide_size, wide_count = cut(last.shape[1], 384)

    def compute(item):
        project(mod_all[item], weight, raw)
        tables = (tables_ref[0], tables_ref[1], tables_ref[2])

        @pl.loop(0, heads, unroll=HEAD_UNROLL)
        def _(head):
            lanes = span(head, LANES)
            queries = turn(unit_norm(raw[0, :, lanes])[0] * gains_ref[0:1, :], tables)
            keys = turn(unit_norm(raw[1, :, lanes])[0] * gains_ref[1:2, :], tables)
            probs = soft(queries.astype(jnp.bfloat16), keys.astype(jnp.bfloat16))
            values = raw[2, :, lanes].astype(jnp.bfloat16)
            mixed[:, lanes] = dot(probs.astype(jnp.bfloat16), values).astype(jnp.bfloat16)

        @pl.loop(0, wide_count)
        def _(index):
            cols = span(index, wide_size)
            part[item, :, cols] = dot(mixed[...], last[:, cols]).astype(jnp.bfloat16)

    @pl.loop(0, count)
    def _(step):
        late, owed = line.far(step - 1)
        item, valid = line.near(step)

        @pl.when(step > 0)
        def _():
            line.receive(step)

            @pl.when(owed)
            def _():
                compute(late)

        @pl.when(valid)
        def _():
            compute(item)

        @pl.when(step > 0)
        def _():
            line.first_sums(step)
            line.relay_sums(step)

    mod_out[...] = mod_all[...]
    line.finish(0, branch_out)
    line.drain()


def block_copy(array, target, slot, block, size, send, recv, peer):
    rows = pl.ds(pl.multiple_of(block * size, size), size)
    source = array.at[rows] if len(array.shape) == 2 else array.at[:, rows]
    return pltpu.make_async_remote_copy(
        src_ref=source,
        dst_ref=target.at[slot],
        send_sem=send,
        recv_sem=recv,
        device_id={"dp": peer},
    )


def attend_back_kernel(
    count,
    wide,
    grad_ref,
    mod_all,
    tables_ref,
    gains_ref,
    narrow_ref,
    weight_hbm,
    last_hbm,
    *rest,
):
    if wide:
        feed_hbm, back_out, weight_out, gain_out, feed_out, *rest = rest
    else:
        back_out, weight_out, gain_out, *rest = rest
    (
        weight,
        last,
        grad_all,
        raw,
        mixed,
        mixed_grad,
        raw_grad,
        kept,
        kept_mixed,
        part,
        land,
        total,
        load_sem,
        ag_send,
        ag_recv,
        rs_send,
        rs_recv,
        *rest,
    ) = rest
    line = Line(count, [(grad_ref, grad_all)], [(part, land)], (ag_send, ag_recv), (rs_send, rs_recv))
    loads = (
        pltpu.make_async_copy(weight_hbm, weight, load_sem.at[0]),
        pltpu.make_async_copy(last_hbm, last, load_sem.at[1]),
    )
    for load in loads:
        load.start()
    line.barrier(wide or 1)
    line.start_own()
    width = last.shape[1]
    here = lax.axis_index("dp")
    if wide:
        feed_land, staged, pair_land, quad_land, fs, fr, ps, pr, qs, qr = rest
        size = width // wide
        half = wide // 2
        parity, seat = lax.rem(here, 2), here // 2
        partner = here + 1 - 2 * parity

        def feed_copy(peer, slot):
            return block_copy(feed_hbm, feed_land, slot, peer, size, fs.at[peer], fr.at[slot], peer)

        def pair_copy(index):
            block = 2 * index + 1 - parity
            return block_copy(
                staged, pair_land, index, block, size, ps.at[index], pr.at[index], partner
            )

        def quad_copy(index, slot):
            block = 2 * index + parity
            return block_copy(
                staged, quad_land, slot, block, size, qs.at[index], qr.at[slot], block
            )

        @pl.loop(1, wide)
        def _(offset):
            peer = lax.rem(here + offset, wide)
            feed_copy(peer, here).start()

    grad_all[line.place] = grad_ref[...]
    total[...] = jnp.zeros_like(total)
    gain_out[...] = jnp.zeros_like(gain_out)
    for load in loads:
        load.wait()
    inner = last.shape[0]
    heads = inner // LANES
    scale = HD ** (-0.5)
    wide_size, wide_count = cut(width, 384)
    inner_size, inner_count = cut(inner, 256)
    tall_size, tall_count = cut(width, 128)
    first_width = kept.shape[2]

    def compute(item):
        project(mod_all[item], weight, raw)
        tables = (tables_ref[0], tables_ref[1], tables_ref[2])

        @pl.loop(0, inner_count)
        def _(index):
            cols = span(index, inner_size)
            mixed_grad[:, cols] = dot_rt(grad_all[item], last[cols, :]).astype(jnp.bfloat16)

        @pl.loop(0, heads, unroll=HEAD_UNROLL)
        def _(head):
            lanes = span(head, LANES)
            query_norm, query_inverse = unit_norm(raw[0, :, lanes])
            key_norm, key_inverse = unit_norm(raw[1, :, lanes])
            values = raw[2, :, lanes].astype(jnp.bfloat16)
            queries = turn(query_norm * gains_ref[0:1, :], tables).astype(jnp.bfloat16)
            keys = turn(key_norm * gains_ref[1:2, :], tables).astype(jnp.bfloat16)
            probs = soft(queries, keys)
            probs_low = probs.astype(jnp.bfloat16)
            mixed[:, lanes] = dot(probs_low, values).astype(jnp.bfloat16)
            grad = mixed_grad[:, lanes]
            prob_grad = dot_rt(grad, values)
            score_grad = (
                probs * (prob_grad - jnp.sum(probs * prob_grad, axis=-1, keepdims=True))
            ).astype(jnp.bfloat16)

            def back(which, value_grad, norm, inverse):
                turned = turn_back(value_grad, tables)
                gained = turned * norm
                gain_out[which] += jnp.sum(gained.reshape(-1, 8, LANES), axis=0)
                scaled = turned * gains_ref[which : which + 1, :]
                mean = jnp.sum(scaled * norm, axis=-1, keepdims=True) * (1.0 / HD)
                raw_grad[which, :, lanes] = (inverse * (scaled - norm * mean)).astype(
                    jnp.bfloat16
                )

            back(0, dot(score_grad, keys) * scale, query_norm, query_inverse)
            back(1, dot_lt(score_grad, queries) * scale, key_norm, key_inverse)
            raw_grad[2, :, lanes] = dot_lt(probs_low, grad).astype(jnp.bfloat16)

        @pl.loop(0, wide_count)
        def _(index):
            cols = span(index, wide_size)
            sums = dot_rt(raw_grad[0], weight[0, cols, :])
            sums += dot_rt(raw_grad[1], weight[1, cols, :])
            sums += dot_rt(raw_grad[2], weight[2, cols, :])
            part[item, :, cols] = sums.astype(jnp.bfloat16)

    def keep(item):
        one = dot(raw_grad[0], narrow_ref[0])
        two = dot(raw_grad[1], narrow_ref[1])
        three = dot(raw_grad[2], narrow_ref[2])
        side = one.shape[1] - LANES
        low = jnp.bfloat16
        kept[item, :, :side] = one[:, :side].astype(low)
        kept[item, :, side : side + LANES] = (one[:, side:] + two[:, :LANES]).astype(low)
        kept[item, :, side + LANES : 2 * side] = two[:, LANES:side].astype(low)
        kept[item, :, 2 * side : 2 * side + LANES] = (two[:, side:] + three[:, :LANES]).astype(low)
        kept[item, :, 2 * side + LANES :] = three[:, LANES:].astype(low)
        kept_mixed[item] = dot(mixed[...], narrow_ref[0]).astype(low)

    def weigh(item):
        @pl.loop(0, tall_count)
        def _(index):
            rows = span(index, tall_size)
            total[rows, :first_width] += dot_lt(mod_all[item, :, rows], kept[item])
            total[rows, first_width:] += dot_lt(grad_all[item, :, rows], kept_mixed[item])

    @pl.loop(0, count)
    def _(step):
        late, owed = line.far(step - 1)
        item, valid = line.near(step)

        @pl.when(step > 0)
        def _():
            older, kept_older = line.far(step - 2)
            old, kept_old = line.near(step - 1)

            @pl.when((step > 1) & kept_older)
            def _():
                weigh(older)

            @pl.when(kept_old)
            def _():
                weigh(old)

            line.receive(step)

            @pl.when(owed)
            def _():
                compute(late)
                keep(late)

        @pl.when(valid)
        def _():
            compute(item)

            @pl.when(step > 0)
            def _():
                line.first_sums(step)

            keep(item)

        @pl.when(step == count - 1)
        def _():
            @pl.when(valid)
            def _():
                weigh(item)

            if wide:
                staged[...] = total[...].astype(jnp.bfloat16)

                @pl.loop(0, half)
                def _(index):
                    pair_copy(index).start()

        @pl.when(step > 0)
        def _():
            line.relay_sums(step)

    if wide:

        @pl.loop(0, half)
        def _(index):
            pair_copy(index).wait_send()
            pair_copy(index).wait_recv()
            rows = pl.ds(pl.multiple_of((2 * index + parity) * size, size), size)
            staged[rows] = (
                staged[rows].astype(jnp.float32) + pair_land[index].astype(jnp.float32)
            ).astype(jnp.bfloat16)

        @pl.loop(1, half)
        def _(offset):
            index = lax.rem(seat + offset, half)
            quad_copy(index, seat).start()

    line.finish(0, back_out)
    line.drain()
    if wide:
        rows = pl.ds(pl.multiple_of(here * size, size), size)
        own = pltpu.make_async_copy(feed_hbm.at[:, rows], feed_land.at[here], load_sem.at[0])
        own.start()

        @pl.loop(1, wide)
        def _(offset):
            peer = lax.rem(here + offset, wide)
            feed_copy(peer, here).wait_send()
            feed_copy(here, peer).wait_recv()

        own.wait()
        for which in range(feed_out.shape[0]):
            feed_out[which] = feed_land[0, which].astype(jnp.float32)

            @pl.loop(1, wide)
            def _(index):
                feed_out[which] += feed_land[index, which].astype(jnp.float32)

        weight_out[...] = staged[rows].astype(jnp.float32)

        @pl.loop(1, half)
        def _(offset):
            index = lax.rem(seat + offset, half)
            quad_copy(index, seat).wait_send()
            quad_copy(seat, index).wait_recv()
            weight_out[...] += quad_land[index].astype(jnp.float32)

    else:
        weight_out[...] = total[...].astype(jnp.bfloat16)


def attend_arrays(project_weight, output_weight, query_gain, key_gain, length):
    inner = project_weight.shape[2]
    heads = inner // HD
    low = jnp.bfloat16
    spot = jnp.arange(heads * LANES)
    real = spot % LANES < HD
    column = spot // LANES * HD + spot % LANES
    spread = (real[None] & (column[None] == jnp.arange(inner)[:, None])).astype(low)
    window = -(-inner // LANES) * LANES
    narrow = jnp.stack(
        [
            real[:, None]
            & (column[:, None] + index * (inner % LANES) == jnp.arange(window)[None, :])
            for index in range(3)
        ]
    ).astype(low)
    weight = jnp.einsum("dke,eh->kdh", project_weight, spread, preferred_element_type=low)
    last = jnp.einsum("ed,eh->hd", output_weight, spread, preferred_element_type=low)
    pad = LANES - HD
    gains = jnp.pad(jnp.stack([query_gain, key_gain]).astype(jnp.float32), ((0, 6), (0, pad)))
    return turn_tables(length), gains, narrow, weight, last


def line_sems(count, gathers, sums):
    return [
        pltpu.SemaphoreType.DMA((2,)),
        pltpu.SemaphoreType.DMA((gathers, 2, count)),
        pltpu.SemaphoreType.DMA((gathers, 2, count)),
        pltpu.SemaphoreType.DMA((sums, 2, count, CHUNKS)),
        pltpu.SemaphoreType.DMA((sums, 2, count, CHUNKS)),
    ]


def attend_pass(mod_in, arrays):
    count = lax.axis_size("tensor")
    tables, gains, _, weight, last = arrays
    item = mod_in.shape
    inner = last.shape[0]
    vmem, any_space = pl.BlockSpec(memory_space=pltpu.VMEM), pl.BlockSpec(memory_space=pl.ANY)
    low = jnp.bfloat16
    return pl.pallas_call(
        functools.partial(attend_kernel, count),
        out_shape=(
            jax.ShapeDtypeStruct(item, jnp.float32),
            jax.ShapeDtypeStruct((count, *item), low),
        ),
        in_specs=[vmem, vmem, vmem, any_space, any_space],
        out_specs=(vmem, vmem),
        scratch_shapes=[
            pltpu.VMEM(weight.shape, low),
            pltpu.VMEM(last.shape, low),
            pltpu.VMEM((count, *item), low),
            pltpu.VMEM((3, item[0], inner), jnp.float32),
            pltpu.VMEM((item[0], inner), low),
            pltpu.VMEM((count, *item), low),
            pltpu.VMEM((count + 1, *item), low),
            *line_sems(count, 1, 1),
        ],
        compiler_params=pltpu.CompilerParams(
            collective_id=6, has_side_effects=True, vmem_limit_bytes=60000000
        ),
        name="attend_pass",
    )(mod_in, tables, gains, weight, last)


def attend_back_pass(attend_grad, mod_all, arrays, feed_weights):
    count, wide = lax.axis_size("tensor"), lax.axis_size("dp")
    tables, gains, narrow, weight, last = arrays
    item = attend_grad.shape
    length, width = item
    inner = last.shape[0]
    vmem, any_space = pl.BlockSpec(memory_space=pltpu.VMEM), pl.BlockSpec(memory_space=pl.ANY)
    low, high = jnp.bfloat16, jnp.float32
    window = narrow.shape[2]
    first_width = 3 * window - 2 * LANES
    columns = first_width + window
    if width % (16 * wide):
        wide = 0
    size = width // wide if wide else width
    outs = [
        jax.ShapeDtypeStruct(item, high),
        jax.ShapeDtypeStruct((size, columns), high if wide else low),
        jax.ShapeDtypeStruct((2, 8, LANES), high),
    ]
    scratch = [
        pltpu.VMEM(weight.shape, low),
        pltpu.VMEM(last.shape, low),
        pltpu.VMEM((count, *item), low),
        pltpu.VMEM((3, length, inner), high),
        pltpu.VMEM((length, inner), low),
        pltpu.VMEM((length, inner), low),
        pltpu.VMEM((3, length, inner), low),
        pltpu.VMEM((count, length, first_width), low),
        pltpu.VMEM((count, length, window), low),
        pltpu.VMEM((count, *item), low),
        pltpu.VMEM((count + 1, *item), low),
        pltpu.VMEM((width, columns), high),
        *line_sems(count, 1, 1),
    ]
    ins = [attend_grad, mod_all, tables, gains, narrow, weight, last]
    specs = [vmem, vmem, vmem, vmem, vmem, any_space, any_space]
    if wide:
        ins.append(feed_weights)
        specs.append(any_space)
        kinds, _, units = feed_weights.shape
        outs.append(jax.ShapeDtypeStruct((kinds, size, units), high))
        half = wide // 2
        scratch += [
            pltpu.VMEM((wide, kinds, size, units), low),
            pltpu.VMEM((width, columns), low),
            pltpu.VMEM((half, size, columns), low),
            pltpu.VMEM((half, size, columns), low),
        ]
        for number in (wide, wide, half, half, half, half):
            scratch.append(pltpu.SemaphoreType.DMA((number,)))
    results = pl.pallas_call(
        functools.partial(attend_back_kernel, count, wide),
        out_shape=tuple(outs),
        in_specs=specs,
        out_specs=tuple([vmem] * len(outs)),
        scratch_shapes=scratch,
        compiler_params=pltpu.CompilerParams(
            collective_id=7, has_side_effects=True, vmem_limit_bytes=66000000
        ),
        name="attend_back_pass",
    )(*ins)
    if wide:
        return results

    def scatter(value, axis):
        return lax.psum_scatter(value, "dp", scatter_dimension=axis, tiled=True).astype(high)

    back, weights, gain_parts = results
    return back, scatter(weights, 0), gain_parts, scatter(feed_weights, 1)


def tail_kernel(
    grads_ref,
    small_ref,
    weight_ref,
    slope_ref,
    forward_ref,
    feat_ref,
    label_ref,
    rows_ref,
    pick_ref,
    small_out,
    modulate_out,
    embed_out,
    class_out,
    time_out,
    bias_out,
    grads_land,
    grads_mine,
    grads_land_dp,
    small_one,
    small_mid,
    small_two,
    part,
    part_land,
    cond,
    cond_land,
    forward_land,
    feat_land,
    label_land,
    grads_all,
    cond_all,
    forward_all,
    feat_all,
    label_all,
    *sems,
):
    deep, wide = part_land.shape[0], cond_land.shape[0]
    items = cond.shape[0]
    axes = (("dp", wide), ("tensor", deep))
    hello = pltpu.get_barrier_semaphore()
    for axis, count in axes:
        here = lax.axis_index(axis)

        @pl.loop(1, count)
        def _(offset):
            pl.semaphore_signal(
                hello, inc=1, device_id={axis: lax.rem(here + offset, count)}
            )

    pl.semaphore_wait(hello, wide + deep - 2)
    low = jnp.bfloat16

    def exchange(number, axis, source, target, split=False):
        count = target.shape[0]
        here = lax.axis_index(axis)
        send, recv = sems[2 * number], sems[2 * number + 1]

        def copy(peer, slot):
            return pltpu.make_async_remote_copy(
                src_ref=source.at[peer] if split else source,
                dst_ref=target.at[slot],
                send_sem=send.at[peer],
                recv_sem=recv.at[slot],
                device_id={axis: peer},
            )

        def start():
            @pl.loop(1, count)
            def _(offset):
                copy(lax.rem(here + offset, count), here).start()

            target[here] = source[here] if split else source[...]

        def finish():
            @pl.loop(1, count)
            def _(offset):
                peer = lax.rem(here + offset, count)
                copy(peer, here).wait_send()
                copy(peer, peer).wait_recv()

        return start, finish

    start_grads, finish_grads = exchange(0, "tensor", grads_ref, grads_land, True)
    start_small, finish_small = exchange(1, "dp", small_ref, small_one)
    start_sums, finish_sums = exchange(2, "tensor", small_mid, small_two)
    start_part, finish_part = exchange(3, "tensor", part, part_land)
    start_mine, finish_mine = exchange(4, "dp", grads_mine, grads_land_dp)
    start_cond, finish_cond = exchange(5, "dp", cond, cond_land)
    start_forward, finish_forward = exchange(6, "dp", forward_ref, forward_land, True)
    start_feat, finish_feat = exchange(7, "dp", feat_ref, feat_land)
    start_label, finish_label = exchange(8, "dp", label_ref, label_land)

    start_grads()
    start_small()
    start_forward()
    start_feat()
    start_label()
    finish_grads()
    kinds = grads_mine.shape[0]
    for item in range(items):
        piece = grads_land[item].astype(jnp.float32)
        for kind in range(kinds):
            grads_all[kind, item : item + 1, :] = piece[kind : kind + 1, :]
    total = jnp.zeros(part.shape, jnp.float32)
    for kind in range(kinds):
        mine = grads_all[kind, :items, :].astype(low)
        grads_mine[kind] = mine
        total += dot_rt(mine, weight_ref[kind])
    part[...] = total
    start_part()
    start_mine()
    finish_small()
    small_mid[...] = small_one[0]

    @pl.loop(1, wide)
    def _(index):
        small_mid[...] += small_one[index]

    start_sums()
    finish_part()
    total = part_land[0]
    for index in range(1, deep):
        total += part_land[index]
    cond[...] = (total * slope_ref[...]).astype(low)
    start_cond()
    finish_forward()
    finish_feat()
    finish_label()
    for index in range(wide):
        rows = pl.ds(index * items, items)
        for kind in range(forward_all.shape[0]):
            forward_all[kind, rows, :] = forward_land[index, kind]
        feat_all[rows, :] = feat_land[index]
        label_all[rows, :] = label_land[index]
    finish_mine()
    for index in range(wide):
        rows = pl.ds(index * items, items)
        for kind in range(kinds):
            grads_all[kind, rows, :] = grads_land_dp[index, kind].astype(jnp.float32)
    active = forward_all[0].astype(low)
    for kind in range(kinds):
        modulate_out[kind] = dot_lt(active, grads_all[kind].astype(low))
    finish_sums()
    small_out[...] = small_two[0]

    @pl.loop(1, deep)
    def _(index):
        small_out[...] += small_two[index]

    finish_cond()
    for index in range(wide):
        cond_all[pl.ds(index * items, items), :] = cond_land[index].astype(jnp.float32)
    every = cond_all[...].astype(low)
    embed_out[...] = dot_lt(forward_all[1].astype(low), every)
    picked = dot(every, pick_ref[...]).astype(low)
    classes = class_out.shape[0]
    label = jnp.broadcast_to(label_all[:, 0:1], (label_all.shape[0], classes))
    lane = lax.broadcasted_iota(jnp.int32, label.shape, 1)
    hot = jnp.where(label == lane, 1.0, 0.0).astype(low)
    class_out[...] = dot_lt(hot, picked)
    earlier = (dot_rt(every, rows_ref[...]) * forward_all[2]).astype(low)
    time_out[...] = dot_lt(feat_all[...].astype(low), earlier)
    bias_out[0:1, :] = jnp.sum(picked.astype(jnp.float32), axis=0, keepdims=True)
    bias_out[1:2, :] = jnp.sum(earlier.astype(jnp.float32), axis=0, keepdims=True)


def tail_pass(grads, small, weight, slope, forward, feat, label, rows, pick, classes):
    deep, kinds, slab = grads.shape
    wide, parts, items, share = forward.shape
    width = weight.shape[1]
    batch = wide * items
    freq = feat.shape[1]
    low, high = jnp.bfloat16, jnp.float32
    vmem = pl.BlockSpec(memory_space=pltpu.VMEM)
    shapes = (
        (small.shape, high),
        ((kinds, share, slab), high),
        ((share, width), high),
        ((classes, share), high),
        ((freq, share), high),
        ((2, share), high),
    )
    scratch = (
        ((deep, kinds, slab), low),
        ((kinds, items, slab), low),
        ((wide, kinds, items, slab), low),
        ((wide, *small.shape), high),
        (small.shape, high),
        ((deep, *small.shape), high),
        ((items, width), high),
        ((deep, items, width), high),
        ((items, width), low),
        ((wide, items, width), low),
        (forward.shape, high),
        ((wide, items, freq), high),
        ((wide, items, LANES), jnp.int32),
        ((kinds, batch, slab), high),
        ((batch, width), high),
        ((parts, batch, share), high),
        ((batch, freq), high),
        ((batch, LANES), jnp.int32),
    )
    sems = []
    for number in (deep, wide, deep, deep, wide, wide, wide, wide, wide):
        sems += [pltpu.SemaphoreType.DMA((number,))] * 2
    return pl.pallas_call(
        tail_kernel,
        out_shape=tuple(jax.ShapeDtypeStruct(*shape) for shape in shapes),
        in_specs=[vmem] * 9,
        out_specs=tuple([vmem] * 6),
        scratch_shapes=[pltpu.VMEM(*shape) for shape in scratch] + sems,
        compiler_params=pltpu.CompilerParams(
            collective_id=3, has_side_effects=True, vmem_limit_bytes=60000000
        ),
        name="tail_pass",
    )(grads, small, weight, slope, forward, feat, label, rows, pick)


def shards(
    tokens,
    timesteps,
    labels,
    item_counts,
    cotangent,
    project_weight,
    query_gain,
    key_gain,
    output_weight,
    output_bias,
    expand_weight,
    down_weight,
    down_bias,
    modulate_weight,
    modulate_bias,
    time_weight,
    time_bias,
    embed_weight,
    embed_bias,
    class_table,
):
    local_items, length, width = tokens.shape
    items = timesteps.shape[0]
    slab = modulate_weight.shape[2]
    heads_here = project_weight.shape[2] // HD
    scale = HD ** (-0.5)
    first_item = lax.axis_index("tensor") * local_items
    live = (first_item + jnp.arange(local_items) < item_counts[0]).astype(jnp.float32)[
        :, None, None
    ]
    index = lax.axis_index("dp")
    time_feat = time_features(timesteps).astype(jnp.bfloat16)
    pre_hidden = jnp.dot(
        time_feat, time_weight, preferred_element_type=jnp.float32
    ) + time_bias.astype(jnp.float32)
    time_hidden = jax.nn.silu(pre_hidden).astype(jnp.bfloat16)
    condition = (
        jnp.dot(time_hidden, embed_weight, preferred_element_type=jnp.float32)
        + embed_bias.astype(jnp.float32)
        + jnp.take(class_table, labels, axis=0).astype(jnp.float32)
    )
    cond_act = jax.nn.silu(condition).astype(jnp.bfloat16)
    modulation_part = (
        jnp.einsum("bd,dke->bke", cond_act, modulate_weight, preferred_element_type=jnp.float32)
        + modulate_bias.astype(jnp.float32)
    ).astype(jnp.bfloat16)
    (modulation_local,) = swap("modulation_swap", 2, [(modulation_part, "tensor", True)])
    modulation_local = jnp.transpose(modulation_local, (1, 0, 2)).reshape(1, 6, width)
    modulation_local = modulation_local.astype(jnp.float32)
    local_parts = [modulation_local[:, which][:, None, :] for which in range(6)]
    attend_shift, attend_scale, attend_gate, feed_shift, feed_scale, feed_gate = local_parts
    positions = jnp.arange(length)
    token_local = tokens.astype(jnp.float32)
    normed_local, inverse_local = layer_norm(token_local)
    mod_in = normed_local * (1.0 + attend_scale) + attend_shift
    arrays = attend_arrays(project_weight, output_weight, query_gain, key_gain, length)
    attend_total, mod_all = attend_pass(mod_in[0].astype(jnp.bfloat16), arrays)
    attend_branch = attend_total[None] + output_bias.astype(jnp.float32)
    residual = token_local + attend_gate * attend_branch
    normed_two, inverse_two = layer_norm(residual)
    mod_two = (normed_two * (1.0 + feed_scale) + feed_shift).astype(jnp.bfloat16)
    out_grad = cotangent.astype(jnp.float32) * live
    branch_grad = (out_grad * feed_gate).astype(jnp.bfloat16)
    down_bias_part = jnp.sum(branch_grad.astype(jnp.float32), axis=(0, 1))
    feed_total, mod_two_grad, feed_weights = feed_pass(
        mod_two[0], branch_grad[0], expand_weight, down_weight
    )
    feed_branch = feed_total[None] + down_bias.astype(jnp.float32)
    result = (live * (residual + feed_gate * feed_branch)).astype(jnp.bfloat16)
    mod_two_grad = mod_two_grad[None]
    residual_grad = out_grad + layer_norm_back(
        normed_two, inverse_two, mod_two_grad * (1.0 + feed_scale)
    )
    attend_grad = (residual_grad * attend_gate).astype(jnp.bfloat16)
    output_bias_part = jnp.sum(attend_grad.astype(jnp.float32), axis=(0, 1))
    mod_in_grad, attend_weights, gain_parts, feed_weights = attend_back_pass(
        attend_grad[0], mod_all, arrays, feed_weights
    )
    mod_in_grad = mod_in_grad[None]
    query_gain_part, key_gain_part = jnp.sum(gain_parts, axis=1)[:, :HD]
    tokens_grad = (
        residual_grad
        + layer_norm_back(normed_local, inverse_local, mod_in_grad * (1.0 + attend_scale))
    ).astype(jnp.bfloat16)
    modulation_grad_part = jnp.stack(
        [
            jnp.sum(mod_in_grad, axis=1),
            jnp.sum(mod_in_grad * normed_local, axis=1),
            jnp.sum(residual_grad * attend_branch, axis=1),
            jnp.sum(mod_two_grad, axis=1),
            jnp.sum(mod_two_grad * normed_two, axis=1),
            jnp.sum(out_grad * feed_branch, axis=1),
        ],
        axis=1,
    )
    modulation_grad_part = modulation_grad_part[0].astype(jnp.bfloat16)
    small = jnp.concatenate(
        [
            output_bias_part,
            down_bias_part,
            modulation_grad_part.astype(jnp.float32).reshape(-1),
            query_gain_part,
            key_gain_part,
        ]
    )
    small_size = small.shape[0]
    small = jnp.pad(small, (0, -small_size % 1024)).reshape(-1, 128)
    tensor_size, wide = width // slab, lax.axis_size("dp")
    share = width // wide

    def shares(value):
        return jnp.transpose(value.astype(jnp.float32).reshape(items, wide, share), (1, 0, 2))

    def mine(value):
        return lax.dynamic_slice_in_dim(value, index * share, share, 0)

    pick = jnp.arange(width)[:, None] == index * share + jnp.arange(share)[None, :]
    small, modulate_grad, embed_grad, class_grad, time_grad, biases = tail_pass(
        jnp.transpose(modulation_grad_part.reshape(6, tensor_size, slab), (1, 0, 2)),
        small,
        jnp.transpose(modulate_weight, (1, 0, 2)),
        silu_slope(condition),
        jnp.stack([shares(cond_act), shares(time_hidden), shares(silu_slope(pre_hidden))], axis=1),
        time_feat.astype(jnp.float32),
        jnp.broadcast_to(labels[:, None], (items, LANES)),
        mine(embed_weight),
        pick.astype(jnp.bfloat16),
        class_table.shape[0],
    )
    modulate_grad = jnp.transpose(modulate_grad, (1, 0, 2))
    embed_bias_grad, time_bias_grad = biases
    small = small.reshape(-1)
    output_bias_grad = small[:width]
    down_bias_grad = small[width : 2 * width]
    modulate_bias_grad = small[2 * width : 8 * width].reshape(6, width)
    query_gain_grad = small[8 * width : 8 * width + HD]
    key_gain_grad = small[8 * width + HD : 8 * width + 2 * HD]
    inner = heads_here * HD
    first_width = attend_weights.shape[1] - -(-inner // LANES) * LANES
    project_grad = attend_weights[:, : 3 * inner].reshape(-1, 3, inner)
    output_weight_grad = attend_weights[:, first_width : first_width + inner].T
    expand_grad = jnp.transpose(feed_weights[:2], (1, 0, 2))
    down_grad = feed_weights[2].T
    return (
        result,
        tokens_grad,
        project_grad,
        query_gain_grad,
        key_gain_grad,
        output_weight_grad,
        output_bias_grad,
        expand_grad,
        down_grad,
        down_bias_grad,
        modulate_grad,
        modulate_bias_grad,
        time_grad,
        time_bias_grad,
        embed_grad,
        embed_bias_grad,
        class_grad,
    )


def solution(mesh):
    return jax.shard_map(
        shards,
        mesh=mesh,
        in_specs=(
            P(("dp", "tensor"), None, None),
            P("dp"),
            P("dp"),
            P("dp"),
            P(("dp", "tensor"), None, None),
            P(None, None, "tensor"),
            P(),
            P(),
            P("tensor", None),
            P(),
            P(None, None, "tensor"),
            P("tensor", None),
            P(),
            P(None, None, "tensor"),
            P(None, "tensor"),
            P(),
            P(),
            P(),
            P(),
            P(),
        ),
        out_specs=(
            P(("dp", "tensor"), None, None),
            P(("dp", "tensor"), None, None),
            P("dp", None, "tensor"),
            P(),
            P(),
            P("tensor", "dp"),
            P(),
            P("dp", None, "tensor"),
            P("tensor", "dp"),
            P(),
            P("dp", None, "tensor"),
            P(),
            P(None, "dp"),
            P("dp"),
            P("dp", None),
            P("dp"),
            P(None, "dp"),
        ),
        check_vma=False,
    )
```

```python
import functools
import math

import jax
import jax.numpy as jnp
from jax import lax
from jax.experimental import pallas as pl
from jax.experimental.pallas import tpu as pltpu
from jax.sharding import PartitionSpec as P

HD = 72
FREQ = 256
GRID = 16


EPS = 1e-06


def layer_norm(value):
    center = value - jnp.mean(value, axis=-1, keepdims=True)
    inverse = lax.rsqrt(jnp.mean(center * center, axis=-1, keepdims=True) + EPS)
    return (center * inverse, inverse)


def layer_norm_back(normed, inverse, grad):
    return inverse * (
        grad
        - jnp.mean(grad, axis=-1, keepdims=True)
        - normed * jnp.mean(grad * normed, axis=-1, keepdims=True)
    )


def silu_slope(value):
    sigma = jax.nn.sigmoid(value)
    return sigma * (1.0 + value * (1.0 - sigma))


def rotate(value, positions):
    quarter = HD // 4
    rates = 10000.0 ** (-jnp.arange(quarter, dtype=jnp.float32) / quarter)
    places = ((positions // GRID).astype(jnp.float32), (positions % GRID).astype(jnp.float32))
    pieces = []
    for which_half in range(2):
        half_value = value[..., which_half * 2 * quarter : (which_half + 1) * 2 * quarter]
        angle = places[which_half][:, None] * rates[None, :]
        cosine = jnp.cos(angle)[None, :, None, :]
        sine = jnp.sin(angle)[None, :, None, :]
        first = half_value[..., :quarter]
        second = half_value[..., quarter:]
        pieces.append(first * cosine - second * sine)
        pieces.append(second * cosine + first * sine)
    return jnp.concatenate(pieces, axis=-1)


def head_prepare(raw, gain, positions):
    scaled = raw * lax.rsqrt(jnp.mean(raw * raw, axis=-1, keepdims=True) + EPS) * gain
    return rotate(scaled, positions)


def time_features(steps_in):
    half = FREQ // 2
    rates = jnp.exp(-math.log(10000.0) * jnp.arange(half, dtype=jnp.float32) / half)
    angle = steps_in.astype(jnp.float32)[:, None] * rates[None, :]
    return jnp.concatenate([jnp.cos(angle), jnp.sin(angle)], axis=-1)


CHUNKS = 8


def rows_of(block, total):
    size = total // CHUNKS
    return pl.ds(pl.multiple_of(block * size, size), size)


class Line:
    def __init__(self, count, gathered, summed, ag_sems, rs_sems):
        self.count = count
        self.place = lax.axis_index("tensor")
        self.gathered = gathered
        self.summed = summed
        self.ag_send, self.ag_recv = ag_sems
        self.rs_send, self.rs_recv = rs_sems

    def barrier(self, wide=1):
        place, count = self.place, self.count
        sem = pltpu.get_barrier_semaphore()

        @pl.when(place > 0)
        def _():
            pl.semaphore_signal(sem, inc=1, device_id={"tensor": place - 1})

        @pl.when(place < count - 1)
        def _():
            pl.semaphore_signal(sem, inc=1, device_id={"tensor": place + 1})

        peers = jnp.where(place > 0, 1, 0) + jnp.where(place < count - 1, 1, 0)
        here = lax.axis_index("dp")

        @pl.loop(1, wide)
        def _(offset):
            peer = lax.rem(here + offset, wide)
            pl.semaphore_signal(sem, inc=1, device_id={"dp": peer})

        pl.semaphore_wait(sem, peers + (wide - 1))

    def item_copy(self, which, way, item, own=False):
        mine, everyone = self.gathered[which]
        target = self.place + (1 if way == 0 else -1)
        return pltpu.make_async_remote_copy(
            src_ref=mine if own else everyone.at[item],
            dst_ref=everyone.at[item],
            send_sem=self.ag_send.at[which, way, item],
            recv_sem=self.ag_recv.at[which, way, item],
            device_id={"tensor": target},
        )

    def can(self, way):
        return self.place < self.count - 1 if way == 0 else self.place > 0

    def sum_copy(self, which, way, item, block):
        part, landed = self.summed[which]
        target = self.place + (1 if way == 0 else -1)
        slot = item
        if way == 1:
            slot = jnp.where(item == target, self.count, item)
        rows = rows_of(block, part.shape[1])
        return pltpu.make_async_remote_copy(
            src_ref=part.at[item, rows],
            dst_ref=landed.at[slot, rows],
            send_sem=self.rs_send.at[which, way, item, block],
            recv_sem=self.rs_recv.at[which, way, item, block],
            device_id={"tensor": target},
        )

    def landed_slot(self, way, item):
        return jnp.where(item == self.place, self.count, item) if way == 1 else item

    def wait_sum(self, which, way, item, block):
        part, landed = self.summed[which]
        rows = rows_of(block, part.shape[1])
        view = landed.at[self.landed_slot(way, item), rows]
        pltpu.make_async_remote_copy(
            src_ref=view,
            dst_ref=view,
            send_sem=self.rs_send.at[which, way, item, block],
            recv_sem=self.rs_recv.at[which, way, item, block],
            device_id={"tensor": self.place},
        ).wait_recv()
        return view

    def start_own(self):
        for which in range(len(self.gathered)):
            for way in range(2):

                @pl.when(self.can(way))
                def _():
                    self.item_copy(which, way, self.place, own=True).start()

    def receive(self, step):
        place, count = self.place, self.count
        for which in range(len(self.gathered)):
            for way in range(2):
                item = place - step if way == 0 else place + step

                @pl.when((item >= 0) & (item < count))
                def _():
                    self.item_copy(which, way, item).wait_recv()

                    @pl.when(self.can(way))
                    def _():
                        self.item_copy(which, way, item).start()

    def items(self, step):
        place, count = self.place, self.count
        low, high = place - step, place + step
        return ((low, (low >= 0)), (high, (high < count) & (step > 0)))

    def moves(self, step):
        place, count = self.place, self.count
        return (
            (0, step, step > place, place),
            (1, count - 1 - step, count - 1 - step < place, count - 1 - place),
        )

    def first_sums(self, step, which=0):
        @pl.loop(0, CHUNKS)
        def _(block):
            for way, item, further, hop in self.moves(step):

                @pl.when(further & (hop == 0))
                def _():
                    self.sum_copy(which, way, item, block).start()

    def relay_sums(self, step, which=0):
        part, landed = self.summed[which]

        @pl.loop(0, CHUNKS + self.count - 3)
        def _(turn):
            for distance in range(1, self.count - 1):
                block = turn - (distance - 1)
                for way, item, further, hop in self.moves(step):

                    @pl.when(further & (hop == distance) & (block >= 0) & (block < CHUNKS))
                    def _():
                        rows = rows_of(block, part.shape[1])
                        view = self.wait_sum(which, way, item, block)
                        total = part[item, rows].astype(jnp.float32) + view[...].astype(
                            jnp.float32
                        )
                        part[item, rows] = total.astype(part.dtype)
                        self.sum_copy(which, way, item, block).start()

    def each(self, first, second, body):
        @pl.loop(0, 2)
        def _(turn):
            item = jnp.where(turn == 0, first[0], second[0])
            valid = ((turn == 0) & first[1]) | ((turn == 1) & second[1])

            @pl.when(valid)
            def _():
                body(item)

    def near(self, step):
        place, count = self.place, self.count
        low = place >= step
        return jnp.where(low, place - step, place + step), low | (place + step < count)

    def far(self, step):
        place, count = self.place, self.count
        return place + step, (step > 0) & (place >= step) & (place + step < count)

    def finish(self, which, out):
        place, count = self.place, self.count
        part, landed = self.summed[which]

        @pl.loop(0, CHUNKS)
        def _(block):
            rows = rows_of(block, part.shape[1])
            out[rows] = part[place, rows].astype(jnp.float32)
            for way in range(2):

                @pl.when(place > 0 if way == 0 else place < count - 1)
                def _():
                    view = self.wait_sum(which, way, place, block)
                    out[rows] += view[...].astype(jnp.float32)

    def drain(self):
        place, count = self.place, self.count

        @pl.loop(0, count)
        def _(item):
            for way in range(2):
                passed = item <= place if way == 0 else item >= place

                @pl.when(passed & self.can(way))
                def _():
                    for which in range(len(self.gathered)):
                        self.item_copy(which, way, item).wait_send()

                further = item > place if way == 0 else item < place

                @pl.when(further)
                def _():
                    @pl.loop(0, CHUNKS)
                    def _(block):
                        for which in range(len(self.summed)):
                            self.sum_copy(which, way, item, block).wait_send()


def dot(left, right):
    return jnp.dot(left, right, preferred_element_type=jnp.float32)


def dot_rt(left, right):
    return lax.dot_general(
        left, right, (((1,), (1,)), ((), ())), preferred_element_type=jnp.float32
    )


def dot_lt(left, right):
    return lax.dot_general(
        left, right, (((0,), (0,)), ((), ())), preferred_element_type=jnp.float32
    )


def cut(total, most):
    size = max(s for s in range(128, most + 1, 128) if total % s == 0)
    return size, total // size


def span(index, size):
    return pl.ds(pl.multiple_of(index * size, size), size)


def feed_kernel(
    count,
    mod_ref,
    grad_all,
    expand_hbm,
    down_hbm,
    back_out,
    weight_hbm,
    part_hbm,
    expand,
    down,
    mod_all,
    hidden,
    slopes,
    feed_part,
    back_part,
    back_land,
    total,
    weights,
    load_sem,
    ag_send,
    ag_recv,
    rs_send,
    rs_recv,
    out_sem,
):
    line = Line(
        count, [(mod_ref, mod_all)], [(back_part, back_land)], (ag_send, ag_recv), (rs_send, rs_recv)
    )
    width, units = expand.shape[1], expand.shape[2]
    loads = (
        pltpu.make_async_copy(expand_hbm, expand, load_sem.at[0]),
        pltpu.make_async_copy(down_hbm, down, load_sem.at[1]),
    )
    for load in loads:
        load.start()
    line.barrier()
    line.start_own()
    mod_all[line.place] = mod_ref[...]
    total[...] = jnp.zeros_like(total)
    for load in loads:
        load.wait()
    unit_size, unit_count = cut(units, 256)
    wide_size, wide_count = cut(width, 384)
    tall_size, tall_count = cut(width, 128)

    def put(item):
        return pltpu.make_async_copy(feed_part.at[item], part_hbm.at[item], out_sem.at[item])

    def compute(item):
        @pl.loop(0, unit_count)
        def _(index):
            cols = span(index, unit_size)
            mod = mod_all[item]
            gate = dot(mod, expand[0, :, cols])
            upper = dot(mod, expand[1, :, cols])
            back = dot_rt(grad_all[item], down[cols, :])
            sigma = jax.nn.sigmoid(gate)
            active = gate * sigma
            hidden[item, :, cols] = (active * upper).astype(jnp.bfloat16)
            slopes[0, item, :, cols] = (
                back * upper * (sigma * (1.0 + gate * (1.0 - sigma)))
            ).astype(jnp.bfloat16)
            slopes[1, item, :, cols] = (back * active).astype(jnp.bfloat16)

        @pl.loop(0, wide_count)
        def _(index):
            cols = span(index, wide_size)
            back_part[item, :, cols] = (
                dot_rt(slopes[0, item], expand[0, cols, :])
                + dot_rt(slopes[1, item], expand[1, cols, :])
            ).astype(jnp.bfloat16)

    def spread(item):
        @pl.loop(0, wide_count)
        def _(index):
            cols = span(index, wide_size)
            feed_part[item, :, cols] = dot(hidden[item], down[:, cols]).astype(jnp.bfloat16)

        put(item).start()

        @pl.loop(0, tall_count)
        def _(index):
            rows = span(index, tall_size)
            mod = mod_all[item, :, rows]
            total[0, rows, :] += dot_lt(mod, slopes[0, item])
            total[1, rows, :] += dot_lt(mod, slopes[1, item])
            total[2, rows, :] += dot_lt(grad_all[item, :, rows], hidden[item])

    @pl.loop(0, count)
    def _(step):
        @pl.when(step > 0)
        def _():
            line.each(line.far(step - 2), line.near(step - 1), spread)
            line.receive(step)

        line.each(line.far(step - 1), line.near(step), compute)

        @pl.when(step > 0)
        def _():
            line.first_sums(step)
            line.relay_sums(step)

    line.each((0, False), line.near(count - 1), spread)
    weights[...] = total[...].astype(jnp.bfloat16)
    store = pltpu.make_async_copy(weights, weight_hbm, load_sem.at[0])
    store.start()
    line.finish(0, back_out)
    line.drain()
    store.wait()

    @pl.loop(0, count)
    def _(item):
        put(item).wait()


def feed_pass(mod_two, branch_grads, expand_weight, down_weight):
    count = lax.axis_size("tensor")
    length, width = mod_two.shape
    units = down_weight.shape[0]
    expand = jnp.transpose(expand_weight, (1, 0, 2))
    vmem, any_space = pl.BlockSpec(memory_space=pltpu.VMEM), pl.BlockSpec(memory_space=pl.ANY)
    low = jnp.bfloat16
    item = (length, width)
    return pl.pallas_call(
        functools.partial(feed_kernel, count),
        out_shape=(
            jax.ShapeDtypeStruct(item, jnp.float32),
            jax.ShapeDtypeStruct((3, width, units), low),
            jax.ShapeDtypeStruct((count, *item), low),
        ),
        in_specs=[vmem, vmem, any_space, any_space],
        out_specs=(vmem, any_space, any_space),
        scratch_shapes=[
            pltpu.VMEM((2, width, units), low),
            pltpu.VMEM((units, width), low),
            pltpu.VMEM((count, *item), low),
            pltpu.VMEM((count, length, units), low),
            pltpu.VMEM((2, count, length, units), low),
            pltpu.VMEM((count, *item), low),
            pltpu.VMEM((count, *item), low),
            pltpu.VMEM((count + 1, *item), low),
            pltpu.VMEM((3, width, units), jnp.float32),
            pltpu.VMEM((3, width, units), low),
            *line_sems(count, 1, 1),
            pltpu.SemaphoreType.DMA((count,)),
        ],
        compiler_params=pltpu.CompilerParams(
            collective_id=1, has_side_effects=True, vmem_limit_bytes=64000000
        ),
        name="feed_pass",
    )(mod_two, branch_grads, expand, down_weight)


def swap_kernel(jobs, total, *refs):
    n = len(jobs)
    ins, outs = refs[:n], refs[n + total : 2 * n + total]
    sems = refs[2 * n + 2 * total :]
    places = [lax.axis_index(axis) for axis, _, _ in jobs]
    hello = pltpu.get_barrier_semaphore()
    axes = []
    for axis, count, _ in jobs:
        if (axis, count) not in axes:
            axes.append((axis, count))
    if total:
        axes = [("dp", lax.axis_size("dp")), ("tensor", lax.axis_size("tensor"))]
    for axis, count in axes:
        here = lax.axis_index(axis)

        @pl.loop(1, count)
        def _(offset):
            peer = lax.rem(here + offset, count)
            pl.semaphore_signal(hello, inc=1, device_id={axis: peer})

    pl.semaphore_wait(hello, sum(count - 1 for _, count in axes))

    def copy(source, target, send, recv, axis, peer, slot):
        return pltpu.make_async_remote_copy(
            src_ref=source,
            dst_ref=target.at[slot],
            send_sem=send.at[peer],
            recv_sem=recv.at[slot],
            device_id={axis: peer},
        )

    def start(source, target, send, recv, axis, count, split):
        here = lax.axis_index(axis)

        @pl.loop(1, count)
        def _(offset):
            peer = lax.rem(here + offset, count)
            piece = source.at[peer] if split else source
            copy(piece, target, send, recv, axis, peer, here).start()

        target[here] = source[here] if split else source[...]

    def finish(source, target, send, recv, axis, count, split):
        here = lax.axis_index(axis)

        @pl.loop(1, count)
        def _(offset):
            peer = lax.rem(here + offset, count)
            piece = source.at[peer] if split else source
            step = copy(piece, target, send, recv, axis, peer, peer)
            step.wait_recv()
            step.wait_send()

    work = []
    for index, (axis, count, split) in enumerate(jobs):
        work.append((ins[index], outs[index], sems[2 * index], sems[2 * index + 1], axis, count, split))
    if total:
        source, result = refs[n], refs[2 * n + total]
        one, two, middle, s1, r1, s2, r2 = sems[2 * n :]
        wide, deep = lax.axis_size("dp"), lax.axis_size("tensor")
        first = (source, one, s1, r1, "dp", wide, False)
        start(*first)
    for job in work:
        start(*job)
    if total:
        finish(*first)
        middle[...] = one[0]

        @pl.loop(1, wide)
        def _(index):
            middle[...] += one[index]

        second = (middle, two, s2, r2, "tensor", deep, False)
        start(*second)
    for job in work:
        finish(*job)
    if total:
        finish(*second)
        result[...] = two[0]

        @pl.loop(1, deep)
        def _(index):
            result[...] += two[index]


def swap(name, number, jobs, total=None):
    vmem = pl.BlockSpec(memory_space=pltpu.VMEM)
    plan, arrays, shapes, scratch = [], [], [], []
    for array, axis, split in jobs:
        count = lax.axis_size(axis)
        plan.append((axis, count, split))
        arrays.append(array)
        piece = array.shape[1:] if split else array.shape
        shapes.append(jax.ShapeDtypeStruct((count, *piece), array.dtype))
        scratch += [pltpu.SemaphoreType.DMA((count,)), pltpu.SemaphoreType.DMA((count,))]
    if total is not None:
        wide, deep = lax.axis_size("dp"), lax.axis_size("tensor")
        arrays.append(total)
        shapes.append(jax.ShapeDtypeStruct(total.shape, total.dtype))
        scratch += [
            pltpu.VMEM((wide, *total.shape), total.dtype),
            pltpu.VMEM((deep, *total.shape), total.dtype),
            pltpu.VMEM(total.shape, total.dtype),
        ]
        for count in (wide, wide, deep, deep):
            scratch.append(pltpu.SemaphoreType.DMA((count,)))
    return pl.pallas_call(
        functools.partial(swap_kernel, tuple(plan), int(total is not None)),
        out_shape=tuple(shapes),
        in_specs=[vmem] * len(arrays),
        out_specs=tuple([vmem] * len(shapes)),
        scratch_shapes=scratch,
        compiler_params=pltpu.CompilerParams(collective_id=number, has_side_effects=True),
        name=name,
    )(*arrays)


LANES = 128
HEAD_UNROLL = 2


def turn(value, tables):
    return (
        value * tables[0]
        + pltpu.roll(value, LANES - HD // 4, 1) * tables[1]
        + pltpu.roll(value, HD // 4, 1) * tables[2]
    )


def turn_back(grad, tables):
    return (
        grad * tables[0]
        + pltpu.roll(grad * tables[1], HD // 4, 1)
        + pltpu.roll(grad * tables[2], LANES - HD // 4, 1)
    )


def turn_tables(length):
    quarter = HD // 4
    lane = jnp.arange(LANES)
    rates = 10000.0 ** (-(lane % quarter).astype(jnp.float32) / quarter)
    positions = jnp.arange(length)[:, None]
    place = jnp.where(lane < 2 * quarter, positions // GRID, positions % GRID)
    angle = place.astype(jnp.float32) * rates
    real = lane < HD
    early = (lane // quarter) % 2 == 0
    cosine = jnp.where(real, jnp.cos(angle), 0.0)
    sine = jnp.sin(angle)
    return jnp.stack(
        [
            cosine,
            jnp.where(real & early, -sine, 0.0),
            jnp.where(real & ~early, sine, 0.0),
        ]
    )


def unit_norm(raw):
    inverse = lax.rsqrt(jnp.sum(raw * raw, axis=-1, keepdims=True) * (1.0 / HD) + EPS)
    return raw * inverse, inverse


def project(mod, weight, raw):
    @pl.loop(0, weight.shape[0])
    def _(index):
        raw[index] = dot(mod, weight[index])


def soft(queries, keys):
    grown = jnp.exp2(dot_rt(queries, keys) * (HD ** (-0.5) / math.log(2.0)))
    return grown * (1.0 / jnp.sum(grown, axis=-1, keepdims=True))


def attend_kernel(
    count,
    mod_ref,
    tables_ref,
    gains_ref,
    weight_hbm,
    last_hbm,
    branch_out,
    mod_out,
    weight,
    last,
    mod_all,
    raw,
    mixed,
    part,
    land,
    load_sem,
    ag_send,
    ag_recv,
    rs_send,
    rs_recv,
):
    line = Line(count, [(mod_ref, mod_all)], [(part, land)], (ag_send, ag_recv), (rs_send, rs_recv))
    loads = (
        pltpu.make_async_copy(weight_hbm, weight, load_sem.at[0]),
        pltpu.make_async_copy(last_hbm, last, load_sem.at[1]),
    )
    for load in loads:
        load.start()
    line.barrier()
    line.start_own()
    mod_all[line.place] = mod_ref[...]
    for load in loads:
        load.wait()
    heads = last.shape[0] // LANES
    wide_size, wide_count = cut(last.shape[1], 384)

    def compute(item):
        project(mod_all[item], weight, raw)
        tables = (tables_ref[0], tables_ref[1], tables_ref[2])

        @pl.loop(0, heads, unroll=HEAD_UNROLL)
        def _(head):
            lanes = span(head, LANES)
            queries = turn(unit_norm(raw[0, :, lanes])[0] * gains_ref[0:1, :], tables)
            keys = turn(unit_norm(raw[1, :, lanes])[0] * gains_ref[1:2, :], tables)
            probs = soft(queries.astype(jnp.bfloat16), keys.astype(jnp.bfloat16))
            values = raw[2, :, lanes].astype(jnp.bfloat16)
            mixed[:, lanes] = dot(probs.astype(jnp.bfloat16), values).astype(jnp.bfloat16)

        @pl.loop(0, wide_count)
        def _(index):
            cols = span(index, wide_size)
            part[item, :, cols] = dot(mixed[...], last[:, cols]).astype(jnp.bfloat16)

    @pl.loop(0, count)
    def _(step):
        @pl.when(step > 0)
        def _():
            line.receive(step)

        line.each(line.far(step - 1), line.near(step), compute)

        @pl.when(step > 0)
        def _():
            line.first_sums(step)
            line.relay_sums(step)

    mod_out[...] = mod_all[...]
    line.finish(0, branch_out)
    line.drain()


def block_copy(array, target, slot, block, size, send, recv, peer):
    rows = pl.ds(pl.multiple_of(block * size, size), size)
    source = array.at[rows] if len(array.shape) == 2 else array.at[:, rows]
    return pltpu.make_async_remote_copy(
        src_ref=source,
        dst_ref=target.at[slot],
        send_sem=send,
        recv_sem=recv,
        device_id={"dp": peer},
    )


def attend_back_kernel(
    count,
    wide,
    grad_ref,
    mod_all,
    tables_ref,
    gains_ref,
    narrow_ref,
    weight_hbm,
    last_hbm,
    branch_hbm,
    *rest,
):
    if wide:
        feed_hbm, back_out, weight_out, gain_out, branch_out, feed_out, *rest = rest
    else:
        back_out, weight_out, gain_out, branch_out, *rest = rest
    (
        weight,
        last,
        grad_all,
        raw,
        mixed,
        mixed_grad,
        raw_grad,
        kept,
        kept_mixed,
        part,
        land,
        branch_part,
        branch_land,
        total,
        load_sem,
        ag_send,
        ag_recv,
        rs_send,
        rs_recv,
        *rest,
    ) = rest
    line = Line(
        count,
        [(grad_ref, grad_all)],
        [(part, land), (branch_part, branch_land)],
        (ag_send, ag_recv),
        (rs_send, rs_recv),
    )
    loads = (
        pltpu.make_async_copy(weight_hbm, weight, load_sem.at[0]),
        pltpu.make_async_copy(last_hbm, last, load_sem.at[1]),
        pltpu.make_async_copy(branch_hbm, branch_part, load_sem.at[2]),
    )
    for load in loads:
        load.start()
    line.barrier(wide or 1)
    line.start_own()
    width = last.shape[1]
    here = lax.axis_index("dp")
    if wide:
        feed_land, staged, pair_land, quad_land, fs, fr, ps, pr, qs, qr = rest
        size = width // wide
        half = wide // 2
        parity, seat = lax.rem(here, 2), here // 2
        partner = here + 1 - 2 * parity

        def feed_copy(peer, slot):
            return block_copy(feed_hbm, feed_land, slot, peer, size, fs.at[peer], fr.at[slot], peer)

        def pair_copy(index):
            block = 2 * index + 1 - parity
            return block_copy(
                staged, pair_land, index, block, size, ps.at[index], pr.at[index], partner
            )

        def quad_copy(index, slot):
            block = 2 * index + parity
            return block_copy(
                staged, quad_land, slot, block, size, qs.at[index], qr.at[slot], block
            )

        @pl.loop(1, wide)
        def _(offset):
            peer = lax.rem(here + offset, wide)
            feed_copy(peer, here).start()

    grad_all[line.place] = grad_ref[...]
    total[...] = jnp.zeros_like(total)
    gain_out[...] = jnp.zeros_like(gain_out)
    for load in loads:
        load.wait()
    inner = last.shape[0]
    heads = inner // LANES
    scale = HD ** (-0.5)
    wide_size, wide_count = cut(width, 384)
    inner_size, inner_count = cut(inner, 256)
    tall_size, tall_count = cut(width, 128)
    first_width = kept.shape[2]

    def compute(item):
        project(mod_all[item], weight, raw)
        tables = (tables_ref[0], tables_ref[1], tables_ref[2])

        @pl.loop(0, inner_count)
        def _(index):
            cols = span(index, inner_size)
            mixed_grad[:, cols] = dot_rt(grad_all[item], last[cols, :]).astype(jnp.bfloat16)

        @pl.loop(0, heads, unroll=HEAD_UNROLL)
        def _(head):
            lanes = span(head, LANES)
            query_norm, query_inverse = unit_norm(raw[0, :, lanes])
            key_norm, key_inverse = unit_norm(raw[1, :, lanes])
            values = raw[2, :, lanes].astype(jnp.bfloat16)
            queries = turn(query_norm * gains_ref[0:1, :], tables).astype(jnp.bfloat16)
            keys = turn(key_norm * gains_ref[1:2, :], tables).astype(jnp.bfloat16)
            probs = soft(queries, keys)
            probs_low = probs.astype(jnp.bfloat16)
            mixed[:, lanes] = dot(probs_low, values).astype(jnp.bfloat16)
            grad = mixed_grad[:, lanes]
            prob_grad = dot_rt(grad, values)
            score_grad = (
                probs * (prob_grad - jnp.sum(probs * prob_grad, axis=-1, keepdims=True))
            ).astype(jnp.bfloat16)

            def back(which, value_grad, norm, inverse):
                turned = turn_back(value_grad, tables)
                gained = turned * norm
                gain_out[which] += jnp.sum(gained.reshape(-1, 8, LANES), axis=0)
                scaled = turned * gains_ref[which : which + 1, :]
                mean = jnp.sum(scaled * norm, axis=-1, keepdims=True) * (1.0 / HD)
                raw_grad[which, :, lanes] = (inverse * (scaled - norm * mean)).astype(
                    jnp.bfloat16
                )

            back(0, dot(score_grad, keys) * scale, query_norm, query_inverse)
            back(1, dot_lt(score_grad, queries) * scale, key_norm, key_inverse)
            raw_grad[2, :, lanes] = dot_lt(probs_low, grad).astype(jnp.bfloat16)

        @pl.loop(0, wide_count)
        def _(index):
            cols = span(index, wide_size)
            sums = dot_rt(raw_grad[0], weight[0, cols, :])
            sums += dot_rt(raw_grad[1], weight[1, cols, :])
            sums += dot_rt(raw_grad[2], weight[2, cols, :])
            part[item, :, cols] = sums.astype(jnp.bfloat16)

    def keep(item):
        one = dot(raw_grad[0], narrow_ref[0])
        two = dot(raw_grad[1], narrow_ref[1])
        three = dot(raw_grad[2], narrow_ref[2])
        side = one.shape[1] - LANES
        low = jnp.bfloat16
        kept[item, :, :side] = one[:, :side].astype(low)
        kept[item, :, side : side + LANES] = (one[:, side:] + two[:, :LANES]).astype(low)
        kept[item, :, side + LANES : 2 * side] = two[:, LANES:side].astype(low)
        kept[item, :, 2 * side : 2 * side + LANES] = (two[:, side:] + three[:, :LANES]).astype(low)
        kept[item, :, 2 * side + LANES :] = three[:, LANES:].astype(low)
        kept_mixed[item] = dot(mixed[...], narrow_ref[0]).astype(low)

    def weigh(item):
        @pl.loop(0, tall_count)
        def _(index):
            rows = span(index, tall_size)
            total[rows, :first_width] += dot_lt(mod_all[item, :, rows], kept[item])
            total[rows, first_width:] += dot_lt(grad_all[item, :, rows], kept_mixed[item])

    def work(item):
        compute(item)
        keep(item)

    line.first_sums(1, 1)

    @pl.loop(0, count)
    def _(step):
        @pl.when(step > 0)
        def _():
            line.each(line.far(step - 2), line.near(step - 1), weigh)
            line.receive(step)

        line.each(line.far(step - 1), line.near(step), work)

        @pl.when(step > 0)
        def _():
            line.first_sums(step)

            @pl.when(step < count - 1)
            def _():
                line.first_sums(step + 1, 1)

        @pl.when(step == count - 1)
        def _():
            line.each((0, False), line.near(step), weigh)
            if wide:
                staged[...] = total[...].astype(jnp.bfloat16)

                @pl.loop(0, half)
                def _(index):
                    pair_copy(index).start()

        @pl.when(step > 0)
        def _():
            line.relay_sums(step, 1)
            line.relay_sums(step)

    if wide:

        @pl.loop(0, half)
        def _(index):
            pair_copy(index).wait_send()
            pair_copy(index).wait_recv()
            rows = pl.ds(pl.multiple_of((2 * index + parity) * size, size), size)
            staged[rows] = (
                staged[rows].astype(jnp.float32) + pair_land[index].astype(jnp.float32)
            ).astype(jnp.bfloat16)

        @pl.loop(1, half)
        def _(offset):
            index = lax.rem(seat + offset, half)
            quad_copy(index, seat).start()

    line.finish(1, branch_out)
    line.finish(0, back_out)
    line.drain()
    if wide:
        rows = pl.ds(pl.multiple_of(here * size, size), size)
        own = pltpu.make_async_copy(feed_hbm.at[:, rows], feed_land.at[here], load_sem.at[0])
        own.start()

        @pl.loop(1, wide)
        def _(offset):
            peer = lax.rem(here + offset, wide)
            feed_copy(peer, here).wait_send()
            feed_copy(here, peer).wait_recv()

        own.wait()
        for which in range(feed_out.shape[0]):
            feed_out[which] = feed_land[0, which].astype(jnp.float32)

            @pl.loop(1, wide)
            def _(index):
                feed_out[which] += feed_land[index, which].astype(jnp.float32)

        weight_out[...] = staged[rows].astype(jnp.float32)

        @pl.loop(1, half)
        def _(offset):
            index = lax.rem(seat + offset, half)
            quad_copy(index, seat).wait_send()
            quad_copy(seat, index).wait_recv()
            weight_out[...] += quad_land[index].astype(jnp.float32)

    else:
        weight_out[...] = total[...].astype(jnp.bfloat16)


def attend_arrays(project_weight, output_weight, query_gain, key_gain, length):
    inner = project_weight.shape[2]
    heads = inner // HD
    low = jnp.bfloat16
    spot = jnp.arange(heads * LANES)
    real = spot % LANES < HD
    column = spot // LANES * HD + spot % LANES
    spread = (real[None] & (column[None] == jnp.arange(inner)[:, None])).astype(low)
    window = -(-inner // LANES) * LANES
    narrow = jnp.stack(
        [
            real[:, None]
            & (column[:, None] + index * (inner % LANES) == jnp.arange(window)[None, :])
            for index in range(3)
        ]
    ).astype(low)
    weight = jnp.einsum("dke,eh->kdh", project_weight, spread, preferred_element_type=low)
    last = jnp.einsum("ed,eh->hd", output_weight, spread, preferred_element_type=low)
    pad = LANES - HD
    gains = jnp.pad(jnp.stack([query_gain, key_gain]).astype(jnp.float32), ((0, 6), (0, pad)))
    return turn_tables(length), gains, narrow, weight, last


def line_sems(count, gathers, sums):
    return [
        pltpu.SemaphoreType.DMA((3,)),
        pltpu.SemaphoreType.DMA((gathers, 2, count)),
        pltpu.SemaphoreType.DMA((gathers, 2, count)),
        pltpu.SemaphoreType.DMA((sums, 2, count, CHUNKS)),
        pltpu.SemaphoreType.DMA((sums, 2, count, CHUNKS)),
    ]


def attend_pass(mod_in, arrays):
    count = lax.axis_size("tensor")
    tables, gains, _, weight, last = arrays
    item = mod_in.shape
    inner = last.shape[0]
    vmem, any_space = pl.BlockSpec(memory_space=pltpu.VMEM), pl.BlockSpec(memory_space=pl.ANY)
    low = jnp.bfloat16
    return pl.pallas_call(
        functools.partial(attend_kernel, count),
        out_shape=(
            jax.ShapeDtypeStruct(item, jnp.float32),
            jax.ShapeDtypeStruct((count, *item), low),
        ),
        in_specs=[vmem, vmem, vmem, any_space, any_space],
        out_specs=(vmem, vmem),
        scratch_shapes=[
            pltpu.VMEM(weight.shape, low),
            pltpu.VMEM(last.shape, low),
            pltpu.VMEM((count, *item), low),
            pltpu.VMEM((3, item[0], inner), jnp.float32),
            pltpu.VMEM((item[0], inner), low),
            pltpu.VMEM((count, *item), low),
            pltpu.VMEM((count + 1, *item), low),
            *line_sems(count, 1, 1),
        ],
        compiler_params=pltpu.CompilerParams(
            collective_id=6, has_side_effects=True, vmem_limit_bytes=60000000
        ),
        name="attend_pass",
    )(mod_in, tables, gains, weight, last)


def attend_back_pass(attend_grad, mod_all, arrays, feed_parts, feed_weights):
    count, wide = lax.axis_size("tensor"), lax.axis_size("dp")
    tables, gains, narrow, weight, last = arrays
    item = attend_grad.shape
    length, width = item
    inner = last.shape[0]
    vmem, any_space = pl.BlockSpec(memory_space=pltpu.VMEM), pl.BlockSpec(memory_space=pl.ANY)
    low, high = jnp.bfloat16, jnp.float32
    window = narrow.shape[2]
    first_width = 3 * window - 2 * LANES
    columns = first_width + window
    if width % (16 * wide):
        wide = 0
    size = width // wide if wide else width
    outs = [
        jax.ShapeDtypeStruct(item, high),
        jax.ShapeDtypeStruct((size, columns), high if wide else low),
        jax.ShapeDtypeStruct((2, 8, LANES), high),
        jax.ShapeDtypeStruct(item, high),
    ]
    scratch = [
        pltpu.VMEM(weight.shape, low),
        pltpu.VMEM(last.shape, low),
        pltpu.VMEM((count, *item), low),
        pltpu.VMEM((3, length, inner), high),
        pltpu.VMEM((length, inner), low),
        pltpu.VMEM((length, inner), low),
        pltpu.VMEM((3, length, inner), low),
        pltpu.VMEM((count, length, first_width), low),
        pltpu.VMEM((count, length, window), low),
        pltpu.VMEM((count, *item), low),
        pltpu.VMEM((count + 1, *item), low),
        pltpu.VMEM((count, *item), low),
        pltpu.VMEM((count + 1, *item), low),
        pltpu.VMEM((width, columns), high),
        *line_sems(count, 1, 2),
    ]
    ins = [attend_grad, mod_all, tables, gains, narrow, weight, last, feed_parts]
    specs = [vmem, vmem, vmem, vmem, vmem, any_space, any_space, any_space]
    if wide:
        ins.append(feed_weights)
        specs.append(any_space)
        kinds, _, units = feed_weights.shape
        outs.append(jax.ShapeDtypeStruct((kinds, size, units), high))
        half = wide // 2
        scratch += [
            pltpu.VMEM((wide, kinds, size, units), low),
            pltpu.VMEM((width, columns), low),
            pltpu.VMEM((half, size, columns), low),
            pltpu.VMEM((half, size, columns), low),
        ]
        for number in (wide, wide, half, half, half, half):
            scratch.append(pltpu.SemaphoreType.DMA((number,)))
    results = pl.pallas_call(
        functools.partial(attend_back_kernel, count, wide),
        out_shape=tuple(outs),
        in_specs=specs,
        out_specs=tuple([vmem] * len(outs)),
        scratch_shapes=scratch,
        compiler_params=pltpu.CompilerParams(
            collective_id=7, has_side_effects=True, vmem_limit_bytes=66000000
        ),
        name="attend_back_pass",
    )(*ins)
    if wide:
        return results

    def scatter(value, axis):
        return lax.psum_scatter(value, "dp", scatter_dimension=axis, tiled=True).astype(high)

    back, weights, gain_parts, branch = results
    return back, scatter(weights, 0), gain_parts, branch, scatter(feed_weights, 1)


def tail_kernel(
    grads_ref,
    small_ref,
    weight_ref,
    slope_ref,
    forward_ref,
    feat_ref,
    label_ref,
    rows_ref,
    pick_ref,
    small_out,
    modulate_out,
    embed_out,
    class_out,
    time_out,
    bias_out,
    grads_land,
    grads_mine,
    grads_land_dp,
    small_one,
    small_mid,
    small_two,
    part,
    part_land,
    cond,
    cond_land,
    forward_land,
    feat_land,
    label_land,
    grads_all,
    cond_all,
    forward_all,
    feat_all,
    label_all,
    *sems,
):
    deep, wide = part_land.shape[0], cond_land.shape[0]
    items = cond.shape[0]
    axes = (("dp", wide), ("tensor", deep))
    hello = pltpu.get_barrier_semaphore()
    for axis, count in axes:
        here = lax.axis_index(axis)

        @pl.loop(1, count)
        def _(offset):
            pl.semaphore_signal(
                hello, inc=1, device_id={axis: lax.rem(here + offset, count)}
            )

    pl.semaphore_wait(hello, wide + deep - 2)
    low = jnp.bfloat16

    def exchange(number, axis, source, target, split=False):
        count = target.shape[0]
        here = lax.axis_index(axis)
        send, recv = sems[2 * number], sems[2 * number + 1]

        def copy(peer, slot):
            return pltpu.make_async_remote_copy(
                src_ref=source.at[peer] if split else source,
                dst_ref=target.at[slot],
                send_sem=send.at[peer],
                recv_sem=recv.at[slot],
                device_id={axis: peer},
            )

        def start():
            @pl.loop(1, count)
            def _(offset):
                copy(lax.rem(here + offset, count), here).start()

            target[here] = source[here] if split else source[...]

        def finish():
            @pl.loop(1, count)
            def _(offset):
                peer = lax.rem(here + offset, count)
                copy(peer, here).wait_send()
                copy(peer, peer).wait_recv()

        return start, finish

    start_grads, finish_grads = exchange(0, "tensor", grads_ref, grads_land, True)
    start_small, finish_small = exchange(1, "dp", small_ref, small_one)
    start_sums, finish_sums = exchange(2, "tensor", small_mid, small_two)
    start_part, finish_part = exchange(3, "tensor", part, part_land)
    start_mine, finish_mine = exchange(4, "dp", grads_mine, grads_land_dp)
    start_cond, finish_cond = exchange(5, "dp", cond, cond_land)
    start_forward, finish_forward = exchange(6, "dp", forward_ref, forward_land, True)
    start_feat, finish_feat = exchange(7, "dp", feat_ref, feat_land)
    start_label, finish_label = exchange(8, "dp", label_ref, label_land)

    start_grads()
    start_small()
    start_forward()
    start_feat()
    start_label()
    finish_grads()
    kinds = grads_mine.shape[0]
    for item in range(items):
        piece = grads_land[item].astype(jnp.float32)
        for kind in range(kinds):
            grads_all[kind, item : item + 1, :] = piece[kind : kind + 1, :]
    total = jnp.zeros(part.shape, jnp.float32)
    for kind in range(kinds):
        mine = grads_all[kind, :items, :].astype(low)
        grads_mine[kind] = mine
        total += dot_rt(mine, weight_ref[kind])
    part[...] = total
    start_part()
    start_mine()
    finish_small()
    small_mid[...] = small_one[0]

    @pl.loop(1, wide)
    def _(index):
        small_mid[...] += small_one[index]

    start_sums()
    finish_part()
    total = part_land[0]
    for index in range(1, deep):
        total += part_land[index]
    cond[...] = (total * slope_ref[...]).astype(low)
    start_cond()
    finish_forward()
    finish_feat()
    finish_label()
    for index in range(wide):
        rows = pl.ds(index * items, items)
        for kind in range(forward_all.shape[0]):
            forward_all[kind, rows, :] = forward_land[index, kind]
        feat_all[rows, :] = feat_land[index]
        label_all[rows, :] = label_land[index]
    finish_mine()
    for index in range(wide):
        rows = pl.ds(index * items, items)
        for kind in range(kinds):
            grads_all[kind, rows, :] = grads_land_dp[index, kind].astype(jnp.float32)
    active = forward_all[0].astype(low)
    for kind in range(kinds):
        modulate_out[kind] = dot_lt(active, grads_all[kind].astype(low))
    finish_sums()
    small_out[...] = small_two[0]

    @pl.loop(1, deep)
    def _(index):
        small_out[...] += small_two[index]

    finish_cond()
    for index in range(wide):
        cond_all[pl.ds(index * items, items), :] = cond_land[index].astype(jnp.float32)
    every = cond_all[...].astype(low)
    embed_out[...] = dot_lt(forward_all[1].astype(low), every)
    picked = dot(every, pick_ref[...]).astype(low)
    classes = class_out.shape[0]
    label = jnp.broadcast_to(label_all[:, 0:1], (label_all.shape[0], classes))
    lane = lax.broadcasted_iota(jnp.int32, label.shape, 1)
    hot = jnp.where(label == lane, 1.0, 0.0).astype(low)
    class_out[...] = dot_lt(hot, picked)
    earlier = (dot_rt(every, rows_ref[...]) * forward_all[2]).astype(low)
    time_out[...] = dot_lt(feat_all[...].astype(low), earlier)
    bias_out[0:1, :] = jnp.sum(picked.astype(jnp.float32), axis=0, keepdims=True)
    bias_out[1:2, :] = jnp.sum(earlier.astype(jnp.float32), axis=0, keepdims=True)


def tail_pass(grads, small, weight, slope, forward, feat, label, rows, pick, classes):
    deep, kinds, slab = grads.shape
    wide, parts, items, share = forward.shape
    width = weight.shape[1]
    batch = wide * items
    freq = feat.shape[1]
    low, high = jnp.bfloat16, jnp.float32
    vmem = pl.BlockSpec(memory_space=pltpu.VMEM)
    shapes = (
        (small.shape, high),
        ((kinds, share, slab), high),
        ((share, width), high),
        ((classes, share), high),
        ((freq, share), high),
        ((2, share), high),
    )
    scratch = (
        ((deep, kinds, slab), low),
        ((kinds, items, slab), low),
        ((wide, kinds, items, slab), low),
        ((wide, *small.shape), high),
        (small.shape, high),
        ((deep, *small.shape), high),
        ((items, width), high),
        ((deep, items, width), high),
        ((items, width), low),
        ((wide, items, width), low),
        (forward.shape, high),
        ((wide, items, freq), high),
        ((wide, items, LANES), jnp.int32),
        ((kinds, batch, slab), high),
        ((batch, width), high),
        ((parts, batch, share), high),
        ((batch, freq), high),
        ((batch, LANES), jnp.int32),
    )
    sems = []
    for number in (deep, wide, deep, deep, wide, wide, wide, wide, wide):
        sems += [pltpu.SemaphoreType.DMA((number,))] * 2
    return pl.pallas_call(
        tail_kernel,
        out_shape=tuple(jax.ShapeDtypeStruct(*shape) for shape in shapes),
        in_specs=[vmem] * 9,
        out_specs=tuple([vmem] * 6),
        scratch_shapes=[pltpu.VMEM(*shape) for shape in scratch] + sems,
        compiler_params=pltpu.CompilerParams(
            collective_id=3, has_side_effects=True, vmem_limit_bytes=60000000
        ),
        name="tail_pass",
    )(grads, small, weight, slope, forward, feat, label, rows, pick)


def line_gather(value, axis):
    count = lax.axis_size(axis)
    ups, downs = [value], [value]
    for _ in range(count - 1):
        ups.append(lax.ppermute(ups[-1], axis, [(i, i + 1) for i in range(count - 1)]))
        downs.append(lax.ppermute(downs[-1], axis, [(i + 1, i) for i in range(count - 1)]))
    row = jnp.concatenate(ups[:0:-1] + downs, axis=0)
    return lax.dynamic_slice_in_dim(row, count - 1 - lax.axis_index(axis), count, 0)


def shards(
    tokens,
    timesteps,
    labels,
    item_counts,
    cotangent,
    project_weight,
    query_gain,
    key_gain,
    output_weight,
    output_bias,
    expand_weight,
    down_weight,
    down_bias,
    modulate_weight,
    modulate_bias,
    time_weight,
    time_bias,
    embed_weight,
    embed_bias,
    class_table,
):
    local_items, length, width = tokens.shape
    items = timesteps.shape[0]
    slab = modulate_weight.shape[2]
    heads_here = project_weight.shape[2] // HD
    scale = HD ** (-0.5)
    first_item = lax.axis_index("tensor") * local_items
    live = (first_item + jnp.arange(local_items) < item_counts[0]).astype(jnp.float32)[
        :, None, None
    ]
    index = lax.axis_index("dp")
    time_feat = time_features(timesteps).astype(jnp.bfloat16)
    pre_hidden = jnp.dot(
        time_feat, time_weight, preferred_element_type=jnp.float32
    ) + time_bias.astype(jnp.float32)
    time_hidden = jax.nn.silu(pre_hidden).astype(jnp.bfloat16)
    condition = (
        jnp.dot(time_hidden, embed_weight, preferred_element_type=jnp.float32)
        + embed_bias.astype(jnp.float32)
        + jnp.take(class_table, labels, axis=0).astype(jnp.float32)
    )
    cond_act = jax.nn.silu(condition).astype(jnp.bfloat16)
    modulation_part = (
        jnp.einsum("bd,dke->bke", cond_act, modulate_weight, preferred_element_type=jnp.float32)
        + modulate_bias.astype(jnp.float32)
    ).astype(jnp.bfloat16)
    cotangents = line_gather(cotangent, "tensor")
    (modulation,) = swap("modulation_swap", 2, [(modulation_part, "tensor", False)])
    modulation = jnp.transpose(modulation, (1, 2, 0, 3)).reshape(items, 6, width)
    modulation = modulation.astype(jnp.float32)
    modulation_local = lax.dynamic_slice_in_dim(modulation, first_item, local_items, 0)
    local_parts = [modulation_local[:, which][:, None, :] for which in range(6)]
    attend_shift, attend_scale, attend_gate, feed_shift, feed_scale, feed_gate = local_parts
    positions = jnp.arange(length)
    token_local = tokens.astype(jnp.float32)
    normed_local, inverse_local = layer_norm(token_local)
    mod_in = normed_local * (1.0 + attend_scale) + attend_shift
    arrays = attend_arrays(project_weight, output_weight, query_gain, key_gain, length)
    attend_total, mod_all = attend_pass(mod_in[0].astype(jnp.bfloat16), arrays)
    attend_branch = attend_total[None] + output_bias.astype(jnp.float32)
    residual = token_local + attend_gate * attend_branch
    normed_two, inverse_two = layer_norm(residual)
    mod_two = (normed_two * (1.0 + feed_scale) + feed_shift).astype(jnp.bfloat16)
    out_grad = cotangent.astype(jnp.float32) * live
    live_all = (jnp.arange(items) < item_counts[0]).astype(jnp.float32)[:, None, None]
    branch_grads = (
        cotangents.astype(jnp.float32) * live_all * modulation[:, 5][:, None, :]
    ).astype(jnp.bfloat16)
    branch_grad = (out_grad * feed_gate).astype(jnp.bfloat16)
    down_bias_part = jnp.sum(branch_grad.astype(jnp.float32), axis=(0, 1))
    mod_two_grad, feed_weights, feed_parts = feed_pass(
        mod_two[0], branch_grads, expand_weight, down_weight
    )
    mod_two_grad = mod_two_grad[None]
    residual_grad = out_grad + layer_norm_back(
        normed_two, inverse_two, mod_two_grad * (1.0 + feed_scale)
    )
    attend_grad = (residual_grad * attend_gate).astype(jnp.bfloat16)
    output_bias_part = jnp.sum(attend_grad.astype(jnp.float32), axis=(0, 1))
    mod_in_grad, attend_weights, gain_parts, feed_total, feed_weights = attend_back_pass(
        attend_grad[0], mod_all, arrays, feed_parts, feed_weights
    )
    feed_branch = feed_total[None] + down_bias.astype(jnp.float32)
    result = (live * (residual + feed_gate * feed_branch)).astype(jnp.bfloat16)
    mod_in_grad = mod_in_grad[None]
    query_gain_part, key_gain_part = jnp.sum(gain_parts, axis=1)[:, :HD]
    tokens_grad = (
        residual_grad
        + layer_norm_back(normed_local, inverse_local, mod_in_grad * (1.0 + attend_scale))
    ).astype(jnp.bfloat16)
    modulation_grad_part = jnp.stack(
        [
            jnp.sum(mod_in_grad, axis=1),
            jnp.sum(mod_in_grad * normed_local, axis=1),
            jnp.sum(residual_grad * attend_branch, axis=1),
            jnp.sum(mod_two_grad, axis=1),
            jnp.sum(mod_two_grad * normed_two, axis=1),
            jnp.sum(out_grad * feed_branch, axis=1),
        ],
        axis=1,
    )
    modulation_grad_part = modulation_grad_part[0].astype(jnp.bfloat16)
    small = jnp.concatenate(
        [
            output_bias_part,
            down_bias_part,
            modulation_grad_part.astype(jnp.float32).reshape(-1),
            query_gain_part,
            key_gain_part,
        ]
    )
    small_size = small.shape[0]
    small = jnp.pad(small, (0, -small_size % 1024)).reshape(-1, 128)
    tensor_size, wide = width // slab, lax.axis_size("dp")
    share = width // wide

    def shares(value):
        return jnp.transpose(value.astype(jnp.float32).reshape(items, wide, share), (1, 0, 2))

    def mine(value):
        return lax.dynamic_slice_in_dim(value, index * share, share, 0)

    pick = jnp.arange(width)[:, None] == index * share + jnp.arange(share)[None, :]
    small, modulate_grad, embed_grad, class_grad, time_grad, biases = tail_pass(
        jnp.transpose(modulation_grad_part.reshape(6, tensor_size, slab), (1, 0, 2)),
        small,
        jnp.transpose(modulate_weight, (1, 0, 2)),
        silu_slope(condition),
        jnp.stack([shares(cond_act), shares(time_hidden), shares(silu_slope(pre_hidden))], axis=1),
        time_feat.astype(jnp.float32),
        jnp.broadcast_to(labels[:, None], (items, LANES)),
        mine(embed_weight),
        pick.astype(jnp.bfloat16),
        class_table.shape[0],
    )
    modulate_grad = jnp.transpose(modulate_grad, (1, 0, 2))
    embed_bias_grad, time_bias_grad = biases
    small = small.reshape(-1)
    output_bias_grad = small[:width]
    down_bias_grad = small[width : 2 * width]
    modulate_bias_grad = small[2 * width : 8 * width].reshape(6, width)
    query_gain_grad = small[8 * width : 8 * width + HD]
    key_gain_grad = small[8 * width + HD : 8 * width + 2 * HD]
    inner = heads_here * HD
    first_width = attend_weights.shape[1] - -(-inner // LANES) * LANES
    project_grad = attend_weights[:, : 3 * inner].reshape(-1, 3, inner)
    output_weight_grad = attend_weights[:, first_width : first_width + inner].T
    expand_grad = jnp.transpose(feed_weights[:2], (1, 0, 2))
    down_grad = feed_weights[2].T
    return (
        result,
        tokens_grad,
        project_grad,
        query_gain_grad,
        key_gain_grad,
        output_weight_grad,
        output_bias_grad,
        expand_grad,
        down_grad,
        down_bias_grad,
        modulate_grad,
        modulate_bias_grad,
        time_grad,
        time_bias_grad,
        embed_grad,
        embed_bias_grad,
        class_grad,
    )


def solution(mesh):
    return jax.shard_map(
        shards,
        mesh=mesh,
        in_specs=(
            P(("dp", "tensor"), None, None),
            P("dp"),
            P("dp"),
            P("dp"),
            P(("dp", "tensor"), None, None),
            P(None, None, "tensor"),
            P(),
            P(),
            P("tensor", None),
            P(),
            P(None, None, "tensor"),
            P("tensor", None),
            P(),
            P(None, None, "tensor"),
            P(None, "tensor"),
            P(),
            P(),
            P(),
            P(),
            P(),
        ),
        out_specs=(
            P(("dp", "tensor"), None, None),
            P(("dp", "tensor"), None, None),
            P("dp", None, "tensor"),
            P(),
            P(),
            P("tensor", "dp"),
            P(),
            P("dp", None, "tensor"),
            P("tensor", "dp"),
            P(),
            P("dp", None, "tensor"),
            P(),
            P(None, "dp"),
            P("dp"),
            P("dp", None),
            P("dp"),
            P(None, "dp"),
        ),
        check_vma=False,
    )
```

```python
import functools
import math

import jax
import jax.numpy as jnp
from jax import lax
from jax.experimental import pallas as pl
from jax.experimental.pallas import tpu as pltpu
from jax.sharding import PartitionSpec as P

HD = 72
FREQ = 256
GRID = 16


EPS = 1e-06


def layer_norm(value):
    center = value - jnp.mean(value, axis=-1, keepdims=True)
    inverse = lax.rsqrt(jnp.mean(center * center, axis=-1, keepdims=True) + EPS)
    return (center * inverse, inverse)


def layer_norm_back(normed, inverse, grad):
    return inverse * (
        grad
        - jnp.mean(grad, axis=-1, keepdims=True)
        - normed * jnp.mean(grad * normed, axis=-1, keepdims=True)
    )


def silu_slope(value):
    sigma = jax.nn.sigmoid(value)
    return sigma * (1.0 + value * (1.0 - sigma))


def rotate(value, positions):
    quarter = HD // 4
    rates = 10000.0 ** (-jnp.arange(quarter, dtype=jnp.float32) / quarter)
    places = ((positions // GRID).astype(jnp.float32), (positions % GRID).astype(jnp.float32))
    pieces = []
    for which_half in range(2):
        half_value = value[..., which_half * 2 * quarter : (which_half + 1) * 2 * quarter]
        angle = places[which_half][:, None] * rates[None, :]
        cosine = jnp.cos(angle)[None, :, None, :]
        sine = jnp.sin(angle)[None, :, None, :]
        first = half_value[..., :quarter]
        second = half_value[..., quarter:]
        pieces.append(first * cosine - second * sine)
        pieces.append(second * cosine + first * sine)
    return jnp.concatenate(pieces, axis=-1)


def head_prepare(raw, gain, positions):
    scaled = raw * lax.rsqrt(jnp.mean(raw * raw, axis=-1, keepdims=True) + EPS) * gain
    return rotate(scaled, positions)


def time_features(steps_in):
    half = FREQ // 2
    rates = jnp.exp(-math.log(10000.0) * jnp.arange(half, dtype=jnp.float32) / half)
    angle = steps_in.astype(jnp.float32)[:, None] * rates[None, :]
    return jnp.concatenate([jnp.cos(angle), jnp.sin(angle)], axis=-1)


CHUNKS = 8


def rows_of(block, total):
    size = total // CHUNKS
    return pl.ds(pl.multiple_of(block * size, size), size)


class Line:
    def __init__(self, count, gathered, summed, ag_sems, rs_sems):
        self.count = count
        self.place = lax.axis_index("tensor")
        self.gathered = gathered
        self.summed = summed
        self.ag_send, self.ag_recv = ag_sems
        self.rs_send, self.rs_recv = rs_sems

    def barrier(self, wide=1):
        place, count = self.place, self.count
        sem = pltpu.get_barrier_semaphore()

        @pl.when(place > 0)
        def _():
            pl.semaphore_signal(sem, inc=1, device_id={"tensor": place - 1})

        @pl.when(place < count - 1)
        def _():
            pl.semaphore_signal(sem, inc=1, device_id={"tensor": place + 1})

        peers = jnp.where(place > 0, 1, 0) + jnp.where(place < count - 1, 1, 0)
        here = lax.axis_index("dp")

        @pl.loop(1, wide)
        def _(offset):
            peer = lax.rem(here + offset, wide)
            pl.semaphore_signal(sem, inc=1, device_id={"dp": peer})

        pl.semaphore_wait(sem, peers + (wide - 1))

    def item_copy(self, which, way, item, own=False):
        mine, everyone = self.gathered[which]
        target = self.place + (1 if way == 0 else -1)
        return pltpu.make_async_remote_copy(
            src_ref=mine if own else everyone.at[item],
            dst_ref=everyone.at[item],
            send_sem=self.ag_send.at[which, way, item],
            recv_sem=self.ag_recv.at[which, way, item],
            device_id={"tensor": target},
        )

    def can(self, way):
        return self.place < self.count - 1 if way == 0 else self.place > 0

    def sum_copy(self, which, way, item, block):
        part, landed = self.summed[which]
        target = self.place + (1 if way == 0 else -1)
        slot = item
        if way == 1:
            slot = jnp.where(item == target, self.count, item)
        rows = rows_of(block, part.shape[1])
        return pltpu.make_async_remote_copy(
            src_ref=part.at[item, rows],
            dst_ref=landed.at[slot, rows],
            send_sem=self.rs_send.at[which, way, item, block],
            recv_sem=self.rs_recv.at[which, way, item, block],
            device_id={"tensor": target},
        )

    def landed_slot(self, way, item):
        return jnp.where(item == self.place, self.count, item) if way == 1 else item

    def wait_sum(self, which, way, item, block):
        part, landed = self.summed[which]
        rows = rows_of(block, part.shape[1])
        view = landed.at[self.landed_slot(way, item), rows]
        pltpu.make_async_remote_copy(
            src_ref=view,
            dst_ref=view,
            send_sem=self.rs_send.at[which, way, item, block],
            recv_sem=self.rs_recv.at[which, way, item, block],
            device_id={"tensor": self.place},
        ).wait_recv()
        return view

    def start_own(self):
        for which in range(len(self.gathered)):
            for way in range(2):

                @pl.when(self.can(way))
                def _():
                    self.item_copy(which, way, self.place, own=True).start()

    def receive(self, step):
        place, count = self.place, self.count
        for which in range(len(self.gathered)):
            for way in range(2):
                item = place - step if way == 0 else place + step

                @pl.when((item >= 0) & (item < count))
                def _():
                    self.item_copy(which, way, item).wait_recv()

                    @pl.when(self.can(way))
                    def _():
                        self.item_copy(which, way, item).start()

    def items(self, step):
        place, count = self.place, self.count
        low, high = place - step, place + step
        return ((low, (low >= 0)), (high, (high < count) & (step > 0)))

    def moves(self, step):
        place, count = self.place, self.count
        return (
            (0, step, step > place, place),
            (1, count - 1 - step, count - 1 - step < place, count - 1 - place),
        )

    def first_sums(self, step, arrays=(0,)):
        @pl.loop(0, CHUNKS)
        def _(block):
            for way, item, further, hop in self.moves(step):

                @pl.when(further & (hop == 0))
                def _():
                    for which in arrays:
                        self.sum_copy(which, way, item, block).start()

    def relay_sums(self, step, arrays=(0,)):
        @pl.loop(0, CHUNKS + self.count - 3)
        def _(turn):
            for distance in range(1, self.count - 1):
                block = turn - (distance - 1)
                for way, item, further, hop in self.moves(step):

                    @pl.when(further & (hop == distance) & (block >= 0) & (block < CHUNKS))
                    def _():
                        for which in arrays:
                            part, landed = self.summed[which]
                            rows = rows_of(block, part.shape[1])
                            view = self.wait_sum(which, way, item, block)
                            total = part[item, rows].astype(jnp.float32) + view[...].astype(
                                jnp.float32
                            )
                            part[item, rows] = total.astype(part.dtype)
                            self.sum_copy(which, way, item, block).start()

    def each(self, first, second, body):
        @pl.loop(0, 2)
        def _(turn):
            item = jnp.where(turn == 0, first[0], second[0])
            valid = ((turn == 0) & first[1]) | ((turn == 1) & second[1])

            @pl.when(valid)
            def _():
                body(item)

    def near(self, step):
        place, count = self.place, self.count
        low = place >= step
        return jnp.where(low, place - step, place + step), low | (place + step < count)

    def far(self, step):
        place, count = self.place, self.count
        return place + step, (step > 0) & (place >= step) & (place + step < count)

    def finish(self, which, out):
        place, count = self.place, self.count
        part, landed = self.summed[which]

        @pl.loop(0, CHUNKS)
        def _(block):
            rows = rows_of(block, part.shape[1])
            out[rows] = part[place, rows].astype(jnp.float32)
            for way in range(2):

                @pl.when(place > 0 if way == 0 else place < count - 1)
                def _():
                    view = self.wait_sum(which, way, place, block)
                    out[rows] += view[...].astype(jnp.float32)

    def drain(self):
        place, count = self.place, self.count

        @pl.loop(0, count)
        def _(item):
            for way in range(2):
                passed = item <= place if way == 0 else item >= place

                @pl.when(passed & self.can(way))
                def _():
                    for which in range(len(self.gathered)):
                        self.item_copy(which, way, item).wait_send()

                further = item > place if way == 0 else item < place

                @pl.when(further)
                def _():
                    @pl.loop(0, CHUNKS)
                    def _(block):
                        for which in range(len(self.summed)):
                            self.sum_copy(which, way, item, block).wait_send()


def dot(left, right):
    return jnp.dot(left, right, preferred_element_type=jnp.float32)


def dot_rt(left, right):
    return lax.dot_general(
        left, right, (((1,), (1,)), ((), ())), preferred_element_type=jnp.float32
    )


def dot_lt(left, right):
    return lax.dot_general(
        left, right, (((0,), (0,)), ((), ())), preferred_element_type=jnp.float32
    )


def cut(total, most):
    size = max(s for s in range(128, most + 1, 128) if total % s == 0)
    return size, total // size


def span(index, size):
    return pl.ds(pl.multiple_of(index * size, size), size)


def feed_kernel(
    count,
    mod_ref,
    grad_ref,
    expand_hbm,
    down_hbm,
    feed_out,
    back_out,
    weight_hbm,
    expand,
    down,
    mod_all,
    grad_all,
    hidden,
    slopes,
    feed_part,
    back_part,
    feed_land,
    back_land,
    total,
    weights,
    load_sem,
    ag_send,
    ag_recv,
    rs_send,
    rs_recv,
):
    line = Line(
        count,
        [(mod_ref, mod_all), (grad_ref, grad_all)],
        [(back_part, back_land), (feed_part, feed_land)],
        (ag_send, ag_recv),
        (rs_send, rs_recv),
    )
    width, units = expand.shape[1], expand.shape[2]
    loads = (
        pltpu.make_async_copy(expand_hbm, expand, load_sem.at[0]),
        pltpu.make_async_copy(down_hbm, down, load_sem.at[1]),
    )
    for load in loads:
        load.start()
    line.barrier()
    line.start_own()
    mod_all[line.place] = mod_ref[...]
    grad_all[line.place] = grad_ref[...]
    total[...] = jnp.zeros_like(total)
    for load in loads:
        load.wait()
    unit_size, unit_count = cut(units, 256)
    wide_size, wide_count = cut(width, 384)
    tall_size, tall_count = cut(width, 128)

    def compute(item):
        @pl.loop(0, unit_count)
        def _(index):
            cols = span(index, unit_size)
            mod = mod_all[item]
            gate = dot(mod, expand[0, :, cols])
            upper = dot(mod, expand[1, :, cols])
            back = dot_rt(grad_all[item], down[cols, :])
            sigma = jax.nn.sigmoid(gate)
            active = gate * sigma
            hidden[item, :, cols] = (active * upper).astype(jnp.bfloat16)
            slopes[0, item, :, cols] = (
                back * upper * (sigma * (1.0 + gate * (1.0 - sigma)))
            ).astype(jnp.bfloat16)
            slopes[1, item, :, cols] = (back * active).astype(jnp.bfloat16)

        @pl.loop(0, wide_count)
        def _(index):
            cols = span(index, wide_size)
            back_part[item, :, cols] = (
                dot_rt(slopes[0, item], expand[0, cols, :])
                + dot_rt(slopes[1, item], expand[1, cols, :])
            ).astype(jnp.bfloat16)
            feed_part[item, :, cols] = dot(hidden[item], down[:, cols]).astype(jnp.bfloat16)

    def weigh(item):
        @pl.loop(0, tall_count)
        def _(index):
            rows = span(index, tall_size)
            mod = mod_all[item, :, rows]
            total[0, rows, :] += dot_lt(mod, slopes[0, item])
            total[1, rows, :] += dot_lt(mod, slopes[1, item])
            total[2, rows, :] += dot_lt(grad_all[item, :, rows], hidden[item])

    @pl.loop(0, count)
    def _(step):
        @pl.when(step > 0)
        def _():
            line.each(line.far(step - 1), line.near(step - 1), weigh)
            line.receive(step)

        line.each(line.far(step), line.near(step), compute)

        @pl.when(step > 0)
        def _():
            line.first_sums(step, (0, 1))
            line.relay_sums(step, (0, 1))

    line.each((0, False), line.near(count - 1), weigh)
    weights[...] = total[...].astype(jnp.bfloat16)
    store = pltpu.make_async_copy(weights, weight_hbm, load_sem.at[0])
    store.start()
    line.finish(0, back_out)
    line.finish(1, feed_out)
    line.drain()
    store.wait()


def feed_pass(mod_two, branch_grad, expand_weight, down_weight):
    count = lax.axis_size("tensor")
    length, width = mod_two.shape
    units = down_weight.shape[0]
    expand = jnp.transpose(expand_weight, (1, 0, 2))
    vmem, any_space = pl.BlockSpec(memory_space=pltpu.VMEM), pl.BlockSpec(memory_space=pl.ANY)
    low = jnp.bfloat16
    item = (length, width)
    return pl.pallas_call(
        functools.partial(feed_kernel, count),
        out_shape=(
            jax.ShapeDtypeStruct(item, jnp.float32),
            jax.ShapeDtypeStruct(item, jnp.float32),
            jax.ShapeDtypeStruct((3, width, units), low),
        ),
        in_specs=[vmem, vmem, any_space, any_space],
        out_specs=(vmem, vmem, any_space),
        scratch_shapes=[
            pltpu.VMEM((2, width, units), low),
            pltpu.VMEM((units, width), low),
            pltpu.VMEM((count, *item), low),
            pltpu.VMEM((count, *item), low),
            pltpu.VMEM((count, length, units), low),
            pltpu.VMEM((2, count, length, units), low),
            pltpu.VMEM((count, *item), low),
            pltpu.VMEM((count, *item), low),
            pltpu.VMEM((count + 1, *item), low),
            pltpu.VMEM((count + 1, *item), low),
            pltpu.VMEM((3, width, units), jnp.float32),
            pltpu.VMEM((3, width, units), low),
            *line_sems(count, 2, 2),
        ],
        compiler_params=pltpu.CompilerParams(
            collective_id=1, has_side_effects=True, vmem_limit_bytes=64000000
        ),
        name="feed_pass",
    )(mod_two, branch_grad, expand, down_weight)


def swap_kernel(jobs, total, *refs):
    n = len(jobs)
    ins, outs = refs[:n], refs[n + total : 2 * n + total]
    sems = refs[2 * n + 2 * total :]
    places = [lax.axis_index(axis) for axis, _, _ in jobs]
    hello = pltpu.get_barrier_semaphore()
    axes = []
    for axis, count, _ in jobs:
        if (axis, count) not in axes:
            axes.append((axis, count))
    if total:
        axes = [("dp", lax.axis_size("dp")), ("tensor", lax.axis_size("tensor"))]
    for axis, count in axes:
        here = lax.axis_index(axis)

        @pl.loop(1, count)
        def _(offset):
            peer = lax.rem(here + offset, count)
            pl.semaphore_signal(hello, inc=1, device_id={axis: peer})

    pl.semaphore_wait(hello, sum(count - 1 for _, count in axes))

    def copy(source, target, send, recv, axis, peer, slot):
        return pltpu.make_async_remote_copy(
            src_ref=source,
            dst_ref=target.at[slot],
            send_sem=send.at[peer],
            recv_sem=recv.at[slot],
            device_id={axis: peer},
        )

    def start(source, target, send, recv, axis, count, split):
        here = lax.axis_index(axis)

        @pl.loop(1, count)
        def _(offset):
            peer = lax.rem(here + offset, count)
            piece = source.at[peer] if split else source
            copy(piece, target, send, recv, axis, peer, here).start()

        target[here] = source[here] if split else source[...]

    def finish(source, target, send, recv, axis, count, split):
        here = lax.axis_index(axis)

        @pl.loop(1, count)
        def _(offset):
            peer = lax.rem(here + offset, count)
            piece = source.at[peer] if split else source
            step = copy(piece, target, send, recv, axis, peer, peer)
            step.wait_recv()
            step.wait_send()

    work = []
    for index, (axis, count, split) in enumerate(jobs):
        work.append((ins[index], outs[index], sems[2 * index], sems[2 * index + 1], axis, count, split))
    if total:
        source, result = refs[n], refs[2 * n + total]
        one, two, middle, s1, r1, s2, r2 = sems[2 * n :]
        wide, deep = lax.axis_size("dp"), lax.axis_size("tensor")
        first = (source, one, s1, r1, "dp", wide, False)
        start(*first)
    for job in work:
        start(*job)
    if total:
        finish(*first)
        middle[...] = one[0]

        @pl.loop(1, wide)
        def _(index):
            middle[...] += one[index]

        second = (middle, two, s2, r2, "tensor", deep, False)
        start(*second)
    for job in work:
        finish(*job)
    if total:
        finish(*second)
        result[...] = two[0]

        @pl.loop(1, deep)
        def _(index):
            result[...] += two[index]


def swap(name, number, jobs, total=None):
    vmem = pl.BlockSpec(memory_space=pltpu.VMEM)
    plan, arrays, shapes, scratch = [], [], [], []
    for array, axis, split in jobs:
        count = lax.axis_size(axis)
        plan.append((axis, count, split))
        arrays.append(array)
        piece = array.shape[1:] if split else array.shape
        shapes.append(jax.ShapeDtypeStruct((count, *piece), array.dtype))
        scratch += [pltpu.SemaphoreType.DMA((count,)), pltpu.SemaphoreType.DMA((count,))]
    if total is not None:
        wide, deep = lax.axis_size("dp"), lax.axis_size("tensor")
        arrays.append(total)
        shapes.append(jax.ShapeDtypeStruct(total.shape, total.dtype))
        scratch += [
            pltpu.VMEM((wide, *total.shape), total.dtype),
            pltpu.VMEM((deep, *total.shape), total.dtype),
            pltpu.VMEM(total.shape, total.dtype),
        ]
        for count in (wide, wide, deep, deep):
            scratch.append(pltpu.SemaphoreType.DMA((count,)))
    return pl.pallas_call(
        functools.partial(swap_kernel, tuple(plan), int(total is not None)),
        out_shape=tuple(shapes),
        in_specs=[vmem] * len(arrays),
        out_specs=tuple([vmem] * len(shapes)),
        scratch_shapes=scratch,
        compiler_params=pltpu.CompilerParams(collective_id=number, has_side_effects=True),
        name=name,
    )(*arrays)


LANES = 128
HEAD_UNROLL = 2


def turn(value, tables):
    return (
        value * tables[0]
        + pltpu.roll(value, LANES - HD // 4, 1) * tables[1]
        + pltpu.roll(value, HD // 4, 1) * tables[2]
    )


def turn_back(grad, tables):
    return (
        grad * tables[0]
        + pltpu.roll(grad * tables[1], HD // 4, 1)
        + pltpu.roll(grad * tables[2], LANES - HD // 4, 1)
    )


def turn_tables(length):
    quarter = HD // 4
    lane = jnp.arange(LANES)
    rates = 10000.0 ** (-(lane % quarter).astype(jnp.float32) / quarter)
    positions = jnp.arange(length)[:, None]
    place = jnp.where(lane < 2 * quarter, positions // GRID, positions % GRID)
    angle = place.astype(jnp.float32) * rates
    real = lane < HD
    early = (lane // quarter) % 2 == 0
    cosine = jnp.where(real, jnp.cos(angle), 0.0)
    sine = jnp.sin(angle)
    return jnp.stack(
        [
            cosine,
            jnp.where(real & early, -sine, 0.0),
            jnp.where(real & ~early, sine, 0.0),
        ]
    )


def unit_norm(raw):
    inverse = lax.rsqrt(jnp.sum(raw * raw, axis=-1, keepdims=True) * (1.0 / HD) + EPS)
    return raw * inverse, inverse


def project(mod, weight, raw):
    @pl.loop(0, weight.shape[0])
    def _(index):
        raw[index] = dot(mod, weight[index])


def soft(queries, keys):
    grown = jnp.exp2(dot_rt(queries, keys) * (HD ** (-0.5) / math.log(2.0)))
    return grown * (1.0 / jnp.sum(grown, axis=-1, keepdims=True))


def attend_kernel(
    count,
    mod_ref,
    tables_ref,
    gains_ref,
    weight_hbm,
    last_hbm,
    branch_out,
    mod_out,
    weight,
    last,
    mod_all,
    raw,
    mixed,
    part,
    land,
    load_sem,
    ag_send,
    ag_recv,
    rs_send,
    rs_recv,
):
    line = Line(count, [(mod_ref, mod_all)], [(part, land)], (ag_send, ag_recv), (rs_send, rs_recv))
    loads = (
        pltpu.make_async_copy(weight_hbm, weight, load_sem.at[0]),
        pltpu.make_async_copy(last_hbm, last, load_sem.at[1]),
    )
    for load in loads:
        load.start()
    line.barrier()
    line.start_own()
    mod_all[line.place] = mod_ref[...]
    for load in loads:
        load.wait()
    heads = last.shape[0] // LANES
    wide_size, wide_count = cut(last.shape[1], 384)

    def compute(item):
        project(mod_all[item], weight, raw)
        tables = (tables_ref[0], tables_ref[1], tables_ref[2])

        @pl.loop(0, heads, unroll=HEAD_UNROLL)
        def _(head):
            lanes = span(head, LANES)
            queries = turn(unit_norm(raw[0, :, lanes])[0] * gains_ref[0:1, :], tables)
            keys = turn(unit_norm(raw[1, :, lanes])[0] * gains_ref[1:2, :], tables)
            probs = soft(queries.astype(jnp.bfloat16), keys.astype(jnp.bfloat16))
            values = raw[2, :, lanes].astype(jnp.bfloat16)
            mixed[:, lanes] = dot(probs.astype(jnp.bfloat16), values).astype(jnp.bfloat16)

        @pl.loop(0, wide_count)
        def _(index):
            cols = span(index, wide_size)
            part[item, :, cols] = dot(mixed[...], last[:, cols]).astype(jnp.bfloat16)

    @pl.loop(0, count)
    def _(step):
        @pl.when(step > 0)
        def _():
            line.receive(step)

        line.each(line.far(step - 1), line.near(step), compute)

        @pl.when(step > 0)
        def _():
            line.first_sums(step)
            line.relay_sums(step)

    mod_out[...] = mod_all[...]
    line.finish(0, branch_out)
    line.drain()


def block_copy(array, target, slot, block, size, send, recv, peer):
    rows = pl.ds(pl.multiple_of(block * size, size), size)
    source = array.at[rows] if len(array.shape) == 2 else array.at[:, rows]
    return pltpu.make_async_remote_copy(
        src_ref=source,
        dst_ref=target.at[slot],
        send_sem=send,
        recv_sem=recv,
        device_id={"dp": peer},
    )


def attend_back_kernel(
    count,
    wide,
    grad_ref,
    mod_all,
    tables_ref,
    gains_ref,
    narrow_ref,
    weight_hbm,
    last_hbm,
    *rest,
):
    if wide:
        feed_hbm, back_out, weight_out, gain_out, feed_out, *rest = rest
    else:
        back_out, weight_out, gain_out, *rest = rest
    (
        weight,
        last,
        grad_all,
        raw,
        mixed,
        mixed_grad,
        raw_grad,
        kept,
        kept_mixed,
        part,
        land,
        total,
        load_sem,
        ag_send,
        ag_recv,
        rs_send,
        rs_recv,
        *rest,
    ) = rest
    line = Line(count, [(grad_ref, grad_all)], [(part, land)], (ag_send, ag_recv), (rs_send, rs_recv))
    loads = (
        pltpu.make_async_copy(weight_hbm, weight, load_sem.at[0]),
        pltpu.make_async_copy(last_hbm, last, load_sem.at[1]),
    )
    for load in loads:
        load.start()
    line.barrier(wide or 1)
    line.start_own()
    width = last.shape[1]
    here = lax.axis_index("dp")
    if wide:
        feed_land, staged, pair_land, quad_land, fs, fr, ps, pr, qs, qr = rest
        size = width // wide
        half = wide // 2
        parity, seat = lax.rem(here, 2), here // 2
        partner = here + 1 - 2 * parity

        def feed_copy(peer, slot):
            return block_copy(feed_hbm, feed_land, slot, peer, size, fs.at[peer], fr.at[slot], peer)

        def pair_copy(index):
            block = 2 * index + 1 - parity
            return block_copy(
                staged, pair_land, index, block, size, ps.at[index], pr.at[index], partner
            )

        def quad_copy(index, slot):
            block = 2 * index + parity
            return block_copy(
                staged, quad_land, slot, block, size, qs.at[index], qr.at[slot], block
            )

        @pl.loop(1, wide)
        def _(offset):
            peer = lax.rem(here + offset, wide)
            feed_copy(peer, here).start()

    grad_all[line.place] = grad_ref[...]
    total[...] = jnp.zeros_like(total)
    gain_out[...] = jnp.zeros_like(gain_out)
    for load in loads:
        load.wait()
    inner = last.shape[0]
    heads = inner // LANES
    scale = HD ** (-0.5)
    wide_size, wide_count = cut(width, 384)
    inner_size, inner_count = cut(inner, 256)
    tall_size, tall_count = cut(width, 128)
    first_width = kept.shape[2]

    def compute(item):
        project(mod_all[item], weight, raw)
        tables = (tables_ref[0], tables_ref[1], tables_ref[2])

        @pl.loop(0, inner_count)
        def _(index):
            cols = span(index, inner_size)
            mixed_grad[:, cols] = dot_rt(grad_all[item], last[cols, :]).astype(jnp.bfloat16)

        @pl.loop(0, heads, unroll=HEAD_UNROLL)
        def _(head):
            lanes = span(head, LANES)
            query_norm, query_inverse = unit_norm(raw[0, :, lanes])
            key_norm, key_inverse = unit_norm(raw[1, :, lanes])
            values = raw[2, :, lanes].astype(jnp.bfloat16)
            queries = turn(query_norm * gains_ref[0:1, :], tables).astype(jnp.bfloat16)
            keys = turn(key_norm * gains_ref[1:2, :], tables).astype(jnp.bfloat16)
            probs = soft(queries, keys)
            probs_low = probs.astype(jnp.bfloat16)
            mixed[:, lanes] = dot(probs_low, values).astype(jnp.bfloat16)
            grad = mixed_grad[:, lanes]
            prob_grad = dot_rt(grad, values)
            score_grad = (
                probs * (prob_grad - jnp.sum(probs * prob_grad, axis=-1, keepdims=True))
            ).astype(jnp.bfloat16)

            def back(which, value_grad, norm, inverse):
                turned = turn_back(value_grad, tables)
                gained = turned * norm
                gain_out[which] += jnp.sum(gained.reshape(-1, 8, LANES), axis=0)
                scaled = turned * gains_ref[which : which + 1, :]
                mean = jnp.sum(scaled * norm, axis=-1, keepdims=True) * (1.0 / HD)
                raw_grad[which, :, lanes] = (inverse * (scaled - norm * mean)).astype(
                    jnp.bfloat16
                )

            back(0, dot(score_grad, keys) * scale, query_norm, query_inverse)
            back(1, dot_lt(score_grad, queries) * scale, key_norm, key_inverse)
            raw_grad[2, :, lanes] = dot_lt(probs_low, grad).astype(jnp.bfloat16)

        @pl.loop(0, wide_count)
        def _(index):
            cols = span(index, wide_size)
            sums = dot_rt(raw_grad[0], weight[0, cols, :])
            sums += dot_rt(raw_grad[1], weight[1, cols, :])
            sums += dot_rt(raw_grad[2], weight[2, cols, :])
            part[item, :, cols] = sums.astype(jnp.bfloat16)

    def keep(item):
        one = dot(raw_grad[0], narrow_ref[0])
        two = dot(raw_grad[1], narrow_ref[1])
        three = dot(raw_grad[2], narrow_ref[2])
        side = one.shape[1] - LANES
        low = jnp.bfloat16
        kept[item, :, :side] = one[:, :side].astype(low)
        kept[item, :, side : side + LANES] = (one[:, side:] + two[:, :LANES]).astype(low)
        kept[item, :, side + LANES : 2 * side] = two[:, LANES:side].astype(low)
        kept[item, :, 2 * side : 2 * side + LANES] = (two[:, side:] + three[:, :LANES]).astype(low)
        kept[item, :, 2 * side + LANES :] = three[:, LANES:].astype(low)
        kept_mixed[item] = dot(mixed[...], narrow_ref[0]).astype(low)

    def weigh(item):
        @pl.loop(0, tall_count)
        def _(index):
            rows = span(index, tall_size)
            total[rows, :first_width] += dot_lt(mod_all[item, :, rows], kept[item])
            total[rows, first_width:] += dot_lt(grad_all[item, :, rows], kept_mixed[item])

    def work(item):
        compute(item)
        keep(item)

    @pl.loop(0, count)
    def _(step):
        @pl.when(step > 0)
        def _():
            line.each(line.far(step - 2), line.near(step - 1), weigh)
            line.receive(step)

        line.each(line.far(step - 1), line.near(step), work)

        @pl.when(step > 0)
        def _():
            line.first_sums(step)

        @pl.when(step == count - 1)
        def _():
            line.each((0, False), line.near(step), weigh)
            if wide:
                staged[...] = total[...].astype(jnp.bfloat16)

                @pl.loop(0, half)
                def _(index):
                    pair_copy(index).start()

                @pl.loop(0, half)
                def _(index):
                    pair_copy(index).wait_send()
                    pair_copy(index).wait_recv()
                    rows = pl.ds(pl.multiple_of((2 * index + parity) * size, size), size)
                    staged[rows] = (
                        staged[rows].astype(jnp.float32) + pair_land[index].astype(jnp.float32)
                    ).astype(jnp.bfloat16)

                @pl.loop(1, half)
                def _(offset):
                    quad_copy(lax.rem(seat + offset, half), seat).start()

        @pl.when(step > 0)
        def _():
            line.relay_sums(step)

    if wide:
        rows = pl.ds(pl.multiple_of(here * size, size), size)
        own = pltpu.make_async_copy(feed_hbm.at[:, rows], feed_land.at[here], load_sem.at[0])
        own.start()

        @pl.loop(1, wide)
        def _(offset):
            peer = lax.rem(here + offset, wide)
            feed_copy(peer, here).wait_send()
            feed_copy(here, peer).wait_recv()

        own.wait()
        for which in range(feed_out.shape[0]):
            total_here = feed_land[0, which].astype(jnp.float32)
            for index in range(1, wide):
                total_here += feed_land[index, which].astype(jnp.float32)
            feed_out[which] = total_here

    line.finish(0, back_out)
    line.drain()
    if wide:
        weight_out[...] = staged[rows].astype(jnp.float32)

        @pl.loop(1, half)
        def _(offset):
            index = lax.rem(seat + offset, half)
            quad_copy(index, seat).wait_send()
            quad_copy(seat, index).wait_recv()
            weight_out[...] += quad_land[index].astype(jnp.float32)

    else:
        weight_out[...] = total[...].astype(jnp.bfloat16)


def attend_arrays(project_weight, output_weight, query_gain, key_gain, length):
    inner = project_weight.shape[2]
    heads = inner // HD
    low = jnp.bfloat16
    spot = jnp.arange(heads * LANES)
    real = spot % LANES < HD
    column = spot // LANES * HD + spot % LANES
    spread = (real[None] & (column[None] == jnp.arange(inner)[:, None])).astype(low)
    window = -(-inner // LANES) * LANES
    narrow = jnp.stack(
        [
            real[:, None]
            & (column[:, None] + index * (inner % LANES) == jnp.arange(window)[None, :])
            for index in range(3)
        ]
    ).astype(low)
    weight = jnp.einsum("dke,eh->kdh", project_weight, spread, preferred_element_type=low)
    last = jnp.einsum("ed,eh->hd", output_weight, spread, preferred_element_type=low)
    pad = LANES - HD
    gains = jnp.pad(jnp.stack([query_gain, key_gain]).astype(jnp.float32), ((0, 6), (0, pad)))
    return turn_tables(length), gains, narrow, weight, last


def line_sems(count, gathers, sums):
    return [
        pltpu.SemaphoreType.DMA((2,)),
        pltpu.SemaphoreType.DMA((gathers, 2, count)),
        pltpu.SemaphoreType.DMA((gathers, 2, count)),
        pltpu.SemaphoreType.DMA((sums, 2, count, CHUNKS)),
        pltpu.SemaphoreType.DMA((sums, 2, count, CHUNKS)),
    ]


def attend_pass(mod_in, arrays):
    count = lax.axis_size("tensor")
    tables, gains, _, weight, last = arrays
    item = mod_in.shape
    inner = last.shape[0]
    vmem, any_space = pl.BlockSpec(memory_space=pltpu.VMEM), pl.BlockSpec(memory_space=pl.ANY)
    low = jnp.bfloat16
    return pl.pallas_call(
        functools.partial(attend_kernel, count),
        out_shape=(
            jax.ShapeDtypeStruct(item, jnp.float32),
            jax.ShapeDtypeStruct((count, *item), low),
        ),
        in_specs=[vmem, vmem, vmem, any_space, any_space],
        out_specs=(vmem, vmem),
        scratch_shapes=[
            pltpu.VMEM(weight.shape, low),
            pltpu.VMEM(last.shape, low),
            pltpu.VMEM((count, *item), low),
            pltpu.VMEM((3, item[0], inner), jnp.float32),
            pltpu.VMEM((item[0], inner), low),
            pltpu.VMEM((count, *item), low),
            pltpu.VMEM((count + 1, *item), low),
            *line_sems(count, 1, 1),
        ],
        compiler_params=pltpu.CompilerParams(
            collective_id=6, has_side_effects=True, vmem_limit_bytes=60000000
        ),
        name="attend_pass",
    )(mod_in, tables, gains, weight, last)


def attend_back_pass(attend_grad, mod_all, arrays, feed_weights):
    count, wide = lax.axis_size("tensor"), lax.axis_size("dp")
    tables, gains, narrow, weight, last = arrays
    item = attend_grad.shape
    length, width = item
    inner = last.shape[0]
    vmem, any_space = pl.BlockSpec(memory_space=pltpu.VMEM), pl.BlockSpec(memory_space=pl.ANY)
    low, high = jnp.bfloat16, jnp.float32
    window = narrow.shape[2]
    first_width = 3 * window - 2 * LANES
    columns = first_width + window
    if width % (16 * wide):
        wide = 0
    size = width // wide if wide else width
    outs = [
        jax.ShapeDtypeStruct(item, high),
        jax.ShapeDtypeStruct((size, columns), high if wide else low),
        jax.ShapeDtypeStruct((2, 8, LANES), high),
    ]
    scratch = [
        pltpu.VMEM(weight.shape, low),
        pltpu.VMEM(last.shape, low),
        pltpu.VMEM((count, *item), low),
        pltpu.VMEM((3, length, inner), high),
        pltpu.VMEM((length, inner), low),
        pltpu.VMEM((length, inner), low),
        pltpu.VMEM((3, length, inner), low),
        pltpu.VMEM((count, length, first_width), low),
        pltpu.VMEM((count, length, window), low),
        pltpu.VMEM((count, *item), low),
        pltpu.VMEM((count + 1, *item), low),
        pltpu.VMEM((width, columns), high),
        *line_sems(count, 1, 1),
    ]
    ins = [attend_grad, mod_all, tables, gains, narrow, weight, last]
    specs = [vmem, vmem, vmem, vmem, vmem, any_space, any_space]
    if wide:
        ins.append(feed_weights)
        specs.append(any_space)
        kinds, _, units = feed_weights.shape
        outs.append(jax.ShapeDtypeStruct((kinds, size, units), high))
        half = wide // 2
        scratch += [
            pltpu.VMEM((wide, kinds, size, units), low),
            pltpu.VMEM((width, columns), low),
            pltpu.VMEM((half, size, columns), low),
            pltpu.VMEM((half, size, columns), low),
        ]
        for number in (wide, wide, half, half, half, half):
            scratch.append(pltpu.SemaphoreType.DMA((number,)))
    results = pl.pallas_call(
        functools.partial(attend_back_kernel, count, wide),
        out_shape=tuple(outs),
        in_specs=specs,
        out_specs=tuple([vmem] * len(outs)),
        scratch_shapes=scratch,
        compiler_params=pltpu.CompilerParams(
            collective_id=7, has_side_effects=True, vmem_limit_bytes=66000000
        ),
        name="attend_back_pass",
    )(*ins)
    if wide:
        return results

    def scatter(value, axis):
        return lax.psum_scatter(value, "dp", scatter_dimension=axis, tiled=True).astype(high)

    back, weights, gain_parts = results
    return back, scatter(weights, 0), gain_parts, scatter(feed_weights, 1)


def tail_kernel(
    grads_ref,
    small_ref,
    weight_ref,
    slope_ref,
    forward_ref,
    feat_ref,
    label_ref,
    rows_ref,
    pick_ref,
    small_out,
    modulate_out,
    embed_out,
    class_out,
    time_out,
    bias_out,
    grads_land,
    grads_mine,
    grads_land_dp,
    small_one,
    small_mid,
    small_two,
    part,
    part_land,
    cond,
    cond_land,
    forward_land,
    feat_land,
    label_land,
    grads_all,
    cond_all,
    forward_all,
    feat_all,
    label_all,
    *sems,
):
    deep, wide = part_land.shape[0], cond_land.shape[0]
    items = cond.shape[0]
    axes = (("dp", wide), ("tensor", deep))
    hello = pltpu.get_barrier_semaphore()
    for axis, count in axes:
        here = lax.axis_index(axis)

        @pl.loop(1, count)
        def _(offset):
            pl.semaphore_signal(
                hello, inc=1, device_id={axis: lax.rem(here + offset, count)}
            )

    pl.semaphore_wait(hello, wide + deep - 2)
    low = jnp.bfloat16

    def exchange(number, axis, source, target, split=False):
        count = target.shape[0]
        here = lax.axis_index(axis)
        send, recv = sems[2 * number], sems[2 * number + 1]

        def copy(peer, slot):
            return pltpu.make_async_remote_copy(
                src_ref=source.at[peer] if split else source,
                dst_ref=target.at[slot],
                send_sem=send.at[peer],
                recv_sem=recv.at[slot],
                device_id={axis: peer},
            )

        def start():
            @pl.loop(1, count)
            def _(offset):
                copy(lax.rem(here + offset, count), here).start()

            target[here] = source[here] if split else source[...]

        def finish():
            @pl.loop(1, count)
            def _(offset):
                peer = lax.rem(here + offset, count)
                copy(peer, here).wait_send()
                copy(peer, peer).wait_recv()

        return start, finish

    start_grads, finish_grads = exchange(0, "tensor", grads_ref, grads_land, True)
    start_small, finish_small = exchange(1, "dp", small_ref, small_one)
    start_sums, finish_sums = exchange(2, "tensor", small_mid, small_two)
    start_part, finish_part = exchange(3, "tensor", part, part_land)
    start_mine, finish_mine = exchange(4, "dp", grads_mine, grads_land_dp)
    start_cond, finish_cond = exchange(5, "dp", cond, cond_land)
    start_forward, finish_forward = exchange(6, "dp", forward_ref, forward_land, True)
    start_feat, finish_feat = exchange(7, "dp", feat_ref, feat_land)
    start_label, finish_label = exchange(8, "dp", label_ref, label_land)

    start_grads()
    start_small()
    start_forward()
    start_feat()
    start_label()
    finish_grads()
    kinds = grads_mine.shape[0]
    for item in range(items):
        piece = grads_land[item].astype(jnp.float32)
        for kind in range(kinds):
            grads_all[kind, item : item + 1, :] = piece[kind : kind + 1, :]
    total = jnp.zeros(part.shape, jnp.float32)
    for kind in range(kinds):
        mine = grads_all[kind, :items, :].astype(low)
        grads_mine[kind] = mine
        total += dot_rt(mine, weight_ref[kind])
    part[...] = total
    start_part()
    start_mine()
    finish_small()
    small_mid[...] = small_one[0]

    @pl.loop(1, wide)
    def _(index):
        small_mid[...] += small_one[index]

    start_sums()
    finish_part()
    total = part_land[0]
    for index in range(1, deep):
        total += part_land[index]
    cond[...] = (total * slope_ref[...]).astype(low)
    start_cond()
    finish_forward()
    finish_feat()
    finish_label()
    for index in range(wide):
        rows = pl.ds(index * items, items)
        for kind in range(forward_all.shape[0]):
            forward_all[kind, rows, :] = forward_land[index, kind]
        feat_all[rows, :] = feat_land[index]
        label_all[rows, :] = label_land[index]
    finish_mine()
    for index in range(wide):
        rows = pl.ds(index * items, items)
        for kind in range(kinds):
            grads_all[kind, rows, :] = grads_land_dp[index, kind].astype(jnp.float32)
    active = forward_all[0].astype(low)
    for kind in range(kinds):
        modulate_out[kind] = dot_lt(active, grads_all[kind].astype(low))
    finish_sums()
    small_out[...] = small_two[0]

    @pl.loop(1, deep)
    def _(index):
        small_out[...] += small_two[index]

    finish_cond()
    for index in range(wide):
        cond_all[pl.ds(index * items, items), :] = cond_land[index].astype(jnp.float32)
    every = cond_all[...].astype(low)
    embed_out[...] = dot_lt(forward_all[1].astype(low), every)
    picked = dot(every, pick_ref[...]).astype(low)
    classes = class_out.shape[0]
    label = jnp.broadcast_to(label_all[:, 0:1], (label_all.shape[0], classes))
    lane = lax.broadcasted_iota(jnp.int32, label.shape, 1)
    hot = jnp.where(label == lane, 1.0, 0.0).astype(low)
    class_out[...] = dot_lt(hot, picked)
    earlier = (dot_rt(every, rows_ref[...]) * forward_all[2]).astype(low)
    time_out[...] = dot_lt(feat_all[...].astype(low), earlier)
    bias_out[0:1, :] = jnp.sum(picked.astype(jnp.float32), axis=0, keepdims=True)
    bias_out[1:2, :] = jnp.sum(earlier.astype(jnp.float32), axis=0, keepdims=True)


def tail_pass(grads, small, weight, slope, forward, feat, label, rows, pick, classes):
    deep, kinds, slab = grads.shape
    wide, parts, items, share = forward.shape
    width = weight.shape[1]
    batch = wide * items
    freq = feat.shape[1]
    low, high = jnp.bfloat16, jnp.float32
    vmem = pl.BlockSpec(memory_space=pltpu.VMEM)
    shapes = (
        (small.shape, high),
        ((kinds, share, slab), high),
        ((share, width), high),
        ((classes, share), high),
        ((freq, share), high),
        ((2, share), high),
    )
    scratch = (
        ((deep, kinds, slab), low),
        ((kinds, items, slab), low),
        ((wide, kinds, items, slab), low),
        ((wide, *small.shape), high),
        (small.shape, high),
        ((deep, *small.shape), high),
        ((items, width), high),
        ((deep, items, width), high),
        ((items, width), low),
        ((wide, items, width), low),
        (forward.shape, high),
        ((wide, items, freq), high),
        ((wide, items, LANES), jnp.int32),
        ((kinds, batch, slab), high),
        ((batch, width), high),
        ((parts, batch, share), high),
        ((batch, freq), high),
        ((batch, LANES), jnp.int32),
    )
    sems = []
    for number in (deep, wide, deep, deep, wide, wide, wide, wide, wide):
        sems += [pltpu.SemaphoreType.DMA((number,))] * 2
    return pl.pallas_call(
        tail_kernel,
        out_shape=tuple(jax.ShapeDtypeStruct(*shape) for shape in shapes),
        in_specs=[vmem] * 9,
        out_specs=tuple([vmem] * 6),
        scratch_shapes=[pltpu.VMEM(*shape) for shape in scratch] + sems,
        compiler_params=pltpu.CompilerParams(
            collective_id=3, has_side_effects=True, vmem_limit_bytes=60000000
        ),
        name="tail_pass",
    )(grads, small, weight, slope, forward, feat, label, rows, pick)


def shards(
    tokens,
    timesteps,
    labels,
    item_counts,
    cotangent,
    project_weight,
    query_gain,
    key_gain,
    output_weight,
    output_bias,
    expand_weight,
    down_weight,
    down_bias,
    modulate_weight,
    modulate_bias,
    time_weight,
    time_bias,
    embed_weight,
    embed_bias,
    class_table,
):
    local_items, length, width = tokens.shape
    items = timesteps.shape[0]
    slab = modulate_weight.shape[2]
    heads_here = project_weight.shape[2] // HD
    scale = HD ** (-0.5)
    first_item = lax.axis_index("tensor") * local_items
    live = (first_item + jnp.arange(local_items) < item_counts[0]).astype(jnp.float32)[
        :, None, None
    ]
    index = lax.axis_index("dp")
    time_feat = time_features(timesteps).astype(jnp.bfloat16)
    pre_hidden = jnp.dot(
        time_feat, time_weight, preferred_element_type=jnp.float32
    ) + time_bias.astype(jnp.float32)
    time_hidden = jax.nn.silu(pre_hidden).astype(jnp.bfloat16)
    condition = (
        jnp.dot(time_hidden, embed_weight, preferred_element_type=jnp.float32)
        + embed_bias.astype(jnp.float32)
        + jnp.take(class_table, labels, axis=0).astype(jnp.float32)
    )
    cond_act = jax.nn.silu(condition).astype(jnp.bfloat16)
    modulation_part = (
        jnp.einsum("bd,dke->bke", cond_act, modulate_weight, preferred_element_type=jnp.float32)
        + modulate_bias.astype(jnp.float32)
    ).astype(jnp.bfloat16)
    (modulation_local,) = swap("modulation_swap", 2, [(modulation_part, "tensor", True)])
    modulation_local = jnp.transpose(modulation_local, (1, 0, 2)).reshape(1, 6, width)
    modulation_local = modulation_local.astype(jnp.float32)
    local_parts = [modulation_local[:, which][:, None, :] for which in range(6)]
    attend_shift, attend_scale, attend_gate, feed_shift, feed_scale, feed_gate = local_parts
    positions = jnp.arange(length)
    token_local = tokens.astype(jnp.float32)
    normed_local, inverse_local = layer_norm(token_local)
    mod_in = normed_local * (1.0 + attend_scale) + attend_shift
    arrays = attend_arrays(project_weight, output_weight, query_gain, key_gain, length)
    attend_total, mod_all = attend_pass(mod_in[0].astype(jnp.bfloat16), arrays)
    attend_branch = attend_total[None] + output_bias.astype(jnp.float32)
    residual = token_local + attend_gate * attend_branch
    normed_two, inverse_two = layer_norm(residual)
    mod_two = (normed_two * (1.0 + feed_scale) + feed_shift).astype(jnp.bfloat16)
    out_grad = cotangent.astype(jnp.float32) * live
    branch_grad = (out_grad * feed_gate).astype(jnp.bfloat16)
    down_bias_part = jnp.sum(branch_grad.astype(jnp.float32), axis=(0, 1))
    feed_total, mod_two_grad, feed_weights = feed_pass(
        mod_two[0], branch_grad[0], expand_weight, down_weight
    )
    feed_branch = feed_total[None] + down_bias.astype(jnp.float32)
    result = (live * (residual + feed_gate * feed_branch)).astype(jnp.bfloat16)
    mod_two_grad = mod_two_grad[None]
    residual_grad = out_grad + layer_norm_back(
        normed_two, inverse_two, mod_two_grad * (1.0 + feed_scale)
    )
    attend_grad = (residual_grad * attend_gate).astype(jnp.bfloat16)
    output_bias_part = jnp.sum(attend_grad.astype(jnp.float32), axis=(0, 1))
    mod_in_grad, attend_weights, gain_parts, feed_weights = attend_back_pass(
        attend_grad[0], mod_all, arrays, feed_weights
    )
    mod_in_grad = mod_in_grad[None]
    query_gain_part, key_gain_part = jnp.sum(gain_parts, axis=1)[:, :HD]
    tokens_grad = (
        residual_grad
        + layer_norm_back(normed_local, inverse_local, mod_in_grad * (1.0 + attend_scale))
    ).astype(jnp.bfloat16)
    modulation_grad_part = jnp.stack(
        [
            jnp.sum(mod_in_grad, axis=1),
            jnp.sum(mod_in_grad * normed_local, axis=1),
            jnp.sum(residual_grad * attend_branch, axis=1),
            jnp.sum(mod_two_grad, axis=1),
            jnp.sum(mod_two_grad * normed_two, axis=1),
            jnp.sum(out_grad * feed_branch, axis=1),
        ],
        axis=1,
    )
    modulation_grad_part = modulation_grad_part[0].astype(jnp.bfloat16)
    small = jnp.concatenate(
        [
            output_bias_part,
            down_bias_part,
            modulation_grad_part.astype(jnp.float32).reshape(-1),
            query_gain_part,
            key_gain_part,
        ]
    )
    small_size = small.shape[0]
    small = jnp.pad(small, (0, -small_size % 1024)).reshape(-1, 128)
    tensor_size, wide = width // slab, lax.axis_size("dp")
    share = width // wide

    def shares(value):
        return jnp.transpose(value.astype(jnp.float32).reshape(items, wide, share), (1, 0, 2))

    def mine(value):
        return lax.dynamic_slice_in_dim(value, index * share, share, 0)

    pick = jnp.arange(width)[:, None] == index * share + jnp.arange(share)[None, :]
    small, modulate_grad, embed_grad, class_grad, time_grad, biases = tail_pass(
        jnp.transpose(modulation_grad_part.reshape(6, tensor_size, slab), (1, 0, 2)),
        small,
        jnp.transpose(modulate_weight, (1, 0, 2)),
        silu_slope(condition),
        jnp.stack([shares(cond_act), shares(time_hidden), shares(silu_slope(pre_hidden))], axis=1),
        time_feat.astype(jnp.float32),
        jnp.broadcast_to(labels[:, None], (items, LANES)),
        mine(embed_weight),
        pick.astype(jnp.bfloat16),
        class_table.shape[0],
    )
    modulate_grad = jnp.transpose(modulate_grad, (1, 0, 2))
    embed_bias_grad, time_bias_grad = biases
    small = small.reshape(-1)
    output_bias_grad = small[:width]
    down_bias_grad = small[width : 2 * width]
    modulate_bias_grad = small[2 * width : 8 * width].reshape(6, width)
    query_gain_grad = small[8 * width : 8 * width + HD]
    key_gain_grad = small[8 * width + HD : 8 * width + 2 * HD]
    inner = heads_here * HD
    first_width = attend_weights.shape[1] - -(-inner // LANES) * LANES
    project_grad = attend_weights[:, : 3 * inner].reshape(-1, 3, inner)
    output_weight_grad = attend_weights[:, first_width : first_width + inner].T
    expand_grad = jnp.transpose(feed_weights[:2], (1, 0, 2))
    down_grad = feed_weights[2].T
    return (
        result,
        tokens_grad,
        project_grad,
        query_gain_grad,
        key_gain_grad,
        output_weight_grad,
        output_bias_grad,
        expand_grad,
        down_grad,
        down_bias_grad,
        modulate_grad,
        modulate_bias_grad,
        time_grad,
        time_bias_grad,
        embed_grad,
        embed_bias_grad,
        class_grad,
    )


def solution(mesh):
    return jax.shard_map(
        shards,
        mesh=mesh,
        in_specs=(
            P(("dp", "tensor"), None, None),
            P("dp"),
            P("dp"),
            P("dp"),
            P(("dp", "tensor"), None, None),
            P(None, None, "tensor"),
            P(),
            P(),
            P("tensor", None),
            P(),
            P(None, None, "tensor"),
            P("tensor", None),
            P(),
            P(None, None, "tensor"),
            P(None, "tensor"),
            P(),
            P(),
            P(),
            P(),
            P(),
        ),
        out_specs=(
            P(("dp", "tensor"), None, None),
            P(("dp", "tensor"), None, None),
            P("dp", None, "tensor"),
            P(),
            P(),
            P("tensor", "dp"),
            P(),
            P("dp", None, "tensor"),
            P("tensor", "dp"),
            P(),
            P("dp", None, "tensor"),
            P(),
            P(None, "dp"),
            P("dp"),
            P("dp", None),
            P("dp"),
            P(None, "dp"),
        ),
        check_vma=False,
    )
```

```python
import functools
import math

import jax
import jax.numpy as jnp
from jax import lax
from jax.experimental import pallas as pl
from jax.experimental.pallas import tpu as pltpu
from jax.sharding import PartitionSpec as P

HD = 72
FREQ = 256
GRID = 16


EPS = 1e-06


def layer_norm(value):
    center = value - jnp.mean(value, axis=-1, keepdims=True)
    inverse = lax.rsqrt(jnp.mean(center * center, axis=-1, keepdims=True) + EPS)
    return (center * inverse, inverse)


def layer_norm_back(normed, inverse, grad):
    return inverse * (
        grad
        - jnp.mean(grad, axis=-1, keepdims=True)
        - normed * jnp.mean(grad * normed, axis=-1, keepdims=True)
    )


def silu_slope(value):
    sigma = jax.nn.sigmoid(value)
    return sigma * (1.0 + value * (1.0 - sigma))


def rotate(value, positions):
    quarter = HD // 4
    rates = 10000.0 ** (-jnp.arange(quarter, dtype=jnp.float32) / quarter)
    places = ((positions // GRID).astype(jnp.float32), (positions % GRID).astype(jnp.float32))
    pieces = []
    for which_half in range(2):
        half_value = value[..., which_half * 2 * quarter : (which_half + 1) * 2 * quarter]
        angle = places[which_half][:, None] * rates[None, :]
        cosine = jnp.cos(angle)[None, :, None, :]
        sine = jnp.sin(angle)[None, :, None, :]
        first = half_value[..., :quarter]
        second = half_value[..., quarter:]
        pieces.append(first * cosine - second * sine)
        pieces.append(second * cosine + first * sine)
    return jnp.concatenate(pieces, axis=-1)


def head_prepare(raw, gain, positions):
    scaled = raw * lax.rsqrt(jnp.mean(raw * raw, axis=-1, keepdims=True) + EPS) * gain
    return rotate(scaled, positions)


def time_features(steps_in):
    half = FREQ // 2
    rates = jnp.exp(-math.log(10000.0) * jnp.arange(half, dtype=jnp.float32) / half)
    angle = steps_in.astype(jnp.float32)[:, None] * rates[None, :]
    return jnp.concatenate([jnp.cos(angle), jnp.sin(angle)], axis=-1)


CHUNKS = 8


def rows_of(block, total):
    size = total // CHUNKS
    return pl.ds(pl.multiple_of(block * size, size), size)


class Line:
    def __init__(self, count, gathered, summed, ag_sems, rs_sems):
        self.count = count
        self.place = lax.axis_index("tensor")
        self.gathered = gathered
        self.summed = summed
        self.ag_send, self.ag_recv = ag_sems
        self.rs_send, self.rs_recv = rs_sems

    def barrier(self, wide=1):
        place, count = self.place, self.count
        sem = pltpu.get_barrier_semaphore()

        @pl.when(place > 0)
        def _():
            pl.semaphore_signal(sem, inc=1, device_id={"tensor": place - 1})

        @pl.when(place < count - 1)
        def _():
            pl.semaphore_signal(sem, inc=1, device_id={"tensor": place + 1})

        peers = jnp.where(place > 0, 1, 0) + jnp.where(place < count - 1, 1, 0)
        here = lax.axis_index("dp")

        @pl.loop(1, wide)
        def _(offset):
            peer = lax.rem(here + offset, wide)
            pl.semaphore_signal(sem, inc=1, device_id={"dp": peer})

        pl.semaphore_wait(sem, peers + (wide - 1))

    def item_copy(self, which, way, item, own=False):
        mine, everyone = self.gathered[which]
        target = self.place + (1 if way == 0 else -1)
        return pltpu.make_async_remote_copy(
            src_ref=mine if own else everyone.at[item],
            dst_ref=everyone.at[item],
            send_sem=self.ag_send.at[which, way, item],
            recv_sem=self.ag_recv.at[which, way, item],
            device_id={"tensor": target},
        )

    def can(self, way):
        return self.place < self.count - 1 if way == 0 else self.place > 0

    def sum_copy(self, which, way, item, block):
        part, landed = self.summed[which]
        target = self.place + (1 if way == 0 else -1)
        slot = item
        if way == 1:
            slot = jnp.where(item == target, self.count, item)
        rows = rows_of(block, part.shape[1])
        return pltpu.make_async_remote_copy(
            src_ref=part.at[item, rows],
            dst_ref=landed.at[slot, rows],
            send_sem=self.rs_send.at[which, way, item, block],
            recv_sem=self.rs_recv.at[which, way, item, block],
            device_id={"tensor": target},
        )

    def landed_slot(self, way, item):
        return jnp.where(item == self.place, self.count, item) if way == 1 else item

    def wait_sum(self, which, way, item, block):
        part, landed = self.summed[which]
        rows = rows_of(block, part.shape[1])
        view = landed.at[self.landed_slot(way, item), rows]
        pltpu.make_async_remote_copy(
            src_ref=view,
            dst_ref=view,
            send_sem=self.rs_send.at[which, way, item, block],
            recv_sem=self.rs_recv.at[which, way, item, block],
            device_id={"tensor": self.place},
        ).wait_recv()
        return view

    def start_own(self):
        for which in range(len(self.gathered)):
            for way in range(2):

                @pl.when(self.can(way))
                def _():
                    self.item_copy(which, way, self.place, own=True).start()

    def receive(self, step):
        place, count = self.place, self.count
        for which in range(len(self.gathered)):
            for way in range(2):
                item = place - step if way == 0 else place + step

                @pl.when((item >= 0) & (item < count))
                def _():
                    self.item_copy(which, way, item).wait_recv()

                    @pl.when(self.can(way))
                    def _():
                        self.item_copy(which, way, item).start()

    def items(self, step):
        place, count = self.place, self.count
        low, high = place - step, place + step
        return ((low, (low >= 0)), (high, (high < count) & (step > 0)))

    def moves(self, step):
        place, count = self.place, self.count
        return (
            (0, step, step > place, place),
            (1, count - 1 - step, count - 1 - step < place, count - 1 - place),
        )

    def first_sums(self, step, arrays=(0,)):
        @pl.loop(0, CHUNKS)
        def _(block):
            for way, item, further, hop in self.moves(step):

                @pl.when(further & (hop == 0))
                def _():
                    for which in arrays:
                        self.sum_copy(which, way, item, block).start()

    def relay_sums(self, step, arrays=(0,)):
        @pl.loop(0, CHUNKS + self.count - 3)
        def _(turn):
            for distance in range(1, self.count - 1):
                block = turn - (distance - 1)
                for way, item, further, hop in self.moves(step):

                    @pl.when(further & (hop == distance) & (block >= 0) & (block < CHUNKS))
                    def _():
                        for which in arrays:
                            part, landed = self.summed[which]
                            rows = rows_of(block, part.shape[1])
                            view = self.wait_sum(which, way, item, block)
                            total = part[item, rows].astype(jnp.float32) + view[...].astype(
                                jnp.float32
                            )
                            part[item, rows] = total.astype(part.dtype)
                            self.sum_copy(which, way, item, block).start()

    def each(self, first, second, body):
        @pl.loop(0, 2)
        def _(turn):
            item = jnp.where(turn == 0, first[0], second[0])
            valid = ((turn == 0) & first[1]) | ((turn == 1) & second[1])

            @pl.when(valid)
            def _():
                body(item)

    def near(self, step):
        place, count = self.place, self.count
        low = place >= step
        return jnp.where(low, place - step, place + step), low | (place + step < count)

    def far(self, step):
        place, count = self.place, self.count
        return place + step, (step > 0) & (place >= step) & (place + step < count)

    def finish(self, which, out):
        place, count = self.place, self.count
        part, landed = self.summed[which]

        @pl.loop(0, CHUNKS)
        def _(block):
            rows = rows_of(block, part.shape[1])
            out[rows] = part[place, rows].astype(jnp.float32)
            for way in range(2):

                @pl.when(place > 0 if way == 0 else place < count - 1)
                def _():
                    view = self.wait_sum(which, way, place, block)
                    out[rows] += view[...].astype(jnp.float32)

    def drain(self):
        place, count = self.place, self.count

        @pl.loop(0, count)
        def _(item):
            for way in range(2):
                passed = item <= place if way == 0 else item >= place

                @pl.when(passed & self.can(way))
                def _():
                    for which in range(len(self.gathered)):
                        self.item_copy(which, way, item).wait_send()

                further = item > place if way == 0 else item < place

                @pl.when(further)
                def _():
                    @pl.loop(0, CHUNKS)
                    def _(block):
                        for which in range(len(self.summed)):
                            self.sum_copy(which, way, item, block).wait_send()


def dot(left, right):
    return jnp.dot(left, right, preferred_element_type=jnp.float32)


def dot_rt(left, right):
    return lax.dot_general(
        left, right, (((1,), (1,)), ((), ())), preferred_element_type=jnp.float32
    )


def dot_lt(left, right):
    return lax.dot_general(
        left, right, (((0,), (0,)), ((), ())), preferred_element_type=jnp.float32
    )


def cut(total, most):
    size = max(s for s in range(128, most + 1, 128) if total % s == 0)
    return size, total // size


def span(index, size):
    return pl.ds(pl.multiple_of(index * size, size), size)


def feed_kernel(
    count,
    mod_ref,
    grad_ref,
    expand_hbm,
    down_hbm,
    feed_out,
    back_out,
    weight_hbm,
    expand,
    down,
    mod_all,
    grad_all,
    hidden,
    slopes,
    feed_part,
    back_part,
    feed_land,
    back_land,
    total,
    weights,
    load_sem,
    ag_send,
    ag_recv,
    rs_send,
    rs_recv,
):
    line = Line(
        count,
        [(mod_ref, mod_all), (grad_ref, grad_all)],
        [(back_part, back_land), (feed_part, feed_land)],
        (ag_send, ag_recv),
        (rs_send, rs_recv),
    )
    width, units = expand.shape[1], expand.shape[2]
    loads = (
        pltpu.make_async_copy(expand_hbm, expand, load_sem.at[0]),
        pltpu.make_async_copy(down_hbm, down, load_sem.at[1]),
    )
    for load in loads:
        load.start()
    line.barrier()
    line.start_own()
    mod_all[line.place] = mod_ref[...]
    grad_all[line.place] = grad_ref[...]
    total[...] = jnp.zeros_like(total)
    for load in loads:
        load.wait()
    unit_size, unit_count = cut(units, 256)
    wide_size, wide_count = cut(width, 384)
    tall_size, tall_count = cut(width, 128)

    def compute(item):
        @pl.loop(0, unit_count)
        def _(index):
            cols = span(index, unit_size)
            mod = mod_all[item]
            gate = dot(mod, expand[0, :, cols])
            upper = dot(mod, expand[1, :, cols])
            back = dot_rt(grad_all[item], down[cols, :])
            sigma = jax.nn.sigmoid(gate)
            active = gate * sigma
            hidden[item, :, cols] = (active * upper).astype(jnp.bfloat16)
            slopes[0, item, :, cols] = (
                back * upper * (sigma * (1.0 + gate * (1.0 - sigma)))
            ).astype(jnp.bfloat16)
            slopes[1, item, :, cols] = (back * active).astype(jnp.bfloat16)

        @pl.loop(0, wide_count)
        def _(index):
            cols = span(index, wide_size)
            back_part[item, :, cols] = (
                dot_rt(slopes[0, item], expand[0, cols, :])
                + dot_rt(slopes[1, item], expand[1, cols, :])
            ).astype(jnp.bfloat16)
            feed_part[item, :, cols] = dot(hidden[item], down[:, cols]).astype(jnp.bfloat16)

    def weigh(item):
        @pl.loop(0, tall_count)
        def _(index):
            rows = span(index, tall_size)
            mod = mod_all[item, :, rows]
            total[0, rows, :] += dot_lt(mod, slopes[0, item])
            total[1, rows, :] += dot_lt(mod, slopes[1, item])
            total[2, rows, :] += dot_lt(grad_all[item, :, rows], hidden[item])

    @pl.loop(0, count)
    def _(step):
        @pl.when(step > 0)
        def _():
            line.each(line.far(step - 1), line.near(step - 1), weigh)
            line.receive(step)

        line.each(line.far(step), line.near(step), compute)

        @pl.when(step > 0)
        def _():
            line.first_sums(step, (0, 1))
            line.relay_sums(step, (0, 1))

    line.each((0, False), line.near(count - 1), weigh)
    weights[...] = total[...].astype(jnp.bfloat16)
    store = pltpu.make_async_copy(weights, weight_hbm, load_sem.at[0])
    store.start()
    line.finish(0, back_out)
    line.finish(1, feed_out)
    line.drain()
    store.wait()


def feed_pass(mod_two, branch_grad, expand_weight, down_weight):
    count = lax.axis_size("tensor")
    length, width = mod_two.shape
    units = down_weight.shape[0]
    expand = jnp.transpose(expand_weight, (1, 0, 2))
    vmem, any_space = pl.BlockSpec(memory_space=pltpu.VMEM), pl.BlockSpec(memory_space=pl.ANY)
    low = jnp.bfloat16
    item = (length, width)
    return pl.pallas_call(
        functools.partial(feed_kernel, count),
        out_shape=(
            jax.ShapeDtypeStruct(item, jnp.float32),
            jax.ShapeDtypeStruct(item, jnp.float32),
            jax.ShapeDtypeStruct((3, width, units), low),
        ),
        in_specs=[vmem, vmem, any_space, any_space],
        out_specs=(vmem, vmem, any_space),
        scratch_shapes=[
            pltpu.VMEM((2, width, units), low),
            pltpu.VMEM((units, width), low),
            pltpu.VMEM((count, *item), low),
            pltpu.VMEM((count, *item), low),
            pltpu.VMEM((count, length, units), low),
            pltpu.VMEM((2, count, length, units), low),
            pltpu.VMEM((count, *item), low),
            pltpu.VMEM((count, *item), low),
            pltpu.VMEM((count + 1, *item), low),
            pltpu.VMEM((count + 1, *item), low),
            pltpu.VMEM((3, width, units), jnp.float32),
            pltpu.VMEM((3, width, units), low),
            *line_sems(count, 2, 2),
        ],
        compiler_params=pltpu.CompilerParams(
            collective_id=1, has_side_effects=True, vmem_limit_bytes=64000000
        ),
        name="feed_pass",
    )(mod_two, branch_grad, expand, down_weight)


def swap_kernel(jobs, total, *refs):
    n = len(jobs)
    ins, outs = refs[:n], refs[n + total : 2 * n + total]
    sems = refs[2 * n + 2 * total :]
    places = [lax.axis_index(axis) for axis, _, _ in jobs]
    hello = pltpu.get_barrier_semaphore()
    axes = []
    for axis, count, _ in jobs:
        if (axis, count) not in axes:
            axes.append((axis, count))
    if total:
        axes = [("dp", lax.axis_size("dp")), ("tensor", lax.axis_size("tensor"))]
    for axis, count in axes:
        here = lax.axis_index(axis)

        @pl.loop(1, count)
        def _(offset):
            peer = lax.rem(here + offset, count)
            pl.semaphore_signal(hello, inc=1, device_id={axis: peer})

    pl.semaphore_wait(hello, sum(count - 1 for _, count in axes))

    def copy(source, target, send, recv, axis, peer, slot):
        return pltpu.make_async_remote_copy(
            src_ref=source,
            dst_ref=target.at[slot],
            send_sem=send.at[peer],
            recv_sem=recv.at[slot],
            device_id={axis: peer},
        )

    def start(source, target, send, recv, axis, count, split):
        here = lax.axis_index(axis)

        @pl.loop(1, count)
        def _(offset):
            peer = lax.rem(here + offset, count)
            piece = source.at[peer] if split else source
            copy(piece, target, send, recv, axis, peer, here).start()

        target[here] = source[here] if split else source[...]

    def finish(source, target, send, recv, axis, count, split):
        here = lax.axis_index(axis)

        @pl.loop(1, count)
        def _(offset):
            peer = lax.rem(here + offset, count)
            piece = source.at[peer] if split else source
            step = copy(piece, target, send, recv, axis, peer, peer)
            step.wait_recv()
            step.wait_send()

    work = []
    for index, (axis, count, split) in enumerate(jobs):
        work.append((ins[index], outs[index], sems[2 * index], sems[2 * index + 1], axis, count, split))
    if total:
        source, result = refs[n], refs[2 * n + total]
        one, two, middle, s1, r1, s2, r2 = sems[2 * n :]
        wide, deep = lax.axis_size("dp"), lax.axis_size("tensor")
        first = (source, one, s1, r1, "dp", wide, False)
        start(*first)
    for job in work:
        start(*job)
    if total:
        finish(*first)
        middle[...] = one[0]

        @pl.loop(1, wide)
        def _(index):
            middle[...] += one[index]

        second = (middle, two, s2, r2, "tensor", deep, False)
        start(*second)
    for job in work:
        finish(*job)
    if total:
        finish(*second)
        result[...] = two[0]

        @pl.loop(1, deep)
        def _(index):
            result[...] += two[index]


def swap(name, number, jobs, total=None):
    vmem = pl.BlockSpec(memory_space=pltpu.VMEM)
    plan, arrays, shapes, scratch = [], [], [], []
    for array, axis, split in jobs:
        count = lax.axis_size(axis)
        plan.append((axis, count, split))
        arrays.append(array)
        piece = array.shape[1:] if split else array.shape
        shapes.append(jax.ShapeDtypeStruct((count, *piece), array.dtype))
        scratch += [pltpu.SemaphoreType.DMA((count,)), pltpu.SemaphoreType.DMA((count,))]
    if total is not None:
        wide, deep = lax.axis_size("dp"), lax.axis_size("tensor")
        arrays.append(total)
        shapes.append(jax.ShapeDtypeStruct(total.shape, total.dtype))
        scratch += [
            pltpu.VMEM((wide, *total.shape), total.dtype),
            pltpu.VMEM((deep, *total.shape), total.dtype),
            pltpu.VMEM(total.shape, total.dtype),
        ]
        for count in (wide, wide, deep, deep):
            scratch.append(pltpu.SemaphoreType.DMA((count,)))
    return pl.pallas_call(
        functools.partial(swap_kernel, tuple(plan), int(total is not None)),
        out_shape=tuple(shapes),
        in_specs=[vmem] * len(arrays),
        out_specs=tuple([vmem] * len(shapes)),
        scratch_shapes=scratch,
        compiler_params=pltpu.CompilerParams(collective_id=number, has_side_effects=True),
        name=name,
    )(*arrays)


LANES = 128
HEAD_UNROLL = 2


def turn(value, tables):
    return (
        value * tables[0]
        + pltpu.roll(value, LANES - HD // 4, 1) * tables[1]
        + pltpu.roll(value, HD // 4, 1) * tables[2]
    )


def turn_back(grad, tables):
    return (
        grad * tables[0]
        + pltpu.roll(grad * tables[1], HD // 4, 1)
        + pltpu.roll(grad * tables[2], LANES - HD // 4, 1)
    )


def turn_tables(length):
    quarter = HD // 4
    lane = jnp.arange(LANES)
    rates = 10000.0 ** (-(lane % quarter).astype(jnp.float32) / quarter)
    positions = jnp.arange(length)[:, None]
    place = jnp.where(lane < 2 * quarter, positions // GRID, positions % GRID)
    angle = place.astype(jnp.float32) * rates
    real = lane < HD
    early = (lane // quarter) % 2 == 0
    cosine = jnp.where(real, jnp.cos(angle), 0.0)
    sine = jnp.sin(angle)
    return jnp.stack(
        [
            cosine,
            jnp.where(real & early, -sine, 0.0),
            jnp.where(real & ~early, sine, 0.0),
        ]
    )


def unit_norm(raw):
    inverse = lax.rsqrt(jnp.sum(raw * raw, axis=-1, keepdims=True) * (1.0 / HD) + EPS)
    return raw * inverse, inverse


def project(mod, weight, raw):
    @pl.loop(0, weight.shape[0])
    def _(index):
        raw[index] = dot_rt(mod, weight[index])


def padded_loads(weight_hbm, last_hbm, weight, last, sem):
    heads = last.shape[0] // LANES
    loads = []
    for head in range(heads):
        rows, to = pl.ds(head * HD, HD), pl.ds(head * LANES, HD)
        rest = pl.ds(head * LANES + HD, LANES - HD)
        for part in range(3):
            weight[part, rest, :] = jnp.zeros((LANES - HD, weight.shape[2]), weight.dtype)
            loads.append(
                pltpu.make_async_copy(
                    weight_hbm.at[part, rows], weight.at[part, to], sem.at[len(loads)]
                )
            )
        last[rest, :] = jnp.zeros((LANES - HD, last.shape[1]), last.dtype)
        loads.append(pltpu.make_async_copy(last_hbm.at[rows], last.at[to], sem.at[len(loads)]))
    for load in loads:
        load.start()
    return loads


def soft(queries, keys):
    grown = jnp.exp2(dot_rt(queries, keys) * (HD ** (-0.5) / math.log(2.0)))
    return grown * (1.0 / jnp.sum(grown, axis=-1, keepdims=True))


def attend_kernel(
    count,
    mod_ref,
    tables_ref,
    gains_ref,
    weight_hbm,
    last_hbm,
    branch_out,
    mod_out,
    weight,
    last,
    mod_all,
    raw,
    mixed,
    part,
    land,
    load_sem,
    ag_send,
    ag_recv,
    rs_send,
    rs_recv,
):
    line = Line(count, [(mod_ref, mod_all)], [(part, land)], (ag_send, ag_recv), (rs_send, rs_recv))
    loads = padded_loads(weight_hbm, last_hbm, weight, last, load_sem)
    line.barrier()
    line.start_own()
    mod_all[line.place] = mod_ref[...]
    for load in loads:
        load.wait()
    heads = last.shape[0] // LANES
    wide_size, wide_count = cut(last.shape[1], 384)

    def compute(item):
        project(mod_all[item], weight, raw)
        tables = (tables_ref[0], tables_ref[1], tables_ref[2])

        @pl.loop(0, heads, unroll=HEAD_UNROLL)
        def _(head):
            lanes = span(head, LANES)
            queries = turn(unit_norm(raw[0, :, lanes])[0] * gains_ref[0:1, :], tables)
            keys = turn(unit_norm(raw[1, :, lanes])[0] * gains_ref[1:2, :], tables)
            probs = soft(queries.astype(jnp.bfloat16), keys.astype(jnp.bfloat16))
            values = raw[2, :, lanes].astype(jnp.bfloat16)
            mixed[:, lanes] = dot(probs.astype(jnp.bfloat16), values).astype(jnp.bfloat16)

        @pl.loop(0, wide_count)
        def _(index):
            cols = span(index, wide_size)
            part[item, :, cols] = dot(mixed[...], last[:, cols]).astype(jnp.bfloat16)

    @pl.loop(0, count)
    def _(step):
        @pl.when(step > 0)
        def _():
            line.receive(step)

        line.each(line.far(step - 1), line.near(step), compute)

        @pl.when(step > 0)
        def _():
            line.first_sums(step)
            line.relay_sums(step)

    mod_out[...] = mod_all[...]
    line.finish(0, branch_out)
    line.drain()


def block_copy(array, target, slot, block, size, send, recv, peer):
    rows = pl.ds(pl.multiple_of(block * size, size), size)
    source = array.at[rows] if len(array.shape) == 2 else array.at[:, rows]
    return pltpu.make_async_remote_copy(
        src_ref=source,
        dst_ref=target.at[slot],
        send_sem=send,
        recv_sem=recv,
        device_id={"dp": peer},
    )


def attend_back_kernel(
    count,
    wide,
    grad_ref,
    mod_all,
    tables_ref,
    gains_ref,
    weight_hbm,
    last_hbm,
    *rest,
):
    if wide:
        feed_hbm, back_out, weight_out, gain_out, feed_out, *rest = rest
    else:
        back_out, weight_out, gain_out, *rest = rest
    (
        weight,
        last,
        narrow,
        grad_all,
        raw,
        mixed,
        mixed_grad,
        raw_grad,
        kept,
        kept_mixed,
        part,
        land,
        total,
        load_sem,
        ag_send,
        ag_recv,
        rs_send,
        rs_recv,
        *rest,
    ) = rest
    line = Line(count, [(grad_ref, grad_all)], [(part, land)], (ag_send, ag_recv), (rs_send, rs_recv))
    loads = padded_loads(weight_hbm, last_hbm, weight, last, load_sem)
    line.barrier(wide or 1)
    line.start_own()
    width = last.shape[1]
    here = lax.axis_index("dp")
    if wide:
        feed_land, staged, pair_land, quad_land, fs, fr, ps, pr, qs, qr = rest
        size = width // wide
        half = wide // 2
        parity, seat = lax.rem(here, 2), here // 2
        partner = here + 1 - 2 * parity

        def feed_copy(peer, slot):
            return block_copy(feed_hbm, feed_land, slot, peer, size, fs.at[peer], fr.at[slot], peer)

        def pair_copy(index):
            block = 2 * index + 1 - parity
            return block_copy(
                staged, pair_land, index, block, size, ps.at[index], pr.at[index], partner
            )

        def quad_copy(index, slot):
            block = 2 * index + parity
            return block_copy(
                staged, quad_land, slot, block, size, qs.at[index], qr.at[slot], block
            )

        @pl.loop(1, wide)
        def _(offset):
            peer = lax.rem(here + offset, wide)
            feed_copy(peer, here).start()

    grad_all[line.place] = grad_ref[...]
    padded_row = lax.broadcasted_iota(jnp.int32, narrow.shape[1:], 0)
    lane = padded_row & (LANES - 1)
    column = (padded_row >> 7) * HD + lane
    target = lax.broadcasted_iota(jnp.int32, narrow.shape[1:], 1)
    offset = last.shape[0] // LANES * HD % LANES
    for part_index in range(3):
        hit = (lane < HD) & (column + part_index * offset == target)
        narrow[part_index] = jnp.where(hit, 1.0, 0.0).astype(jnp.bfloat16)
    total[...] = jnp.zeros_like(total)
    gain_out[...] = jnp.zeros_like(gain_out)
    for load in loads:
        load.wait()
    inner = last.shape[0]
    heads = inner // LANES
    scale = HD ** (-0.5)
    wide_size, wide_count = cut(width, 384)
    inner_size, inner_count = cut(inner, 256)
    tall_size, tall_count = cut(width, 128)
    first_width = kept.shape[2]

    def compute(item):
        project(mod_all[item], weight, raw)
        tables = (tables_ref[0], tables_ref[1], tables_ref[2])

        @pl.loop(0, inner_count)
        def _(index):
            cols = span(index, inner_size)
            mixed_grad[:, cols] = dot_rt(grad_all[item], last[cols, :]).astype(jnp.bfloat16)

        @pl.loop(0, heads, unroll=HEAD_UNROLL)
        def _(head):
            lanes = span(head, LANES)
            query_norm, query_inverse = unit_norm(raw[0, :, lanes])
            key_norm, key_inverse = unit_norm(raw[1, :, lanes])
            values = raw[2, :, lanes].astype(jnp.bfloat16)
            queries = turn(query_norm * gains_ref[0:1, :], tables).astype(jnp.bfloat16)
            keys = turn(key_norm * gains_ref[1:2, :], tables).astype(jnp.bfloat16)
            probs = soft(queries, keys)
            probs_low = probs.astype(jnp.bfloat16)
            mixed[:, lanes] = dot(probs_low, values).astype(jnp.bfloat16)
            grad = mixed_grad[:, lanes]
            prob_grad = dot_rt(grad, values)
            score_grad = (
                probs * (prob_grad - jnp.sum(probs * prob_grad, axis=-1, keepdims=True))
            ).astype(jnp.bfloat16)

            def back(which, value_grad, norm, inverse):
                turned = turn_back(value_grad, tables)
                gained = turned * norm
                gain_out[which] += jnp.sum(gained.reshape(-1, 8, LANES), axis=0)
                scaled = turned * gains_ref[which : which + 1, :]
                mean = jnp.sum(scaled * norm, axis=-1, keepdims=True) * (1.0 / HD)
                raw_grad[which, :, lanes] = (inverse * (scaled - norm * mean)).astype(
                    jnp.bfloat16
                )

            back(0, dot(score_grad, keys) * scale, query_norm, query_inverse)
            back(1, dot_lt(score_grad, queries) * scale, key_norm, key_inverse)
            raw_grad[2, :, lanes] = dot_lt(probs_low, grad).astype(jnp.bfloat16)

        @pl.loop(0, wide_count)
        def _(index):
            cols = span(index, wide_size)
            sums = dot(raw_grad[0], weight[0, :, cols])
            sums += dot(raw_grad[1], weight[1, :, cols])
            sums += dot(raw_grad[2], weight[2, :, cols])
            part[item, :, cols] = sums.astype(jnp.bfloat16)

    def keep(item):
        one = dot(raw_grad[0], narrow[0])
        two = dot(raw_grad[1], narrow[1])
        three = dot(raw_grad[2], narrow[2])
        side = one.shape[1] - LANES
        low = jnp.bfloat16
        kept[item, :, :side] = one[:, :side].astype(low)
        kept[item, :, side : side + LANES] = (one[:, side:] + two[:, :LANES]).astype(low)
        kept[item, :, side + LANES : 2 * side] = two[:, LANES:side].astype(low)
        kept[item, :, 2 * side : 2 * side + LANES] = (two[:, side:] + three[:, :LANES]).astype(low)
        kept[item, :, 2 * side + LANES :] = three[:, LANES:].astype(low)
        kept_mixed[item] = dot(mixed[...], narrow[0]).astype(low)

    def weigh(item):
        @pl.loop(0, tall_count)
        def _(index):
            rows = span(index, tall_size)
            total[rows, :first_width] += dot_lt(mod_all[item, :, rows], kept[item])
            total[rows, first_width:] += dot_lt(grad_all[item, :, rows], kept_mixed[item])

    def work(item):
        compute(item)
        keep(item)

    @pl.loop(0, count)
    def _(step):
        @pl.when(step > 0)
        def _():
            line.each(line.far(step - 2), line.near(step - 1), weigh)
            line.receive(step)

        line.each(line.far(step - 1), line.near(step), work)

        @pl.when(step > 0)
        def _():
            line.first_sums(step)

        @pl.when(step == count - 1)
        def _():
            line.each((0, False), line.near(step), weigh)
            if wide:
                staged[...] = total[...].astype(jnp.bfloat16)

                @pl.loop(0, half)
                def _(index):
                    pair_copy(index).start()

                @pl.loop(0, half)
                def _(index):
                    pair_copy(index).wait_send()
                    pair_copy(index).wait_recv()
                    rows = pl.ds(pl.multiple_of((2 * index + parity) * size, size), size)
                    staged[rows] = (
                        staged[rows].astype(jnp.float32) + pair_land[index].astype(jnp.float32)
                    ).astype(jnp.bfloat16)

                @pl.loop(1, half)
                def _(offset):
                    quad_copy(lax.rem(seat + offset, half), seat).start()

        @pl.when(step > 0)
        def _():
            line.relay_sums(step)

    if wide:
        rows = pl.ds(pl.multiple_of(here * size, size), size)
        own = pltpu.make_async_copy(feed_hbm.at[:, rows], feed_land.at[here], load_sem.at[0])
        own.start()

        @pl.loop(1, wide)
        def _(offset):
            peer = lax.rem(here + offset, wide)
            feed_copy(peer, here).wait_send()
            feed_copy(here, peer).wait_recv()

        own.wait()
        for which in range(feed_out.shape[0]):
            total_here = feed_land[0, which].astype(jnp.float32)
            for index in range(1, wide):
                total_here += feed_land[index, which].astype(jnp.float32)
            feed_out[which] = total_here

    line.finish(0, back_out)
    line.drain()
    if wide:
        weight_out[...] = staged[rows].astype(jnp.float32)

        @pl.loop(1, half)
        def _(offset):
            index = lax.rem(seat + offset, half)
            quad_copy(index, seat).wait_send()
            quad_copy(seat, index).wait_recv()
            weight_out[...] += quad_land[index].astype(jnp.float32)

    else:
        weight_out[...] = total[...].astype(jnp.bfloat16)


def attend_arrays(project_weight, output_weight, query_gain, key_gain, length):
    gains = jnp.stack([query_gain, key_gain]).astype(jnp.float32)
    gains = jnp.pad(gains, ((0, 6), (0, LANES - HD)))
    return turn_tables(length), gains, jnp.transpose(project_weight, (1, 2, 0)), output_weight


def line_sems(count, gathers, sums, loads=2):
    return [
        pltpu.SemaphoreType.DMA((loads,)),
        pltpu.SemaphoreType.DMA((gathers, 2, count)),
        pltpu.SemaphoreType.DMA((gathers, 2, count)),
        pltpu.SemaphoreType.DMA((sums, 2, count, CHUNKS)),
        pltpu.SemaphoreType.DMA((sums, 2, count, CHUNKS)),
    ]


def attend_pass(mod_in, arrays):
    count = lax.axis_size("tensor")
    tables, gains, weight, last = arrays
    item = mod_in.shape
    width = item[1]
    heads = last.shape[0] // HD
    inner = heads * LANES
    vmem, any_space = pl.BlockSpec(memory_space=pltpu.VMEM), pl.BlockSpec(memory_space=pl.ANY)
    low = jnp.bfloat16
    return pl.pallas_call(
        functools.partial(attend_kernel, count),
        out_shape=(
            jax.ShapeDtypeStruct(item, jnp.float32),
            jax.ShapeDtypeStruct((count, *item), low),
        ),
        in_specs=[vmem, vmem, vmem, any_space, any_space],
        out_specs=(vmem, vmem),
        scratch_shapes=[
            pltpu.VMEM((3, inner, width), low),
            pltpu.VMEM((inner, width), low),
            pltpu.VMEM((count, *item), low),
            pltpu.VMEM((3, item[0], inner), jnp.float32),
            pltpu.VMEM((item[0], inner), low),
            pltpu.VMEM((count, *item), low),
            pltpu.VMEM((count + 1, *item), low),
            *line_sems(count, 1, 1, 4 * heads),
        ],
        compiler_params=pltpu.CompilerParams(
            collective_id=6, has_side_effects=True, vmem_limit_bytes=60000000
        ),
        name="attend_pass",
    )(mod_in, tables, gains, weight, last)


def attend_back_pass(attend_grad, mod_all, arrays, feed_weights):
    count, wide = lax.axis_size("tensor"), lax.axis_size("dp")
    tables, gains, weight, last = arrays
    item = attend_grad.shape
    length, width = item
    heads = last.shape[0] // HD
    inner = heads * LANES
    vmem, any_space = pl.BlockSpec(memory_space=pltpu.VMEM), pl.BlockSpec(memory_space=pl.ANY)
    low, high = jnp.bfloat16, jnp.float32
    window = -(-last.shape[0] // LANES) * LANES
    first_width = 3 * window - 2 * LANES
    columns = first_width + window
    if width % (16 * wide):
        wide = 0
    size = width // wide if wide else width
    outs = [
        jax.ShapeDtypeStruct(item, high),
        jax.ShapeDtypeStruct((size, columns), high if wide else low),
        jax.ShapeDtypeStruct((2, 8, LANES), high),
    ]
    scratch = [
        pltpu.VMEM((3, inner, width), low),
        pltpu.VMEM((inner, width), low),
        pltpu.VMEM((3, inner, window), low),
        pltpu.VMEM((count, *item), low),
        pltpu.VMEM((3, length, inner), high),
        pltpu.VMEM((length, inner), low),
        pltpu.VMEM((length, inner), low),
        pltpu.VMEM((3, length, inner), low),
        pltpu.VMEM((count, length, first_width), low),
        pltpu.VMEM((count, length, window), low),
        pltpu.VMEM((count, *item), low),
        pltpu.VMEM((count + 1, *item), low),
        pltpu.VMEM((width, columns), high),
        *line_sems(count, 1, 1, 4 * heads),
    ]
    ins = [attend_grad, mod_all, tables, gains, weight, last]
    specs = [vmem, vmem, vmem, vmem, any_space, any_space]
    if wide:
        ins.append(feed_weights)
        specs.append(any_space)
        kinds, _, units = feed_weights.shape
        outs.append(jax.ShapeDtypeStruct((kinds, size, units), high))
        half = wide // 2
        scratch += [
            pltpu.VMEM((wide, kinds, size, units), low),
            pltpu.VMEM((width, columns), low),
            pltpu.VMEM((half, size, columns), low),
            pltpu.VMEM((half, size, columns), low),
        ]
        for number in (wide, wide, half, half, half, half):
            scratch.append(pltpu.SemaphoreType.DMA((number,)))
    results = pl.pallas_call(
        functools.partial(attend_back_kernel, count, wide),
        out_shape=tuple(outs),
        in_specs=specs,
        out_specs=tuple([vmem] * len(outs)),
        scratch_shapes=scratch,
        compiler_params=pltpu.CompilerParams(
            collective_id=7, has_side_effects=True, vmem_limit_bytes=66000000
        ),
        name="attend_back_pass",
    )(*ins)
    if wide:
        return results

    def scatter(value, axis):
        return lax.psum_scatter(value, "dp", scatter_dimension=axis, tiled=True).astype(high)

    back, weights, gain_parts = results
    return back, scatter(weights, 0), gain_parts, scatter(feed_weights, 1)


def tail_kernel(
    grads_ref,
    small_ref,
    weight_ref,
    slope_ref,
    forward_ref,
    feat_ref,
    label_ref,
    rows_hbm,
    small_out,
    modulate_out,
    embed_out,
    class_out,
    time_out,
    bias_out,
    grads_land,
    grads_mine,
    grads_land_dp,
    small_one,
    small_mid,
    small_two,
    part,
    part_land,
    cond,
    cond_land,
    forward_land,
    feat_land,
    label_land,
    grads_all,
    cond_all,
    forward_all,
    feat_all,
    label_all,
    rows,
    load_sem,
    *sems,
):
    deep, wide = part_land.shape[0], cond_land.shape[0]
    items = cond.shape[0]
    share = rows.shape[0]
    seat = lax.axis_index("dp") * share
    start_row = seat if rows_hbm.shape[0] > share else 0
    if share % 16 == 0:
        start_row = pl.multiple_of(start_row, 16)
    load = pltpu.make_async_copy(rows_hbm.at[pl.ds(start_row, share)], rows, load_sem)
    load.start()
    axes = (("dp", wide), ("tensor", deep))
    hello = pltpu.get_barrier_semaphore()
    for axis, count in axes:
        here = lax.axis_index(axis)

        @pl.loop(1, count)
        def _(offset):
            pl.semaphore_signal(
                hello, inc=1, device_id={axis: lax.rem(here + offset, count)}
            )

    pl.semaphore_wait(hello, wide + deep - 2)
    low = jnp.bfloat16

    def exchange(number, axis, source, target, split=False):
        count = target.shape[0]
        here = lax.axis_index(axis)
        send, recv = sems[2 * number], sems[2 * number + 1]

        def copy(peer, slot):
            return pltpu.make_async_remote_copy(
                src_ref=source.at[peer] if split else source,
                dst_ref=target.at[slot],
                send_sem=send.at[peer],
                recv_sem=recv.at[slot],
                device_id={axis: peer},
            )

        def start():
            @pl.loop(1, count)
            def _(offset):
                copy(lax.rem(here + offset, count), here).start()

            target[here] = source[here] if split else source[...]

        def finish():
            @pl.loop(1, count)
            def _(offset):
                peer = lax.rem(here + offset, count)
                copy(peer, here).wait_send()
                copy(peer, peer).wait_recv()

        return start, finish

    start_grads, finish_grads = exchange(0, "tensor", grads_ref, grads_land, True)
    start_small, finish_small = exchange(1, "dp", small_ref, small_one)
    start_sums, finish_sums = exchange(2, "tensor", small_mid, small_two)
    start_part, finish_part = exchange(3, "tensor", part, part_land)
    start_mine, finish_mine = exchange(4, "dp", grads_mine, grads_land_dp)
    start_cond, finish_cond = exchange(5, "dp", cond, cond_land)
    start_forward, finish_forward = exchange(6, "dp", forward_ref, forward_land, True)
    start_feat, finish_feat = exchange(7, "dp", feat_ref, feat_land)
    start_label, finish_label = exchange(8, "dp", label_ref, label_land)

    start_grads()
    start_small()
    start_forward()
    start_feat()
    start_label()
    finish_grads()
    kinds = grads_mine.shape[0]
    for item in range(items):
        piece = grads_land[item].astype(jnp.float32)
        for kind in range(kinds):
            grads_all[kind, item : item + 1, :] = piece[kind : kind + 1, :]
    total = jnp.zeros(part.shape, jnp.float32)
    for kind in range(kinds):
        mine = grads_all[kind, :items, :].astype(low)
        grads_mine[kind] = mine
        total += dot(mine, weight_ref[kind])
    part[...] = total
    start_part()
    start_mine()
    finish_small()
    small_mid[...] = small_one[0]

    @pl.loop(1, wide)
    def _(index):
        small_mid[...] += small_one[index]

    start_sums()
    finish_part()
    total = part_land[0]
    for index in range(1, deep):
        total += part_land[index]
    cond[...] = (total * slope_ref[...]).astype(low)
    start_cond()
    finish_forward()
    finish_feat()
    finish_label()
    for index in range(wide):
        batch = pl.ds(index * items, items)
        for kind in range(forward_all.shape[0]):
            forward_all[kind, batch, :] = forward_land[index, kind]
        feat_all[batch, :] = feat_land[index]
        label_all[batch, :] = label_land[index]
    finish_mine()
    for index in range(wide):
        batch = pl.ds(index * items, items)
        for kind in range(kinds):
            grads_all[kind, batch, :] = grads_land_dp[index, kind].astype(jnp.float32)
    active = forward_all[0].astype(low)
    for kind in range(kinds):
        modulate_out[kind] = dot_lt(active, grads_all[kind].astype(low))
    finish_sums()
    small_out[...] = small_two[0]

    @pl.loop(1, deep)
    def _(index):
        small_out[...] += small_two[index]

    finish_cond()
    for index in range(wide):
        cond_all[pl.ds(index * items, items), :] = cond_land[index].astype(jnp.float32)
    every = cond_all[...].astype(low)
    embed_out[...] = dot_lt(forward_all[1].astype(low), every)
    width = every.shape[1]
    spot = lax.broadcasted_iota(jnp.int32, (width, share), 0)
    pick = jnp.where(spot == seat + lax.broadcasted_iota(jnp.int32, (width, share), 1), 1.0, 0.0)
    picked = dot(every, pick.astype(low)).astype(low)
    classes = class_out.shape[1]
    label = jnp.broadcast_to(label_all[:, 0:1], (label_all.shape[0], classes))
    lane = lax.broadcasted_iota(jnp.int32, label.shape, 1)
    hot = jnp.where(label == lane, 1.0, 0.0).astype(low)
    class_out[...] = dot_lt(picked, hot)
    load.wait()
    earlier = (dot_rt(every, rows[...]) * forward_all[2]).astype(low)
    time_out[...] = dot_lt(earlier, feat_all[...].astype(low))
    bias_out[0:1, :] = jnp.sum(picked.astype(jnp.float32), axis=0, keepdims=True)
    bias_out[1:2, :] = jnp.sum(earlier.astype(jnp.float32), axis=0, keepdims=True)


def tail_pass(grads, small, weight, slope, forward, feat, label, rows, classes):
    deep, kinds, slab = grads.shape
    wide, parts, items, share = forward.shape
    width = weight.shape[2]
    batch = wide * items
    freq = feat.shape[1]
    low, high = jnp.bfloat16, jnp.float32
    vmem = pl.BlockSpec(memory_space=pltpu.VMEM)
    shapes = (
        (small.shape, high),
        ((kinds, share, slab), high),
        ((share, width), high),
        ((share, classes), high),
        ((share, freq), high),
        ((2, share), high),
    )
    scratch = (
        ((deep, kinds, slab), low),
        ((kinds, items, slab), low),
        ((wide, kinds, items, slab), low),
        ((wide, *small.shape), high),
        (small.shape, high),
        ((deep, *small.shape), high),
        ((items, width), high),
        ((deep, items, width), high),
        ((items, width), low),
        ((wide, items, width), low),
        (forward.shape, high),
        ((wide, items, freq), high),
        ((wide, items, LANES), jnp.int32),
        ((kinds, batch, slab), high),
        ((batch, width), high),
        ((parts, batch, share), high),
        ((batch, freq), high),
        ((batch, LANES), jnp.int32),
        ((share, width), low),
    )
    sems = [pltpu.SemaphoreType.DMA]
    for number in (deep, wide, deep, deep, wide, wide, wide, wide, wide):
        sems += [pltpu.SemaphoreType.DMA((number,))] * 2
    return pl.pallas_call(
        tail_kernel,
        out_shape=tuple(jax.ShapeDtypeStruct(*shape) for shape in shapes),
        in_specs=[vmem] * 7 + [pl.BlockSpec(memory_space=pl.ANY)],
        out_specs=tuple([vmem] * 6),
        scratch_shapes=[pltpu.VMEM(*shape) for shape in scratch] + sems,
        compiler_params=pltpu.CompilerParams(
            collective_id=3, has_side_effects=True, vmem_limit_bytes=60000000
        ),
        name="tail_pass",
    )(grads, small, weight, slope, forward, feat, label, rows)


def shards(
    tokens,
    timesteps,
    labels,
    item_counts,
    cotangent,
    project_weight,
    query_gain,
    key_gain,
    output_weight,
    output_bias,
    expand_weight,
    down_weight,
    down_bias,
    modulate_weight,
    modulate_bias,
    time_weight,
    time_bias,
    embed_weight,
    embed_bias,
    class_table,
):
    local_items, length, width = tokens.shape
    items = timesteps.shape[0]
    slab = modulate_weight.shape[2]
    heads_here = project_weight.shape[2] // HD
    scale = HD ** (-0.5)
    first_item = lax.axis_index("tensor") * local_items
    live = (first_item + jnp.arange(local_items) < item_counts[0]).astype(jnp.float32)[
        :, None, None
    ]
    index = lax.axis_index("dp")
    time_feat = time_features(timesteps).astype(jnp.bfloat16)
    pre_hidden = jnp.dot(
        time_feat, time_weight, preferred_element_type=jnp.float32
    ) + time_bias.astype(jnp.float32)
    time_hidden = jax.nn.silu(pre_hidden).astype(jnp.bfloat16)
    condition = (
        jnp.dot(time_hidden, embed_weight, preferred_element_type=jnp.float32)
        + embed_bias.astype(jnp.float32)
        + class_table.at[labels].get(mode="promise_in_bounds").astype(jnp.float32)
    )
    cond_act = jax.nn.silu(condition).astype(jnp.bfloat16)
    modulation_part = (
        jnp.einsum("bd,dke->bke", cond_act, modulate_weight, preferred_element_type=jnp.float32)
        + modulate_bias.astype(jnp.float32)
    ).astype(jnp.bfloat16)
    (modulation_local,) = swap("modulation_swap", 2, [(modulation_part, "tensor", True)])
    modulation_local = jnp.transpose(modulation_local, (1, 0, 2)).reshape(1, 6, width)
    modulation_local = modulation_local.astype(jnp.float32)
    local_parts = [modulation_local[:, which][:, None, :] for which in range(6)]
    attend_shift, attend_scale, attend_gate, feed_shift, feed_scale, feed_gate = local_parts
    positions = jnp.arange(length)
    token_local = tokens.astype(jnp.float32)
    normed_local, inverse_local = layer_norm(token_local)
    mod_in = normed_local * (1.0 + attend_scale) + attend_shift
    arrays = attend_arrays(project_weight, output_weight, query_gain, key_gain, length)
    attend_total, mod_all = attend_pass(mod_in[0].astype(jnp.bfloat16), arrays)
    attend_branch = attend_total[None] + output_bias.astype(jnp.float32)
    residual = token_local + attend_gate * attend_branch
    normed_two, inverse_two = layer_norm(residual)
    mod_two = (normed_two * (1.0 + feed_scale) + feed_shift).astype(jnp.bfloat16)
    out_grad = cotangent.astype(jnp.float32) * live
    branch_grad = (out_grad * feed_gate).astype(jnp.bfloat16)
    down_bias_part = jnp.sum(branch_grad.astype(jnp.float32), axis=(0, 1))
    feed_total, mod_two_grad, feed_weights = feed_pass(
        mod_two[0], branch_grad[0], expand_weight, down_weight
    )
    feed_branch = feed_total[None] + down_bias.astype(jnp.float32)
    result = (live * (residual + feed_gate * feed_branch)).astype(jnp.bfloat16)
    mod_two_grad = mod_two_grad[None]
    residual_grad = out_grad + layer_norm_back(
        normed_two, inverse_two, mod_two_grad * (1.0 + feed_scale)
    )
    attend_grad = (residual_grad * attend_gate).astype(jnp.bfloat16)
    output_bias_part = jnp.sum(attend_grad.astype(jnp.float32), axis=(0, 1))
    mod_in_grad, attend_weights, gain_parts, feed_weights = attend_back_pass(
        attend_grad[0], mod_all, arrays, feed_weights
    )
    mod_in_grad = mod_in_grad[None]
    query_gain_part, key_gain_part = jnp.sum(gain_parts, axis=1)[:, :HD]
    tokens_grad = (
        residual_grad
        + layer_norm_back(normed_local, inverse_local, mod_in_grad * (1.0 + attend_scale))
    ).astype(jnp.bfloat16)
    modulation_grad_part = jnp.stack(
        [
            jnp.sum(mod_in_grad, axis=1),
            jnp.sum(mod_in_grad * normed_local, axis=1),
            jnp.sum(residual_grad * attend_branch, axis=1),
            jnp.sum(mod_two_grad, axis=1),
            jnp.sum(mod_two_grad * normed_two, axis=1),
            jnp.sum(out_grad * feed_branch, axis=1),
        ],
        axis=1,
    )
    modulation_grad_part = modulation_grad_part[0].astype(jnp.bfloat16)
    small = jnp.concatenate(
        [
            output_bias_part,
            down_bias_part,
            modulation_grad_part.astype(jnp.float32).reshape(-1),
            query_gain_part,
            key_gain_part,
        ]
    )
    small_size = small.shape[0]
    small = jnp.pad(small, (0, -small_size % 1024)).reshape(-1, 128)
    tensor_size, wide = width // slab, lax.axis_size("dp")
    share = width // wide

    def shares(value):
        return jnp.transpose(value.astype(jnp.float32).reshape(items, wide, share), (1, 0, 2))

    rows = embed_weight
    if share % 16:
        rows = lax.dynamic_slice_in_dim(embed_weight, index * share, share, 0)
    small, modulate_grad, embed_grad, class_grad, time_grad, biases = tail_pass(
        jnp.transpose(modulation_grad_part.reshape(6, tensor_size, slab), (1, 0, 2)),
        small,
        jnp.transpose(modulate_weight, (1, 2, 0)),
        silu_slope(condition),
        jnp.stack([shares(cond_act), shares(time_hidden), shares(silu_slope(pre_hidden))], axis=1),
        time_feat.astype(jnp.float32),
        jnp.broadcast_to(labels[:, None], (items, LANES)),
        rows,
        class_table.shape[0],
    )
    class_grad, time_grad = class_grad.T, time_grad.T
    modulate_grad = jnp.transpose(modulate_grad, (1, 0, 2))
    embed_bias_grad, time_bias_grad = biases
    small = small.reshape(-1)
    output_bias_grad = small[:width]
    down_bias_grad = small[width : 2 * width]
    modulate_bias_grad = small[2 * width : 8 * width].reshape(6, width)
    query_gain_grad = small[8 * width : 8 * width + HD]
    key_gain_grad = small[8 * width + HD : 8 * width + 2 * HD]
    inner = heads_here * HD
    first_width = attend_weights.shape[1] - -(-inner // LANES) * LANES
    project_grad = attend_weights[:, : 3 * inner].reshape(-1, 3, inner)
    output_weight_grad = attend_weights[:, first_width : first_width + inner].T
    expand_grad = jnp.transpose(feed_weights[:2], (1, 0, 2))
    down_grad = feed_weights[2].T
    return (
        result,
        tokens_grad,
        project_grad,
        query_gain_grad,
        key_gain_grad,
        output_weight_grad,
        output_bias_grad,
        expand_grad,
        down_grad,
        down_bias_grad,
        modulate_grad,
        modulate_bias_grad,
        time_grad,
        time_bias_grad,
        embed_grad,
        embed_bias_grad,
        class_grad,
    )


def solution(mesh):
    return jax.shard_map(
        shards,
        mesh=mesh,
        in_specs=(
            P(("dp", "tensor"), None, None),
            P("dp"),
            P("dp"),
            P("dp"),
            P(("dp", "tensor"), None, None),
            P(None, None, "tensor"),
            P(),
            P(),
            P("tensor", None),
            P(),
            P(None, None, "tensor"),
            P("tensor", None),
            P(),
            P(None, None, "tensor"),
            P(None, "tensor"),
            P(),
            P(),
            P(),
            P(),
            P(),
        ),
        out_specs=(
            P(("dp", "tensor"), None, None),
            P(("dp", "tensor"), None, None),
            P("dp", None, "tensor"),
            P(),
            P(),
            P("tensor", "dp"),
            P(),
            P("dp", None, "tensor"),
            P("tensor", "dp"),
            P(),
            P("dp", None, "tensor"),
            P(),
            P(None, "dp"),
            P("dp"),
            P("dp", None),
            P("dp"),
            P(None, "dp"),
        ),
        check_vma=False,
    )
```

```python
import functools
import math

import jax
import jax.numpy as jnp
from jax import lax
from jax.experimental import pallas as pl
from jax.experimental.pallas import tpu as pltpu
from jax.sharding import PartitionSpec as P

HD = 72
FREQ = 256
GRID = 16


EPS = 1e-06


def layer_norm(value):
    center = value - jnp.mean(value, axis=-1, keepdims=True)
    inverse = lax.rsqrt(jnp.mean(center * center, axis=-1, keepdims=True) + EPS)
    return (center * inverse, inverse)


def layer_norm_back(normed, inverse, grad):
    return inverse * (
        grad
        - jnp.mean(grad, axis=-1, keepdims=True)
        - normed * jnp.mean(grad * normed, axis=-1, keepdims=True)
    )


def silu_slope(value):
    sigma = jax.nn.sigmoid(value)
    return sigma * (1.0 + value * (1.0 - sigma))


def time_features(steps_in):
    half = FREQ // 2
    rates = jnp.exp(-math.log(10000.0) * jnp.arange(half, dtype=jnp.float32) / half)
    angle = steps_in.astype(jnp.float32)[:, None] * rates[None, :]
    return jnp.concatenate([jnp.cos(angle), jnp.sin(angle)], axis=-1)


FEED_BLOCKS, ATTEND_BLOCKS = 8, 4


def rows_of(block, total, blocks):
    size = total // blocks
    return pl.ds(pl.multiple_of(block * size, size), size)


class Line:
    def __init__(self, count, blocks, gathered, summed, ag_sems, rs_sems):
        self.count = count
        self.blocks = blocks
        self.place = lax.axis_index("tensor")
        self.gathered = gathered
        self.summed = summed
        self.ag_send, self.ag_recv = ag_sems
        self.rs_send, self.rs_recv = rs_sems

    def barrier(self, wide=1):
        place, count = self.place, self.count
        sem = pltpu.get_barrier_semaphore()

        @pl.when(place > 0)
        def _():
            pl.semaphore_signal(sem, inc=1, device_id={"tensor": place - 1})

        @pl.when(place < count - 1)
        def _():
            pl.semaphore_signal(sem, inc=1, device_id={"tensor": place + 1})

        peers = jnp.where(place > 0, 1, 0) + jnp.where(place < count - 1, 1, 0)
        here = lax.axis_index("dp")

        @pl.loop(1, wide)
        def _(offset):
            peer = lax.rem(here + offset, wide)
            pl.semaphore_signal(sem, inc=1, device_id={"dp": peer})

        pl.semaphore_wait(sem, peers + (wide - 1))

    def item_copy(self, which, way, item, own=False):
        mine, everyone = self.gathered[which]
        target = self.place + (1 if way == 0 else -1)
        return pltpu.make_async_remote_copy(
            src_ref=mine if own else everyone.at[item],
            dst_ref=everyone.at[item],
            send_sem=self.ag_send.at[which, way, item],
            recv_sem=self.ag_recv.at[which, way, item],
            device_id={"tensor": target},
        )

    def can(self, way):
        return self.place < self.count - 1 if way == 0 else self.place > 0

    def sum_copy(self, which, way, item, block):
        part, landed = self.summed[which]
        target = self.place + (1 if way == 0 else -1)
        slot = item
        if way == 1:
            slot = jnp.where(item == target, self.count, item)
        rows = rows_of(block, part.shape[1], self.blocks)
        return pltpu.make_async_remote_copy(
            src_ref=part.at[item, rows],
            dst_ref=landed.at[slot, rows],
            send_sem=self.rs_send.at[which, way, item, block],
            recv_sem=self.rs_recv.at[which, way, item, block],
            device_id={"tensor": target},
        )

    def landed_slot(self, way, item):
        return jnp.where(item == self.place, self.count, item) if way == 1 else item

    def wait_sum(self, which, way, item, block):
        part, landed = self.summed[which]
        rows = rows_of(block, part.shape[1], self.blocks)
        view = landed.at[self.landed_slot(way, item), rows]
        pltpu.make_async_remote_copy(
            src_ref=view,
            dst_ref=view,
            send_sem=self.rs_send.at[which, way, item, block],
            recv_sem=self.rs_recv.at[which, way, item, block],
            device_id={"tensor": self.place},
        ).wait_recv()
        return view

    def start_own(self):
        for which in range(len(self.gathered)):
            for way in range(2):

                @pl.when(self.can(way))
                def _():
                    self.item_copy(which, way, self.place, own=True).start()

    def receive(self, step):
        place, count = self.place, self.count
        for which in range(len(self.gathered)):
            for way in range(2):
                item = place - step if way == 0 else place + step

                @pl.when((item >= 0) & (item < count))
                def _():
                    self.item_copy(which, way, item).wait_recv()

                    @pl.when(self.can(way))
                    def _():
                        self.item_copy(which, way, item).start()

    def items(self, step):
        place, count = self.place, self.count
        low, high = place - step, place + step
        return ((low, (low >= 0)), (high, (high < count) & (step > 0)))

    def moves(self, step):
        place, count = self.place, self.count
        return (
            (0, step, step > place, place),
            (1, count - 1 - step, count - 1 - step < place, count - 1 - place),
        )

    def first_sums(self, step, arrays=(0,)):
        @pl.loop(0, self.blocks)
        def _(block):
            for way, item, further, hop in self.moves(step):

                @pl.when(further & (hop == 0))
                def _():
                    for which in arrays:
                        self.sum_copy(which, way, item, block).start()

    def relay_sums(self, step, arrays=(0,)):
        @pl.loop(0, self.blocks + self.count - 3)
        def _(turn):
            for distance in range(1, self.count - 1):
                block = turn - (distance - 1)
                for way, item, further, hop in self.moves(step):

                    @pl.when(further & (hop == distance) & (block >= 0) & (block < self.blocks))
                    def _():
                        for which in arrays:
                            part, landed = self.summed[which]
                            rows = rows_of(block, part.shape[1], self.blocks)
                            view = self.wait_sum(which, way, item, block)
                            total = part[item, rows].astype(jnp.float32) + view[...].astype(
                                jnp.float32
                            )
                            part[item, rows] = total.astype(part.dtype)
                            self.sum_copy(which, way, item, block).start()

    def each(self, first, second, body):
        @pl.loop(0, 2)
        def _(turn):
            item = jnp.where(turn == 0, first[0], second[0])
            valid = ((turn == 0) & first[1]) | ((turn == 1) & second[1])

            @pl.when(valid)
            def _():
                body(item)

    def near(self, step):
        place, count = self.place, self.count
        low = place >= step
        return jnp.where(low, place - step, place + step), low | (place + step < count)

    def far(self, step):
        place, count = self.place, self.count
        return place + step, (step > 0) & (place >= step) & (place + step < count)

    def finish(self, which, out):
        place, count = self.place, self.count
        part, landed = self.summed[which]

        @pl.loop(0, self.blocks)
        def _(block):
            rows = rows_of(block, part.shape[1], self.blocks)
            out[rows] = part[place, rows].astype(jnp.float32)
            for way in range(2):

                @pl.when(place > 0 if way == 0 else place < count - 1)
                def _():
                    view = self.wait_sum(which, way, place, block)
                    out[rows] += view[...].astype(jnp.float32)

    def drain(self):
        place, count = self.place, self.count

        @pl.loop(0, count)
        def _(item):
            for way in range(2):
                passed = item <= place if way == 0 else item >= place

                @pl.when(passed & self.can(way))
                def _():
                    for which in range(len(self.gathered)):
                        self.item_copy(which, way, item).wait_send()

                further = item > place if way == 0 else item < place

                @pl.when(further)
                def _():
                    @pl.loop(0, self.blocks)
                    def _(block):
                        for which in range(len(self.summed)):
                            self.sum_copy(which, way, item, block).wait_send()


def dot(left, right):
    return jnp.dot(left, right, preferred_element_type=jnp.float32)


def dot_rt(left, right):
    return lax.dot_general(
        left, right, (((1,), (1,)), ((), ())), preferred_element_type=jnp.float32
    )


def dot_lt(left, right):
    return lax.dot_general(
        left, right, (((0,), (0,)), ((), ())), preferred_element_type=jnp.float32
    )


def cut(total, most):
    size = max(s for s in range(128, most + 1, 128) if total % s == 0)
    return size, total // size


def span(index, size):
    return pl.ds(pl.multiple_of(index * size, size), size)


def feed_kernel(
    count,
    mod_ref,
    grad_ref,
    expand_hbm,
    down_hbm,
    feed_out,
    back_out,
    weight_hbm,
    expand,
    down,
    mod_all,
    grad_all,
    hidden,
    slopes,
    feed_part,
    back_part,
    feed_land,
    back_land,
    total,
    weights,
    load_sem,
    ag_send,
    ag_recv,
    rs_send,
    rs_recv,
):
    line = Line(
        count,
        FEED_BLOCKS,
        [(mod_ref, mod_all), (grad_ref, grad_all)],
        [(back_part, back_land), (feed_part, feed_land)],
        (ag_send, ag_recv),
        (rs_send, rs_recv),
    )
    width, units = expand.shape[1], expand.shape[2]
    loads = (
        pltpu.make_async_copy(expand_hbm, expand, load_sem.at[0]),
        pltpu.make_async_copy(down_hbm, down, load_sem.at[1]),
    )
    for load in loads:
        load.start()
    line.barrier()
    line.start_own()
    mod_all[line.place] = mod_ref[...]
    grad_all[line.place] = grad_ref[...]
    total[...] = jnp.zeros_like(total)
    for load in loads:
        load.wait()
    unit_size, unit_count = cut(units, 256)
    wide_size, wide_count = cut(width, 384)
    tall_size, tall_count = cut(width, 128)

    def compute(item):
        @pl.loop(0, unit_count)
        def _(index):
            cols = span(index, unit_size)
            mod = mod_all[item]
            gate = dot(mod, expand[0, :, cols])
            upper = dot(mod, expand[1, :, cols])
            back = dot_rt(grad_all[item], down[cols, :])
            sigma = jax.nn.sigmoid(gate)
            active = gate * sigma
            hidden[item, :, cols] = (active * upper).astype(jnp.bfloat16)
            slopes[0, item, :, cols] = (
                back * upper * (sigma * (1.0 + gate * (1.0 - sigma)))
            ).astype(jnp.bfloat16)
            slopes[1, item, :, cols] = (back * active).astype(jnp.bfloat16)

        @pl.loop(0, wide_count)
        def _(index):
            cols = span(index, wide_size)
            back_part[item, :, cols] = (
                dot_rt(slopes[0, item], expand[0, cols, :])
                + dot_rt(slopes[1, item], expand[1, cols, :])
            ).astype(jnp.bfloat16)
            feed_part[item, :, cols] = dot(hidden[item], down[:, cols]).astype(jnp.bfloat16)

    def weigh(item):
        @pl.loop(0, tall_count)
        def _(index):
            rows = span(index, tall_size)
            mod = mod_all[item, :, rows]
            total[0, rows, :] += dot_lt(mod, slopes[0, item])
            total[1, rows, :] += dot_lt(mod, slopes[1, item])
            total[2, rows, :] += dot_lt(grad_all[item, :, rows], hidden[item])

    @pl.loop(0, count)
    def _(step):
        @pl.when(step > 0)
        def _():
            line.each(line.far(step - 1), line.near(step - 1), weigh)
            line.receive(step)

        line.each(line.far(step), line.near(step), compute)

        @pl.when(step > 0)
        def _():
            line.first_sums(step, (0, 1))
            line.relay_sums(step, (0, 1))

    line.each((0, False), line.near(count - 1), weigh)
    weights[...] = total[...].astype(jnp.bfloat16)
    store = pltpu.make_async_copy(weights, weight_hbm, load_sem.at[0])
    store.start()
    line.finish(0, back_out)
    line.finish(1, feed_out)
    line.drain()
    store.wait()


def feed_pass(mod_two, branch_grad, expand_weight, down_weight):
    count = lax.axis_size("tensor")
    length, width = mod_two.shape
    units = down_weight.shape[0]
    expand = jnp.transpose(expand_weight, (1, 0, 2))
    vmem, any_space = pl.BlockSpec(memory_space=pltpu.VMEM), pl.BlockSpec(memory_space=pl.ANY)
    low = jnp.bfloat16
    item = (length, width)
    return pl.pallas_call(
        functools.partial(feed_kernel, count),
        out_shape=(
            jax.ShapeDtypeStruct(item, jnp.float32),
            jax.ShapeDtypeStruct(item, jnp.float32),
            jax.ShapeDtypeStruct((3, width, units), low),
        ),
        in_specs=[vmem, vmem, any_space, any_space],
        out_specs=(vmem, vmem, any_space),
        scratch_shapes=[
            pltpu.VMEM((2, width, units), low),
            pltpu.VMEM((units, width), low),
            pltpu.VMEM((count, *item), low),
            pltpu.VMEM((count, *item), low),
            pltpu.VMEM((count, length, units), low),
            pltpu.VMEM((2, count, length, units), low),
            pltpu.VMEM((count, *item), low),
            pltpu.VMEM((count, *item), low),
            pltpu.VMEM((count + 1, *item), low),
            pltpu.VMEM((count + 1, *item), low),
            pltpu.VMEM((3, width, units), jnp.float32),
            pltpu.VMEM((3, width, units), low),
            *line_sems(count, FEED_BLOCKS, 2, 2),
        ],
        compiler_params=pltpu.CompilerParams(
            collective_id=1, has_side_effects=True, vmem_limit_bytes=64000000
        ),
        name="feed_pass",
    )(mod_two, branch_grad, expand, down_weight)


LANES = 128
HEAD_UNROLL = 2


def turn(value, tables):
    return (
        value * tables[0]
        + pltpu.roll(value, LANES - HD // 4, 1) * tables[1]
        + pltpu.roll(value, HD // 4, 1) * tables[2]
    )


def turn_back(grad, tables):
    return (
        grad * tables[0]
        + pltpu.roll(grad * tables[1], HD // 4, 1)
        + pltpu.roll(grad * tables[2], LANES - HD // 4, 1)
    )


def turn_tables(length):
    quarter = HD // 4
    lane = jnp.arange(LANES)
    rates = 10000.0 ** (-(lane % quarter).astype(jnp.float32) / quarter)
    positions = jnp.arange(length)[:, None]
    place = jnp.where(lane < 2 * quarter, positions // GRID, positions % GRID)
    angle = place.astype(jnp.float32) * rates
    real = lane < HD
    early = (lane // quarter) % 2 == 0
    cosine = jnp.where(real, jnp.cos(angle), 0.0)
    sine = jnp.sin(angle)
    return jnp.stack(
        [
            cosine,
            jnp.where(real & early, -sine, 0.0),
            jnp.where(real & ~early, sine, 0.0),
        ]
    )


def unit_norm(raw):
    inverse = lax.rsqrt(jnp.sum(raw * raw, axis=-1, keepdims=True) * (1.0 / HD) + EPS)
    return raw * inverse, inverse


def project(mod, weight, raw):
    @pl.loop(0, weight.shape[0])
    def _(index):
        raw[index] = dot_rt(mod, weight[index])


def padded_loads(weight_hbm, last_hbm, weight, last, sem):
    heads = last.shape[0] // LANES
    loads = []
    for head in range(heads):
        rows, to = pl.ds(head * HD, HD), pl.ds(head * LANES, HD)
        rest = pl.ds(head * LANES + HD, LANES - HD)
        for part in range(3):
            weight[part, rest, :] = jnp.zeros((LANES - HD, weight.shape[2]), weight.dtype)
            loads.append(
                pltpu.make_async_copy(
                    weight_hbm.at[part, rows], weight.at[part, to], sem.at[len(loads)]
                )
            )
        last[rest, :] = jnp.zeros((LANES - HD, last.shape[1]), last.dtype)
        loads.append(pltpu.make_async_copy(last_hbm.at[rows], last.at[to], sem.at[len(loads)]))
    for load in loads:
        load.start()
    return loads


def soft(queries, keys):
    grown = jnp.exp2(dot_rt(queries, keys) * (HD ** (-0.5) / math.log(2.0)))
    return grown * (1.0 / jnp.sum(grown, axis=-1, keepdims=True))


def attend_kernel(
    count,
    token_ref,
    slab_ref,
    tables_ref,
    gains_ref,
    weight_hbm,
    last_hbm,
    branch_out,
    mod_out,
    rows_out,
    slab_land,
    mod_own,
    weight,
    last,
    mod_all,
    raw,
    mixed,
    part,
    land,
    load_sem,
    ag_send,
    ag_recv,
    rs_send,
    rs_recv,
    slab_send,
    slab_recv,
):
    line = Line(count, ATTEND_BLOCKS, [(mod_own, mod_all)], [(part, land)], (ag_send, ag_recv), (rs_send, rs_recv))
    loads = padded_loads(weight_hbm, last_hbm, weight, last, load_sem)
    place = line.place
    hello = pltpu.get_barrier_semaphore()

    @pl.loop(1, count)
    def _(offset):
        pl.semaphore_signal(hello, inc=1, device_id={"tensor": lax.rem(place + offset, count)})

    pl.semaphore_wait(hello, count - 1)

    def slab_copy(peer, slot):
        return pltpu.make_async_remote_copy(
            src_ref=slab_ref.at[peer],
            dst_ref=slab_land.at[slot],
            send_sem=slab_send.at[peer],
            recv_sem=slab_recv.at[slot],
            device_id={"tensor": peer},
        )

    @pl.loop(1, count)
    def _(offset):
        slab_copy(lax.rem(place + offset, count), place).start()

    slab_land[place] = slab_ref[place]

    @pl.loop(1, count)
    def _(offset):
        peer = lax.rem(place + offset, count)
        slab_copy(peer, place).wait_send()
        slab_copy(peer, peer).wait_recv()

    rows_out[...] = jnp.concatenate(
        [slab_land[index].astype(jnp.float32) for index in range(count)], axis=1
    )

    @pl.loop(0, ATTEND_BLOCKS)
    def _(block):
        rows = rows_of(block, token_ref.shape[0], ATTEND_BLOCKS)
        value = token_ref[rows].astype(jnp.float32)
        center = value - jnp.mean(value, axis=-1, keepdims=True)
        inverse = lax.rsqrt(jnp.mean(center * center, axis=-1, keepdims=True) + EPS)
        mod = center * inverse * (1.0 + rows_out[1:2, :]) + rows_out[0:1, :]
        mod_own[rows] = mod.astype(jnp.bfloat16)
        mod_all[place, rows] = mod.astype(jnp.bfloat16)

    line.start_own()
    for load in loads:
        load.wait()
    heads = last.shape[0] // LANES
    wide_size, wide_count = cut(last.shape[1], 384)

    def compute(item):
        project(mod_all[item], weight, raw)
        tables = (tables_ref[0], tables_ref[1], tables_ref[2])

        @pl.loop(0, heads, unroll=HEAD_UNROLL)
        def _(head):
            lanes = span(head, LANES)
            queries = turn(unit_norm(raw[0, :, lanes])[0] * gains_ref[0:1, :], tables)
            keys = turn(unit_norm(raw[1, :, lanes])[0] * gains_ref[1:2, :], tables)
            probs = soft(queries.astype(jnp.bfloat16), keys.astype(jnp.bfloat16))
            values = raw[2, :, lanes].astype(jnp.bfloat16)
            mixed[:, lanes] = dot(probs.astype(jnp.bfloat16), values).astype(jnp.bfloat16)

        @pl.loop(0, wide_count)
        def _(index):
            cols = span(index, wide_size)
            part[item, :, cols] = dot(mixed[...], last[:, cols]).astype(jnp.bfloat16)

    @pl.loop(0, count)
    def _(step):
        @pl.when(step > 0)
        def _():
            line.receive(step)

        line.each(line.far(step - 1), line.near(step), compute)

        @pl.when(step > 0)
        def _():
            line.first_sums(step)
            line.relay_sums(step)

    mod_out[...] = mod_all[...]
    line.finish(0, branch_out)
    line.drain()


def block_copy(array, target, slot, block, size, send, recv, peer):
    rows = pl.ds(pl.multiple_of(block * size, size), size)
    source = array.at[rows] if len(array.shape) == 2 else array.at[:, rows]
    return pltpu.make_async_remote_copy(
        src_ref=source,
        dst_ref=target.at[slot],
        send_sem=send,
        recv_sem=recv,
        device_id={"dp": peer},
    )


def attend_back_kernel(
    count,
    wide,
    grad_ref,
    mod_all,
    tables_ref,
    gains_ref,
    weight_hbm,
    last_hbm,
    *rest,
):
    if wide:
        feed_hbm, back_out, weight_out, gain_out, feed_out, *rest = rest
    else:
        back_out, weight_out, gain_out, *rest = rest
    (
        weight,
        last,
        narrow,
        grad_all,
        raw,
        mixed,
        mixed_grad,
        raw_grad,
        kept,
        kept_mixed,
        part,
        land,
        total,
        load_sem,
        ag_send,
        ag_recv,
        rs_send,
        rs_recv,
        *rest,
    ) = rest
    line = Line(count, ATTEND_BLOCKS, [(grad_ref, grad_all)], [(part, land)], (ag_send, ag_recv), (rs_send, rs_recv))
    loads = padded_loads(weight_hbm, last_hbm, weight, last, load_sem)
    line.barrier(wide or 1)
    line.start_own()
    width = last.shape[1]
    here = lax.axis_index("dp")
    if wide:
        feed_land, staged, pair_land, quad_land, fs, fr, ps, pr, qs, qr = rest
        size = width // wide
        half = wide // 2
        parity, seat = lax.rem(here, 2), here // 2
        partner = here + 1 - 2 * parity

        def feed_copy(peer, slot):
            return block_copy(feed_hbm, feed_land, slot, peer, size, fs.at[peer], fr.at[slot], peer)

        def pair_copy(index):
            block = 2 * index + 1 - parity
            return block_copy(
                staged, pair_land, index, block, size, ps.at[index], pr.at[index], partner
            )

        def quad_copy(index, slot):
            block = 2 * index + parity
            return block_copy(
                staged, quad_land, slot, block, size, qs.at[index], qr.at[slot], block
            )

        @pl.loop(1, wide)
        def _(offset):
            peer = lax.rem(here + offset, wide)
            feed_copy(peer, here).start()

    grad_all[line.place] = grad_ref[...]
    padded_row = lax.broadcasted_iota(jnp.int32, narrow.shape[1:], 0)
    lane = padded_row & (LANES - 1)
    column = (padded_row >> 7) * HD + lane
    target = lax.broadcasted_iota(jnp.int32, narrow.shape[1:], 1)
    offset = last.shape[0] // LANES * HD % LANES
    for part_index in range(3):
        hit = (lane < HD) & (column + part_index * offset == target)
        narrow[part_index] = jnp.where(hit, 1.0, 0.0).astype(jnp.bfloat16)
    total[...] = jnp.zeros_like(total)
    gain_out[...] = jnp.zeros_like(gain_out)
    for load in loads:
        load.wait()
    inner = last.shape[0]
    heads = inner // LANES
    scale = HD ** (-0.5)
    wide_size, wide_count = cut(width, 384)
    inner_size, inner_count = cut(inner, 256)
    tall_size, tall_count = cut(width, 128)
    first_width = kept.shape[2]

    def compute(item):
        project(mod_all[item], weight, raw)
        tables = (tables_ref[0], tables_ref[1], tables_ref[2])

        @pl.loop(0, inner_count)
        def _(index):
            cols = span(index, inner_size)
            mixed_grad[:, cols] = dot_rt(grad_all[item], last[cols, :]).astype(jnp.bfloat16)

        @pl.loop(0, heads, unroll=HEAD_UNROLL)
        def _(head):
            lanes = span(head, LANES)
            query_norm, query_inverse = unit_norm(raw[0, :, lanes])
            key_norm, key_inverse = unit_norm(raw[1, :, lanes])
            values = raw[2, :, lanes].astype(jnp.bfloat16)
            queries = turn(query_norm * gains_ref[0:1, :], tables).astype(jnp.bfloat16)
            keys = turn(key_norm * gains_ref[1:2, :], tables).astype(jnp.bfloat16)
            probs = soft(queries, keys)
            probs_low = probs.astype(jnp.bfloat16)
            mixed[:, lanes] = dot(probs_low, values).astype(jnp.bfloat16)
            grad = mixed_grad[:, lanes]
            prob_grad = dot_rt(grad, values)
            score_grad = (
                probs * (prob_grad - jnp.sum(probs * prob_grad, axis=-1, keepdims=True))
            ).astype(jnp.bfloat16)

            def back(which, value_grad, norm, inverse):
                turned = turn_back(value_grad, tables)
                gained = turned * norm
                gain_out[which] += jnp.sum(gained.reshape(-1, 8, LANES), axis=0)
                scaled = turned * gains_ref[which : which + 1, :]
                mean = jnp.sum(scaled * norm, axis=-1, keepdims=True) * (1.0 / HD)
                raw_grad[which, :, lanes] = (inverse * (scaled - norm * mean)).astype(
                    jnp.bfloat16
                )

            back(0, dot(score_grad, keys) * scale, query_norm, query_inverse)
            back(1, dot_lt(score_grad, queries) * scale, key_norm, key_inverse)
            raw_grad[2, :, lanes] = dot_lt(probs_low, grad).astype(jnp.bfloat16)

        @pl.loop(0, wide_count)
        def _(index):
            cols = span(index, wide_size)
            sums = dot(raw_grad[0], weight[0, :, cols])
            sums += dot(raw_grad[1], weight[1, :, cols])
            sums += dot(raw_grad[2], weight[2, :, cols])
            part[item, :, cols] = sums.astype(jnp.bfloat16)

    def keep(item):
        one = dot(raw_grad[0], narrow[0])
        two = dot(raw_grad[1], narrow[1])
        three = dot(raw_grad[2], narrow[2])
        side = one.shape[1] - LANES
        low = jnp.bfloat16
        kept[item, :, :side] = one[:, :side].astype(low)
        kept[item, :, side : side + LANES] = (one[:, side:] + two[:, :LANES]).astype(low)
        kept[item, :, side + LANES : 2 * side] = two[:, LANES:side].astype(low)
        kept[item, :, 2 * side : 2 * side + LANES] = (two[:, side:] + three[:, :LANES]).astype(low)
        kept[item, :, 2 * side + LANES :] = three[:, LANES:].astype(low)
        kept_mixed[item] = dot(mixed[...], narrow[0]).astype(low)

    def weigh(item):
        @pl.loop(0, tall_count)
        def _(index):
            rows = span(index, tall_size)
            total[rows, :first_width] += dot_lt(mod_all[item, :, rows], kept[item])
            total[rows, first_width:] += dot_lt(grad_all[item, :, rows], kept_mixed[item])

    def work(item):
        compute(item)
        keep(item)

    @pl.loop(0, count)
    def _(step):
        @pl.when(step > 0)
        def _():
            line.each(line.far(step - 2), line.near(step - 1), weigh)
            line.receive(step)

        line.each(line.far(step - 1), line.near(step), work)

        @pl.when(step > 0)
        def _():
            line.first_sums(step)

        @pl.when(step == count - 1)
        def _():
            line.each((0, False), line.near(step), weigh)
            if wide:
                staged[...] = total[...].astype(jnp.bfloat16)

                @pl.loop(0, half)
                def _(index):
                    pair_copy(index).start()

                @pl.loop(0, half)
                def _(index):
                    pair_copy(index).wait_send()
                    pair_copy(index).wait_recv()
                    rows = pl.ds(pl.multiple_of((2 * index + parity) * size, size), size)
                    staged[rows] = (
                        staged[rows].astype(jnp.float32) + pair_land[index].astype(jnp.float32)
                    ).astype(jnp.bfloat16)

                @pl.loop(1, half)
                def _(offset):
                    quad_copy(lax.rem(seat + offset, half), seat).start()

        @pl.when(step > 0)
        def _():
            line.relay_sums(step)

    if wide:
        rows = pl.ds(pl.multiple_of(here * size, size), size)
        own = pltpu.make_async_copy(feed_hbm.at[:, rows], feed_land.at[here], load_sem.at[0])
        own.start()

        @pl.loop(1, wide)
        def _(offset):
            peer = lax.rem(here + offset, wide)
            feed_copy(peer, here).wait_send()
            feed_copy(here, peer).wait_recv()

        own.wait()
        for which in range(feed_out.shape[0]):
            total_here = feed_land[0, which].astype(jnp.float32)
            for index in range(1, wide):
                total_here += feed_land[index, which].astype(jnp.float32)
            feed_out[which] = total_here

    line.finish(0, back_out)
    line.drain()
    if wide:
        weight_out[...] = staged[rows].astype(jnp.float32)

        @pl.loop(1, half)
        def _(offset):
            index = lax.rem(seat + offset, half)
            quad_copy(index, seat).wait_send()
            quad_copy(seat, index).wait_recv()
            weight_out[...] += quad_land[index].astype(jnp.float32)

    else:
        weight_out[...] = total[...].astype(jnp.bfloat16)


def attend_arrays(project_weight, output_weight, query_gain, key_gain, length):
    gains = jnp.stack([query_gain, key_gain]).astype(jnp.float32)
    gains = jnp.pad(gains, ((0, 6), (0, LANES - HD)))
    return turn_tables(length), gains, jnp.transpose(project_weight, (1, 2, 0)), output_weight


def line_sems(count, blocks, gathers, sums, loads=2):
    return [
        pltpu.SemaphoreType.DMA((loads,)),
        pltpu.SemaphoreType.DMA((gathers, 2, count)),
        pltpu.SemaphoreType.DMA((gathers, 2, count)),
        pltpu.SemaphoreType.DMA((sums, 2, count, blocks)),
        pltpu.SemaphoreType.DMA((sums, 2, count, blocks)),
    ]


def attend_pass(tokens, slabs, arrays):
    count = lax.axis_size("tensor")
    tables, gains, weight, last = arrays
    item = tokens.shape
    width = item[1]
    heads = last.shape[0] // HD
    inner = heads * LANES
    vmem, any_space = pl.BlockSpec(memory_space=pltpu.VMEM), pl.BlockSpec(memory_space=pl.ANY)
    low = jnp.bfloat16
    return pl.pallas_call(
        functools.partial(attend_kernel, count),
        out_shape=(
            jax.ShapeDtypeStruct(item, jnp.float32),
            jax.ShapeDtypeStruct((count, *item), low),
            jax.ShapeDtypeStruct((slabs.shape[1], width), jnp.float32),
        ),
        in_specs=[vmem, vmem, vmem, vmem, any_space, any_space],
        out_specs=(vmem, vmem, vmem),
        scratch_shapes=[
            pltpu.VMEM(slabs.shape, low),
            pltpu.VMEM(item, low),
            pltpu.VMEM((3, inner, width), low),
            pltpu.VMEM((inner, width), low),
            pltpu.VMEM((count, *item), low),
            pltpu.VMEM((3, item[0], inner), jnp.float32),
            pltpu.VMEM((item[0], inner), low),
            pltpu.VMEM((count, *item), low),
            pltpu.VMEM((count + 1, *item), low),
            *line_sems(count, ATTEND_BLOCKS, 1, 1, 4 * heads),
            pltpu.SemaphoreType.DMA((count,)),
            pltpu.SemaphoreType.DMA((count,)),
        ],
        compiler_params=pltpu.CompilerParams(
            collective_id=6, has_side_effects=True, vmem_limit_bytes=60000000
        ),
        name="attend_pass",
    )(tokens, slabs, tables, gains, weight, last)


def attend_back_pass(attend_grad, mod_all, arrays, feed_weights):
    count, wide = lax.axis_size("tensor"), lax.axis_size("dp")
    tables, gains, weight, last = arrays
    item = attend_grad.shape
    length, width = item
    heads = last.shape[0] // HD
    inner = heads * LANES
    vmem, any_space = pl.BlockSpec(memory_space=pltpu.VMEM), pl.BlockSpec(memory_space=pl.ANY)
    low, high = jnp.bfloat16, jnp.float32
    window = -(-last.shape[0] // LANES) * LANES
    first_width = 3 * window - 2 * LANES
    columns = first_width + window
    if width % (16 * wide):
        wide = 0
    size = width // wide if wide else width
    outs = [
        jax.ShapeDtypeStruct(item, high),
        jax.ShapeDtypeStruct((size, columns), high if wide else low),
        jax.ShapeDtypeStruct((2, 8, LANES), high),
    ]
    scratch = [
        pltpu.VMEM((3, inner, width), low),
        pltpu.VMEM((inner, width), low),
        pltpu.VMEM((3, inner, window), low),
        pltpu.VMEM((count, *item), low),
        pltpu.VMEM((3, length, inner), high),
        pltpu.VMEM((length, inner), low),
        pltpu.VMEM((length, inner), low),
        pltpu.VMEM((3, length, inner), low),
        pltpu.VMEM((count, length, first_width), low),
        pltpu.VMEM((count, length, window), low),
        pltpu.VMEM((count, *item), low),
        pltpu.VMEM((count + 1, *item), low),
        pltpu.VMEM((width, columns), high),
        *line_sems(count, ATTEND_BLOCKS, 1, 1, 4 * heads),
    ]
    ins = [attend_grad, mod_all, tables, gains, weight, last]
    specs = [vmem, vmem, vmem, vmem, any_space, any_space]
    if wide:
        ins.append(feed_weights)
        specs.append(any_space)
        kinds, _, units = feed_weights.shape
        outs.append(jax.ShapeDtypeStruct((kinds, size, units), high))
        half = wide // 2
        scratch += [
            pltpu.VMEM((wide, kinds, size, units), low),
            pltpu.VMEM((width, columns), low),
            pltpu.VMEM((half, size, columns), low),
            pltpu.VMEM((half, size, columns), low),
        ]
        for number in (wide, wide, half, half, half, half):
            scratch.append(pltpu.SemaphoreType.DMA((number,)))
    results = pl.pallas_call(
        functools.partial(attend_back_kernel, count, wide),
        out_shape=tuple(outs),
        in_specs=specs,
        out_specs=tuple([vmem] * len(outs)),
        scratch_shapes=scratch,
        compiler_params=pltpu.CompilerParams(
            collective_id=7, has_side_effects=True, vmem_limit_bytes=66000000
        ),
        name="attend_back_pass",
    )(*ins)
    if wide:
        return results

    def scatter(value, axis):
        return lax.psum_scatter(value, "dp", scatter_dimension=axis, tiled=True).astype(high)

    back, weights, gain_parts = results
    return back, scatter(weights, 0), gain_parts, scatter(feed_weights, 1)


def tail_kernel(
    grads_ref,
    small_ref,
    weight_ref,
    slope_ref,
    forward_ref,
    feat_ref,
    label_ref,
    rows_hbm,
    small_out,
    modulate_out,
    embed_out,
    class_out,
    time_out,
    bias_out,
    grads_land,
    grads_mine,
    grads_land_dp,
    small_one,
    small_mid,
    small_two,
    part,
    part_land,
    cond,
    cond_land,
    forward_land,
    feat_land,
    label_land,
    grads_all,
    cond_all,
    forward_all,
    feat_all,
    label_all,
    rows,
    load_sem,
    *sems,
):
    deep, wide = part_land.shape[0], cond_land.shape[0]
    items = cond.shape[0]
    share = rows.shape[0]
    seat = lax.axis_index("dp") * share
    start_row = seat if rows_hbm.shape[0] > share else 0
    if share % 16 == 0:
        start_row = pl.multiple_of(start_row, 16)
    load = pltpu.make_async_copy(rows_hbm.at[pl.ds(start_row, share)], rows, load_sem)
    load.start()
    axes = (("dp", wide), ("tensor", deep))
    hello = pltpu.get_barrier_semaphore()
    for axis, count in axes:
        here = lax.axis_index(axis)

        @pl.loop(1, count)
        def _(offset):
            pl.semaphore_signal(
                hello, inc=1, device_id={axis: lax.rem(here + offset, count)}
            )

    pl.semaphore_wait(hello, wide + deep - 2)
    low = jnp.bfloat16

    def exchange(number, axis, source, target, split=False):
        count = target.shape[0]
        here = lax.axis_index(axis)
        send, recv = sems[2 * number], sems[2 * number + 1]

        def copy(peer, slot):
            return pltpu.make_async_remote_copy(
                src_ref=source.at[peer] if split else source,
                dst_ref=target.at[slot],
                send_sem=send.at[peer],
                recv_sem=recv.at[slot],
                device_id={axis: peer},
            )

        def start():
            @pl.loop(1, count)
            def _(offset):
                copy(lax.rem(here + offset, count), here).start()

            target[here] = source[here] if split else source[...]

        def finish():
            @pl.loop(1, count)
            def _(offset):
                peer = lax.rem(here + offset, count)
                copy(peer, here).wait_send()
                copy(peer, peer).wait_recv()

        return start, finish

    start_grads, finish_grads = exchange(0, "tensor", grads_ref, grads_land, True)
    start_small, finish_small = exchange(1, "dp", small_ref, small_one)
    start_sums, finish_sums = exchange(2, "tensor", small_mid, small_two)
    start_part, finish_part = exchange(3, "tensor", part, part_land)
    start_mine, finish_mine = exchange(4, "dp", grads_mine, grads_land_dp)
    start_cond, finish_cond = exchange(5, "dp", cond, cond_land)
    start_forward, finish_forward = exchange(6, "dp", forward_ref, forward_land, True)
    start_feat, finish_feat = exchange(7, "dp", feat_ref, feat_land)
    start_label, finish_label = exchange(8, "dp", label_ref, label_land)

    start_grads()
    start_small()
    start_forward()
    start_feat()
    start_label()
    finish_grads()
    kinds = grads_mine.shape[0]
    for item in range(items):
        piece = grads_land[item].astype(jnp.float32)
        for kind in range(kinds):
            grads_all[kind, item : item + 1, :] = piece[kind : kind + 1, :]
    total = jnp.zeros(part.shape, jnp.float32)
    for kind in range(kinds):
        mine = grads_all[kind, :items, :].astype(low)
        grads_mine[kind] = mine
        total += dot(mine, weight_ref[kind])
    part[...] = total
    start_part()
    start_mine()
    finish_small()
    small_mid[...] = small_one[0]

    @pl.loop(1, wide)
    def _(index):
        small_mid[...] += small_one[index]

    start_sums()
    finish_part()
    total = part_land[0]
    for index in range(1, deep):
        total += part_land[index]
    cond[...] = (total * slope_ref[...]).astype(low)
    start_cond()
    finish_forward()
    finish_feat()
    finish_label()
    for index in range(wide):
        batch = pl.ds(index * items, items)
        for kind in range(forward_all.shape[0]):
            forward_all[kind, batch, :] = forward_land[index, kind]
        feat_all[batch, :] = feat_land[index].astype(jnp.float32)
        label_all[batch, :] = label_land[index]
    finish_mine()
    for index in range(wide):
        batch = pl.ds(index * items, items)
        for kind in range(kinds):
            grads_all[kind, batch, :] = grads_land_dp[index, kind].astype(jnp.float32)
    active = forward_all[0].astype(low)
    for kind in range(kinds):
        modulate_out[kind] = dot_lt(active, grads_all[kind].astype(low))
    finish_sums()
    small_out[...] = small_two[0]

    @pl.loop(1, deep)
    def _(index):
        small_out[...] += small_two[index]

    finish_cond()
    for index in range(wide):
        cond_all[pl.ds(index * items, items), :] = cond_land[index].astype(jnp.float32)
    every = cond_all[...].astype(low)
    embed_out[...] = dot_lt(forward_all[1].astype(low), every)
    width = every.shape[1]
    spot = lax.broadcasted_iota(jnp.int32, (width, share), 0)
    pick = jnp.where(spot == seat + lax.broadcasted_iota(jnp.int32, (width, share), 1), 1.0, 0.0)
    picked = dot(every, pick.astype(low)).astype(low)
    classes = class_out.shape[1]
    label = jnp.broadcast_to(label_all[:, 0:1], (label_all.shape[0], classes))
    lane = lax.broadcasted_iota(jnp.int32, label.shape, 1)
    hot = jnp.where(label == lane, 1.0, 0.0).astype(low)
    class_out[...] = dot_lt(picked, hot)
    load.wait()
    earlier = (dot_rt(every, rows[...]) * forward_all[2]).astype(low)
    time_out[...] = dot_lt(earlier, feat_all[...].astype(low))
    bias_out[0:1, :] = jnp.sum(picked.astype(jnp.float32), axis=0, keepdims=True)
    bias_out[1:2, :] = jnp.sum(earlier.astype(jnp.float32), axis=0, keepdims=True)


def tail_pass(grads, small, weight, slope, forward, feat, label, rows, classes):
    deep, kinds, slab = grads.shape
    wide, parts, items, share = forward.shape
    width = weight.shape[2]
    batch = wide * items
    freq = feat.shape[1]
    low, high = jnp.bfloat16, jnp.float32
    vmem = pl.BlockSpec(memory_space=pltpu.VMEM)
    shapes = (
        (small.shape, high),
        ((kinds, share, slab), high),
        ((share, width), high),
        ((share, classes), high),
        ((share, freq), high),
        ((2, share), high),
    )
    scratch = (
        ((deep, kinds, slab), low),
        ((kinds, items, slab), low),
        ((wide, kinds, items, slab), low),
        ((wide, *small.shape), high),
        (small.shape, high),
        ((deep, *small.shape), high),
        ((items, width), high),
        ((deep, items, width), high),
        ((items, width), low),
        ((wide, items, width), low),
        (forward.shape, high),
        ((wide, items, freq), low),
        ((wide, items, LANES), jnp.int32),
        ((kinds, batch, slab), high),
        ((batch, width), high),
        ((parts, batch, share), high),
        ((batch, freq), high),
        ((batch, LANES), jnp.int32),
        ((share, width), low),
    )
    sems = [pltpu.SemaphoreType.DMA]
    for number in (deep, wide, deep, deep, wide, wide, wide, wide, wide):
        sems += [pltpu.SemaphoreType.DMA((number,))] * 2
    return pl.pallas_call(
        tail_kernel,
        out_shape=tuple(jax.ShapeDtypeStruct(*shape) for shape in shapes),
        in_specs=[vmem] * 7 + [pl.BlockSpec(memory_space=pl.ANY)],
        out_specs=tuple([vmem] * 6),
        scratch_shapes=[pltpu.VMEM(*shape) for shape in scratch] + sems,
        compiler_params=pltpu.CompilerParams(
            collective_id=3, has_side_effects=True, vmem_limit_bytes=60000000
        ),
        name="tail_pass",
    )(grads, small, weight, slope, forward, feat, label, rows)


def shards(
    tokens,
    timesteps,
    labels,
    item_counts,
    cotangent,
    project_weight,
    query_gain,
    key_gain,
    output_weight,
    output_bias,
    expand_weight,
    down_weight,
    down_bias,
    modulate_weight,
    modulate_bias,
    time_weight,
    time_bias,
    embed_weight,
    embed_bias,
    class_table,
):
    local_items, length, width = tokens.shape
    items = timesteps.shape[0]
    slab = modulate_weight.shape[2]
    heads_here = project_weight.shape[2] // HD
    first_item = lax.axis_index("tensor") * local_items
    live = (first_item + jnp.arange(local_items) < item_counts[0]).astype(jnp.float32)[
        :, None, None
    ]
    index = lax.axis_index("dp")
    time_feat = time_features(timesteps).astype(jnp.bfloat16)
    pre_hidden = jnp.dot(
        time_feat, time_weight, preferred_element_type=jnp.float32
    ) + time_bias.astype(jnp.float32)
    time_hidden = jax.nn.silu(pre_hidden).astype(jnp.bfloat16)
    condition = (
        jnp.dot(time_hidden, embed_weight, preferred_element_type=jnp.float32)
        + embed_bias.astype(jnp.float32)
        + class_table.at[labels].get(mode="promise_in_bounds").astype(jnp.float32)
    )
    cond_act = jax.nn.silu(condition).astype(jnp.bfloat16)
    modulation_part = (
        jnp.einsum("bd,dke->bke", cond_act, modulate_weight, preferred_element_type=jnp.float32)
        + modulate_bias.astype(jnp.float32)
    ).astype(jnp.bfloat16)
    arrays = attend_arrays(project_weight, output_weight, query_gain, key_gain, length)
    attend_total, mod_all, modulation = attend_pass(tokens[0], modulation_part, arrays)
    _, attend_scale, attend_gate, feed_shift, feed_scale, feed_gate = [
        modulation[which][None, None, :] for which in range(6)
    ]
    token_local = tokens.astype(jnp.float32)
    normed_local, inverse_local = layer_norm(token_local)
    attend_branch = attend_total[None] + output_bias.astype(jnp.float32)
    residual = token_local + attend_gate * attend_branch
    normed_two, inverse_two = layer_norm(residual)
    mod_two = (normed_two * (1.0 + feed_scale) + feed_shift).astype(jnp.bfloat16)
    out_grad = cotangent.astype(jnp.float32) * live
    branch_grad = (out_grad * feed_gate).astype(jnp.bfloat16)
    down_bias_part = jnp.sum(branch_grad.astype(jnp.float32), axis=(0, 1))
    feed_total, mod_two_grad, feed_weights = feed_pass(
        mod_two[0], branch_grad[0], expand_weight, down_weight
    )
    feed_branch = feed_total[None] + down_bias.astype(jnp.float32)
    result = (live * (residual + feed_gate * feed_branch)).astype(jnp.bfloat16)
    mod_two_grad = mod_two_grad[None]
    residual_grad = out_grad + layer_norm_back(
        normed_two, inverse_two, mod_two_grad * (1.0 + feed_scale)
    )
    attend_grad = (residual_grad * attend_gate).astype(jnp.bfloat16)
    output_bias_part = jnp.sum(attend_grad.astype(jnp.float32), axis=(0, 1))
    mod_in_grad, attend_weights, gain_parts, feed_weights = attend_back_pass(
        attend_grad[0], mod_all, arrays, feed_weights
    )
    mod_in_grad = mod_in_grad[None]
    query_gain_part, key_gain_part = jnp.sum(gain_parts, axis=1)[:, :HD]
    tokens_grad = (
        residual_grad
        + layer_norm_back(normed_local, inverse_local, mod_in_grad * (1.0 + attend_scale))
    ).astype(jnp.bfloat16)
    modulation_grad_part = jnp.stack(
        [
            jnp.sum(mod_in_grad, axis=1),
            jnp.sum(mod_in_grad * normed_local, axis=1),
            jnp.sum(residual_grad * attend_branch, axis=1),
            jnp.sum(mod_two_grad, axis=1),
            jnp.sum(mod_two_grad * normed_two, axis=1),
            jnp.sum(out_grad * feed_branch, axis=1),
        ],
        axis=1,
    )
    modulation_grad_part = modulation_grad_part[0].astype(jnp.bfloat16)
    gain_row = jnp.pad(
        jnp.concatenate([query_gain_part, key_gain_part])[None], ((0, 0), (0, width - 2 * HD))
    )
    small = jnp.concatenate(
        [
            output_bias_part[None],
            down_bias_part[None],
            modulation_grad_part.astype(jnp.float32),
            gain_row,
        ]
    )
    tensor_size, wide = width // slab, lax.axis_size("dp")
    share = width // wide

    def shares(value):
        return jnp.transpose(value.astype(jnp.float32).reshape(items, wide, share), (1, 0, 2))

    rows = embed_weight
    if share % 16:
        rows = lax.dynamic_slice_in_dim(embed_weight, index * share, share, 0)
    small, modulate_grad, embed_grad, class_grad, time_grad, biases = tail_pass(
        jnp.transpose(modulation_grad_part.reshape(6, tensor_size, slab), (1, 0, 2)),
        small,
        jnp.transpose(modulate_weight, (1, 2, 0)),
        silu_slope(condition),
        jnp.stack([shares(cond_act), shares(time_hidden), shares(silu_slope(pre_hidden))], axis=1),
        time_feat,
        jnp.broadcast_to(labels[:, None], (items, LANES)),
        rows,
        class_table.shape[0],
    )
    class_grad, time_grad = class_grad.T, time_grad.T
    modulate_grad = jnp.transpose(modulate_grad, (1, 0, 2))
    embed_bias_grad, time_bias_grad = biases
    output_bias_grad, down_bias_grad = small[0], small[1]
    modulate_bias_grad = small[2:8]
    query_gain_grad, key_gain_grad = small[8, :HD], small[8, HD : 2 * HD]
    inner = heads_here * HD
    first_width = attend_weights.shape[1] - -(-inner // LANES) * LANES
    project_grad = attend_weights[:, : 3 * inner].reshape(-1, 3, inner)
    output_weight_grad = attend_weights[:, first_width : first_width + inner].T
    expand_grad = jnp.transpose(feed_weights[:2], (1, 0, 2))
    down_grad = feed_weights[2].T
    return (
        result,
        tokens_grad,
        project_grad,
        query_gain_grad,
        key_gain_grad,
        output_weight_grad,
        output_bias_grad,
        expand_grad,
        down_grad,
        down_bias_grad,
        modulate_grad,
        modulate_bias_grad,
        time_grad,
        time_bias_grad,
        embed_grad,
        embed_bias_grad,
        class_grad,
    )


def solution(mesh):
    return jax.shard_map(
        shards,
        mesh=mesh,
        in_specs=(
            P(("dp", "tensor"), None, None),
            P("dp"),
            P("dp"),
            P("dp"),
            P(("dp", "tensor"), None, None),
            P(None, None, "tensor"),
            P(),
            P(),
            P("tensor", None),
            P(),
            P(None, None, "tensor"),
            P("tensor", None),
            P(),
            P(None, None, "tensor"),
            P(None, "tensor"),
            P(),
            P(),
            P(),
            P(),
            P(),
        ),
        out_specs=(
            P(("dp", "tensor"), None, None),
            P(("dp", "tensor"), None, None),
            P("dp", None, "tensor"),
            P(),
            P(),
            P("tensor", "dp"),
            P(),
            P("dp", None, "tensor"),
            P("tensor", "dp"),
            P(),
            P("dp", None, "tensor"),
            P(),
            P(None, "dp"),
            P("dp"),
            P("dp", None),
            P("dp"),
            P(None, "dp"),
        ),
        check_vma=False,
    )
```

```python
import functools
import math

import jax
import jax.numpy as jnp
from jax import lax
from jax.experimental import pallas as pl
from jax.experimental.pallas import tpu as pltpu
from jax.sharding import PartitionSpec as P

HD = 72
FREQ = 256
GRID = 16


EPS = 1e-06


def layer_norm(value):
    center = value - jnp.mean(value, axis=-1, keepdims=True)
    inverse = lax.rsqrt(jnp.mean(center * center, axis=-1, keepdims=True) + EPS)
    return (center * inverse, inverse)


def layer_norm_back(normed, inverse, grad):
    return inverse * (
        grad
        - jnp.mean(grad, axis=-1, keepdims=True)
        - normed * jnp.mean(grad * normed, axis=-1, keepdims=True)
    )


def silu_slope(value):
    sigma = jax.nn.sigmoid(value)
    return sigma * (1.0 + value * (1.0 - sigma))


def time_features(steps_in):
    half = FREQ // 2
    rates = jnp.exp(-math.log(10000.0) * jnp.arange(half, dtype=jnp.float32) / half)
    angle = steps_in.astype(jnp.float32)[:, None] * rates[None, :]
    return jnp.concatenate([jnp.cos(angle), jnp.sin(angle)], axis=-1)


FEED_BLOCKS, ATTEND_BLOCKS = 8, 4


def rows_of(block, total, blocks):
    size = total // blocks
    return pl.ds(pl.multiple_of(block * size, size), size)


class Line:
    def __init__(self, count, blocks, gathered, summed, ag_sems, rs_sems):
        self.count = count
        self.blocks = blocks
        self.place = lax.axis_index("tensor")
        self.gathered = gathered
        self.summed = summed
        self.ag_send, self.ag_recv = ag_sems
        self.rs_send, self.rs_recv = rs_sems

    def barrier(self, wide=1):
        place, count = self.place, self.count
        sem = pltpu.get_barrier_semaphore()

        @pl.when(place > 0)
        def _():
            pl.semaphore_signal(sem, inc=1, device_id={"tensor": place - 1})

        @pl.when(place < count - 1)
        def _():
            pl.semaphore_signal(sem, inc=1, device_id={"tensor": place + 1})

        peers = jnp.where(place > 0, 1, 0) + jnp.where(place < count - 1, 1, 0)
        here = lax.axis_index("dp")

        @pl.loop(1, wide)
        def _(offset):
            peer = lax.rem(here + offset, wide)
            pl.semaphore_signal(sem, inc=1, device_id={"dp": peer})

        pl.semaphore_wait(sem, peers + (wide - 1))

    def item_copy(self, which, way, item, own=False):
        mine, everyone = self.gathered[which]
        target = self.place + (1 if way == 0 else -1)
        return pltpu.make_async_remote_copy(
            src_ref=mine if own else everyone.at[item],
            dst_ref=everyone.at[item],
            send_sem=self.ag_send.at[which, way, item],
            recv_sem=self.ag_recv.at[which, way, item],
            device_id={"tensor": target},
        )

    def can(self, way):
        return self.place < self.count - 1 if way == 0 else self.place > 0

    def sum_copy(self, which, way, item, block):
        part, landed = self.summed[which]
        target = self.place + (1 if way == 0 else -1)
        slot = item
        if way == 1:
            slot = jnp.where(item == target, self.count, item)
        rows = rows_of(block, part.shape[1], self.blocks)
        return pltpu.make_async_remote_copy(
            src_ref=part.at[item, rows],
            dst_ref=landed.at[slot, rows],
            send_sem=self.rs_send.at[which, way, item, block],
            recv_sem=self.rs_recv.at[which, way, item, block],
            device_id={"tensor": target},
        )

    def landed_slot(self, way, item):
        return jnp.where(item == self.place, self.count, item) if way == 1 else item

    def wait_sum(self, which, way, item, block):
        part, landed = self.summed[which]
        rows = rows_of(block, part.shape[1], self.blocks)
        view = landed.at[self.landed_slot(way, item), rows]
        pltpu.make_async_remote_copy(
            src_ref=view,
            dst_ref=view,
            send_sem=self.rs_send.at[which, way, item, block],
            recv_sem=self.rs_recv.at[which, way, item, block],
            device_id={"tensor": self.place},
        ).wait_recv()
        return view

    def start_own(self):
        for which in range(len(self.gathered)):
            for way in range(2):

                @pl.when(self.can(way))
                def _():
                    self.item_copy(which, way, self.place, own=True).start()

    def receive(self, step, arrays=(0,)):
        place, count = self.place, self.count
        for which in arrays:
            for way in range(2):
                item = place - step if way == 0 else place + step

                @pl.when((item >= 0) & (item < count))
                def _():
                    self.item_copy(which, way, item).wait_recv()

                    @pl.when(self.can(way))
                    def _():
                        self.item_copy(which, way, item).start()

    def items(self, step):
        place, count = self.place, self.count
        low, high = place - step, place + step
        return ((low, (low >= 0)), (high, (high < count) & (step > 0)))

    def moves(self, step):
        place, count = self.place, self.count
        return (
            (0, step, step > place, place),
            (1, count - 1 - step, count - 1 - step < place, count - 1 - place),
        )

    def first_sums(self, step, arrays=(0,)):
        @pl.loop(0, self.blocks)
        def _(block):
            for way, item, further, hop in self.moves(step):

                @pl.when(further & (hop == 0))
                def _():
                    for which in arrays:
                        self.sum_copy(which, way, item, block).start()

    def relay_sums(self, step, arrays=(0,)):
        @pl.loop(0, self.blocks + self.count - 3)
        def _(turn):
            for distance in range(1, self.count - 1):
                block = turn - (distance - 1)
                for way, item, further, hop in self.moves(step):

                    @pl.when(further & (hop == distance) & (block >= 0) & (block < self.blocks))
                    def _():
                        for which in arrays:
                            part, landed = self.summed[which]
                            rows = rows_of(block, part.shape[1], self.blocks)
                            view = self.wait_sum(which, way, item, block)
                            total = part[item, rows].astype(jnp.float32) + view[...].astype(
                                jnp.float32
                            )
                            part[item, rows] = total.astype(part.dtype)
                            self.sum_copy(which, way, item, block).start()

    def each(self, first, second, body):
        @pl.loop(0, 2)
        def _(turn):
            item = jnp.where(turn == 0, first[0], second[0])
            valid = ((turn == 0) & first[1]) | ((turn == 1) & second[1])

            @pl.when(valid)
            def _():
                body(item)

    def near(self, step):
        place, count = self.place, self.count
        low = place >= step
        return jnp.where(low, place - step, place + step), low | (place + step < count)

    def far(self, step):
        place, count = self.place, self.count
        return place + step, (step > 0) & (place >= step) & (place + step < count)

    def finish(self, which, out):
        place, count = self.place, self.count
        part, landed = self.summed[which]

        @pl.loop(0, self.blocks)
        def _(block):
            rows = rows_of(block, part.shape[1], self.blocks)
            out[rows] = part[place, rows].astype(jnp.float32)
            for way in range(2):

                @pl.when(place > 0 if way == 0 else place < count - 1)
                def _():
                    view = self.wait_sum(which, way, place, block)
                    out[rows] += view[...].astype(jnp.float32)

    def drain(self):
        place, count = self.place, self.count

        @pl.loop(0, count)
        def _(item):
            for way in range(2):
                passed = item <= place if way == 0 else item >= place

                @pl.when(passed & self.can(way))
                def _():
                    for which in range(len(self.gathered)):
                        self.item_copy(which, way, item).wait_send()

                further = item > place if way == 0 else item < place

                @pl.when(further)
                def _():
                    @pl.loop(0, self.blocks)
                    def _(block):
                        for which in range(len(self.summed)):
                            self.sum_copy(which, way, item, block).wait_send()


def dot(left, right):
    return jnp.dot(left, right, preferred_element_type=jnp.float32)


def dot_rt(left, right):
    return lax.dot_general(
        left, right, (((1,), (1,)), ((), ())), preferred_element_type=jnp.float32
    )


def dot_lt(left, right):
    return lax.dot_general(
        left, right, (((0,), (0,)), ((), ())), preferred_element_type=jnp.float32
    )


def cut(total, most):
    size = max(s for s in range(128, most + 1, 128) if total % s == 0)
    return size, total // size


def span(index, size):
    return pl.ds(pl.multiple_of(index * size, size), size)


def feed_kernel(
    count,
    mod_ref,
    grad_ref,
    expand_hbm,
    down_hbm,
    feed_out,
    back_out,
    weight_hbm,
    expand,
    down,
    mod_all,
    grad_all,
    hidden,
    slopes,
    feed_part,
    back_part,
    feed_land,
    back_land,
    total,
    weights,
    gates,
    load_sem,
    ag_send,
    ag_recv,
    rs_send,
    rs_recv,
):
    line = Line(
        count,
        FEED_BLOCKS,
        [(mod_ref, mod_all), (grad_ref, grad_all)],
        [(back_part, back_land), (feed_part, feed_land)],
        (ag_send, ag_recv),
        (rs_send, rs_recv),
    )
    width, units = expand.shape[1], expand.shape[2]
    loads = (
        pltpu.make_async_copy(expand_hbm, expand, load_sem.at[0]),
        pltpu.make_async_copy(down_hbm, down, load_sem.at[1]),
    )
    for load in loads:
        load.start()
    line.barrier()
    line.start_own()
    mod_all[line.place] = mod_ref[...]
    grad_all[line.place] = grad_ref[...]
    total[...] = jnp.zeros_like(total)
    for load in loads:
        load.wait()
    unit_size, unit_count = cut(units, 256)
    wide_size, wide_count = cut(width, 384)
    tall_size, tall_count = cut(width, 128)

    def ahead(item):
        @pl.loop(0, unit_count)
        def _(index):
            cols = span(index, unit_size)
            mod = mod_all[item]
            gate = dot(mod, expand[0, :, cols])
            upper = dot(mod, expand[1, :, cols])
            gates[0, item, :, cols] = gate
            gates[1, item, :, cols] = upper
            hidden[item, :, cols] = (gate * jax.nn.sigmoid(gate) * upper).astype(jnp.bfloat16)

        @pl.loop(0, wide_count)
        def _(index):
            cols = span(index, wide_size)
            feed_part[item, :, cols] = dot(hidden[item], down[:, cols]).astype(jnp.bfloat16)

    def behind(item):
        @pl.loop(0, unit_count)
        def _(index):
            cols = span(index, unit_size)
            back = dot_rt(grad_all[item], down[cols, :])
            gate = gates[0, item, :, cols]
            sigma = jax.nn.sigmoid(gate)
            slopes[0, item, :, cols] = (
                back * gates[1, item, :, cols] * (sigma * (1.0 + gate * (1.0 - sigma)))
            ).astype(jnp.bfloat16)
            slopes[1, item, :, cols] = (back * (gate * sigma)).astype(jnp.bfloat16)

        @pl.loop(0, wide_count)
        def _(index):
            cols = span(index, wide_size)
            back_part[item, :, cols] = (
                dot_rt(slopes[0, item], expand[0, cols, :])
                + dot_rt(slopes[1, item], expand[1, cols, :])
            ).astype(jnp.bfloat16)

    def weigh(item):
        @pl.loop(0, tall_count)
        def _(index):
            rows = span(index, tall_size)
            mod = mod_all[item, :, rows]
            total[0, rows, :] += dot_lt(mod, slopes[0, item])
            total[1, rows, :] += dot_lt(mod, slopes[1, item])
            total[2, rows, :] += dot_lt(grad_all[item, :, rows], hidden[item])

    @pl.loop(0, count)
    def _(step):
        @pl.when(step > 0)
        def _():
            line.each(line.far(step - 1), line.near(step - 1), weigh)
            line.receive(step, (0,))

        line.each(line.far(step), line.near(step), ahead)

        @pl.when(step > 0)
        def _():
            line.first_sums(step, (1,))
            line.receive(step, (1,))

        line.each(line.far(step), line.near(step), behind)

        @pl.when(step > 0)
        def _():
            line.first_sums(step, (0,))
            line.relay_sums(step, (1,))
            line.relay_sums(step, (0,))

    line.each((0, False), line.near(count - 1), weigh)
    weights[...] = total[...].astype(jnp.bfloat16)
    store = pltpu.make_async_copy(weights, weight_hbm, load_sem.at[0])
    store.start()
    line.finish(1, feed_out)
    line.finish(0, back_out)
    line.drain()
    store.wait()


def feed_pass(mod_two, branch_grad, expand_weight, down_weight):
    count = lax.axis_size("tensor")
    length, width = mod_two.shape
    units = down_weight.shape[0]
    expand = jnp.transpose(expand_weight, (1, 0, 2))
    vmem, any_space = pl.BlockSpec(memory_space=pltpu.VMEM), pl.BlockSpec(memory_space=pl.ANY)
    low = jnp.bfloat16
    item = (length, width)
    return pl.pallas_call(
        functools.partial(feed_kernel, count),
        out_shape=(
            jax.ShapeDtypeStruct(item, jnp.float32),
            jax.ShapeDtypeStruct(item, jnp.float32),
            jax.ShapeDtypeStruct((3, width, units), low),
        ),
        in_specs=[vmem, vmem, any_space, any_space],
        out_specs=(vmem, vmem, any_space),
        scratch_shapes=[
            pltpu.VMEM((2, width, units), low),
            pltpu.VMEM((units, width), low),
            pltpu.VMEM((count, *item), low),
            pltpu.VMEM((count, *item), low),
            pltpu.VMEM((count, length, units), low),
            pltpu.VMEM((2, count, length, units), low),
            pltpu.VMEM((count, *item), low),
            pltpu.VMEM((count, *item), low),
            pltpu.VMEM((count + 1, *item), low),
            pltpu.VMEM((count + 1, *item), low),
            pltpu.VMEM((3, width, units), jnp.float32),
            pltpu.VMEM((3, width, units), low),
            pltpu.VMEM((2, count, length, units), jnp.float32),
            *line_sems(count, FEED_BLOCKS, 2, 2),
        ],
        compiler_params=pltpu.CompilerParams(
            collective_id=1, has_side_effects=True, vmem_limit_bytes=64000000
        ),
        name="feed_pass",
    )(mod_two, branch_grad, expand, down_weight)


LANES = 128
HEAD_UNROLL = 2


def turn(value, tables):
    return (
        value * tables[0]
        + pltpu.roll(value, LANES - HD // 4, 1) * tables[1]
        + pltpu.roll(value, HD // 4, 1) * tables[2]
    )


def turn_back(grad, tables):
    return (
        grad * tables[0]
        + pltpu.roll(grad * tables[1], HD // 4, 1)
        + pltpu.roll(grad * tables[2], LANES - HD // 4, 1)
    )


def turn_tables(length):
    quarter = HD // 4
    lane = jnp.arange(LANES)
    rates = 10000.0 ** (-(lane % quarter).astype(jnp.float32) / quarter)
    positions = jnp.arange(length)[:, None]
    place = jnp.where(lane < 2 * quarter, positions // GRID, positions % GRID)
    angle = place.astype(jnp.float32) * rates
    real = lane < HD
    early = (lane // quarter) % 2 == 0
    cosine = jnp.where(real, jnp.cos(angle), 0.0)
    sine = jnp.sin(angle)
    return jnp.stack(
        [
            cosine,
            jnp.where(real & early, -sine, 0.0),
            jnp.where(real & ~early, sine, 0.0),
        ]
    )


def unit_norm(raw):
    inverse = lax.rsqrt(jnp.sum(raw * raw, axis=-1, keepdims=True) * (1.0 / HD) + EPS)
    return raw * inverse, inverse


def project(mod, weight, raw):
    @pl.loop(0, weight.shape[0])
    def _(index):
        raw[index] = dot_rt(mod, weight[index])


def padded_loads(weight_hbm, last_hbm, weight, last, sem):
    heads = last.shape[0] // LANES
    loads = []
    for head in range(heads):
        rows, to = pl.ds(head * HD, HD), pl.ds(head * LANES, HD)
        rest = pl.ds(head * LANES + HD, LANES - HD)
        for part in range(3):
            weight[part, rest, :] = jnp.zeros((LANES - HD, weight.shape[2]), weight.dtype)
            loads.append(
                pltpu.make_async_copy(
                    weight_hbm.at[part, rows], weight.at[part, to], sem.at[len(loads)]
                )
            )
        last[rest, :] = jnp.zeros((LANES - HD, last.shape[1]), last.dtype)
        loads.append(pltpu.make_async_copy(last_hbm.at[rows], last.at[to], sem.at[len(loads)]))
    for load in loads:
        load.start()
    return loads


def soft(queries, keys):
    grown = jnp.exp2(dot_rt(queries, keys) * (HD ** (-0.5) / math.log(2.0)))
    return grown * (1.0 / jnp.sum(grown, axis=-1, keepdims=True))


def attend_kernel(
    count,
    token_ref,
    slab_ref,
    tables_ref,
    gains_ref,
    weight_hbm,
    last_hbm,
    branch_out,
    mod_out,
    rows_out,
    slab_land,
    mod_own,
    weight,
    last,
    mod_all,
    raw,
    mixed,
    part,
    land,
    load_sem,
    ag_send,
    ag_recv,
    rs_send,
    rs_recv,
    slab_send,
    slab_recv,
):
    line = Line(count, ATTEND_BLOCKS, [(mod_own, mod_all)], [(part, land)], (ag_send, ag_recv), (rs_send, rs_recv))
    loads = padded_loads(weight_hbm, last_hbm, weight, last, load_sem)
    place = line.place
    hello = pltpu.get_barrier_semaphore()

    @pl.loop(1, count)
    def _(offset):
        pl.semaphore_signal(hello, inc=1, device_id={"tensor": lax.rem(place + offset, count)})

    pl.semaphore_wait(hello, count - 1)

    def slab_copy(peer, slot):
        return pltpu.make_async_remote_copy(
            src_ref=slab_ref.at[peer],
            dst_ref=slab_land.at[slot],
            send_sem=slab_send.at[peer],
            recv_sem=slab_recv.at[slot],
            device_id={"tensor": peer},
        )

    @pl.loop(1, count)
    def _(offset):
        slab_copy(lax.rem(place + offset, count), place).start()

    slab_land[place] = slab_ref[place]

    @pl.loop(1, count)
    def _(offset):
        peer = lax.rem(place + offset, count)
        slab_copy(peer, place).wait_send()
        slab_copy(peer, peer).wait_recv()

    rows_out[...] = jnp.concatenate(
        [slab_land[index].astype(jnp.float32) for index in range(count)], axis=1
    )

    @pl.loop(0, ATTEND_BLOCKS)
    def _(block):
        rows = rows_of(block, token_ref.shape[0], ATTEND_BLOCKS)
        value = token_ref[rows].astype(jnp.float32)
        center = value - jnp.mean(value, axis=-1, keepdims=True)
        inverse = lax.rsqrt(jnp.mean(center * center, axis=-1, keepdims=True) + EPS)
        mod = center * inverse * (1.0 + rows_out[1:2, :]) + rows_out[0:1, :]
        mod_own[rows] = mod.astype(jnp.bfloat16)
        mod_all[place, rows] = mod.astype(jnp.bfloat16)

    line.start_own()
    for load in loads:
        load.wait()
    heads = last.shape[0] // LANES
    wide_size, wide_count = cut(last.shape[1], 384)

    def compute(item):
        project(mod_all[item], weight, raw)
        tables = (tables_ref[0], tables_ref[1], tables_ref[2])

        @pl.loop(0, heads, unroll=HEAD_UNROLL)
        def _(head):
            lanes = span(head, LANES)
            queries = turn(unit_norm(raw[0, :, lanes])[0] * gains_ref[0:1, :], tables)
            keys = turn(unit_norm(raw[1, :, lanes])[0] * gains_ref[1:2, :], tables)
            probs = soft(queries.astype(jnp.bfloat16), keys.astype(jnp.bfloat16))
            values = raw[2, :, lanes].astype(jnp.bfloat16)
            mixed[:, lanes] = dot(probs.astype(jnp.bfloat16), values).astype(jnp.bfloat16)

        @pl.loop(0, wide_count)
        def _(index):
            cols = span(index, wide_size)
            part[item, :, cols] = dot(mixed[...], last[:, cols]).astype(jnp.bfloat16)

    @pl.loop(0, count)
    def _(step):
        @pl.when(step > 0)
        def _():
            line.receive(step)

        line.each(line.far(step - 1), line.near(step), compute)

        @pl.when(step > 0)
        def _():
            line.first_sums(step)
            line.relay_sums(step)

    mod_out[...] = mod_all[...]
    line.finish(0, branch_out)
    line.drain()


def block_copy(array, target, slot, block, size, send, recv, peer):
    rows = pl.ds(pl.multiple_of(block * size, size), size)
    source = array.at[rows] if len(array.shape) == 2 else array.at[:, rows]
    return pltpu.make_async_remote_copy(
        src_ref=source,
        dst_ref=target.at[slot],
        send_sem=send,
        recv_sem=recv,
        device_id={"dp": peer},
    )


def attend_back_kernel(
    count,
    wide,
    grad_ref,
    mod_all,
    tables_ref,
    gains_ref,
    weight_hbm,
    last_hbm,
    *rest,
):
    if wide:
        feed_hbm, back_out, weight_out, gain_out, feed_out, *rest = rest
    else:
        back_out, weight_out, gain_out, *rest = rest
    (
        weight,
        last,
        narrow,
        grad_all,
        raw,
        mixed,
        mixed_grad,
        raw_grad,
        kept,
        kept_mixed,
        part,
        land,
        total,
        load_sem,
        ag_send,
        ag_recv,
        rs_send,
        rs_recv,
        *rest,
    ) = rest
    line = Line(count, ATTEND_BLOCKS, [(grad_ref, grad_all)], [(part, land)], (ag_send, ag_recv), (rs_send, rs_recv))
    loads = padded_loads(weight_hbm, last_hbm, weight, last, load_sem)
    line.barrier(wide or 1)
    line.start_own()
    width = last.shape[1]
    here = lax.axis_index("dp")
    if wide:
        feed_land, staged, pair_land, quad_land, fs, fr, ps, pr, qs, qr = rest
        size = width // wide
        half = wide // 2
        parity, seat = lax.rem(here, 2), here // 2
        partner = here + 1 - 2 * parity

        def feed_copy(peer, slot):
            return block_copy(feed_hbm, feed_land, slot, peer, size, fs.at[peer], fr.at[slot], peer)

        def pair_copy(index):
            block = 2 * index + 1 - parity
            return block_copy(
                staged, pair_land, index, block, size, ps.at[index], pr.at[index], partner
            )

        def quad_copy(index, slot):
            block = 2 * index + parity
            return block_copy(
                staged, quad_land, slot, block, size, qs.at[index], qr.at[slot], block
            )

        @pl.loop(1, wide)
        def _(offset):
            peer = lax.rem(here + offset, wide)
            feed_copy(peer, here).start()

    grad_all[line.place] = grad_ref[...]
    padded_row = lax.broadcasted_iota(jnp.int32, narrow.shape[1:], 0)
    lane = padded_row & (LANES - 1)
    column = (padded_row >> 7) * HD + lane
    target = lax.broadcasted_iota(jnp.int32, narrow.shape[1:], 1)
    offset = last.shape[0] // LANES * HD % LANES
    for part_index in range(3):
        hit = (lane < HD) & (column + part_index * offset == target)
        narrow[part_index] = jnp.where(hit, 1.0, 0.0).astype(jnp.bfloat16)
    total[...] = jnp.zeros_like(total)
    gain_out[...] = jnp.zeros_like(gain_out)
    for load in loads:
        load.wait()
    inner = last.shape[0]
    heads = inner // LANES
    scale = HD ** (-0.5)
    wide_size, wide_count = cut(width, 384)
    inner_size, inner_count = cut(inner, 256)
    tall_size, tall_count = cut(width, 128)
    first_width = kept.shape[2]

    def compute(item):
        project(mod_all[item], weight, raw)
        tables = (tables_ref[0], tables_ref[1], tables_ref[2])

        @pl.loop(0, inner_count)
        def _(index):
            cols = span(index, inner_size)
            mixed_grad[:, cols] = dot_rt(grad_all[item], last[cols, :]).astype(jnp.bfloat16)

        @pl.loop(0, heads, unroll=HEAD_UNROLL)
        def _(head):
            lanes = span(head, LANES)
            query_norm, query_inverse = unit_norm(raw[0, :, lanes])
            key_norm, key_inverse = unit_norm(raw[1, :, lanes])
            values = raw[2, :, lanes].astype(jnp.bfloat16)
            queries = turn(query_norm * gains_ref[0:1, :], tables).astype(jnp.bfloat16)
            keys = turn(key_norm * gains_ref[1:2, :], tables).astype(jnp.bfloat16)
            probs = soft(queries, keys)
            probs_low = probs.astype(jnp.bfloat16)
            mixed[:, lanes] = dot(probs_low, values).astype(jnp.bfloat16)
            grad = mixed_grad[:, lanes]
            prob_grad = dot_rt(grad, values)
            score_grad = (
                probs * (prob_grad - jnp.sum(probs * prob_grad, axis=-1, keepdims=True))
            ).astype(jnp.bfloat16)

            def back(which, value_grad, norm, inverse):
                turned = turn_back(value_grad, tables)
                gained = turned * norm
                gain_out[which] += jnp.sum(gained.reshape(-1, 8, LANES), axis=0)
                scaled = turned * gains_ref[which : which + 1, :]
                mean = jnp.sum(scaled * norm, axis=-1, keepdims=True) * (1.0 / HD)
                raw_grad[which, :, lanes] = (inverse * (scaled - norm * mean)).astype(
                    jnp.bfloat16
                )

            back(0, dot(score_grad, keys) * scale, query_norm, query_inverse)
            back(1, dot_lt(score_grad, queries) * scale, key_norm, key_inverse)
            raw_grad[2, :, lanes] = dot_lt(probs_low, grad).astype(jnp.bfloat16)

        @pl.loop(0, wide_count)
        def _(index):
            cols = span(index, wide_size)
            sums = dot(raw_grad[0], weight[0, :, cols])
            sums += dot(raw_grad[1], weight[1, :, cols])
            sums += dot(raw_grad[2], weight[2, :, cols])
            part[item, :, cols] = sums.astype(jnp.bfloat16)

    def keep(item):
        one = dot(raw_grad[0], narrow[0])
        two = dot(raw_grad[1], narrow[1])
        three = dot(raw_grad[2], narrow[2])
        side = one.shape[1] - LANES
        low = jnp.bfloat16
        kept[item, :, :side] = one[:, :side].astype(low)
        kept[item, :, side : side + LANES] = (one[:, side:] + two[:, :LANES]).astype(low)
        kept[item, :, side + LANES : 2 * side] = two[:, LANES:side].astype(low)
        kept[item, :, 2 * side : 2 * side + LANES] = (two[:, side:] + three[:, :LANES]).astype(low)
        kept[item, :, 2 * side + LANES :] = three[:, LANES:].astype(low)
        kept_mixed[item] = dot(mixed[...], narrow[0]).astype(low)

    def weigh(item):
        @pl.loop(0, tall_count)
        def _(index):
            rows = span(index, tall_size)
            total[rows, :first_width] += dot_lt(mod_all[item, :, rows], kept[item])
            total[rows, first_width:] += dot_lt(grad_all[item, :, rows], kept_mixed[item])

    def work(item):
        compute(item)
        keep(item)

    @pl.loop(0, count)
    def _(step):
        @pl.when(step > 0)
        def _():
            line.each(line.far(step - 2), line.near(step - 1), weigh)
            line.receive(step)

        line.each(line.far(step - 1), line.near(step), work)

        @pl.when(step > 0)
        def _():
            line.first_sums(step)

        @pl.when(step == count - 1)
        def _():
            line.each((0, False), line.near(step), weigh)
            if wide:
                staged[...] = total[...].astype(jnp.bfloat16)

                @pl.loop(0, half)
                def _(index):
                    pair_copy(index).start()

                @pl.loop(0, half)
                def _(index):
                    pair_copy(index).wait_send()
                    pair_copy(index).wait_recv()
                    rows = pl.ds(pl.multiple_of((2 * index + parity) * size, size), size)
                    staged[rows] = (
                        staged[rows].astype(jnp.float32) + pair_land[index].astype(jnp.float32)
                    ).astype(jnp.bfloat16)

                @pl.loop(1, half)
                def _(offset):
                    quad_copy(lax.rem(seat + offset, half), seat).start()

        @pl.when(step > 0)
        def _():
            line.relay_sums(step)

    if wide:
        rows = pl.ds(pl.multiple_of(here * size, size), size)
        own = pltpu.make_async_copy(feed_hbm.at[:, rows], feed_land.at[here], load_sem.at[0])
        own.start()

        @pl.loop(1, wide)
        def _(offset):
            peer = lax.rem(here + offset, wide)
            feed_copy(peer, here).wait_send()
            feed_copy(here, peer).wait_recv()

        own.wait()
        for which in range(feed_out.shape[0]):
            total_here = feed_land[0, which].astype(jnp.float32)
            for index in range(1, wide):
                total_here += feed_land[index, which].astype(jnp.float32)
            feed_out[which] = total_here

    line.finish(0, back_out)
    line.drain()
    if wide:
        weight_out[...] = staged[rows].astype(jnp.float32)

        @pl.loop(1, half)
        def _(offset):
            index = lax.rem(seat + offset, half)
            quad_copy(index, seat).wait_send()
            quad_copy(seat, index).wait_recv()
            weight_out[...] += quad_land[index].astype(jnp.float32)

    else:
        weight_out[...] = total[...].astype(jnp.bfloat16)


def attend_arrays(project_weight, output_weight, query_gain, key_gain, length):
    gains = jnp.stack([query_gain, key_gain]).astype(jnp.float32)
    gains = jnp.pad(gains, ((0, 6), (0, LANES - HD)))
    return turn_tables(length), gains, jnp.transpose(project_weight, (1, 2, 0)), output_weight


def line_sems(count, blocks, gathers, sums, loads=2):
    return [
        pltpu.SemaphoreType.DMA((loads,)),
        pltpu.SemaphoreType.DMA((gathers, 2, count)),
        pltpu.SemaphoreType.DMA((gathers, 2, count)),
        pltpu.SemaphoreType.DMA((sums, 2, count, blocks)),
        pltpu.SemaphoreType.DMA((sums, 2, count, blocks)),
    ]


def attend_pass(tokens, slabs, arrays):
    count = lax.axis_size("tensor")
    tables, gains, weight, last = arrays
    item = tokens.shape
    width = item[1]
    heads = last.shape[0] // HD
    inner = heads * LANES
    vmem, any_space = pl.BlockSpec(memory_space=pltpu.VMEM), pl.BlockSpec(memory_space=pl.ANY)
    low = jnp.bfloat16
    return pl.pallas_call(
        functools.partial(attend_kernel, count),
        out_shape=(
            jax.ShapeDtypeStruct(item, jnp.float32),
            jax.ShapeDtypeStruct((count, *item), low),
            jax.ShapeDtypeStruct((slabs.shape[1], width), jnp.float32),
        ),
        in_specs=[vmem, vmem, vmem, vmem, any_space, any_space],
        out_specs=(vmem, vmem, vmem),
        scratch_shapes=[
            pltpu.VMEM(slabs.shape, low),
            pltpu.VMEM(item, low),
            pltpu.VMEM((3, inner, width), low),
            pltpu.VMEM((inner, width), low),
            pltpu.VMEM((count, *item), low),
            pltpu.VMEM((3, item[0], inner), jnp.float32),
            pltpu.VMEM((item[0], inner), low),
            pltpu.VMEM((count, *item), low),
            pltpu.VMEM((count + 1, *item), low),
            *line_sems(count, ATTEND_BLOCKS, 1, 1, 4 * heads),
            pltpu.SemaphoreType.DMA((count,)),
            pltpu.SemaphoreType.DMA((count,)),
        ],
        compiler_params=pltpu.CompilerParams(
            collective_id=6, has_side_effects=True, vmem_limit_bytes=60000000
        ),
        name="attend_pass",
    )(tokens, slabs, tables, gains, weight, last)


def attend_back_pass(attend_grad, mod_all, arrays, feed_weights):
    count, wide = lax.axis_size("tensor"), lax.axis_size("dp")
    tables, gains, weight, last = arrays
    item = attend_grad.shape
    length, width = item
    heads = last.shape[0] // HD
    inner = heads * LANES
    vmem, any_space = pl.BlockSpec(memory_space=pltpu.VMEM), pl.BlockSpec(memory_space=pl.ANY)
    low, high = jnp.bfloat16, jnp.float32
    window = -(-last.shape[0] // LANES) * LANES
    first_width = 3 * window - 2 * LANES
    columns = first_width + window
    if width % (16 * wide):
        wide = 0
    size = width // wide if wide else width
    outs = [
        jax.ShapeDtypeStruct(item, high),
        jax.ShapeDtypeStruct((size, columns), high if wide else low),
        jax.ShapeDtypeStruct((2, 8, LANES), high),
    ]
    scratch = [
        pltpu.VMEM((3, inner, width), low),
        pltpu.VMEM((inner, width), low),
        pltpu.VMEM((3, inner, window), low),
        pltpu.VMEM((count, *item), low),
        pltpu.VMEM((3, length, inner), high),
        pltpu.VMEM((length, inner), low),
        pltpu.VMEM((length, inner), low),
        pltpu.VMEM((3, length, inner), low),
        pltpu.VMEM((count, length, first_width), low),
        pltpu.VMEM((count, length, window), low),
        pltpu.VMEM((count, *item), low),
        pltpu.VMEM((count + 1, *item), low),
        pltpu.VMEM((width, columns), high),
        *line_sems(count, ATTEND_BLOCKS, 1, 1, 4 * heads),
    ]
    ins = [attend_grad, mod_all, tables, gains, weight, last]
    specs = [vmem, vmem, vmem, vmem, any_space, any_space]
    if wide:
        ins.append(feed_weights)
        specs.append(any_space)
        kinds, _, units = feed_weights.shape
        outs.append(jax.ShapeDtypeStruct((kinds, size, units), high))
        half = wide // 2
        scratch += [
            pltpu.VMEM((wide, kinds, size, units), low),
            pltpu.VMEM((width, columns), low),
            pltpu.VMEM((half, size, columns), low),
            pltpu.VMEM((half, size, columns), low),
        ]
        for number in (wide, wide, half, half, half, half):
            scratch.append(pltpu.SemaphoreType.DMA((number,)))
    results = pl.pallas_call(
        functools.partial(attend_back_kernel, count, wide),
        out_shape=tuple(outs),
        in_specs=specs,
        out_specs=tuple([vmem] * len(outs)),
        scratch_shapes=scratch,
        compiler_params=pltpu.CompilerParams(
            collective_id=7, has_side_effects=True, vmem_limit_bytes=66000000
        ),
        name="attend_back_pass",
    )(*ins)
    if wide:
        return results

    def scatter(value, axis):
        return lax.psum_scatter(value, "dp", scatter_dimension=axis, tiled=True).astype(high)

    back, weights, gain_parts = results
    return back, scatter(weights, 0), gain_parts, scatter(feed_weights, 1)


def tail_kernel(
    grads_ref,
    small_ref,
    weight_ref,
    slope_ref,
    forward_ref,
    feat_ref,
    label_ref,
    rows_hbm,
    small_out,
    modulate_out,
    embed_out,
    class_out,
    time_out,
    bias_out,
    grads_land,
    grads_mine,
    grads_land_dp,
    small_one,
    small_mid,
    small_two,
    part,
    part_land,
    cond,
    cond_land,
    forward_land,
    feat_land,
    label_land,
    grads_all,
    cond_all,
    forward_all,
    feat_all,
    label_all,
    rows,
    load_sem,
    *sems,
):
    deep, wide = part_land.shape[0], cond_land.shape[0]
    items = cond.shape[0]
    share = rows.shape[0]
    seat = lax.axis_index("dp") * share
    start_row = seat if rows_hbm.shape[0] > share else 0
    if share % 16 == 0:
        start_row = pl.multiple_of(start_row, 16)
    load = pltpu.make_async_copy(rows_hbm.at[pl.ds(start_row, share)], rows, load_sem)
    load.start()
    axes = (("dp", wide), ("tensor", deep))
    hello = pltpu.get_barrier_semaphore()
    for axis, count in axes:
        here = lax.axis_index(axis)

        @pl.loop(1, count)
        def _(offset):
            pl.semaphore_signal(
                hello, inc=1, device_id={axis: lax.rem(here + offset, count)}
            )

    pl.semaphore_wait(hello, wide + deep - 2)
    low = jnp.bfloat16

    def exchange(number, axis, source, target, split=False):
        count = target.shape[0]
        here = lax.axis_index(axis)
        send, recv = sems[2 * number], sems[2 * number + 1]

        def copy(peer, slot):
            return pltpu.make_async_remote_copy(
                src_ref=source.at[peer] if split else source,
                dst_ref=target.at[slot],
                send_sem=send.at[peer],
                recv_sem=recv.at[slot],
                device_id={axis: peer},
            )

        def start():
            @pl.loop(1, count)
            def _(offset):
                copy(lax.rem(here + offset, count), here).start()

            target[here] = source[here] if split else source[...]

        def finish():
            @pl.loop(1, count)
            def _(offset):
                peer = lax.rem(here + offset, count)
                copy(peer, here).wait_send()
                copy(peer, peer).wait_recv()

        return start, finish

    start_grads, finish_grads = exchange(0, "tensor", grads_ref, grads_land, True)
    start_small, finish_small = exchange(1, "dp", small_ref, small_one)
    start_sums, finish_sums = exchange(2, "tensor", small_mid, small_two)
    start_part, finish_part = exchange(3, "tensor", part, part_land)
    start_mine, finish_mine = exchange(4, "dp", grads_mine, grads_land_dp)
    start_cond, finish_cond = exchange(5, "dp", cond, cond_land)
    start_forward, finish_forward = exchange(6, "dp", forward_ref, forward_land, True)
    start_feat, finish_feat = exchange(7, "dp", feat_ref, feat_land)
    start_label, finish_label = exchange(8, "dp", label_ref, label_land)

    start_grads()
    start_small()
    start_forward()
    start_feat()
    start_label()
    finish_grads()
    kinds = grads_mine.shape[0]
    for item in range(items):
        piece = grads_land[item].astype(jnp.float32)
        for kind in range(kinds):
            grads_all[kind, item : item + 1, :] = piece[kind : kind + 1, :]
    total = jnp.zeros(part.shape, jnp.float32)
    for kind in range(kinds):
        mine = grads_all[kind, :items, :].astype(low)
        grads_mine[kind] = mine
        total += dot(mine, weight_ref[kind])
    part[...] = total
    start_part()
    start_mine()
    finish_small()
    small_mid[...] = small_one[0]

    @pl.loop(1, wide)
    def _(index):
        small_mid[...] += small_one[index]

    start_sums()
    finish_part()
    total = part_land[0]
    for index in range(1, deep):
        total += part_land[index]
    cond[...] = (total * slope_ref[...]).astype(low)
    start_cond()
    finish_forward()
    finish_feat()
    finish_label()
    for index in range(wide):
        batch = pl.ds(index * items, items)
        for kind in range(forward_all.shape[0]):
            forward_all[kind, batch, :] = forward_land[index, kind]
        feat_all[batch, :] = feat_land[index].astype(jnp.float32)
        label_all[batch, :] = label_land[index]
    finish_mine()
    for index in range(wide):
        batch = pl.ds(index * items, items)
        for kind in range(kinds):
            grads_all[kind, batch, :] = grads_land_dp[index, kind].astype(jnp.float32)
    active = forward_all[0].astype(low)
    for kind in range(kinds):
        modulate_out[kind] = dot_lt(active, grads_all[kind].astype(low))
    finish_sums()
    small_out[...] = small_two[0]

    @pl.loop(1, deep)
    def _(index):
        small_out[...] += small_two[index]

    finish_cond()
    for index in range(wide):
        cond_all[pl.ds(index * items, items), :] = cond_land[index].astype(jnp.float32)
    every = cond_all[...].astype(low)
    embed_out[...] = dot_lt(forward_all[1].astype(low), every)
    width = every.shape[1]
    spot = lax.broadcasted_iota(jnp.int32, (width, share), 0)
    pick = jnp.where(spot == seat + lax.broadcasted_iota(jnp.int32, (width, share), 1), 1.0, 0.0)
    picked = dot(every, pick.astype(low)).astype(low)
    classes = class_out.shape[1]
    label = jnp.broadcast_to(label_all[:, 0:1], (label_all.shape[0], classes))
    lane = lax.broadcasted_iota(jnp.int32, label.shape, 1)
    hot = jnp.where(label == lane, 1.0, 0.0).astype(low)
    class_out[...] = dot_lt(picked, hot)
    load.wait()
    earlier = (dot_rt(every, rows[...]) * forward_all[2]).astype(low)
    time_out[...] = dot_lt(earlier, feat_all[...].astype(low))
    bias_out[0:1, :] = jnp.sum(picked.astype(jnp.float32), axis=0, keepdims=True)
    bias_out[1:2, :] = jnp.sum(earlier.astype(jnp.float32), axis=0, keepdims=True)


def tail_pass(grads, small, weight, slope, forward, feat, label, rows, classes):
    deep, kinds, slab = grads.shape
    wide, parts, items, share = forward.shape
    width = weight.shape[2]
    batch = wide * items
    freq = feat.shape[1]
    low, high = jnp.bfloat16, jnp.float32
    vmem = pl.BlockSpec(memory_space=pltpu.VMEM)
    shapes = (
        (small.shape, high),
        ((kinds, share, slab), high),
        ((share, width), high),
        ((share, classes), high),
        ((share, freq), high),
        ((2, share), high),
    )
    scratch = (
        ((deep, kinds, slab), low),
        ((kinds, items, slab), low),
        ((wide, kinds, items, slab), low),
        ((wide, *small.shape), high),
        (small.shape, high),
        ((deep, *small.shape), high),
        ((items, width), high),
        ((deep, items, width), high),
        ((items, width), low),
        ((wide, items, width), low),
        (forward.shape, high),
        ((wide, items, freq), low),
        ((wide, items, LANES), jnp.int32),
        ((kinds, batch, slab), high),
        ((batch, width), high),
        ((parts, batch, share), high),
        ((batch, freq), high),
        ((batch, LANES), jnp.int32),
        ((share, width), low),
    )
    sems = [pltpu.SemaphoreType.DMA]
    for number in (deep, wide, deep, deep, wide, wide, wide, wide, wide):
        sems += [pltpu.SemaphoreType.DMA((number,))] * 2
    return pl.pallas_call(
        tail_kernel,
        out_shape=tuple(jax.ShapeDtypeStruct(*shape) for shape in shapes),
        in_specs=[vmem] * 7 + [pl.BlockSpec(memory_space=pl.ANY)],
        out_specs=tuple([vmem] * 6),
        scratch_shapes=[pltpu.VMEM(*shape) for shape in scratch] + sems,
        compiler_params=pltpu.CompilerParams(
            collective_id=3, has_side_effects=True, vmem_limit_bytes=60000000
        ),
        name="tail_pass",
    )(grads, small, weight, slope, forward, feat, label, rows)


def shards(
    tokens,
    timesteps,
    labels,
    item_counts,
    cotangent,
    project_weight,
    query_gain,
    key_gain,
    output_weight,
    output_bias,
    expand_weight,
    down_weight,
    down_bias,
    modulate_weight,
    modulate_bias,
    time_weight,
    time_bias,
    embed_weight,
    embed_bias,
    class_table,
):
    local_items, length, width = tokens.shape
    items = timesteps.shape[0]
    slab = modulate_weight.shape[2]
    heads_here = project_weight.shape[2] // HD
    first_item = lax.axis_index("tensor") * local_items
    live = (first_item + jnp.arange(local_items) < item_counts[0]).astype(jnp.float32)[
        :, None, None
    ]
    index = lax.axis_index("dp")
    time_feat = time_features(timesteps).astype(jnp.bfloat16)
    pre_hidden = jnp.dot(
        time_feat, time_weight, preferred_element_type=jnp.float32
    ) + time_bias.astype(jnp.float32)
    time_hidden = jax.nn.silu(pre_hidden).astype(jnp.bfloat16)
    condition = (
        jnp.dot(time_hidden, embed_weight, preferred_element_type=jnp.float32)
        + embed_bias.astype(jnp.float32)
        + class_table.at[labels].get(mode="promise_in_bounds").astype(jnp.float32)
    )
    cond_act = jax.nn.silu(condition).astype(jnp.bfloat16)
    modulation_part = (
        jnp.einsum("bd,dke->bke", cond_act, modulate_weight, preferred_element_type=jnp.float32)
        + modulate_bias.astype(jnp.float32)
    ).astype(jnp.bfloat16)
    arrays = attend_arrays(project_weight, output_weight, query_gain, key_gain, length)
    attend_total, mod_all, modulation = attend_pass(tokens[0], modulation_part, arrays)
    _, attend_scale, attend_gate, feed_shift, feed_scale, feed_gate = [
        modulation[which][None, None, :] for which in range(6)
    ]
    token_local = tokens.astype(jnp.float32)
    normed_local, inverse_local = layer_norm(token_local)
    attend_branch = attend_total[None] + output_bias.astype(jnp.float32)
    residual = token_local + attend_gate * attend_branch
    normed_two, inverse_two = layer_norm(residual)
    mod_two = (normed_two * (1.0 + feed_scale) + feed_shift).astype(jnp.bfloat16)
    out_grad = cotangent.astype(jnp.float32) * live
    branch_grad = (out_grad * feed_gate).astype(jnp.bfloat16)
    down_bias_part = jnp.sum(branch_grad.astype(jnp.float32), axis=(0, 1))
    feed_total, mod_two_grad, feed_weights = feed_pass(
        mod_two[0], branch_grad[0], expand_weight, down_weight
    )
    feed_branch = feed_total[None] + down_bias.astype(jnp.float32)
    result = (live * (residual + feed_gate * feed_branch)).astype(jnp.bfloat16)
    mod_two_grad = mod_two_grad[None]
    residual_grad = out_grad + layer_norm_back(
        normed_two, inverse_two, mod_two_grad * (1.0 + feed_scale)
    )
    attend_grad = (residual_grad * attend_gate).astype(jnp.bfloat16)
    output_bias_part = jnp.sum(attend_grad.astype(jnp.float32), axis=(0, 1))
    mod_in_grad, attend_weights, gain_parts, feed_weights = attend_back_pass(
        attend_grad[0], mod_all, arrays, feed_weights
    )
    mod_in_grad = mod_in_grad[None]
    query_gain_part, key_gain_part = jnp.sum(gain_parts, axis=1)[:, :HD]
    tokens_grad = (
        residual_grad
        + layer_norm_back(normed_local, inverse_local, mod_in_grad * (1.0 + attend_scale))
    ).astype(jnp.bfloat16)
    modulation_grad_part = jnp.stack(
        [
            jnp.sum(mod_in_grad, axis=1),
            jnp.sum(mod_in_grad * normed_local, axis=1),
            jnp.sum(residual_grad * attend_branch, axis=1),
            jnp.sum(mod_two_grad, axis=1),
            jnp.sum(mod_two_grad * normed_two, axis=1),
            jnp.sum(out_grad * feed_branch, axis=1),
        ],
        axis=1,
    )
    modulation_grad_part = modulation_grad_part[0].astype(jnp.bfloat16)
    small = jnp.concatenate(
        [
            output_bias_part,
            down_bias_part,
            modulation_grad_part.astype(jnp.float32).reshape(-1),
            query_gain_part,
            key_gain_part,
        ]
    )
    small_size = small.shape[0]
    small = jnp.pad(small, (0, -small_size % 1024)).reshape(-1, 128)
    tensor_size, wide = width // slab, lax.axis_size("dp")
    share = width // wide

    def shares(value):
        return jnp.transpose(value.astype(jnp.float32).reshape(items, wide, share), (1, 0, 2))

    rows = embed_weight
    if share % 16:
        rows = lax.dynamic_slice_in_dim(embed_weight, index * share, share, 0)
    small, modulate_grad, embed_grad, class_grad, time_grad, biases = tail_pass(
        jnp.transpose(modulation_grad_part.reshape(6, tensor_size, slab), (1, 0, 2)),
        small,
        jnp.transpose(modulate_weight, (1, 2, 0)),
        silu_slope(condition),
        jnp.stack([shares(cond_act), shares(time_hidden), shares(silu_slope(pre_hidden))], axis=1),
        time_feat,
        jnp.broadcast_to(labels[:, None], (items, LANES)),
        rows,
        class_table.shape[0],
    )
    class_grad, time_grad = class_grad.T, time_grad.T
    modulate_grad = jnp.transpose(modulate_grad, (1, 0, 2))
    embed_bias_grad, time_bias_grad = biases
    small = small.reshape(-1)
    output_bias_grad = small[:width]
    down_bias_grad = small[width : 2 * width]
    modulate_bias_grad = small[2 * width : 8 * width].reshape(6, width)
    query_gain_grad = small[8 * width : 8 * width + HD]
    key_gain_grad = small[8 * width + HD : 8 * width + 2 * HD]
    inner = heads_here * HD
    first_width = attend_weights.shape[1] - -(-inner // LANES) * LANES
    project_grad = attend_weights[:, : 3 * inner].reshape(-1, 3, inner)
    output_weight_grad = attend_weights[:, first_width : first_width + inner].T
    expand_grad = jnp.transpose(feed_weights[:2], (1, 0, 2))
    down_grad = feed_weights[2].T
    return (
        result,
        tokens_grad,
        project_grad,
        query_gain_grad,
        key_gain_grad,
        output_weight_grad,
        output_bias_grad,
        expand_grad,
        down_grad,
        down_bias_grad,
        modulate_grad,
        modulate_bias_grad,
        time_grad,
        time_bias_grad,
        embed_grad,
        embed_bias_grad,
        class_grad,
    )


def solution(mesh):
    return jax.shard_map(
        shards,
        mesh=mesh,
        in_specs=(
            P(("dp", "tensor"), None, None),
            P("dp"),
            P("dp"),
            P("dp"),
            P(("dp", "tensor"), None, None),
            P(None, None, "tensor"),
            P(),
            P(),
            P("tensor", None),
            P(),
            P(None, None, "tensor"),
            P("tensor", None),
            P(),
            P(None, None, "tensor"),
            P(None, "tensor"),
            P(),
            P(),
            P(),
            P(),
            P(),
        ),
        out_specs=(
            P(("dp", "tensor"), None, None),
            P(("dp", "tensor"), None, None),
            P("dp", None, "tensor"),
            P(),
            P(),
            P("tensor", "dp"),
            P(),
            P("dp", None, "tensor"),
            P("tensor", "dp"),
            P(),
            P("dp", None, "tensor"),
            P(),
            P(None, "dp"),
            P("dp"),
            P("dp", None),
            P("dp"),
            P(None, "dp"),
        ),
        check_vma=False,
    )
```

```python
import functools
import math

import jax
import jax.numpy as jnp
from jax import lax
from jax.experimental import pallas as pl
from jax.experimental.pallas import tpu as pltpu
from jax.sharding import PartitionSpec as P

HD = 72
FREQ = 256
GRID = 16


EPS = 1e-06


def layer_norm(value):
    center = value - jnp.mean(value, axis=-1, keepdims=True)
    inverse = lax.rsqrt(jnp.mean(center * center, axis=-1, keepdims=True) + EPS)
    return (center * inverse, inverse)


def layer_norm_back(normed, inverse, grad):
    return inverse * (
        grad
        - jnp.mean(grad, axis=-1, keepdims=True)
        - normed * jnp.mean(grad * normed, axis=-1, keepdims=True)
    )


def silu_slope(value):
    sigma = jax.nn.sigmoid(value)
    return sigma * (1.0 + value * (1.0 - sigma))


def time_features(steps_in):
    half = FREQ // 2
    rates = jnp.exp(-math.log(10000.0) * jnp.arange(half, dtype=jnp.float32) / half)
    angle = steps_in.astype(jnp.float32)[:, None] * rates[None, :]
    return jnp.concatenate([jnp.cos(angle), jnp.sin(angle)], axis=-1)


FEED_BLOCKS, ATTEND_BLOCKS = 8, 4


def rows_of(block, total, blocks):
    size = total // blocks
    return pl.ds(pl.multiple_of(block * size, size), size)


class Line:
    def __init__(self, count, blocks, gathered, summed, ag_sems, rs_sems):
        self.count = count
        self.blocks = blocks
        self.place = lax.axis_index("tensor")
        self.gathered = gathered
        self.summed = summed
        self.ag_send, self.ag_recv = ag_sems
        self.rs_send, self.rs_recv = rs_sems

    def barrier(self, wide=1):
        place, count = self.place, self.count
        sem = pltpu.get_barrier_semaphore()

        @pl.when(place > 0)
        def _():
            pl.semaphore_signal(sem, inc=1, device_id={"tensor": place - 1})

        @pl.when(place < count - 1)
        def _():
            pl.semaphore_signal(sem, inc=1, device_id={"tensor": place + 1})

        peers = jnp.where(place > 0, 1, 0) + jnp.where(place < count - 1, 1, 0)
        here = lax.axis_index("dp")

        @pl.loop(1, wide)
        def _(offset):
            peer = lax.rem(here + offset, wide)
            pl.semaphore_signal(sem, inc=1, device_id={"dp": peer})

        pl.semaphore_wait(sem, peers + (wide - 1))

    def item_copy(self, which, way, item, own=False):
        mine, everyone = self.gathered[which]
        target = self.place + (1 if way == 0 else -1)
        return pltpu.make_async_remote_copy(
            src_ref=mine if own else everyone.at[item],
            dst_ref=everyone.at[item],
            send_sem=self.ag_send.at[which, way, item],
            recv_sem=self.ag_recv.at[which, way, item],
            device_id={"tensor": target},
        )

    def can(self, way):
        return self.place < self.count - 1 if way == 0 else self.place > 0

    def sum_copy(self, which, way, item, block):
        part, landed = self.summed[which]
        target = self.place + (1 if way == 0 else -1)
        slot = item
        if way == 1:
            slot = jnp.where(item == target, self.count, item)
        rows = rows_of(block, part.shape[1], self.blocks)
        return pltpu.make_async_remote_copy(
            src_ref=part.at[item, rows],
            dst_ref=landed.at[slot, rows],
            send_sem=self.rs_send.at[which, way, item, block],
            recv_sem=self.rs_recv.at[which, way, item, block],
            device_id={"tensor": target},
        )

    def landed_slot(self, way, item):
        return jnp.where(item == self.place, self.count, item) if way == 1 else item

    def wait_sum(self, which, way, item, block):
        part, landed = self.summed[which]
        rows = rows_of(block, part.shape[1], self.blocks)
        view = landed.at[self.landed_slot(way, item), rows]
        pltpu.make_async_remote_copy(
            src_ref=view,
            dst_ref=view,
            send_sem=self.rs_send.at[which, way, item, block],
            recv_sem=self.rs_recv.at[which, way, item, block],
            device_id={"tensor": self.place},
        ).wait_recv()
        return view

    def start_own(self):
        for which in range(len(self.gathered)):
            for way in range(2):

                @pl.when(self.can(way))
                def _():
                    self.item_copy(which, way, self.place, own=True).start()

    def receive(self, step):
        place, count = self.place, self.count
        for which in range(len(self.gathered)):
            for way in range(2):
                item = place - step if way == 0 else place + step

                @pl.when((item >= 0) & (item < count))
                def _():
                    self.item_copy(which, way, item).wait_recv()

                    @pl.when(self.can(way))
                    def _():
                        self.item_copy(which, way, item).start()

    def items(self, step):
        place, count = self.place, self.count
        low, high = place - step, place + step
        return ((low, (low >= 0)), (high, (high < count) & (step > 0)))

    def moves(self, step):
        place, count = self.place, self.count
        return (
            (0, step, step > place, place),
            (1, count - 1 - step, count - 1 - step < place, count - 1 - place),
        )

    def first_sums(self, step, arrays=(0,)):
        @pl.loop(0, self.blocks)
        def _(block):
            for way, item, further, hop in self.moves(step):

                @pl.when(further & (hop == 0))
                def _():
                    for which in arrays:
                        self.sum_copy(which, way, item, block).start()

    def relay_sums(self, step, arrays=(0,)):
        @pl.loop(0, self.blocks + self.count - 3)
        def _(turn):
            for distance in range(1, self.count - 1):
                block = turn - (distance - 1)
                for way, item, further, hop in self.moves(step):

                    @pl.when(further & (hop == distance) & (block >= 0) & (block < self.blocks))
                    def _():
                        for which in arrays:
                            part, landed = self.summed[which]
                            rows = rows_of(block, part.shape[1], self.blocks)
                            view = self.wait_sum(which, way, item, block)
                            total = part[item, rows].astype(jnp.float32) + view[...].astype(
                                jnp.float32
                            )
                            part[item, rows] = total.astype(part.dtype)
                            self.sum_copy(which, way, item, block).start()

    def each(self, first, second, body):
        @pl.loop(0, 2)
        def _(turn):
            item = jnp.where(turn == 0, first[0], second[0])
            valid = ((turn == 0) & first[1]) | ((turn == 1) & second[1])

            @pl.when(valid)
            def _():
                body(item)

    def near(self, step):
        place, count = self.place, self.count
        low = place >= step
        return jnp.where(low, place - step, place + step), low | (place + step < count)

    def far(self, step):
        place, count = self.place, self.count
        return place + step, (step > 0) & (place >= step) & (place + step < count)

    def finish(self, which, out):
        place, count = self.place, self.count
        part, landed = self.summed[which]

        @pl.loop(0, self.blocks)
        def _(block):
            rows = rows_of(block, part.shape[1], self.blocks)
            out[rows] = part[place, rows].astype(jnp.float32)
            for way in range(2):

                @pl.when(place > 0 if way == 0 else place < count - 1)
                def _():
                    view = self.wait_sum(which, way, place, block)
                    out[rows] += view[...].astype(jnp.float32)

    def drain(self):
        place, count = self.place, self.count

        @pl.loop(0, count)
        def _(item):
            for way in range(2):
                passed = item <= place if way == 0 else item >= place

                @pl.when(passed & self.can(way))
                def _():
                    for which in range(len(self.gathered)):
                        self.item_copy(which, way, item).wait_send()

                further = item > place if way == 0 else item < place

                @pl.when(further)
                def _():
                    @pl.loop(0, self.blocks)
                    def _(block):
                        for which in range(len(self.summed)):
                            self.sum_copy(which, way, item, block).wait_send()


def dot(left, right):
    return jnp.dot(left, right, preferred_element_type=jnp.float32)


def dot_rt(left, right):
    return lax.dot_general(
        left, right, (((1,), (1,)), ((), ())), preferred_element_type=jnp.float32
    )


def dot_lt(left, right):
    return lax.dot_general(
        left, right, (((0,), (0,)), ((), ())), preferred_element_type=jnp.float32
    )


def cut(total, most):
    size = max(s for s in range(128, most + 1, 128) if total % s == 0)
    return size, total // size


def span(index, size):
    return pl.ds(pl.multiple_of(index * size, size), size)


def feed_kernel(
    count,
    mod_ref,
    grad_ref,
    expand_hbm,
    down_hbm,
    feed_out,
    back_out,
    weight_hbm,
    expand,
    down,
    mod_all,
    grad_all,
    hidden,
    slopes,
    feed_part,
    back_part,
    feed_land,
    back_land,
    total,
    weights,
    load_sem,
    ag_send,
    ag_recv,
    rs_send,
    rs_recv,
):
    line = Line(
        count,
        FEED_BLOCKS,
        [(mod_ref, mod_all), (grad_ref, grad_all)],
        [(back_part, back_land), (feed_part, feed_land)],
        (ag_send, ag_recv),
        (rs_send, rs_recv),
    )
    width, units = expand.shape[1], expand.shape[2]
    loads = (
        pltpu.make_async_copy(expand_hbm, expand, load_sem.at[0]),
        pltpu.make_async_copy(down_hbm, down, load_sem.at[1]),
    )
    for load in loads:
        load.start()
    line.barrier()
    line.start_own()
    mod_all[line.place] = mod_ref[...]
    grad_all[line.place] = grad_ref[...]
    total[...] = jnp.zeros_like(total)
    for load in loads:
        load.wait()
    unit_size, unit_count = cut(units, 256)
    wide_size, wide_count = cut(width, 384)
    tall_size, tall_count = cut(width, 128)

    def compute(item):
        @pl.loop(0, unit_count)
        def _(index):
            cols = span(index, unit_size)
            mod = mod_all[item]
            gate = dot(mod, expand[0, :, cols])
            upper = dot(mod, expand[1, :, cols])
            back = dot_rt(grad_all[item], down[cols, :])
            sigma = jax.nn.sigmoid(gate)
            active = gate * sigma
            hidden[item, :, cols] = (active * upper).astype(jnp.bfloat16)
            slopes[0, item, :, cols] = (
                back * upper * (sigma * (1.0 + gate * (1.0 - sigma)))
            ).astype(jnp.bfloat16)
            slopes[1, item, :, cols] = (back * active).astype(jnp.bfloat16)

        @pl.loop(0, wide_count)
        def _(index):
            cols = span(index, wide_size)
            back_part[item, :, cols] = (
                dot_rt(slopes[0, item], expand[0, cols, :])
                + dot_rt(slopes[1, item], expand[1, cols, :])
            ).astype(jnp.bfloat16)
            feed_part[item, :, cols] = dot(hidden[item], down[:, cols]).astype(jnp.bfloat16)

    def weigh(item):
        @pl.loop(0, tall_count)
        def _(index):
            rows = span(index, tall_size)
            mod = mod_all[item, :, rows]
            total[0, rows, :] += dot_lt(mod, slopes[0, item])
            total[1, rows, :] += dot_lt(mod, slopes[1, item])
            total[2, rows, :] += dot_lt(grad_all[item, :, rows], hidden[item])

    @pl.loop(0, count)
    def _(step):
        @pl.when(step > 0)
        def _():
            line.each(line.far(step - 1), line.near(step - 1), weigh)
            line.receive(step)

        line.each(line.far(step), line.near(step), compute)

        @pl.when(step > 0)
        def _():
            line.first_sums(step, (0, 1))
            line.relay_sums(step, (0, 1))

    line.each((0, False), line.near(count - 1), weigh)
    weights[...] = total[...].astype(jnp.bfloat16)
    store = pltpu.make_async_copy(weights, weight_hbm, load_sem.at[0])
    store.start()
    line.finish(0, back_out)
    line.finish(1, feed_out)
    line.drain()
    store.wait()


def feed_pass(mod_two, branch_grad, expand_weight, down_weight):
    count = lax.axis_size("tensor")
    length, width = mod_two.shape
    units = down_weight.shape[0]
    expand = jnp.transpose(expand_weight, (1, 0, 2))
    vmem, any_space = pl.BlockSpec(memory_space=pltpu.VMEM), pl.BlockSpec(memory_space=pl.ANY)
    low = jnp.bfloat16
    item = (length, width)
    return pl.pallas_call(
        functools.partial(feed_kernel, count),
        out_shape=(
            jax.ShapeDtypeStruct(item, jnp.float32),
            jax.ShapeDtypeStruct(item, jnp.float32),
            jax.ShapeDtypeStruct((3, width, units), low),
        ),
        in_specs=[vmem, vmem, any_space, any_space],
        out_specs=(vmem, vmem, any_space),
        scratch_shapes=[
            pltpu.VMEM((2, width, units), low),
            pltpu.VMEM((units, width), low),
            pltpu.VMEM((count, *item), low),
            pltpu.VMEM((count, *item), low),
            pltpu.VMEM((count, length, units), low),
            pltpu.VMEM((2, count, length, units), low),
            pltpu.VMEM((count, *item), low),
            pltpu.VMEM((count, *item), low),
            pltpu.VMEM((count + 1, *item), low),
            pltpu.VMEM((count + 1, *item), low),
            pltpu.VMEM((3, width, units), jnp.float32),
            pltpu.VMEM((3, width, units), low),
            *line_sems(count, FEED_BLOCKS, 2, 2),
        ],
        compiler_params=pltpu.CompilerParams(
            collective_id=1, has_side_effects=True, vmem_limit_bytes=64000000
        ),
        name="feed_pass",
    )(mod_two, branch_grad, expand, down_weight)


LANES = 128
HEAD_UNROLL = 2


def turn(value, tables):
    return (
        value * tables[0]
        + pltpu.roll(value, LANES - HD // 4, 1) * tables[1]
        + pltpu.roll(value, HD // 4, 1) * tables[2]
    )


def turn_back(grad, tables):
    return (
        grad * tables[0]
        + pltpu.roll(grad * tables[1], HD // 4, 1)
        + pltpu.roll(grad * tables[2], LANES - HD // 4, 1)
    )


def turn_tables(length):
    quarter = HD // 4
    lane = jnp.arange(LANES)
    rates = 10000.0 ** (-(lane % quarter).astype(jnp.float32) / quarter)
    positions = jnp.arange(length)[:, None]
    place = jnp.where(lane < 2 * quarter, positions // GRID, positions % GRID)
    angle = place.astype(jnp.float32) * rates
    real = lane < HD
    early = (lane // quarter) % 2 == 0
    cosine = jnp.where(real, jnp.cos(angle), 0.0)
    sine = jnp.sin(angle)
    return jnp.stack(
        [
            cosine,
            jnp.where(real & early, -sine, 0.0),
            jnp.where(real & ~early, sine, 0.0),
        ]
    )


def unit_norm(raw):
    inverse = lax.rsqrt(jnp.sum(raw * raw, axis=-1, keepdims=True) * (1.0 / HD) + EPS)
    return raw * inverse, inverse


def project(mod, weight, raw):
    @pl.loop(0, weight.shape[0])
    def _(index):
        raw[index] = dot_rt(mod, weight[index])


def padded_loads(weight_hbm, last_hbm, weight, last, sem):
    heads = last.shape[0] // LANES
    loads = []
    for head in range(heads):
        rows, to = pl.ds(head * HD, HD), pl.ds(head * LANES, HD)
        rest = pl.ds(head * LANES + HD, LANES - HD)
        for part in range(3):
            weight[part, rest, :] = jnp.zeros((LANES - HD, weight.shape[2]), weight.dtype)
            loads.append(
                pltpu.make_async_copy(
                    weight_hbm.at[part, rows], weight.at[part, to], sem.at[len(loads)]
                )
            )
        last[rest, :] = jnp.zeros((LANES - HD, last.shape[1]), last.dtype)
        loads.append(pltpu.make_async_copy(last_hbm.at[rows], last.at[to], sem.at[len(loads)]))
    for load in loads:
        load.start()
    return loads


def soft(queries, keys):
    grown = jnp.exp2(dot_rt(queries, keys) * (HD ** (-0.5) / math.log(2.0)))
    return grown * (1.0 / jnp.sum(grown, axis=-1, keepdims=True))


def attend_kernel(
    count,
    token_ref,
    slab_ref,
    tables_ref,
    gains_ref,
    weight_hbm,
    last_hbm,
    branch_out,
    mod_out,
    rows_out,
    slab_land,
    mod_own,
    weight,
    last,
    mod_all,
    raw,
    mixed,
    part,
    land,
    load_sem,
    ag_send,
    ag_recv,
    rs_send,
    rs_recv,
    slab_send,
    slab_recv,
):
    line = Line(count, ATTEND_BLOCKS, [(mod_own, mod_all)], [(part, land)], (ag_send, ag_recv), (rs_send, rs_recv))
    loads = padded_loads(weight_hbm, last_hbm, weight, last, load_sem)
    place = line.place
    hello = pltpu.get_barrier_semaphore()

    @pl.loop(1, count)
    def _(offset):
        pl.semaphore_signal(hello, inc=1, device_id={"tensor": lax.rem(place + offset, count)})

    pl.semaphore_wait(hello, count - 1)

    def slab_copy(peer, slot):
        return pltpu.make_async_remote_copy(
            src_ref=slab_ref.at[peer],
            dst_ref=slab_land.at[slot],
            send_sem=slab_send.at[peer],
            recv_sem=slab_recv.at[slot],
            device_id={"tensor": peer},
        )

    @pl.loop(1, count)
    def _(offset):
        slab_copy(lax.rem(place + offset, count), place).start()

    slab_land[place] = slab_ref[place]

    @pl.loop(1, count)
    def _(offset):
        peer = lax.rem(place + offset, count)
        slab_copy(peer, place).wait_send()
        slab_copy(peer, peer).wait_recv()

    rows_out[...] = jnp.concatenate(
        [slab_land[index].astype(jnp.float32) for index in range(count)], axis=1
    )

    @pl.loop(0, ATTEND_BLOCKS)
    def _(block):
        rows = rows_of(block, token_ref.shape[0], ATTEND_BLOCKS)
        value = token_ref[rows].astype(jnp.float32)
        center = value - jnp.mean(value, axis=-1, keepdims=True)
        inverse = lax.rsqrt(jnp.mean(center * center, axis=-1, keepdims=True) + EPS)
        mod = center * inverse * (1.0 + rows_out[1:2, :]) + rows_out[0:1, :]
        mod_own[rows] = mod.astype(jnp.bfloat16)
        mod_all[place, rows] = mod.astype(jnp.bfloat16)

    line.start_own()
    for load in loads:
        load.wait()
    heads = last.shape[0] // LANES
    wide_size, wide_count = cut(last.shape[1], 384)

    def compute(item):
        project(mod_all[item], weight, raw)
        tables = (tables_ref[0], tables_ref[1], tables_ref[2])

        @pl.loop(0, heads, unroll=HEAD_UNROLL)
        def _(head):
            lanes = span(head, LANES)
            queries = turn(unit_norm(raw[0, :, lanes])[0] * gains_ref[0:1, :], tables)
            keys = turn(unit_norm(raw[1, :, lanes])[0] * gains_ref[1:2, :], tables)
            probs = soft(queries.astype(jnp.bfloat16), keys.astype(jnp.bfloat16))
            values = raw[2, :, lanes].astype(jnp.bfloat16)
            mixed[:, lanes] = dot(probs.astype(jnp.bfloat16), values).astype(jnp.bfloat16)

        @pl.loop(0, wide_count)
        def _(index):
            cols = span(index, wide_size)
            part[item, :, cols] = dot(mixed[...], last[:, cols]).astype(jnp.bfloat16)

    @pl.loop(0, count)
    def _(step):
        @pl.when(step > 0)
        def _():
            line.receive(step)

        line.each(line.far(step - 1), line.near(step), compute)

        @pl.when(step > 0)
        def _():
            line.first_sums(step)
            line.relay_sums(step)

    mod_out[...] = mod_all[...]
    line.finish(0, branch_out)
    line.drain()


def block_copy(array, target, slot, block, size, send, recv, peer):
    rows = pl.ds(pl.multiple_of(block * size, size), size)
    source = array.at[rows] if len(array.shape) == 2 else array.at[:, rows]
    return pltpu.make_async_remote_copy(
        src_ref=source,
        dst_ref=target.at[slot],
        send_sem=send,
        recv_sem=recv,
        device_id={"dp": peer},
    )


def attend_back_kernel(
    count,
    wide,
    grad_ref,
    mod_all,
    tables_ref,
    gains_ref,
    weight_hbm,
    last_hbm,
    *rest,
):
    if wide:
        feed_hbm, back_out, weight_out, gain_out, feed_out, *rest = rest
    else:
        back_out, weight_out, gain_out, *rest = rest
    (
        weight,
        last,
        narrow,
        grad_all,
        raw,
        mixed,
        mixed_grad,
        raw_grad,
        kept,
        kept_mixed,
        part,
        land,
        total,
        load_sem,
        ag_send,
        ag_recv,
        rs_send,
        rs_recv,
        *rest,
    ) = rest
    line = Line(count, ATTEND_BLOCKS, [(grad_ref, grad_all)], [(part, land)], (ag_send, ag_recv), (rs_send, rs_recv))
    loads = padded_loads(weight_hbm, last_hbm, weight, last, load_sem)
    line.barrier(wide or 1)
    line.start_own()
    width = last.shape[1]
    here = lax.axis_index("dp")
    if wide:
        feed_land, staged, pair_land, quad_land, fs, fr, ps, pr, qs, qr = rest
        size = width // wide
        half = wide // 2
        parity, seat = lax.rem(here, 2), here // 2
        partner = here + 1 - 2 * parity

        def feed_copy(peer, slot):
            return block_copy(feed_hbm, feed_land, slot, peer, size, fs.at[peer], fr.at[slot], peer)

        def pair_copy(index):
            block = 2 * index + 1 - parity
            return block_copy(
                staged, pair_land, index, block, size, ps.at[index], pr.at[index], partner
            )

        def quad_copy(index, slot):
            block = 2 * index + parity
            return block_copy(
                staged, quad_land, slot, block, size, qs.at[index], qr.at[slot], block
            )

        @pl.loop(1, wide)
        def _(offset):
            peer = lax.rem(here + offset, wide)
            feed_copy(peer, here).start()

    grad_all[line.place] = grad_ref[...]
    padded_row = lax.broadcasted_iota(jnp.int32, narrow.shape[1:], 0)
    lane = padded_row & (LANES - 1)
    column = (padded_row >> 7) * HD + lane
    target = lax.broadcasted_iota(jnp.int32, narrow.shape[1:], 1)
    offset = last.shape[0] // LANES * HD % LANES
    for part_index in range(3):
        hit = (lane < HD) & (column + part_index * offset == target)
        narrow[part_index] = jnp.where(hit, 1.0, 0.0).astype(jnp.bfloat16)
    total[...] = jnp.zeros_like(total)
    gain_out[...] = jnp.zeros_like(gain_out)
    for load in loads:
        load.wait()
    inner = last.shape[0]
    heads = inner // LANES
    scale = HD ** (-0.5)
    wide_size, wide_count = cut(width, 384)
    inner_size, inner_count = cut(inner, 256)
    tall_size, tall_count = cut(width, 128)
    first_width = kept.shape[2]

    def compute(item):
        project(mod_all[item], weight, raw)
        tables = (tables_ref[0], tables_ref[1], tables_ref[2])

        @pl.loop(0, inner_count)
        def _(index):
            cols = span(index, inner_size)
            mixed_grad[:, cols] = dot_rt(grad_all[item], last[cols, :]).astype(jnp.bfloat16)

        @pl.loop(0, heads, unroll=HEAD_UNROLL)
        def _(head):
            lanes = span(head, LANES)
            query_norm, query_inverse = unit_norm(raw[0, :, lanes])
            key_norm, key_inverse = unit_norm(raw[1, :, lanes])
            values = raw[2, :, lanes].astype(jnp.bfloat16)
            queries = turn(query_norm * gains_ref[0:1, :], tables).astype(jnp.bfloat16)
            keys = turn(key_norm * gains_ref[1:2, :], tables).astype(jnp.bfloat16)
            probs = soft(queries, keys)
            probs_low = probs.astype(jnp.bfloat16)
            mixed[:, lanes] = dot(probs_low, values).astype(jnp.bfloat16)
            grad = mixed_grad[:, lanes]
            prob_grad = dot_rt(grad, values)
            score_grad = (
                probs * (prob_grad - jnp.sum(probs * prob_grad, axis=-1, keepdims=True))
            ).astype(jnp.bfloat16)

            def back(which, value_grad, norm, inverse):
                turned = turn_back(value_grad, tables)
                gained = turned * norm
                gain_out[which] += jnp.sum(gained.reshape(-1, 8, LANES), axis=0)
                scaled = turned * gains_ref[which : which + 1, :]
                mean = jnp.sum(scaled * norm, axis=-1, keepdims=True) * (1.0 / HD)
                raw_grad[which, :, lanes] = (inverse * (scaled - norm * mean)).astype(
                    jnp.bfloat16
                )

            back(0, dot(score_grad, keys) * scale, query_norm, query_inverse)
            back(1, dot_lt(score_grad, queries) * scale, key_norm, key_inverse)
            raw_grad[2, :, lanes] = dot_lt(probs_low, grad).astype(jnp.bfloat16)

        @pl.loop(0, wide_count)
        def _(index):
            cols = span(index, wide_size)
            sums = dot(raw_grad[0], weight[0, :, cols])
            sums += dot(raw_grad[1], weight[1, :, cols])
            sums += dot(raw_grad[2], weight[2, :, cols])
            part[item, :, cols] = sums.astype(jnp.bfloat16)

    def keep(item):
        one = dot(raw_grad[0], narrow[0])
        two = dot(raw_grad[1], narrow[1])
        three = dot(raw_grad[2], narrow[2])
        side = one.shape[1] - LANES
        low = jnp.bfloat16
        kept[item, :, :side] = one[:, :side].astype(low)
        kept[item, :, side : side + LANES] = (one[:, side:] + two[:, :LANES]).astype(low)
        kept[item, :, side + LANES : 2 * side] = two[:, LANES:side].astype(low)
        kept[item, :, 2 * side : 2 * side + LANES] = (two[:, side:] + three[:, :LANES]).astype(low)
        kept[item, :, 2 * side + LANES :] = three[:, LANES:].astype(low)
        kept_mixed[item] = dot(mixed[...], narrow[0]).astype(low)

    def weigh(item):
        @pl.loop(0, tall_count)
        def _(index):
            rows = span(index, tall_size)
            total[rows, :first_width] += dot_lt(mod_all[item, :, rows], kept[item])
            total[rows, first_width:] += dot_lt(grad_all[item, :, rows], kept_mixed[item])

    def work(item):
        compute(item)
        keep(item)

    @pl.loop(0, count)
    def _(step):
        @pl.when(step > 0)
        def _():
            line.each(line.far(step - 2), line.near(step - 1), weigh)
            line.receive(step)

        line.each(line.far(step - 1), line.near(step), work)

        @pl.when(step > 0)
        def _():
            line.first_sums(step)

        @pl.when(step == count - 1)
        def _():
            line.each((0, False), line.near(step), weigh)
            if wide:
                staged[...] = total[...].astype(jnp.bfloat16)

                @pl.loop(0, half)
                def _(index):
                    pair_copy(index).start()

                @pl.loop(0, half)
                def _(index):
                    pair_copy(index).wait_send()
                    pair_copy(index).wait_recv()
                    rows = pl.ds(pl.multiple_of((2 * index + parity) * size, size), size)
                    staged[rows] = (
                        staged[rows].astype(jnp.float32) + pair_land[index].astype(jnp.float32)
                    ).astype(jnp.bfloat16)

                @pl.loop(1, half)
                def _(offset):
                    quad_copy(lax.rem(seat + offset, half), seat).start()

        @pl.when(step > 0)
        def _():
            line.relay_sums(step)

    if wide:
        rows = pl.ds(pl.multiple_of(here * size, size), size)
        own = pltpu.make_async_copy(feed_hbm.at[:, rows], feed_land.at[here], load_sem.at[0])
        own.start()

        @pl.loop(1, wide)
        def _(offset):
            peer = lax.rem(here + offset, wide)
            feed_copy(peer, here).wait_send()
            feed_copy(here, peer).wait_recv()

        own.wait()
        for which in range(feed_out.shape[0]):
            total_here = feed_land[0, which].astype(jnp.float32)
            for index in range(1, wide):
                total_here += feed_land[index, which].astype(jnp.float32)
            feed_out[which] = total_here

    line.finish(0, back_out)
    line.drain()
    if wide:
        weight_out[...] = staged[rows].astype(jnp.float32)

        @pl.loop(1, half)
        def _(offset):
            index = lax.rem(seat + offset, half)
            quad_copy(index, seat).wait_send()
            quad_copy(seat, index).wait_recv()
            weight_out[...] += quad_land[index].astype(jnp.float32)

    else:
        weight_out[...] = total[...].astype(jnp.bfloat16)


def attend_arrays(project_weight, output_weight, query_gain, key_gain, length):
    gains = jnp.stack([query_gain, key_gain]).astype(jnp.float32)
    gains = jnp.pad(gains, ((0, 6), (0, LANES - HD)))
    return turn_tables(length), gains, jnp.transpose(project_weight, (1, 2, 0)), output_weight


def line_sems(count, blocks, gathers, sums, loads=2):
    return [
        pltpu.SemaphoreType.DMA((loads,)),
        pltpu.SemaphoreType.DMA((gathers, 2, count)),
        pltpu.SemaphoreType.DMA((gathers, 2, count)),
        pltpu.SemaphoreType.DMA((sums, 2, count, blocks)),
        pltpu.SemaphoreType.DMA((sums, 2, count, blocks)),
    ]


def attend_pass(tokens, slabs, arrays):
    count = lax.axis_size("tensor")
    tables, gains, weight, last = arrays
    item = tokens.shape
    width = item[1]
    heads = last.shape[0] // HD
    inner = heads * LANES
    vmem, any_space = pl.BlockSpec(memory_space=pltpu.VMEM), pl.BlockSpec(memory_space=pl.ANY)
    low = jnp.bfloat16
    return pl.pallas_call(
        functools.partial(attend_kernel, count),
        out_shape=(
            jax.ShapeDtypeStruct(item, jnp.float32),
            jax.ShapeDtypeStruct((count, *item), low),
            jax.ShapeDtypeStruct((slabs.shape[1], width), jnp.float32),
        ),
        in_specs=[vmem, vmem, vmem, vmem, any_space, any_space],
        out_specs=(vmem, vmem, vmem),
        scratch_shapes=[
            pltpu.VMEM(slabs.shape, low),
            pltpu.VMEM(item, low),
            pltpu.VMEM((3, inner, width), low),
            pltpu.VMEM((inner, width), low),
            pltpu.VMEM((count, *item), low),
            pltpu.VMEM((3, item[0], inner), jnp.float32),
            pltpu.VMEM((item[0], inner), low),
            pltpu.VMEM((count, *item), low),
            pltpu.VMEM((count + 1, *item), low),
            *line_sems(count, ATTEND_BLOCKS, 1, 1, 4 * heads),
            pltpu.SemaphoreType.DMA((count,)),
            pltpu.SemaphoreType.DMA((count,)),
        ],
        compiler_params=pltpu.CompilerParams(
            collective_id=6, has_side_effects=True, vmem_limit_bytes=60000000
        ),
        name="attend_pass",
    )(tokens, slabs, tables, gains, weight, last)


def attend_back_pass(attend_grad, mod_all, arrays, feed_weights):
    count, wide = lax.axis_size("tensor"), lax.axis_size("dp")
    tables, gains, weight, last = arrays
    item = attend_grad.shape
    length, width = item
    heads = last.shape[0] // HD
    inner = heads * LANES
    vmem, any_space = pl.BlockSpec(memory_space=pltpu.VMEM), pl.BlockSpec(memory_space=pl.ANY)
    low, high = jnp.bfloat16, jnp.float32
    window = -(-last.shape[0] // LANES) * LANES
    first_width = 3 * window - 2 * LANES
    columns = first_width + window
    if width % (16 * wide):
        wide = 0
    size = width // wide if wide else width
    outs = [
        jax.ShapeDtypeStruct(item, high),
        jax.ShapeDtypeStruct((size, columns), high if wide else low),
        jax.ShapeDtypeStruct((2, 8, LANES), high),
    ]
    scratch = [
        pltpu.VMEM((3, inner, width), low),
        pltpu.VMEM((inner, width), low),
        pltpu.VMEM((3, inner, window), low),
        pltpu.VMEM((count, *item), low),
        pltpu.VMEM((3, length, inner), high),
        pltpu.VMEM((length, inner), low),
        pltpu.VMEM((length, inner), low),
        pltpu.VMEM((3, length, inner), low),
        pltpu.VMEM((count, length, first_width), low),
        pltpu.VMEM((count, length, window), low),
        pltpu.VMEM((count, *item), low),
        pltpu.VMEM((count + 1, *item), low),
        pltpu.VMEM((width, columns), high),
        *line_sems(count, ATTEND_BLOCKS, 1, 1, 4 * heads),
    ]
    ins = [attend_grad, mod_all, tables, gains, weight, last]
    specs = [vmem, vmem, vmem, vmem, any_space, any_space]
    if wide:
        ins.append(feed_weights)
        specs.append(any_space)
        kinds, _, units = feed_weights.shape
        outs.append(jax.ShapeDtypeStruct((kinds, size, units), high))
        half = wide // 2
        scratch += [
            pltpu.VMEM((wide, kinds, size, units), low),
            pltpu.VMEM((width, columns), low),
            pltpu.VMEM((half, size, columns), low),
            pltpu.VMEM((half, size, columns), low),
        ]
        for number in (wide, wide, half, half, half, half):
            scratch.append(pltpu.SemaphoreType.DMA((number,)))
    results = pl.pallas_call(
        functools.partial(attend_back_kernel, count, wide),
        out_shape=tuple(outs),
        in_specs=specs,
        out_specs=tuple([vmem] * len(outs)),
        scratch_shapes=scratch,
        compiler_params=pltpu.CompilerParams(
            collective_id=7, has_side_effects=True, vmem_limit_bytes=66000000
        ),
        name="attend_back_pass",
    )(*ins)
    if wide:
        return results

    def scatter(value, axis):
        return lax.psum_scatter(value, "dp", scatter_dimension=axis, tiled=True).astype(high)

    back, weights, gain_parts = results
    return back, scatter(weights, 0), gain_parts, scatter(feed_weights, 1)


def tail_kernel(
    grads_ref,
    small_ref,
    weight_ref,
    slope_ref,
    forward_ref,
    feat_ref,
    label_ref,
    rows_hbm,
    small_out,
    modulate_out,
    embed_out,
    class_out,
    time_out,
    bias_out,
    grads_land,
    grads_mine,
    grads_land_dp,
    small_one,
    small_mid,
    small_two,
    part,
    part_land,
    cond,
    cond_land,
    forward_land,
    feat_land,
    label_land,
    grads_all,
    cond_all,
    forward_all,
    feat_all,
    label_all,
    rows,
    load_sem,
    *sems,
):
    deep, wide = part_land.shape[0], cond_land.shape[0]
    items = cond.shape[0]
    share = rows.shape[0]
    seat = lax.axis_index("dp") * share
    start_row = seat if rows_hbm.shape[0] > share else 0
    if share % 16 == 0:
        start_row = pl.multiple_of(start_row, 16)
    load = pltpu.make_async_copy(rows_hbm.at[pl.ds(start_row, share)], rows, load_sem)
    load.start()
    axes = (("dp", wide), ("tensor", deep))
    hello = pltpu.get_barrier_semaphore()
    for axis, count in axes:
        here = lax.axis_index(axis)

        @pl.loop(1, count)
        def _(offset):
            pl.semaphore_signal(
                hello, inc=1, device_id={axis: lax.rem(here + offset, count)}
            )

    pl.semaphore_wait(hello, wide + deep - 2)
    low = jnp.bfloat16

    def exchange(number, axis, source, target, split=False):
        count = target.shape[0]
        here = lax.axis_index(axis)
        send, recv = sems[2 * number], sems[2 * number + 1]

        def copy(peer, slot):
            return pltpu.make_async_remote_copy(
                src_ref=source.at[peer] if split else source,
                dst_ref=target.at[slot],
                send_sem=send.at[peer],
                recv_sem=recv.at[slot],
                device_id={axis: peer},
            )

        def start():
            @pl.loop(1, count)
            def _(offset):
                copy(lax.rem(here + offset, count), here).start()

            target[here] = source[here] if split else source[...]

        def finish():
            @pl.loop(1, count)
            def _(offset):
                peer = lax.rem(here + offset, count)
                copy(peer, here).wait_send()
                copy(peer, peer).wait_recv()

        return start, finish

    start_grads, finish_grads = exchange(0, "tensor", grads_ref, grads_land, True)
    start_small, finish_small = exchange(1, "dp", small_ref, small_one)
    start_sums, finish_sums = exchange(2, "tensor", small_mid, small_two)
    start_part, finish_part = exchange(3, "tensor", part, part_land)
    start_mine, finish_mine = exchange(4, "dp", grads_mine, grads_land_dp)
    start_cond, finish_cond = exchange(5, "dp", cond, cond_land)
    start_forward, finish_forward = exchange(6, "dp", forward_ref, forward_land, True)
    start_feat, finish_feat = exchange(7, "dp", feat_ref, feat_land)
    start_label, finish_label = exchange(8, "dp", label_ref, label_land)

    start_grads()
    start_small()
    start_forward()
    start_feat()
    start_label()
    finish_grads()
    kinds = grads_mine.shape[0]
    for item in range(items):
        piece = grads_land[item].astype(jnp.float32)
        for kind in range(kinds):
            grads_all[kind, item : item + 1, :] = piece[kind : kind + 1, :]
    total = jnp.zeros(part.shape, jnp.float32)
    for kind in range(kinds):
        mine = grads_all[kind, :items, :].astype(low)
        grads_mine[kind] = mine
        total += dot(mine, weight_ref[kind])
    part[...] = total
    start_part()
    start_mine()
    finish_small()
    small_mid[...] = small_one[0]

    @pl.loop(1, wide)
    def _(index):
        small_mid[...] += small_one[index]

    start_sums()
    finish_part()
    total = part_land[0]
    for index in range(1, deep):
        total += part_land[index]
    cond[...] = (total * slope_ref[...]).astype(low)
    start_cond()
    finish_forward()
    finish_feat()
    finish_label()
    for index in range(wide):
        batch = pl.ds(index * items, items)
        for kind in range(forward_all.shape[0]):
            forward_all[kind, batch, :] = forward_land[index, kind]
        feat_all[batch, :] = feat_land[index].astype(jnp.float32)
        label_all[batch, :] = label_land[index]
    finish_mine()
    for index in range(wide):
        batch = pl.ds(index * items, items)
        for kind in range(kinds):
            grads_all[kind, batch, :] = grads_land_dp[index, kind].astype(jnp.float32)
    active = forward_all[0].astype(low)
    for kind in range(kinds):
        modulate_out[kind] = dot_lt(active, grads_all[kind].astype(low))
    finish_sums()
    small_out[...] = small_two[0]

    @pl.loop(1, deep)
    def _(index):
        small_out[...] += small_two[index]

    finish_cond()
    for index in range(wide):
        cond_all[pl.ds(index * items, items), :] = cond_land[index].astype(jnp.float32)
    every = cond_all[...].astype(low)
    embed_out[...] = dot_lt(forward_all[1].astype(low), every)
    width = every.shape[1]
    spot = lax.broadcasted_iota(jnp.int32, (width, share), 0)
    pick = jnp.where(spot == seat + lax.broadcasted_iota(jnp.int32, (width, share), 1), 1.0, 0.0)
    picked = dot(every, pick.astype(low)).astype(low)
    classes = class_out.shape[1]
    label = jnp.broadcast_to(label_all[:, 0:1], (label_all.shape[0], classes))
    lane = lax.broadcasted_iota(jnp.int32, label.shape, 1)
    hot = jnp.where(label == lane, 1.0, 0.0).astype(low)
    class_out[...] = dot_lt(picked, hot)
    load.wait()
    earlier = (dot_rt(every, rows[...]) * forward_all[2]).astype(low)
    time_out[...] = dot_lt(earlier, feat_all[...].astype(low))
    bias_out[0:1, :] = jnp.sum(picked.astype(jnp.float32), axis=0, keepdims=True)
    bias_out[1:2, :] = jnp.sum(earlier.astype(jnp.float32), axis=0, keepdims=True)


def tail_pass(grads, small, weight, slope, forward, feat, label, rows, classes):
    deep, kinds, slab = grads.shape
    wide, parts, items, share = forward.shape
    width = weight.shape[2]
    batch = wide * items
    freq = feat.shape[1]
    low, high = jnp.bfloat16, jnp.float32
    vmem = pl.BlockSpec(memory_space=pltpu.VMEM)
    shapes = (
        (small.shape, high),
        ((kinds, share, slab), high),
        ((share, width), high),
        ((share, classes), high),
        ((share, freq), high),
        ((2, share), high),
    )
    scratch = (
        ((deep, kinds, slab), low),
        ((kinds, items, slab), low),
        ((wide, kinds, items, slab), low),
        ((wide, *small.shape), high),
        (small.shape, high),
        ((deep, *small.shape), high),
        ((items, width), high),
        ((deep, items, width), high),
        ((items, width), low),
        ((wide, items, width), low),
        (forward.shape, high),
        ((wide, items, freq), low),
        ((wide, items, LANES), jnp.int32),
        ((kinds, batch, slab), high),
        ((batch, width), high),
        ((parts, batch, share), high),
        ((batch, freq), high),
        ((batch, LANES), jnp.int32),
        ((share, width), low),
    )
    sems = [pltpu.SemaphoreType.DMA]
    for number in (deep, wide, deep, deep, wide, wide, wide, wide, wide):
        sems += [pltpu.SemaphoreType.DMA((number,))] * 2
    return pl.pallas_call(
        tail_kernel,
        out_shape=tuple(jax.ShapeDtypeStruct(*shape) for shape in shapes),
        in_specs=[vmem] * 7 + [pl.BlockSpec(memory_space=pl.ANY)],
        out_specs=tuple([vmem] * 6),
        scratch_shapes=[pltpu.VMEM(*shape) for shape in scratch] + sems,
        compiler_params=pltpu.CompilerParams(
            collective_id=3, has_side_effects=True, vmem_limit_bytes=60000000
        ),
        name="tail_pass",
    )(grads, small, weight, slope, forward, feat, label, rows)


def shards(
    tokens,
    timesteps,
    labels,
    item_counts,
    cotangent,
    project_weight,
    query_gain,
    key_gain,
    output_weight,
    output_bias,
    expand_weight,
    down_weight,
    down_bias,
    modulate_weight,
    modulate_bias,
    time_weight,
    time_bias,
    embed_weight,
    embed_bias,
    class_table,
):
    local_items, length, width = tokens.shape
    items = timesteps.shape[0]
    slab = modulate_weight.shape[2]
    heads_here = project_weight.shape[2] // HD
    first_item = lax.axis_index("tensor") * local_items
    live = (first_item + jnp.arange(local_items) < item_counts[0]).astype(jnp.float32)[
        :, None, None
    ]
    index = lax.axis_index("dp")
    time_feat = time_features(timesteps).astype(jnp.bfloat16)
    pre_hidden = jnp.dot(
        time_feat, time_weight, preferred_element_type=jnp.float32
    ) + time_bias.astype(jnp.float32)
    time_hidden = jax.nn.silu(pre_hidden).astype(jnp.bfloat16)
    condition = (
        jnp.dot(time_hidden, embed_weight, preferred_element_type=jnp.float32)
        + embed_bias.astype(jnp.float32)
        + class_table.at[labels].get(mode="promise_in_bounds").astype(jnp.float32)
    )
    cond_act = jax.nn.silu(condition).astype(jnp.bfloat16)
    modulation_part = (
        jnp.einsum("bd,dke->bke", cond_act, modulate_weight, preferred_element_type=jnp.float32)
        + modulate_bias.astype(jnp.float32)
    ).astype(jnp.bfloat16)
    arrays = attend_arrays(project_weight, output_weight, query_gain, key_gain, length)
    attend_total, mod_all, modulation = attend_pass(tokens[0], modulation_part, arrays)
    _, attend_scale, attend_gate, feed_shift, feed_scale, feed_gate = [
        modulation[which][None, None, :] for which in range(6)
    ]
    token_local = tokens.astype(jnp.float32)
    normed_local, inverse_local = layer_norm(token_local)
    attend_branch = attend_total[None] + output_bias.astype(jnp.float32)
    residual = token_local + attend_gate * attend_branch
    normed_two, inverse_two = layer_norm(residual)
    mod_two = (normed_two * (1.0 + feed_scale) + feed_shift).astype(jnp.bfloat16)
    out_grad = cotangent.astype(jnp.float32) * live
    branch_grad = (out_grad * feed_gate).astype(jnp.bfloat16)
    down_bias_part = jnp.sum(branch_grad.astype(jnp.float32), axis=(0, 1))
    feed_total, mod_two_grad, feed_weights = feed_pass(
        mod_two[0], branch_grad[0], expand_weight, down_weight
    )
    feed_branch = feed_total[None] + down_bias.astype(jnp.float32)
    result = (live * (residual + feed_gate * feed_branch)).astype(jnp.bfloat16)
    mod_two_grad = mod_two_grad[None]
    residual_grad = out_grad + layer_norm_back(
        normed_two, inverse_two, mod_two_grad * (1.0 + feed_scale)
    )
    attend_grad = (residual_grad * attend_gate).astype(jnp.bfloat16)
    output_bias_part = jnp.sum(attend_grad.astype(jnp.float32), axis=(0, 1))
    mod_in_grad, attend_weights, gain_parts, feed_weights = attend_back_pass(
        attend_grad[0], mod_all, arrays, feed_weights
    )
    mod_in_grad = mod_in_grad[None]
    query_gain_part, key_gain_part = jnp.sum(gain_parts, axis=1)[:, :HD]
    tokens_grad = (
        residual_grad
        + layer_norm_back(normed_local, inverse_local, mod_in_grad * (1.0 + attend_scale))
    ).astype(jnp.bfloat16)
    modulation_grad_part = jnp.stack(
        [
            jnp.sum(mod_in_grad, axis=1),
            jnp.sum(mod_in_grad * normed_local, axis=1),
            jnp.sum(residual_grad * attend_branch, axis=1),
            jnp.sum(mod_two_grad, axis=1),
            jnp.sum(mod_two_grad * normed_two, axis=1),
            jnp.sum(out_grad * feed_branch, axis=1),
        ],
        axis=1,
    )
    modulation_grad_part = modulation_grad_part[0].astype(jnp.bfloat16)
    small = jnp.concatenate(
        [
            output_bias_part,
            down_bias_part,
            modulation_grad_part.astype(jnp.float32).reshape(-1),
            query_gain_part,
            key_gain_part,
        ]
    )
    small_size = small.shape[0]
    small = jnp.pad(small, (0, -small_size % 1024)).reshape(-1, 128)
    tensor_size, wide = width // slab, lax.axis_size("dp")
    share = width // wide

    def shares(value):
        return jnp.transpose(value.astype(jnp.float32).reshape(items, wide, share), (1, 0, 2))

    rows = embed_weight
    if share % 16:
        rows = lax.dynamic_slice_in_dim(embed_weight, index * share, share, 0)
    small, modulate_grad, embed_grad, class_grad, time_grad, biases = tail_pass(
        jnp.transpose(modulation_grad_part.reshape(6, tensor_size, slab), (1, 0, 2)),
        small,
        jnp.transpose(modulate_weight, (1, 2, 0)),
        silu_slope(condition),
        jnp.stack([shares(cond_act), shares(time_hidden), shares(silu_slope(pre_hidden))], axis=1),
        time_feat,
        jnp.broadcast_to(labels[:, None], (items, LANES)),
        rows,
        class_table.shape[0],
    )
    class_grad, time_grad = class_grad.T, time_grad.T
    modulate_grad = jnp.transpose(modulate_grad, (1, 0, 2))
    embed_bias_grad, time_bias_grad = biases
    small = small.reshape(-1)
    output_bias_grad = small[:width]
    down_bias_grad = small[width : 2 * width]
    modulate_bias_grad = small[2 * width : 8 * width].reshape(6, width)
    query_gain_grad = small[8 * width : 8 * width + HD]
    key_gain_grad = small[8 * width + HD : 8 * width + 2 * HD]
    inner = heads_here * HD
    first_width = attend_weights.shape[1] - -(-inner // LANES) * LANES
    project_grad = attend_weights[:, : 3 * inner].reshape(-1, 3, inner)
    output_weight_grad = attend_weights[:, first_width : first_width + inner].T
    expand_grad = jnp.transpose(feed_weights[:2], (1, 0, 2))
    down_grad = feed_weights[2].T
    return (
        result,
        tokens_grad,
        project_grad,
        query_gain_grad,
        key_gain_grad,
        output_weight_grad,
        output_bias_grad,
        expand_grad,
        down_grad,
        down_bias_grad,
        modulate_grad,
        modulate_bias_grad,
        time_grad,
        time_bias_grad,
        embed_grad,
        embed_bias_grad,
        class_grad,
    )


def solution(mesh):
    return jax.shard_map(
        shards,
        mesh=mesh,
        in_specs=(
            P(("dp", "tensor"), None, None),
            P("dp"),
            P("dp"),
            P("dp"),
            P(("dp", "tensor"), None, None),
            P(None, None, "tensor"),
            P(),
            P(),
            P("tensor", None),
            P(),
            P(None, None, "tensor"),
            P("tensor", None),
            P(),
            P(None, None, "tensor"),
            P(None, "tensor"),
            P(),
            P(),
            P(),
            P(),
            P(),
        ),
        out_specs=(
            P(("dp", "tensor"), None, None),
            P(("dp", "tensor"), None, None),
            P("dp", None, "tensor"),
            P(),
            P(),
            P("tensor", "dp"),
            P(),
            P("dp", None, "tensor"),
            P("tensor", "dp"),
            P(),
            P("dp", None, "tensor"),
            P(),
            P(None, "dp"),
            P("dp"),
            P("dp", None),
            P("dp"),
            P(None, "dp"),
        ),
        check_vma=False,
    )
```
